32 devices in a mesh: rep: 8 (over z, y), shard: 4 (over x, core).
Axes of the slice: x: 2, y: 2, z: 4, core: 2. Of those that a mesh axis runs over, the one named last changes fastest.
Arguments:
- prompt: bfloat16 [8, 1024, 768], P('rep', 'shard'), may hold values from -6 to 6
- conts: bfloat16 [8, 4, 512, 768], P('rep', 'shard'), may hold values from -6 to 6
- prompt_cot: bfloat16 [8, 1024, 768], P('rep', 'shard'), may hold values from -6 to 6
- cont_cot: bfloat16 [8, 4, 512, 768], P('rep', 'shard'), may hold values from -6 to 6
- labels: int32 [8, 4], P('rep', 'shard'), may hold values from 0 to 13
- w_qkv: float32 [768, 2304], P('shard'), may hold values from -0.21875 to 0.21875
- w_out: float32 [768, 768], P('shard'), may hold values from -3.5 to 3.5
- w_in: float32 [768, 3072], P('shard'), may hold values from -0.21875 to 0.21875
- w_ffo: float32 [3072, 768], P('shard'), may hold values from -0.109375 to 0.109375
- layer_biases: float32 [6, 768], replicated, may hold values from -3 to 3
- norm_gains: float32 [2, 768], replicated, may hold values from 0.25 to 1.75
- bias_in: float32 [3072], replicated, may hold values from -3 to 3
- w_student: float32 [768, 128], replicated, may hold values from -0.21875 to 0.21875
- student_vectors: float32 [3, 128], replicated, may hold values from -4 to 4
- w_pool: float32 [128, 128], replicated, may hold values from -0.5 to 0.5
- w_class: float32 [128, 14], replicated, may hold values from -1 to 1
- bias_class: float32 [14], replicated, may hold values from -3 to 3
Outputs:
- prompt_out: bfloat16 [8, 1024, 768], P('rep', 'shard')
- cont_out: bfloat16 [8, 4, 512, 768], P('rep', 'shard')
- logits: float32 [8, 4, 14], P('rep', 'shard')
- prompt_grad: float32 [8, 1024, 768], P('rep', 'shard')
- cont_grad: float32 [8, 4, 512, 768], P('rep', 'shard')
- grad_qkv: float32 [768, 2304], P('shard')
- grad_out: float32 [768, 768], P('shard')
- grad_in: float32 [768, 3072], P('shard')
- grad_ffo: float32 [3072, 768], P('shard')
- grad_biases: float32 [6, 768], replicated
- grad_gains: float32 [2, 768], replicated
- grad_bias_in: float32 [3072], replicated
- grad_student: float32 [768, 128], replicated
- grad_student_vectors: float32 [3, 128], replicated
- grad_pool: float32 [128, 128], replicated
- grad_class: float32 [128, 14], replicated
- grad_bias_class: float32 [14], replicated
The draws below stay inside these ranges and needn't reach their ends.
All inputs are finite; a program needn't handle non-finite values.
Results may differ from the reference program's by a relative error of at most 0.02.
Values may be sent and summed in bfloat16 or wider, within the bound.
A program may use at most 192 MiB of HBM per device.

```python
from functools import partial
import jax
import jax.numpy as jnp
from jax import lax

D = 768
HEADS = 12
DH = 64
FF = 3072
STU = 128
SHEADS = 2
CLASSES = 14
PD = 256
CL = 512
PROMPT = 1024
GROUPS = 8
CONTS = 4


def place_ends(drawn, key, least, high):
    dims = drawn.shape
    index_at = [jax.random.randint(jax.random.fold_in(key, axis), (), 0, dims[axis]) for axis in range(len(dims))]
    drawn = drawn.at[tuple(index_at)].set(least)
    longest = dims.index(max(dims))
    index_at[longest] = (index_at[longest] + 1) % dims[longest]
    return drawn.at[tuple(index_at)].set(high)


def block_scale(own_key, shape, pieces, low, top_value):
    level, own = 1.0, jax.random.fold_in(own_key, 6)
    for dim, blocks in pieces:
        draws = jnp.exp(jax.random.uniform(jax.random.fold_in(own, dim), (blocks,), jnp.float32, low / len(pieces), top_value / len(pieces)))
        level = level * jnp.repeat(draws, shape[dim] // blocks).reshape([-1 if axis == dim else 1 for axis in range(len(shape))])
    return level


def gaussian(stream_key, dims, scale, limit, pieces=(), kind=jnp.bfloat16):
    drawn = jax.random.normal(stream_key, dims, jnp.float32) * scale
    if len(pieces) > 0:
        drawn = block_scale(stream_key, dims, pieces, -0.22, 0.18) * drawn
    return jnp.clip(drawn, min=-limit, max=limit).astype(kind)


def setup_inputs(seed: int = 0) -> dict:
    key_list = jax.random.split(jax.random.key(seed), 18)
    return {
        "prompt": gaussian(key_list[0], (GROUPS, PROMPT, D), 1.0, 6.0, ((0, 8), (1, 4))),
        "conts": gaussian(key_list[1], (GROUPS, CONTS, CL, D), 1.0, 6.0, ((0, 8), (1, 4))),
        "prompt_cot": gaussian(key_list[2], (GROUPS, PROMPT, D), 1.0, 6.0, ((0, 8), (1, 4))),
        "cont_cot": gaussian(key_list[3], (GROUPS, CONTS, CL, D), 1.0, 6.0, ((0, 8), (1, 4))),
        "labels": place_ends(jax.random.randint(key_list[4], (GROUPS, CONTS), 0, CLASSES), jax.random.fold_in(key_list[4], 1), 0, CLASSES - 1).astype(jnp.int32),
        "w_qkv": gaussian(key_list[5], (D, 3 * D), D ** -0.5, 0.21875, ((0, 4),), jnp.float32),
        "w_out": gaussian(key_list[6], (D, D), (max(D // 256, 1)) ** -0.5, 3.5, ((0, 4),), jnp.float32),
        "w_in": gaussian(key_list[7], (D, FF), D ** -0.5, 0.21875, ((0, 4),), jnp.float32),
        "w_ffo": gaussian(key_list[8], (FF, D), FF ** -0.5, 0.109375, ((0, 4),), jnp.float32),
        "layer_biases": gaussian(key_list[9], (6, D), 0.5, 3.0, (), jnp.float32),
        "norm_gains": jnp.clip(1.0 + 0.15 * jax.random.normal(key_list[10], (2, D), jnp.float32), 0.25, 1.75),
        "bias_in": gaussian(key_list[11], (FF,), 0.5, 3.0, (), jnp.float32),
        "w_student": gaussian(key_list[12], (D, STU), D ** -0.5, 0.21875, (), jnp.float32),
        "student_vectors": gaussian(key_list[13], (3, STU), 1.0, 4.0, (), jnp.float32),
        "w_pool": gaussian(key_list[14], (STU, STU), STU ** -0.5, 0.5, (), jnp.float32),
        "w_class": gaussian(key_list[15], (STU, CLASSES), (STU // 4) ** -0.5, 1.0, (), jnp.float32),
        "bias_class": gaussian(key_list[16], (CLASSES,), 0.5, 3.0, (), jnp.float32),
    }


@jax.custom_vjp
def low(v):
    return lax.optimization_barrier(v.astype(jnp.bfloat16)).astype(jnp.float32)

@jax.custom_vjp
def low_back(v):
    return v

def low_keep(v):
    return (low(v), None)

def low_pass(kept, grad):
    return (grad,)

def back_keep(v):
    return (v, None)

def back_low(kept, grad):
    return (low(grad),)
low.defvjp(low_keep, low_pass)
low_back.defvjp(back_keep, back_low)
HIGHEST = lax.Precision.HIGHEST
NEG_BIG = -1e+30

def matmul(left, right):
    return jnp.dot(left, right, precision=HIGHEST, preferred_element_type=jnp.float32)

def softmax_rows(scores):
    largest = lax.optimization_barrier(jnp.max(scores, -1, keepdims=True))
    expo = jnp.exp(scores - largest)
    return expo / lax.optimization_barrier(jnp.sum(expo, -1, keepdims=True))

def layer_norm(values, gain, shift):
    center = values - lax.optimization_barrier(jnp.mean(values, -1, keepdims=True))
    spread = lax.optimization_barrier(jnp.mean(center * center, -1, keepdims=True))
    return center * lax.rsqrt(spread + 1e-05) * gain + shift

def block_attention(kv_prompt, item):
    block_index, query_rows, kv_cont = item
    kv_seen = low_back(kv_prompt)
    keys = jnp.concatenate([kv_seen[:, :D], kv_cont[:, :D]], 0)
    values = jnp.concatenate([kv_seen[:, D:], kv_cont[:, D:]], 0)
    query_h = query_rows.reshape(-1, HEADS, DH)
    key_h = keys.reshape(-1, HEADS, DH)
    value_h = values.reshape(-1, HEADS, DH)
    scores = low_back(jnp.einsum('qhd,khd->hqk', query_h, key_h, precision=HIGHEST) * DH ** (-0.5))
    query_pos = jnp.concatenate([block_index * PD + jnp.arange(PD, dtype=jnp.int32), PROMPT + jnp.arange(CL, dtype=jnp.int32)])
    key_pos = jnp.arange(PROMPT + CL, dtype=jnp.int32)
    scores = jnp.where((key_pos[None, :] <= query_pos[:, None])[None], scores, NEG_BIG)
    attended = jnp.einsum('hqk,khd->qhd', low(softmax_rows(scores)), value_h, precision=HIGHEST)
    return attended.reshape(-1, D)

def student_head(stu_rows, pool_query, bias_pool, w_pool, w_class, bias_class):
    part_w = STU // SHEADS
    parts = stu_rows.reshape(CL, SHEADS, part_w)
    queries = pool_query.reshape(SHEADS, part_w)
    scores = jnp.einsum('tha,ha->ht', parts, queries, precision=HIGHEST) * part_w ** (-0.5)
    weights = softmax_rows(scores)
    pooled = jnp.einsum('ht,tha->ha', weights, parts, precision=HIGHEST).reshape(STU)
    top_layer = jnp.tanh(matmul(pooled, w_pool) + bias_pool)
    return matmul(top_layer, w_class) + bias_class

def group_forward(params, x_prompt, x_conts, cot_all, label_row):
    w_qkv, w_out, w_in, w_ffo, layer_biases, norm_gains, bias_in, w_student, student_vectors, w_pool, w_class, bias_class = params
    tokens = jnp.concatenate([x_prompt, x_conts.reshape(CONTS * CL, D)], 0)
    zero_row = jnp.zeros((D,), jnp.float32)
    bias_three = jnp.concatenate([layer_biases[0], zero_row, layer_biases[1]])
    qkv_raw = matmul(tokens, low(w_qkv)) + bias_three
    queries = low(low_back(qkv_raw[:, :D]))
    kv_prompt = low(qkv_raw[:PROMPT, D:])
    kv_cont = low(low_back(qkv_raw[PROMPT:, D:])).reshape(CONTS, CL, 2 * D)
    query_blocks = jnp.concatenate([queries[:PROMPT].reshape(CONTS, PD, D), queries[PROMPT:].reshape(CONTS, CL, D)], 1)
    blocks = lax.map(jax.checkpoint(partial(block_attention, kv_prompt)), (jnp.arange(CONTS, dtype=jnp.int32), query_blocks, kv_cont))
    attended_raw = jnp.concatenate([blocks[:, :PD].reshape(PROMPT, D), blocks[:, PD:].reshape(CONTS * CL, D)], 0)
    attended = low(low_back(attended_raw))
    branch = low_back(matmul(attended, low(w_out)) + layer_biases[2])
    first = layer_norm(tokens + branch, norm_gains[0], layer_biases[4])
    hidden = low_back(matmul(low(first), low(w_in)) + bias_in)
    ffn = low_back(matmul(low(jax.nn.gelu(hidden, approximate=False)), low(w_ffo)) + layer_biases[3])
    output = layer_norm(first + ffn, norm_gains[1], layer_biases[5])
    out_cont = output[PROMPT:].reshape(CONTS, CL, D)
    stu = low_back(jnp.einsum('cqd,de->cqe', low(out_cont), low(w_student), precision=HIGHEST) + student_vectors[0])
    logit_rows = jax.vmap(student_head, in_axes=(0, None, None, None, None, None))(stu, student_vectors[1], student_vectors[2], w_pool, w_class, bias_class)
    largest = lax.optimization_barrier(jnp.max(logit_rows, -1, keepdims=True))
    log_total = jnp.log(lax.optimization_barrier(jnp.sum(jnp.exp(logit_rows - largest), -1))) + largest[:, 0]
    picked = lax.optimization_barrier(jnp.sum(jnp.where(jnp.arange(CLASSES)[None, :] == label_row[:, None], logit_rows, 0.0), -1))
    objective = jnp.sum(output * cot_all) + jnp.sum(log_total - picked)
    return (objective, (output, logit_rows))

def reference(prompt, conts, prompt_cot, cont_cot, labels, w_qkv, w_out, w_in, w_ffo, layer_biases, norm_gains, bias_in, w_student, student_vectors, w_pool, w_class, bias_class):
    params = (w_qkv, w_out, w_in, w_ffo, layer_biases, norm_gains, bias_in, w_student, student_vectors, w_pool, w_class, bias_class)

    def group_step(totals, item):
        x_prompt, x_conts, cot_prompt, cot_conts, label_row = item
        cot_all = jnp.concatenate([cot_prompt.astype(jnp.float32), cot_conts.astype(jnp.float32).reshape(CONTS * CL, D)], 0)

        def closed(par, xp, xc):
            return group_forward(par, xp, xc, cot_all, label_row)
        objective, pull, extra = jax.vjp(closed, params, x_prompt.astype(jnp.float32), x_conts.astype(jnp.float32), has_aux=True)
        grad_par, grad_prompt, grad_conts = pull(jnp.ones((), jnp.float32))
        totals = jax.tree.map(jnp.add, totals, grad_par)
        output, logit_rows = extra
        outs = (output[:PROMPT].astype(jnp.bfloat16), output[PROMPT:].reshape(CONTS, CL, D).astype(jnp.bfloat16), logit_rows, grad_prompt, grad_conts)
        return (totals, outs)
    zeros = jax.tree.map(jnp.zeros_like, params)
    totals, ys = lax.scan(group_step, zeros, (prompt, conts, prompt_cot, cont_cot, labels))
    return (ys[0], ys[1], ys[2], ys[3], ys[4], totals[0], totals[1], totals[2], totals[3], totals[4], totals[5], totals[6], totals[7], totals[8], totals[9], totals[10], totals[11])
```

```python
import jax
import jax.numpy as jnp
from jax import lax
from jax.experimental import pallas as pl
from jax.experimental.pallas import tpu as pltpu
from jax.sharding import PartitionSpec as P

D = 768
HEADS = 12
DH = 64
STU = 128
SHEADS = 2


HIGHEST = lax.Precision.HIGHEST
NEG_BIG = -1e30


def dot_plain(left, right):
    return jnp.dot(left, right, preferred_element_type=jnp.float32)


def dot_first(left, right):
    return lax.dot_general(
        left, right, (((0,), (0,)), ((), ())), preferred_element_type=jnp.float32
    )


def dot_second(left, right):
    return lax.dot_general(
        left, right, (((1,), (1,)), ((), ())), preferred_element_type=jnp.float32
    )


def layer_norm(values, gain, shift):
    center = values - jnp.mean(values, -1, keepdims=True)
    spread = jnp.mean(center * center, -1, keepdims=True)
    return center * lax.rsqrt(spread + 1e-05) * gain + shift


def gelu_exact(values):
    return jax.nn.gelu(values, approximate=False)


TILE = 256
PAIR = 128
VMEM_ALL = 60 * 1024 * 1024


def rows_dot(left, right):
    return lax.dot_general(
        left, right, (((1,), (1,)), ((), ())), preferred_element_type=jnp.float32
    )


def low_lanes(shape):
    return lax.broadcasted_iota(jnp.int32, shape, len(shape) - 1) < DH


def attend_fwd_pair(shard, prompt_rows, q, kp, vp, kc, vc, att_ref, lse_ref):
    cont_len = kc.shape[0]
    prompt_len = kp.shape[0]
    for start in range(0, prompt_rows + cont_len, TILE):
        q_t = q[start : start + TILE, :] * jnp.asarray(DH ** (-0.5), jnp.bfloat16)
        halves = []
        for parity in range(2):
            keep = low_lanes(q_t.shape) == (parity == 0)
            q_h = jnp.where(keep, q_t, jnp.zeros_like(q_t))
            s_p = rows_dot(q_h, kp[...])
            if start < prompt_rows:
                key = lax.broadcasted_iota(jnp.int32, s_p.shape, 1)
                row = lax.broadcasted_iota(jnp.int32, s_p.shape, 0)
                s_p = jnp.where(key <= row + (shard * prompt_rows + start), s_p, NEG_BIG)
                largest = jnp.max(s_p, 1, keepdims=True)
                p_p = jnp.exp(s_p - largest)
                total = jnp.sum(p_p, 1, keepdims=True)
                o = dot_plain(p_p.astype(jnp.bfloat16), vp[...])
            else:
                seen = start - prompt_rows + TILE
                s_c = rows_dot(q_h, kc[:seen, :])
                key = lax.broadcasted_iota(jnp.int32, s_c.shape, 1)
                row = lax.broadcasted_iota(jnp.int32, s_c.shape, 0)
                s_c = jnp.where(key <= row + (start - prompt_rows), s_c, NEG_BIG)
                largest = jnp.maximum(
                    jnp.max(s_p, 1, keepdims=True), jnp.max(s_c, 1, keepdims=True)
                )
                p_p = jnp.exp(s_p - largest)
                p_c = jnp.exp(s_c - largest)
                total = jnp.sum(p_p, 1, keepdims=True) + jnp.sum(p_c, 1, keepdims=True)
                o = dot_plain(p_p.astype(jnp.bfloat16), vp[...]) + dot_plain(
                    p_c.astype(jnp.bfloat16), vc[:seen, :]
                )
            halves.append((o / total, largest + jnp.log(total)))
        keep = low_lanes((TILE, PAIR))
        att_ref[start : start + TILE, :] = jnp.where(keep, halves[0][0], halves[1][0])
        lse = jnp.where(
            keep,
            jnp.broadcast_to(halves[0][1], (TILE, PAIR)),
            jnp.broadcast_to(halves[1][1], (TILE, PAIR)),
        )
        turned = jnp.transpose(lse)
        lse_ref[0:1, start : start + TILE] = turned[0:1, :]
        lse_ref[1:2, start : start + TILE] = turned[DH : DH + 1, :]


def attend_bwd_pair(
    shard, prompt_rows, q, kp, vp, kc, vc, g, att, lse, dq, dkp, dvp, dkc, dvc, accum
):
    cont_len = kc.shape[0]
    tokens = prompt_rows + cont_len
    prompt_len = kp.shape[0]
    g_t = g[...]
    turned = jnp.transpose(g_t.astype(jnp.float32) * att[...])
    delta = (
        jnp.sum(turned[:DH], 0, keepdims=True),
        jnp.sum(turned[DH:], 0, keepdims=True),
    )
    q_t = q[...] * jnp.asarray(DH ** (-0.5), jnp.bfloat16)
    keep = low_lanes(q_t.shape)
    zero = jnp.zeros_like(q_t)
    q_h = (jnp.where(keep, q_t, zero), jnp.where(keep, zero, q_t))
    g_h = (jnp.where(keep, g_t, zero), jnp.where(keep, zero, g_t))
    accum[...] = jnp.zeros_like(accum)

    def block(key_b, value_b, first, mask):
        key_t = jnp.transpose(key_b.astype(jnp.float32)).astype(jnp.bfloat16)
        g_key = jnp.zeros((TILE, PAIR), jnp.float32)
        g_value = jnp.zeros((TILE, PAIR), jnp.float32)
        for parity in range(2):
            scores = rows_dot(key_b, q_h[parity][first:])
            probs = jnp.exp(scores - lse[parity : parity + 1, first:])
            masked = jnp.where(mask, probs[:, :TILE], 0.0)
            if tokens - first > TILE:
                probs = jnp.concatenate([masked, probs[:, TILE:]], 1)
            else:
                probs = masked
            g_probs = rows_dot(value_b, g_h[parity][first:])
            g_scores = (probs * (g_probs - delta[parity][:, first:])).astype(jnp.bfloat16)
            g_value += dot_plain(probs.astype(jnp.bfloat16), g_h[parity][first:])
            g_key += dot_plain(g_scores, q_h[parity][first:])
            rows = slice(parity * DH, (parity + 1) * DH)
            accum[rows, first:] += dot_plain(key_t[rows], g_scores)
        return g_key.astype(jnp.bfloat16), g_value.astype(jnp.bfloat16)

    ahead = lax.broadcasted_iota(jnp.int32, (TILE, TILE), 0) - lax.broadcasted_iota(
        jnp.int32, (TILE, TILE), 1
    )

    def prompt_block(index, start):
        rows = pl.ds(start, TILE)
        mask = ahead <= shard * prompt_rows - index * TILE
        g_key, g_value = block(kp[rows, :], vp[rows, :], 0, mask)
        dkp[rows, :] = g_key
        dvp[rows, :] = g_value

    blocks = prompt_len // TILE
    if blocks <= 4:
        for index in range(blocks):
            prompt_block(index, index * TILE)
    else:

        def step(index, carry):
            prompt_block(index, pl.multiple_of(index * TILE, TILE))
            return carry

        lax.fori_loop(0, blocks, step, 0)
    for start in range(0, cont_len, TILE):
        rows = slice(start, start + TILE)
        g_key, g_value = block(kc[rows, :], vc[rows, :], prompt_rows + start, ahead <= 0)
        dkc[rows, :] = g_key
        dvc[rows, :] = g_value
    dq[...] = (jnp.transpose(accum[...]) * DH ** (-0.5)).astype(jnp.bfloat16)


def attend_forward(qkv_b, kv_prompt, prompt_rows):
    tokens = qkv_b.shape[0]
    prompt_len = kv_prompt.shape[0]
    cont_len = tokens - prompt_rows
    pairs = HEADS // 2

    def kernel(q, kp, vp, ko, vo, att_ref, lse_ref):
        attend_fwd_pair(
            lax.axis_index("shard"),
            prompt_rows,
            q,
            kp,
            vp,
            ko.at[prompt_rows:, :],
            vo.at[prompt_rows:, :],
            att_ref,
            lse_ref.at[0],
        )

    return pl.pallas_call(
        kernel,
        grid=(pairs,),
        in_specs=[
            pl.BlockSpec((tokens, PAIR), lambda p: (0, p)),
            pl.BlockSpec((prompt_len, PAIR), lambda p: (0, p)),
            pl.BlockSpec((prompt_len, PAIR), lambda p: (0, pairs + p)),
            pl.BlockSpec((tokens, PAIR), lambda p: (0, pairs + p)),
            pl.BlockSpec((tokens, PAIR), lambda p: (0, 2 * pairs + p)),
        ],
        out_specs=[
            pl.BlockSpec((tokens, PAIR), lambda p: (0, p)),
            pl.BlockSpec((1, 8, tokens), lambda p: (p, 0, 0)),
        ],
        out_shape=[
            jax.ShapeDtypeStruct((tokens, D), jnp.float32),
            jax.ShapeDtypeStruct((pairs, 8, tokens), jnp.float32),
        ],
        compiler_params=pltpu.CompilerParams(vmem_limit_bytes=VMEM_ALL),
        name="attend_forward",
    )(qkv_b, kv_prompt, kv_prompt, qkv_b, qkv_b)


def attend_backward(qkv_b, kv_prompt, g_att, att, lse, prompt_rows):
    tokens = qkv_b.shape[0]
    prompt_len = kv_prompt.shape[0]
    cont_len = tokens - prompt_rows
    pairs = HEADS // 2

    def kernel(q, kp, vp, ko, vo, g, a, ls, dq, dkp, dvp, dkc, dvc, accum):
        attend_bwd_pair(
            lax.axis_index("shard"),
            prompt_rows,
            q,
            kp,
            vp,
            ko.at[prompt_rows:, :],
            vo.at[prompt_rows:, :],
            g,
            a,
            ls.at[0],
            dq,
            dkp,
            dvp,
            dkc,
            dvc,
            accum,
        )

    def columns(rows):
        return pl.BlockSpec((rows, PAIR), lambda p: (0, p))

    return pl.pallas_call(
        kernel,
        grid=(pairs,),
        in_specs=[
            columns(tokens),
            columns(prompt_len),
            pl.BlockSpec((prompt_len, PAIR), lambda p: (0, pairs + p)),
            pl.BlockSpec((tokens, PAIR), lambda p: (0, pairs + p)),
            pl.BlockSpec((tokens, PAIR), lambda p: (0, 2 * pairs + p)),
            columns(tokens),
            columns(tokens),
            pl.BlockSpec((1, 8, tokens), lambda p: (p, 0, 0)),
        ],
        out_specs=[
            columns(tokens),
            columns(prompt_len),
            columns(prompt_len),
            columns(cont_len),
            columns(cont_len),
        ],
        out_shape=[
            jax.ShapeDtypeStruct((tokens, D), jnp.bfloat16),
            jax.ShapeDtypeStruct((prompt_len, D), jnp.bfloat16),
            jax.ShapeDtypeStruct((prompt_len, D), jnp.bfloat16),
            jax.ShapeDtypeStruct((cont_len, D), jnp.bfloat16),
            jax.ShapeDtypeStruct((cont_len, D), jnp.bfloat16),
        ],
        scratch_shapes=[pltpu.VMEM((PAIR, tokens), jnp.float32)],
        compiler_params=pltpu.CompilerParams(vmem_limit_bytes=VMEM_ALL),
        name="attend_backward",
    )(qkv_b, kv_prompt, kv_prompt, qkv_b, qkv_b, g_att, att, lse)


MESH_ID = pl.DeviceIdType.MESH


def sum_gradients(g_qkv, g_out, g_in, g_ffo, g_small):
    pieces = 12
    rows = g_qkv.shape[0] // 4
    width, half, quarter = D, D // 2, rows // 4
    s_width, s_half = g_small.shape[1], g_small.shape[1] // 2
    ahead = 3

    def kernel(
        gq, go, gi, gf, gs, out, out_s,
        own, cr, xs, xr, yb, yr, zb, zr, fb,
        own_s, cr_s, xs_s, xr_s, yb_s, yr_s, zb_s, zr_s, fb_s,
        sem_own, c_send, c_recv, x_send, x_recv, y_send, y_recv, z_send, z_recv,
        f_send, f_recv, o_send, o_recv, o_own, g_send, g_recv,
    ):
        rep, shard = lax.axis_index("rep"), lax.axis_index("shard")
        z, y = rep // 2, rep % 2
        x, core = shard // 2, shard % 2
        partner = (rep, 2 * x + 1 - core)
        across = (rep, 2 * (1 - x) + core)
        beside = (2 * z + 1 - y, shard)

        def along(step):
            return (2 * lax.rem(z + step, 4) + y, shard)

        barrier = pltpu.get_barrier_semaphore()
        others = [partner, across, beside, along(1), along(2), along(3)]
        far = (rep, 2 * (1 - x) + 1 - core)
        for other in others + [far]:
            pl.semaphore_signal(barrier, inc=1, device_id=other, device_id_type=MESH_ID)
        pl.semaphore_wait(barrier, len(others) + 1)

        def remote(source, target, send, recv, device):
            return pltpu.make_async_remote_copy(
                src_ref=source,
                dst_ref=target,
                send_sem=send,
                recv_sem=recv,
                device_id=device,
                device_id_type=MESH_ID,
            )

        def source(k, block):
            if k < 4:
                return gf.at[pl.ds(block * 4 * rows + k * rows, rows), :]
            if k < 8:
                return gi.at[pl.ds(block * rows, rows), (k - 4) * width : (k - 3) * width]
            if k < 9:
                return go.at[pl.ds(block * rows, rows), :]
            if k < 12:
                return gq.at[pl.ds(block * rows, rows), (k - 9) * width : (k - 8) * width]
            return gs.at[pl.ds(block * rows, rows), :]

        big = (own, cr, xs, xr, yb, yr, zb, zr, fb, half)
        small = (own_s, cr_s, xs_s, xr_s, yb_s, yr_s, zb_s, zr_s, fb_s, s_half)

        def bufs(k):
            if isinstance(k, int) and k == pieces:
                return small, 0
            return big, k

        def core_copy(k, xx):
            b, i = bufs(k)
            return remote(
                source(k, 2 * xx + 1 - core) if isinstance(k, int) else b[1].at[i, xx],
                b[1].at[i, xx],
                c_send.at[k, xx],
                c_recv.at[k, xx],
                partner,
            )

        def own_copy(k, xx):
            b, i = bufs(k)
            return pltpu.make_async_copy(
                source(k, 2 * xx + core) if isinstance(k, int) else b[0].at[i, xx],
                b[0].at[i, xx],
                sem_own.at[k, xx],
            )

        def x_copy(k):
            b, i = bufs(k)
            return remote(b[2].at[i], b[3].at[i], x_send.at[k], x_recv.at[k], across)

        def y_copy(k):
            b, i = bufs(k)
            return remote(b[4].at[i, 1 - y], b[5].at[i], y_send.at[k], y_recv.at[k], beside)

        def z_copy(k, step, buf, slot, send, recv, target):
            return remote(buf, target, send.at[k, step - 1], recv.at[k, slot], along(step))

        def zs_copy(k, step):
            b, i = bufs(k)
            return z_copy(
                k, step, b[6].at[i, lax.rem(z + step, 4)], z, z_send, z_recv, b[7].at[i, z]
            )

        def zr_wait(k, step):
            b, i = bufs(k)
            slot = lax.rem(z + step, 4)
            z_copy(k, step, b[7].at[i, slot], slot, z_send, z_recv, b[7].at[i, slot]).wait_recv()

        def fs_copy(k, step):
            b, i = bufs(k)
            return z_copy(k, step, b[8].at[i, z], z, f_send, f_recv, b[8].at[i, z])

        def fr_wait(k, step):
            b, i = bufs(k)
            slot = lax.rem(z + step, 4)
            z_copy(k, step, b[8].at[i, slot], slot, f_send, f_recv, b[8].at[i, slot]).wait_recv()

        def final(k, yy):
            if isinstance(k, int) and k == pieces:
                return out_s.at[shard, :, :, pl.ds(pl.multiple_of(yy * s_half, 128), s_half)]
            return out.at[k, :, :, pl.ds(pl.multiple_of(yy * half, 128), half)]

        def o_copy(k):
            b, i = bufs(k)
            return remote(b[8].at[i], final(k, y), o_send.at[k], o_recv.at[k], beside)

        def o_wait(k):
            b, i = bufs(k)
            remote(b[8].at[i], final(k, 1 - y), o_send.at[k], o_recv.at[k], beside).wait_recv()

        def o_local(k):
            b, i = bufs(k)
            return pltpu.make_async_copy(b[8].at[i], final(k, y), o_own.at[k])

        def wide(value):
            return value.astype(jnp.float32)

        def stage_x(k):
            b, i = bufs(k)
            for xx in range(2):
                core_copy(k, xx).wait_recv()
                own_copy(k, xx).wait()
            b[2][i] = (wide(b[0][i, 1 - x]) + wide(b[1][i, 1 - x])).astype(jnp.bfloat16)
            x_copy(k).start()

        def stage_y(k):
            b, i = bufs(k)
            x_copy(k).wait_recv()
            total = (wide(b[0][i, x]) + wide(b[1][i, x]) + wide(b[3][i])).astype(jnp.bfloat16)
            cut = b[9]
            b[4][i, 0] = total[:, :cut]
            b[4][i, 1] = total[:, cut:]
            y_copy(k).start()

        def stage_z(k):
            b, i = bufs(k)
            y_copy(k).wait_recv()
            total = (wide(b[4][i, y]) + wide(b[5][i])).astype(jnp.bfloat16)
            for q in range(4):
                b[6][i, q] = total[q * quarter : (q + 1) * quarter]
            for step in (2, 1, 3):
                zs_copy(k, step).start()

        def stage_f(k):
            b, i = bufs(k)
            total = wide(b[6][i, z])
            for step in (1, 2, 3):
                zr_wait(k, step)
                total += wide(b[7][i, lax.rem(z + step, 4)])
            b[8][i, z] = total.astype(jnp.bfloat16)
            for step in (2, 1, 3):
                fs_copy(k, step).start()

        def stage_o(k):
            for step in (1, 2, 3):
                fr_wait(k, step)
            o_copy(k).start()
            o_local(k).start()

        def g_copy(step):
            return remote(
                out_s.at[shard],
                out_s.at[shard],
                g_send.at[step - 1],
                g_recv.at[shard],
                (rep, lax.rem(shard + step, 4)),
            )

        def stage_g():
            o_wait(pieces)
            o_local(pieces).wait()
            for step in (1, 2, 3):
                g_copy(step).start()

        order = [pieces] + list(range(pieces))
        for k in order:
            for xx in range(2):
                core_copy(k, xx).start()
                own_copy(k, xx).start()
        stage_x(pieces)
        for k in range(ahead):
            stage_x(k)
        small_stages = [stage_y, stage_z, stage_f, stage_o]

        def tick(t, carry):
            @pl.when(t + ahead < pieces)
            def _():
                stage_x(t + ahead)

            for at, stage in enumerate(small_stages):

                @pl.when(t == at)
                def _(stage=stage):
                    stage(pieces)

            @pl.when(t == len(small_stages))
            def _():
                stage_g()

            @pl.when(t < pieces)
            def _():
                stage_y(t)

            for late, stage in ((1, stage_z), (2, stage_f), (3, stage_o)):

                @pl.when((t >= late) & (t < pieces + late))
                def _(late=late, stage=stage):
                    stage(t - late)

            return carry

        lax.fori_loop(0, pieces + 3, tick, 0)

        def finish(k):
            for xx in range(2):
                core_copy(k, xx).wait_send()
            x_copy(k).wait_send()
            y_copy(k).wait_send()
            for step in (1, 2, 3):
                zs_copy(k, step).wait_send()
                fs_copy(k, step).wait_send()
            o_copy(k).wait_send()

        def last(k, carry):
            o_wait(k)
            o_local(k).wait()
            finish(k)
            return carry

        lax.fori_loop(0, pieces, last, 0)
        finish(pieces)
        for step in (1, 2, 3):
            slot = lax.rem(shard + step, 4)
            remote(
                out_s.at[slot], out_s.at[slot], g_send.at[step - 1], g_recv.at[slot], far
            ).wait_recv()
            g_copy(step).wait_send()

    def buffers(count, wide_cols):
        cut = wide_cols // 2
        return [
            pltpu.VMEM((count, 2, rows, wide_cols), jnp.bfloat16),
            pltpu.VMEM((count, 2, rows, wide_cols), jnp.bfloat16),
            pltpu.VMEM((count, rows, wide_cols), jnp.bfloat16),
            pltpu.VMEM((count, rows, wide_cols), jnp.bfloat16),
            pltpu.VMEM((count, 2, rows, cut), jnp.bfloat16),
            pltpu.VMEM((count, rows, cut), jnp.bfloat16),
            pltpu.VMEM((count, 4, quarter, cut), jnp.bfloat16),
            pltpu.VMEM((count, 4, quarter, cut), jnp.bfloat16),
            pltpu.VMEM((count, 4, quarter, cut), jnp.bfloat16),
        ]

    def sems(*dims):
        return pltpu.SemaphoreType.DMA(dims)

    n = pieces + 1
    anywhere = pl.BlockSpec(memory_space=pl.ANY)
    out, out_s = pl.pallas_call(
        kernel,
        in_specs=[anywhere] * 5,
        out_specs=[anywhere, pl.BlockSpec(memory_space=pltpu.VMEM)],
        out_shape=[
            jax.ShapeDtypeStruct((pieces, 4, quarter, width), jnp.bfloat16),
            jax.ShapeDtypeStruct((4, 4, quarter, s_width), jnp.bfloat16),
        ],
        scratch_shapes=buffers(pieces, width)
        + buffers(1, s_width)
        + [
            sems(n, 2), sems(n, 2), sems(n, 2), sems(n), sems(n), sems(n), sems(n),
            sems(n, 3), sems(n, 4), sems(n, 3), sems(n, 4), sems(n), sems(n), sems(n),
            sems(3), sems(4),
        ],
        compiler_params=pltpu.CompilerParams(
            collective_id=0, has_side_effects=True, vmem_limit_bytes=VMEM_ALL
        ),
        name="sum_gradients",
    )(g_qkv, g_out, g_in, g_ffo, g_small)
    return out.reshape(pieces, rows, width), out_s.reshape(4 * rows, s_width)


def student_loss(stu_rows, pool_query, bias_pool, w_pool, w_class, bias_class, label_value):
    part_w = STU // SHEADS
    parts = stu_rows.reshape(stu_rows.shape[0], SHEADS, part_w)
    queries = pool_query.reshape(SHEADS, part_w)
    scores = jnp.einsum("tha,ha->ht", parts, queries, precision=HIGHEST) * part_w ** (-0.5)
    largest = jnp.max(scores, -1, keepdims=True)
    expo = jnp.exp(scores - largest)
    weights = expo / jnp.sum(expo, -1, keepdims=True)
    pooled = jnp.einsum("ht,tha->ha", weights, parts, precision=HIGHEST).reshape(STU)
    top_layer = jnp.tanh(jnp.dot(pooled, w_pool, precision=HIGHEST) + bias_pool)
    logit_row = jnp.dot(top_layer, w_class, precision=HIGHEST) + bias_class
    top_logit = jnp.max(logit_row)
    log_total = jnp.log(jnp.sum(jnp.exp(logit_row - top_logit))) + top_logit
    picked = jnp.sum(jnp.where(jnp.arange(logit_row.shape[0]) == label_value, logit_row, 0.0))
    return (log_total - picked, logit_row)


def sum_native(g_qkvw, g_outw, g_in, g_ffo, small):
    def over(grad):
        part = lax.psum_scatter(
            grad.astype(jnp.bfloat16), "shard", scatter_dimension=0, tiled=True
        )
        return lax.psum(part, "rep").astype(jnp.float32)

    owned = tuple(over(grad) for grad in (g_qkvw, g_outw, g_in, g_ffo))
    return owned, lax.psum(small, ("rep", "shard"))


def sum_direct(g_qkvw, g_outw, g_in, g_ffo, small):
    biases, gains, in_bias, student, vectors, pool, class_w, class_b = small
    parts = [
        biases.reshape(-1, 128),
        gains.reshape(-1, 128),
        in_bias.reshape(-1, 128),
        vectors.reshape(-1, 128),
        pool.reshape(-1, 128),
        jnp.pad(class_w, ((0, 0), (0, 128 - class_w.shape[1]))),
        jnp.pad(class_b[None], ((0, 0), (0, 128 - class_b.shape[0]))),
    ]
    used = sum(part.shape[0] for part in parts)
    side = jnp.concatenate(parts + [jnp.zeros((D - used, 128), jnp.float32)], 0)
    packed = jnp.concatenate([student, side], 1).astype(jnp.bfloat16)
    low = [grad.astype(jnp.bfloat16) for grad in (g_qkvw, g_outw, g_in, g_ffo)]
    out, summed = sum_gradients(*low, packed)
    out = out.astype(jnp.float32)
    summed = summed.astype(jnp.float32)
    owned = (
        jnp.concatenate([out[9], out[10], out[11]], 1),
        out[8],
        jnp.concatenate([out[4], out[5], out[6], out[7]], 1),
        out[:4].reshape(-1, D),
    )
    result, at = [summed[:, :128]], 0
    for part in parts:
        result.append(summed[at : at + part.shape[0], 128:])
        at += part.shape[0]
    return owned, (
        result[1].reshape(biases.shape),
        result[2].reshape(gains.shape),
        result[3].reshape(in_bias.shape),
        result[0],
        result[4].reshape(vectors.shape),
        result[5].reshape(pool.shape),
        result[6][:, : class_w.shape[1]],
        result[7][0, : class_b.shape[0]],
    )


def body(
    prompt,
    conts,
    prompt_cot,
    cont_cot,
    labels,
    w_qkv,
    w_out,
    w_in,
    w_ffo,
    layer_biases,
    norm_gains,
    bias_in,
    w_student,
    student_vectors,
    w_pool,
    w_class,
    bias_class,
):
    prompt_rows = prompt.shape[1]
    cont_len = conts.shape[2]
    prompt_len = prompt_rows * lax.axis_size("shard")
    qkv_low = w_qkv.astype(jnp.bfloat16)
    out_low = w_out.astype(jnp.bfloat16)
    in_low = w_in.astype(jnp.bfloat16)
    ffo_low = w_ffo.astype(jnp.bfloat16)
    qkv_full, out_full, in_full, ffo_full = (
        lax.all_gather(qkv_low, "shard", axis=0, tiled=True),
        lax.all_gather(out_low, "shard", axis=0, tiled=True),
        lax.all_gather(in_low, "shard", axis=0, tiled=True),
        lax.all_gather(ffo_low, "shard", axis=0, tiled=True),
    )
    tokens = jnp.concatenate([prompt[0], conts[0, 0]], 0)
    tokens_f = tokens.astype(jnp.float32)
    zero_row = jnp.zeros((D,), jnp.float32)
    bias_three = jnp.concatenate([layer_biases[0], zero_row, layer_biases[1]])
    qkv_b = (dot_plain(tokens, qkv_full) + bias_three).astype(jnp.bfloat16)
    kv_prompt = lax.all_gather(qkv_b[:prompt_rows, D:], "shard", axis=0, tiled=True)
    attended, log_totals = attend_forward(qkv_b, kv_prompt, prompt_rows)
    att_b = attended.astype(jnp.bfloat16)
    branch = dot_plain(att_b, out_full) + layer_biases[2]
    resid_one = tokens_f + branch
    first = layer_norm(resid_one, norm_gains[0], layer_biases[4])
    first_b = first.astype(jnp.bfloat16)
    hidden = dot_plain(first_b, in_full) + bias_in
    act_b = gelu_exact(hidden).astype(jnp.bfloat16)
    ffn = dot_plain(act_b, ffo_full) + layer_biases[3]
    resid_two = first + ffn
    output = layer_norm(resid_two, norm_gains[1], layer_biases[5])
    output_b = output.astype(jnp.bfloat16)
    cont_b = output_b[prompt_rows:]
    student_low = w_student.astype(jnp.bfloat16)
    stu = dot_plain(cont_b, student_low) + student_vectors[0]

    def loss_closed(stu_rows, pool_query, bias_pool, pool_weight, class_weight, class_bias):
        return student_loss(
            stu_rows, pool_query, bias_pool, pool_weight, class_weight, class_bias, labels[0, 0]
        )

    loss_value, loss_pull, logit_row = jax.vjp(
        loss_closed,
        stu,
        student_vectors[1],
        student_vectors[2],
        w_pool,
        w_class,
        bias_class,
        has_aux=True,
    )
    g_stu, g_query, g_pbias, g_pool, g_class, g_cbias = loss_pull(jnp.ones((), jnp.float32))
    g_stu_b = g_stu.astype(jnp.bfloat16)
    g_sbias = jnp.sum(g_stu_b.astype(jnp.float32), 0)
    g_student = dot_first(cont_b, g_stu_b)
    student_back = dot_second(g_stu_b, student_low)
    g_output = jnp.concatenate([prompt_cot[0], cont_cot[0, 0]], 0).astype(jnp.float32)
    g_output = g_output + jnp.concatenate(
        [jnp.zeros((prompt_rows, D), jnp.float32), student_back], 0
    )
    qkv_back, out_back, in_back, ffo_back = (
        lax.all_gather(qkv_low, "shard", axis=0, tiled=True),
        lax.all_gather(out_low, "shard", axis=0, tiled=True),
        lax.all_gather(in_low, "shard", axis=0, tiled=True),
        lax.all_gather(ffo_low, "shard", axis=0, tiled=True),
    )
    norm_two, norm_two_pull = jax.vjp(layer_norm, resid_two, norm_gains[1], layer_biases[5])
    g_resid_two, g_gain_two, g_shift_two = norm_two_pull(g_output)
    g_ffn_b = g_resid_two.astype(jnp.bfloat16)
    g_ffo = dot_first(act_b, g_ffn_b)
    g_ffo_bias = jnp.sum(g_ffn_b.astype(jnp.float32), 0)
    g_act = dot_second(g_ffn_b, ffo_back)
    gelu_value, gelu_pull = jax.vjp(gelu_exact, hidden)
    g_hidden_b = gelu_pull(g_act)[0].astype(jnp.bfloat16)
    g_in = dot_first(first_b, g_hidden_b)
    g_in_bias = jnp.sum(g_hidden_b.astype(jnp.float32), 0)
    g_first = g_resid_two + dot_second(g_hidden_b, in_back)
    norm_one, norm_one_pull = jax.vjp(layer_norm, resid_one, norm_gains[0], layer_biases[4])
    g_resid_one, g_gain_one, g_shift_one = norm_one_pull(g_first)
    g_branch_b = g_resid_one.astype(jnp.bfloat16)
    g_outw = dot_first(att_b, g_branch_b)
    g_out_bias = jnp.sum(g_branch_b.astype(jnp.float32), 0)
    g_att_b = dot_second(g_branch_b, out_back).astype(jnp.bfloat16)
    query_grad_b, g_keys_p, g_values_p, g_keys_c, g_values_c = attend_backward(
        qkv_b, kv_prompt, g_att_b, attended, log_totals, prompt_rows
    )
    cont_kv_b = jnp.concatenate([g_keys_c, g_values_c], 1)
    block_kv_b = jnp.concatenate([g_keys_p, g_values_p], 1)
    kv_weights = qkv_back[:, D:]
    g_query_w = dot_first(tokens, query_grad_b)
    g_kv_w = dot_first(tokens[prompt_rows:], cont_kv_b)
    g_tokens = g_resid_one + dot_second(query_grad_b, qkv_back[:, :D])
    cont_through = dot_second(cont_kv_b, kv_weights)
    kv_summed = lax.psum_scatter(
        block_kv_b,
        "shard",
        scatter_dimension=0,
        tiled=True,
    ).astype(jnp.float32)
    g_kv_w = g_kv_w + lax.dot_general(
        tokens_f[:prompt_rows],
        kv_summed,
        (((0,), (0,)), ((), ())),
        precision=HIGHEST,
        preferred_element_type=jnp.float32,
    )
    prompt_through = jnp.dot(
        kv_summed,
        kv_weights.astype(jnp.float32).T,
        precision=HIGHEST,
        preferred_element_type=jnp.float32,
    )
    value_cols = jnp.sum(kv_summed[:, D:], 0)
    g_tokens = g_tokens + jnp.concatenate([prompt_through, cont_through], 0)
    g_qkvw = jnp.concatenate([g_query_w, g_kv_w], 1)
    g_query_bias = jnp.sum(query_grad_b.astype(jnp.float32), 0)
    g_value_bias = jnp.sum(cont_kv_b[:, D:].astype(jnp.float32), 0) + value_cols
    g_biases = jnp.stack(
        [g_query_bias, g_value_bias, g_out_bias, g_ffo_bias, g_shift_one, g_shift_two]
    )
    g_gains = jnp.stack([g_gain_one, g_gain_two])
    g_vectors = jnp.stack([g_sbias, g_query, g_pbias])
    small = (g_biases, g_gains, g_in_bias, g_student, g_vectors, g_pool, g_class, g_cbias)
    direct = (lax.axis_size("rep"), lax.axis_size("shard")) == (8, 4)
    owned, summed = (sum_direct if direct else sum_native)(g_qkvw, g_outw, g_in, g_ffo, small)
    owned_qkv, owned_out, owned_in, owned_ffo = owned
    return (
        output_b[:prompt_rows][None],
        output_b[prompt_rows:][None, None],
        logit_row[None, None],
        g_tokens[:prompt_rows][None],
        g_tokens[prompt_rows:][None, None],
        owned_qkv,
        owned_out,
        owned_in,
        owned_ffo,
        summed[0],
        summed[1],
        summed[2],
        summed[3],
        summed[4],
        summed[5],
        summed[6],
        summed[7],
    )


def solution(mesh):
    return jax.shard_map(
        body,
        mesh=mesh,
        in_specs=(
            P("rep", "shard", None),
            P("rep", "shard", None, None),
            P("rep", "shard", None),
            P("rep", "shard", None, None),
            P("rep", "shard"),
            P("shard", None),
            P("shard", None),
            P("shard", None),
            P("shard", None),
            P(),
            P(),
            P(),
            P(),
            P(),
            P(),
            P(),
            P(),
        ),
        out_specs=(
            P("rep", "shard", None),
            P("rep", "shard", None, None),
            P("rep", "shard", None),
            P("rep", "shard", None),
            P("rep", "shard", None, None),
            P("shard", None),
            P("shard", None),
            P("shard", None),
            P("shard", None),
            P(),
            P(),
            P(),
            P(),
            P(),
            P(),
            P(),
            P(),
        ),
        check_vma=False,
    )
```

```python
import jax
import jax.numpy as jnp
from jax import lax
from jax.experimental import pallas as pl
from jax.experimental.pallas import tpu as pltpu
from jax.sharding import PartitionSpec as P

D = 768
HEADS = 12
DH = 64
STU = 128
SHEADS = 2


HIGHEST = lax.Precision.HIGHEST
NEG_BIG = -1e30


def dot_plain(left, right):
    return jnp.dot(left, right, preferred_element_type=jnp.float32)


def dot_first(left, right):
    return lax.dot_general(
        left, right, (((0,), (0,)), ((), ())), preferred_element_type=jnp.float32
    )


def dot_second(left, right):
    return lax.dot_general(
        left, right, (((1,), (1,)), ((), ())), preferred_element_type=jnp.float32
    )


def layer_norm(values, gain, shift):
    center = values - jnp.mean(values, -1, keepdims=True)
    spread = jnp.mean(center * center, -1, keepdims=True)
    return center * lax.rsqrt(spread + 1e-05) * gain + shift


def gelu_exact(values):
    return jax.nn.gelu(values, approximate=False)


TILE = 256
PAIR = 128
VMEM_ALL = 60 * 1024 * 1024


def rows_dot(left, right):
    return lax.dot_general(
        left, right, (((1,), (1,)), ((), ())), preferred_element_type=jnp.float32
    )


def low_lanes(shape):
    return lax.broadcasted_iota(jnp.int32, shape, len(shape) - 1) < DH


def attend_fwd_pair(
    shard, prompt_rows, q, kp, vp, kc, vc, att_ref, lse_ref, between=None
):
    cont_len = kc.shape[0]
    prompt_len = kp.shape[0]
    for start in range(0, prompt_rows + cont_len, TILE):
        q_t = q[start : start + TILE, :] * jnp.asarray(DH ** (-0.5), jnp.bfloat16)
        halves = []
        for parity in range(2):
            keep = low_lanes(q_t.shape) == (parity == 0)
            q_h = jnp.where(keep, q_t, jnp.zeros_like(q_t))
            s_p = rows_dot(q_h, kp[...])
            if start < prompt_rows:
                key = lax.broadcasted_iota(jnp.int32, s_p.shape, 1)
                row = lax.broadcasted_iota(jnp.int32, s_p.shape, 0)
                s_p = jnp.where(key <= row + (shard * prompt_rows + start), s_p, NEG_BIG)
                largest = jnp.max(s_p, 1, keepdims=True)
                p_p = jnp.exp(s_p - largest)
                total = jnp.sum(p_p, 1, keepdims=True)
                o = dot_plain(p_p.astype(jnp.bfloat16), vp[...])
            else:
                seen = start - prompt_rows + TILE
                s_c = rows_dot(q_h, kc[:seen, :])
                key = lax.broadcasted_iota(jnp.int32, s_c.shape, 1)
                row = lax.broadcasted_iota(jnp.int32, s_c.shape, 0)
                s_c = jnp.where(key <= row + (start - prompt_rows), s_c, NEG_BIG)
                largest = jnp.maximum(
                    jnp.max(s_p, 1, keepdims=True), jnp.max(s_c, 1, keepdims=True)
                )
                p_p = jnp.exp(s_p - largest)
                p_c = jnp.exp(s_c - largest)
                total = jnp.sum(p_p, 1, keepdims=True) + jnp.sum(p_c, 1, keepdims=True)
                o = dot_plain(p_p.astype(jnp.bfloat16), vp[...]) + dot_plain(
                    p_c.astype(jnp.bfloat16), vc[:seen, :]
                )
            halves.append((o / total, largest + jnp.log(total)))
        keep = low_lanes((TILE, PAIR))
        att_ref[start : start + TILE, :] = jnp.where(keep, halves[0][0], halves[1][0])
        lse = jnp.where(
            keep,
            jnp.broadcast_to(halves[0][1], (TILE, PAIR)),
            jnp.broadcast_to(halves[1][1], (TILE, PAIR)),
        )
        turned = jnp.transpose(lse)
        lse_ref[0:1, start : start + TILE] = turned[0:1, :]
        lse_ref[1:2, start : start + TILE] = turned[DH : DH + 1, :]
        if between is not None:
            between(start // TILE)


def attend_bwd_pair(
    shard, prompt_rows, q, kp, vp, kc, vc, g, att, lse, dq, dkp, dvp, dkc, dvc, accum
):
    cont_len = kc.shape[0]
    tokens = prompt_rows + cont_len
    prompt_len = kp.shape[0]
    g_t = g[...]
    turned = jnp.transpose(g_t.astype(jnp.float32) * att[...])
    delta = (
        jnp.sum(turned[:DH], 0, keepdims=True),
        jnp.sum(turned[DH:], 0, keepdims=True),
    )
    q_t = q[...] * jnp.asarray(DH ** (-0.5), jnp.bfloat16)
    keep = low_lanes(q_t.shape)
    zero = jnp.zeros_like(q_t)
    q_h = (jnp.where(keep, q_t, zero), jnp.where(keep, zero, q_t))
    g_h = (jnp.where(keep, g_t, zero), jnp.where(keep, zero, g_t))
    accum[...] = jnp.zeros_like(accum)

    def block(key_b, value_b, first, mask):
        key_t = jnp.transpose(key_b.astype(jnp.float32)).astype(jnp.bfloat16)
        g_key = jnp.zeros((TILE, PAIR), jnp.float32)
        g_value = jnp.zeros((TILE, PAIR), jnp.float32)
        for parity in range(2):
            scores = rows_dot(key_b, q_h[parity][first:])
            probs = jnp.exp(scores - lse[parity : parity + 1, first:])
            masked = jnp.where(mask, probs[:, :TILE], 0.0)
            if tokens - first > TILE:
                probs = jnp.concatenate([masked, probs[:, TILE:]], 1)
            else:
                probs = masked
            g_probs = rows_dot(value_b, g_h[parity][first:])
            g_scores = (probs * (g_probs - delta[parity][:, first:])).astype(jnp.bfloat16)
            g_value += dot_plain(probs.astype(jnp.bfloat16), g_h[parity][first:])
            g_key += dot_plain(g_scores, q_h[parity][first:])
            rows = slice(parity * DH, (parity + 1) * DH)
            accum[rows, first:] += dot_plain(key_t[rows], g_scores)
        return g_key.astype(jnp.bfloat16), g_value.astype(jnp.bfloat16)

    ahead = lax.broadcasted_iota(jnp.int32, (TILE, TILE), 0) - lax.broadcasted_iota(
        jnp.int32, (TILE, TILE), 1
    )

    def prompt_block(index, start):
        rows = pl.ds(start, TILE)
        mask = ahead <= shard * prompt_rows - index * TILE
        g_key, g_value = block(kp[rows, :], vp[rows, :], 0, mask)
        dkp[rows, :] = g_key
        dvp[rows, :] = g_value

    blocks = prompt_len // TILE
    if blocks <= 4:
        for index in range(blocks):
            prompt_block(index, index * TILE)
    else:

        def step(index, carry):
            prompt_block(index, pl.multiple_of(index * TILE, TILE))
            return carry

        lax.fori_loop(0, blocks, step, 0)
    for start in range(0, cont_len, TILE):
        rows = slice(start, start + TILE)
        g_key, g_value = block(kc[rows, :], vc[rows, :], prompt_rows + start, ahead <= 0)
        dkc[rows, :] = g_key
        dvc[rows, :] = g_value
    dq[...] = (jnp.transpose(accum[...]) * DH ** (-0.5)).astype(jnp.bfloat16)


def attend_forward(q, kp, vp, kc, vc, prompt_rows):
    tokens, prompt_len, cont_len = q.shape[0], kp.shape[0], kc.shape[0]
    pairs = HEADS // 2

    def kernel(q, kp, vp, kc, vc, att_ref, lse_ref):
        attend_fwd_pair(
            lax.axis_index("shard"), prompt_rows, q, kp, vp, kc, vc, att_ref, lse_ref.at[0]
        )

    def columns(rows):
        return pl.BlockSpec((rows, PAIR), lambda p: (0, p))

    return pl.pallas_call(
        kernel,
        grid=(pairs,),
        in_specs=[columns(rows) for rows in (tokens, prompt_len, prompt_len, cont_len, cont_len)],
        out_specs=[columns(tokens), pl.BlockSpec((1, 8, tokens), lambda p: (p, 0, 0))],
        out_shape=[
            jax.ShapeDtypeStruct((tokens, D), jnp.float32),
            jax.ShapeDtypeStruct((pairs, 8, tokens), jnp.float32),
        ],
        compiler_params=pltpu.CompilerParams(vmem_limit_bytes=VMEM_ALL),
        name="attend_forward",
    )(q, kp, vp, kc, vc)


def attend_backward(q, kp, vp, kc, vc, g_att, att, lse, prompt_rows):
    tokens, prompt_len, cont_len = q.shape[0], kp.shape[0], kc.shape[0]
    pairs = HEADS // 2

    def kernel(q, kp, vp, kc, vc, g, a, ls, dq, dkp, dvp, dkc, dvc, accum):
        attend_bwd_pair(
            lax.axis_index("shard"),
            prompt_rows,
            q,
            kp,
            vp,
            kc,
            vc,
            g,
            a,
            ls.at[0],
            dq,
            dkp,
            dvp,
            dkc,
            dvc,
            accum,
        )

    def columns(rows):
        return pl.BlockSpec((rows, PAIR), lambda p: (0, p))

    sizes = (tokens, prompt_len, prompt_len, cont_len, cont_len)
    return pl.pallas_call(
        kernel,
        grid=(pairs,),
        in_specs=[columns(rows) for rows in sizes + (tokens, tokens)]
        + [pl.BlockSpec((1, 8, tokens), lambda p: (p, 0, 0))],
        out_specs=[columns(rows) for rows in sizes],
        out_shape=[jax.ShapeDtypeStruct((rows, D), jnp.bfloat16) for rows in sizes],
        scratch_shapes=[pltpu.VMEM((PAIR, tokens), jnp.float32)],
        compiler_params=pltpu.CompilerParams(vmem_limit_bytes=VMEM_ALL),
        name="attend_backward",
    )(q, kp, vp, kc, vc, g_att, att, lse)


MESH_ID = pl.DeviceIdType.MESH


def sum_gradients(g_qkv, g_out, g_in, g_ffo, g_small):
    pieces = 12
    rows = g_qkv.shape[0] // 4
    width, half, quarter = D, D // 2, rows // 4
    s_width, s_half = g_small.shape[1], g_small.shape[1] // 2
    ahead = 3

    def kernel(
        gq, go, gi, gf, gs, out, out_s,
        own, cr, xs, xr, yb, yr, zb, zr, fb,
        own_s, cr_s, xs_s, xr_s, yb_s, yr_s, zb_s, zr_s, fb_s,
        sem_own, c_send, c_recv, x_send, x_recv, y_send, y_recv, z_send, z_recv,
        f_send, f_recv, o_send, o_recv, o_own, g_send, g_recv,
    ):
        rep, shard = lax.axis_index("rep"), lax.axis_index("shard")
        z, y = rep // 2, rep % 2
        x, core = shard // 2, shard % 2
        partner = (rep, 2 * x + 1 - core)
        across = (rep, 2 * (1 - x) + core)
        beside = (2 * z + 1 - y, shard)

        def along(step):
            return (2 * lax.rem(z + step, 4) + y, shard)

        barrier = pltpu.get_barrier_semaphore()
        others = [partner, across, beside, along(1), along(2), along(3)]
        far = (rep, 2 * (1 - x) + 1 - core)
        for other in others + [far]:
            pl.semaphore_signal(barrier, inc=1, device_id=other, device_id_type=MESH_ID)
        pl.semaphore_wait(barrier, len(others) + 1)

        def remote(source, target, send, recv, device):
            return pltpu.make_async_remote_copy(
                src_ref=source,
                dst_ref=target,
                send_sem=send,
                recv_sem=recv,
                device_id=device,
                device_id_type=MESH_ID,
            )

        def source(k, block):
            if k < 4:
                return gf.at[pl.ds(block * 4 * rows + k * rows, rows), :]
            if k < 8:
                return gi.at[pl.ds(block * rows, rows), (k - 4) * width : (k - 3) * width]
            if k < 9:
                return go.at[pl.ds(block * rows, rows), :]
            if k < 12:
                return gq.at[pl.ds(block * rows, rows), (k - 9) * width : (k - 8) * width]
            return gs.at[pl.ds(block * rows, rows), :]

        big = (own, cr, xs, xr, yb, yr, zb, zr, fb, half)
        small = (own_s, cr_s, xs_s, xr_s, yb_s, yr_s, zb_s, zr_s, fb_s, s_half)

        def bufs(k):
            if isinstance(k, int) and k == pieces:
                return small, 0
            return big, k

        def core_copy(k, xx):
            b, i = bufs(k)
            return remote(
                source(k, 2 * xx + 1 - core) if isinstance(k, int) else b[1].at[i, xx],
                b[1].at[i, xx],
                c_send.at[k, xx],
                c_recv.at[k, xx],
                partner,
            )

        def own_copy(k, xx):
            b, i = bufs(k)
            return pltpu.make_async_copy(
                source(k, 2 * xx + core) if isinstance(k, int) else b[0].at[i, xx],
                b[0].at[i, xx],
                sem_own.at[k, xx],
            )

        def x_copy(k):
            b, i = bufs(k)
            return remote(b[2].at[i], b[3].at[i], x_send.at[k], x_recv.at[k], across)

        def y_copy(k):
            b, i = bufs(k)
            return remote(b[4].at[i, 1 - y], b[5].at[i], y_send.at[k], y_recv.at[k], beside)

        def z_copy(k, step, buf, slot, send, recv, target):
            return remote(buf, target, send.at[k, step - 1], recv.at[k, slot], along(step))

        def zs_copy(k, step):
            b, i = bufs(k)
            return z_copy(
                k, step, b[6].at[i, lax.rem(z + step, 4)], z, z_send, z_recv, b[7].at[i, z]
            )

        def zr_wait(k, step):
            b, i = bufs(k)
            slot = lax.rem(z + step, 4)
            z_copy(k, step, b[7].at[i, slot], slot, z_send, z_recv, b[7].at[i, slot]).wait_recv()

        def fs_copy(k, step):
            b, i = bufs(k)
            return z_copy(k, step, b[8].at[i, z], z, f_send, f_recv, b[8].at[i, z])

        def fr_wait(k, step):
            b, i = bufs(k)
            slot = lax.rem(z + step, 4)
            z_copy(k, step, b[8].at[i, slot], slot, f_send, f_recv, b[8].at[i, slot]).wait_recv()

        def final(k, yy):
            if isinstance(k, int) and k == pieces:
                return out_s.at[shard, :, :, pl.ds(pl.multiple_of(yy * s_half, 128), s_half)]
            return out.at[k, :, :, pl.ds(pl.multiple_of(yy * half, 128), half)]

        def o_copy(k):
            b, i = bufs(k)
            return remote(b[8].at[i], final(k, y), o_send.at[k], o_recv.at[k], beside)

        def o_wait(k):
            b, i = bufs(k)
            remote(b[8].at[i], final(k, 1 - y), o_send.at[k], o_recv.at[k], beside).wait_recv()

        def o_local(k):
            b, i = bufs(k)
            return pltpu.make_async_copy(b[8].at[i], final(k, y), o_own.at[k])

        def wide(value):
            return value.astype(jnp.float32)

        def stage_x(k):
            b, i = bufs(k)
            for xx in range(2):
                core_copy(k, xx).wait_recv()
                own_copy(k, xx).wait()
            b[2][i] = (wide(b[0][i, 1 - x]) + wide(b[1][i, 1 - x])).astype(jnp.bfloat16)
            x_copy(k).start()

        def stage_y(k):
            b, i = bufs(k)
            x_copy(k).wait_recv()
            total = (wide(b[0][i, x]) + wide(b[1][i, x]) + wide(b[3][i])).astype(jnp.bfloat16)
            cut = b[9]
            b[4][i, 0] = total[:, :cut]
            b[4][i, 1] = total[:, cut:]
            y_copy(k).start()

        def stage_z(k):
            b, i = bufs(k)
            y_copy(k).wait_recv()
            total = (wide(b[4][i, y]) + wide(b[5][i])).astype(jnp.bfloat16)
            for q in range(4):
                b[6][i, q] = total[q * quarter : (q + 1) * quarter]
            for step in (2, 1, 3):
                zs_copy(k, step).start()

        def stage_f(k):
            b, i = bufs(k)
            total = wide(b[6][i, z])
            for step in (1, 2, 3):
                zr_wait(k, step)
                total += wide(b[7][i, lax.rem(z + step, 4)])
            b[8][i, z] = total.astype(jnp.bfloat16)
            for step in (2, 1, 3):
                fs_copy(k, step).start()

        def stage_o(k):
            for step in (1, 2, 3):
                fr_wait(k, step)
            o_copy(k).start()
            o_local(k).start()

        def g_copy(step):
            return remote(
                out_s.at[shard],
                out_s.at[shard],
                g_send.at[step - 1],
                g_recv.at[shard],
                (rep, lax.rem(shard + step, 4)),
            )

        def stage_g():
            o_wait(pieces)
            o_local(pieces).wait()
            for step in (1, 2, 3):
                g_copy(step).start()

        order = [pieces] + list(range(pieces))
        for k in order:
            for xx in range(2):
                core_copy(k, xx).start()
                own_copy(k, xx).start()
        stage_x(pieces)
        for k in range(ahead):
            stage_x(k)
        small_stages = [stage_y, stage_z, stage_f, stage_o]

        def tick(t, carry):
            @pl.when(t + ahead < pieces)
            def _():
                stage_x(t + ahead)

            for at, stage in enumerate(small_stages):

                @pl.when(t == at)
                def _(stage=stage):
                    stage(pieces)

            @pl.when(t == len(small_stages))
            def _():
                stage_g()

            @pl.when(t < pieces)
            def _():
                stage_y(t)

            for late, stage in ((1, stage_z), (2, stage_f), (3, stage_o)):

                @pl.when((t >= late) & (t < pieces + late))
                def _(late=late, stage=stage):
                    stage(t - late)

            return carry

        lax.fori_loop(0, pieces + 3, tick, 0)

        def finish(k):
            for xx in range(2):
                core_copy(k, xx).wait_send()
            x_copy(k).wait_send()
            y_copy(k).wait_send()
            for step in (1, 2, 3):
                zs_copy(k, step).wait_send()
                fs_copy(k, step).wait_send()
            o_copy(k).wait_send()

        def last(k, carry):
            o_wait(k)
            o_local(k).wait()
            finish(k)
            return carry

        lax.fori_loop(0, pieces, last, 0)
        finish(pieces)
        for step in (1, 2, 3):
            slot = lax.rem(shard + step, 4)
            remote(
                out_s.at[slot], out_s.at[slot], g_send.at[step - 1], g_recv.at[slot], far
            ).wait_recv()
            g_copy(step).wait_send()

    def buffers(count, wide_cols):
        cut = wide_cols // 2
        return [
            pltpu.VMEM((count, 2, rows, wide_cols), jnp.bfloat16),
            pltpu.VMEM((count, 2, rows, wide_cols), jnp.bfloat16),
            pltpu.VMEM((count, rows, wide_cols), jnp.bfloat16),
            pltpu.VMEM((count, rows, wide_cols), jnp.bfloat16),
            pltpu.VMEM((count, 2, rows, cut), jnp.bfloat16),
            pltpu.VMEM((count, rows, cut), jnp.bfloat16),
            pltpu.VMEM((count, 4, quarter, cut), jnp.bfloat16),
            pltpu.VMEM((count, 4, quarter, cut), jnp.bfloat16),
            pltpu.VMEM((count, 4, quarter, cut), jnp.bfloat16),
        ]

    def sems(*dims):
        return pltpu.SemaphoreType.DMA(dims)

    n = pieces + 1
    anywhere = pl.BlockSpec(memory_space=pl.ANY)
    out, out_s = pl.pallas_call(
        kernel,
        in_specs=[anywhere] * 5,
        out_specs=[anywhere, pl.BlockSpec(memory_space=pltpu.VMEM)],
        out_shape=[
            jax.ShapeDtypeStruct((pieces, 4, quarter, width), jnp.bfloat16),
            jax.ShapeDtypeStruct((4, 4, quarter, s_width), jnp.bfloat16),
        ],
        scratch_shapes=buffers(pieces, width)
        + buffers(1, s_width)
        + [
            sems(n, 2), sems(n, 2), sems(n, 2), sems(n), sems(n), sems(n), sems(n),
            sems(n, 3), sems(n, 4), sems(n, 3), sems(n, 4), sems(n), sems(n), sems(n),
            sems(3), sems(4),
        ],
        compiler_params=pltpu.CompilerParams(
            collective_id=0, has_side_effects=True, vmem_limit_bytes=VMEM_ALL
        ),
        name="sum_gradients",
    )(g_qkv, g_out, g_in, g_ffo, g_small)
    return out.reshape(pieces, rows, width), out_s.reshape(4 * rows, s_width)


def project_and_attend(prompt, conts, w_qkv, w_out, w_in, w_ffo, layer_biases):
    pieces, early = 12, 6
    rows = w_qkv.shape[0]
    p_rows, cont_len = prompt.shape[0], conts.shape[0]
    tokens = p_rows + cont_len
    p_len = 4 * p_rows
    pairs = HEADS // 2
    tiles = tokens // TILE
    chunk = 2 * PAIR
    chunks = D // chunk
    half_rows = rows // 2

    def kernel(
        xp, xc, wq, wo, wi, wf, bias, w_all_out, wf_out, q_out, kc_out, vc_out, kp_out, vp_out, att_out, lse,
        stage, w_all, q, kc, vc, kp, vp, att,
        load, c_s, c_r, x_s, x_r, y_s, y_r, d_s, d_r, e_s, e_r, w_sem,
        kc_s, kc_r, kx_s, kx_r, kd_s, kd_r, out_sem,
    ):
        rep, shard = lax.axis_index("rep"), lax.axis_index("shard")
        z, y = rep // 2, rep % 2
        x, core = shard // 2, shard % 2
        partner = (rep, 2 * x + 1 - core)
        across = (rep, 2 * (1 - x) + core)
        beside = (2 * z + 1 - y, shard)
        there = 2 * (1 - x) + core

        def remote(ref, send, recv, device):
            return pltpu.make_async_remote_copy(
                src_ref=ref,
                dst_ref=ref,
                send_sem=send,
                recv_sem=recv,
                device_id=device,
                device_id_type=MESH_ID,
            )

        def source(k):
            if k < 3:
                j = (1, 2, 0)[k]
                return wq.at[:, j * D : (j + 1) * D]
            if k < 4:
                return wo
            if k < 8:
                return wi.at[:, (k - 4) * D : (k - 3) * D]
            return wf.at[(k - 8) * rows : (k - 7) * rows, :]

        def loading(k):
            return pltpu.make_async_copy(source(k), stage.at[k], load.at[k])

        for k in range(pieces):
            loading(k).start()
        barrier = pltpu.get_barrier_semaphore()
        for other in (partner, across, beside):
            pl.semaphore_signal(barrier, inc=1, device_id=other, device_id_type=MESH_ID)
        pl.semaphore_wait(barrier, 3)

        def part(k, block, which):
            return w_all.at[k, block, pl.ds(pl.multiple_of(which * half_rows, 16), half_rows), :]

        def core_copy(k):
            return remote(w_all.at[k, shard], c_s.at[k], c_r.at[k], partner)

        def core_arrival(k):
            return remote(w_all.at[k, 2 * x + 1 - core], c_s.at[k], c_r.at[k], partner)

        def x_copy(k):
            return remote(part(k, shard, y), x_s.at[k], x_r.at[k], across)

        def x_arrival(k):
            return remote(part(k, there, y), x_s.at[k], x_r.at[k], across)

        def y_copy(k):
            return remote(part(k, there, y), y_s.at[k], y_r.at[k], beside)

        def y_arrival(k):
            return remote(part(k, there, 1 - y), y_s.at[k], y_r.at[k], beside)

        def d_copy(k):
            return remote(part(k, there, y), d_s.at[k], d_r.at[k], partner)

        def e_copy(k):
            return remote(part(k, there, 1 - y), e_s.at[k], e_r.at[k], partner)

        far = 2 * (1 - x) + 1 - core

        def send_piece(k):
            x_copy(k).start()
            core_copy(k).start()

        def round_piece(k):
            loading(k).wait()
            w_all[k, shard] = stage[k].astype(jnp.bfloat16)

        def serve_x(k):
            x_arrival(k).wait_recv()
            y_copy(k).start()
            d_copy(k).start()

        def serve_y(k):
            y_arrival(k).wait_recv()
            e_copy(k).start()

        def w_store(k):
            if k < 8:
                return pltpu.make_async_copy(w_all.at[k], w_all_out.at[k], w_sem.at[k])
            return pltpu.make_async_copy(w_all.at[k], wf_out.at[:, k - 8], w_sem.at[k])

        def complete(k):
            core_arrival(k).wait_recv()
            remote(part(k, far, y), d_s.at[k], d_r.at[k], partner).wait_recv()
            remote(part(k, far, 1 - y), e_s.at[k], e_r.at[k], partner).wait_recv()
            w_store(k).start()

        def weight(k):
            return w_all[k].reshape(4 * rows, D)

        for k in range(early):
            round_piece(k)
            send_piece(k)
        for k in range(early, pieces):
            round_piece(k)
        for k in range(3):
            serve_x(k)
        for k in range(3):
            serve_y(k)

        own_rows = pl.ds(pl.multiple_of(shard * p_rows, p_rows), p_rows)
        kv = (kp, vp)

        def kv_part(t, g, block):
            lanes = pl.ds(g * chunk if isinstance(g, int) else pl.multiple_of(g * chunk, chunk), chunk)
            return kv[t].at[pl.ds(pl.multiple_of(block * p_rows, p_rows), p_rows), lanes]

        def kv_core(t, g):
            return remote(kv_part(t, g, shard), kc_s.at[g, t], kc_r.at[g, t], partner)

        def kv_across(t, g):
            return remote(kv_part(t, g, shard), kx_s.at[g, t], kx_r.at[g, t], across)

        def kv_forward(t, g):
            return remote(kv_part(t, g, there), kd_s.at[g, t], kd_r.at[g, t], partner)

        complete(0)
        kp[own_rows, :] = dot_plain(xp[...], weight(0)).astype(jnp.bfloat16)
        complete(1)
        vp[own_rows, :] = (dot_plain(xp[...], weight(1)) + bias[1:2, :]).astype(jnp.bfloat16)
        for g in range(chunks):
            for t in range(2):
                kv_across(t, g).start()
                kv_core(t, g).start()
        for k in range(early, pieces):
            send_piece(k)
        kc[...] = dot_plain(xc[...], weight(0)).astype(jnp.bfloat16)
        vc[...] = (dot_plain(xc[...], weight(1)) + bias[1:2, :]).astype(jnp.bfloat16)
        complete(2)
        q[:p_rows, :] = (dot_plain(xp[...], weight(2)) + bias[0:1, :]).astype(jnp.bfloat16)
        q[p_rows:, :] = (dot_plain(xc[...], weight(2)) + bias[0:1, :]).astype(jnp.bfloat16)

        def keep(ref, target, i):
            return pltpu.make_async_copy(ref, target, out_sem.at[i])

        kept = [(q, q_out, 0), (kc, kc_out, 1), (vc, vc_out, 2)]
        for item in kept:
            keep(*item).start()

        def serve_kv(g):
            for t in range(2):
                remote(kv_part(t, g, there), kx_s.at[g, t], kx_r.at[g, t], across).wait_recv()
                kv_forward(t, g).start()

        def complete_kv(g):
            for t in range(2):
                remote(
                    kv_part(t, g, 2 * x + 1 - core), kc_s.at[g, t], kc_r.at[g, t], partner
                ).wait_recv()
                remote(kv_part(t, g, far), kd_s.at[g, t], kd_r.at[g, t], partner).wait_recv()

        serve_kv(0)
        first_slot = {3: 0, 4: 1, 5: 2}
        for k in range(early, pieces):
            first_slot[k] = 10 + 2 * (k - early)
        slots = pairs * tiles
        work = []
        for k in range(3, pieces):
            work += [(first_slot[k], serve_x, k), (first_slot[k] + 2, serve_y, k)]
            work.append((first_slot[k] + 4, complete, k))
        work.sort(key=lambda item: item[0])

        def att_store(p):
            lanes = pl.ds(pl.multiple_of(p * PAIR, PAIR), PAIR)
            return pltpu.make_async_copy(att.at[:, lanes], att_out.at[:, lanes], out_sem.at[5 + p])

        def pair(p, carry):
            @pl.when(p % 2 == 0)
            def _():
                complete_kv(p // 2)

            def between(tile):
                @pl.when((p % 2 == 0) & (p < pairs - 2) & (tile == tiles - 1))
                def _():
                    serve_kv(p // 2 + 1)

                for slot, action, k in work:
                    if slot < slots and slot % tiles == tile:

                        @pl.when(p == slot // tiles)
                        def _(action=action, k=k):
                            action(k)

            lanes = pl.ds(pl.multiple_of(p * PAIR, PAIR), PAIR)
            attend_fwd_pair(
                shard,
                p_rows,
                q.at[:, lanes],
                kp.at[:, lanes],
                vp.at[:, lanes],
                kc.at[:, lanes],
                vc.at[:, lanes],
                att.at[:, lanes],
                lse.at[p],
                between,
            )
            att_store(p).start()
            return carry

        lax.fori_loop(0, pairs, pair, 0)
        kept += [(kp, kp_out, 3), (vp, vp_out, 4)]
        for item in kept[3:]:
            keep(*item).start()
        for slot, action, k in work:
            if slot >= slots:
                action(k)
        for item in kept:
            keep(*item).wait()

        def last_pair(p, carry):
            att_store(p).wait()
            return carry

        lax.fori_loop(0, pairs, last_pair, 0)
        for k in range(pieces):
            w_store(k).wait()
            for copy in (core_copy, x_copy, y_copy, d_copy, e_copy):
                copy(k).wait_send()
        for g in range(chunks):
            for t in range(2):
                for copy in (kv_core, kv_across, kv_forward):
                    copy(t, g).wait_send()

    def sems(*dims):
        return pltpu.SemaphoreType.DMA(dims)

    def low(*dims):
        return jax.ShapeDtypeStruct(dims, jnp.bfloat16)

    anywhere = pl.BlockSpec(memory_space=pl.ANY)
    vmem = pl.BlockSpec(memory_space=pltpu.VMEM)
    n = pieces
    out = pl.pallas_call(
        kernel,
        in_specs=[vmem, vmem, anywhere, anywhere, anywhere, anywhere, vmem],
        out_specs=[anywhere] * 8 + [vmem],
        out_shape=[
            low(8, 4, rows, D),
            low(4, 4, rows, D),
            low(tokens, D),
            low(cont_len, D),
            low(cont_len, D),
            low(p_len, D),
            low(p_len, D),
            jax.ShapeDtypeStruct((tokens, D), jnp.float32),
            jax.ShapeDtypeStruct((pairs, 8, tokens), jnp.float32),
        ],
        scratch_shapes=[
            pltpu.VMEM((n, rows, D), jnp.float32),
            pltpu.VMEM((n, 4, rows, D), jnp.bfloat16),
            pltpu.VMEM((tokens, D), jnp.bfloat16),
            pltpu.VMEM((cont_len, D), jnp.bfloat16),
            pltpu.VMEM((cont_len, D), jnp.bfloat16),
            pltpu.VMEM((p_len, D), jnp.bfloat16),
            pltpu.VMEM((p_len, D), jnp.bfloat16),
            pltpu.VMEM((tokens, D), jnp.float32),
        ]
        + [sems(n)] * 12
        + [sems(chunks, 2)] * 6
        + [sems(5 + pairs)],
        compiler_params=pltpu.CompilerParams(
            collective_id=1, has_side_effects=True, vmem_limit_bytes=VMEM_ALL
        ),
        name="project_and_attend",
    )(prompt, conts, w_qkv, w_out, w_in, w_ffo, layer_biases)
    w_all, wf, q, kc, vc, kp, vp, att, lse = out
    w_all = w_all.reshape(8, 4 * rows, D)
    return w_all, wf.reshape(16 * rows, D), q, kp, vp, kc, vc, att, lse


def project_native(prompt, conts, w_qkv, w_out, w_in, w_ffo, layer_biases):
    rows = prompt.shape[0]

    def gathered(value):
        return lax.all_gather(value.astype(jnp.bfloat16), "shard", axis=0, tiled=True)

    qkv, out, inner, ffo = (gathered(w) for w in (w_qkv, w_out, w_in, w_ffo))
    tokens = jnp.concatenate([prompt, conts], 0)
    bias = jnp.concatenate([layer_biases[0], jnp.zeros((D,), jnp.float32), layer_biases[1]])
    qkv_b = (dot_plain(tokens, qkv) + bias).astype(jnp.bfloat16)
    q, keys, values = (qkv_b[:, i * D : (i + 1) * D] for i in range(3))
    kp, vp = gathered(keys[:rows]), gathered(values[:rows])
    kc, vc = keys[rows:], values[rows:]
    att, lse = attend_forward(q, kp, vp, kc, vc, rows)
    blocks = [qkv[:, D : 2 * D], qkv[:, 2 * D :], qkv[:, :D], out]
    blocks += [inner[:, i * D : (i + 1) * D] for i in range(inner.shape[1] // D)]
    return jnp.stack(blocks), ffo, q, kp, vp, kc, vc, att, lse


def student_loss(stu_rows, pool_query, bias_pool, w_pool, w_class, bias_class, label_value):
    part_w = STU // SHEADS
    parts = stu_rows.reshape(stu_rows.shape[0], SHEADS, part_w)
    queries = pool_query.reshape(SHEADS, part_w)
    scores = jnp.einsum("tha,ha->ht", parts, queries, precision=HIGHEST) * part_w ** (-0.5)
    largest = jnp.max(scores, -1, keepdims=True)
    expo = jnp.exp(scores - largest)
    weights = expo / jnp.sum(expo, -1, keepdims=True)
    pooled = jnp.einsum("ht,tha->ha", weights, parts, precision=HIGHEST).reshape(STU)
    top_layer = jnp.tanh(jnp.dot(pooled, w_pool, precision=HIGHEST) + bias_pool)
    logit_row = jnp.dot(top_layer, w_class, precision=HIGHEST) + bias_class
    top_logit = jnp.max(logit_row)
    log_total = jnp.log(jnp.sum(jnp.exp(logit_row - top_logit))) + top_logit
    picked = jnp.sum(jnp.where(jnp.arange(logit_row.shape[0]) == label_value, logit_row, 0.0))
    return (log_total - picked, logit_row)


def sum_native(g_qkvw, g_outw, g_in, g_ffo, small):
    def over(grad):
        part = lax.psum_scatter(
            grad.astype(jnp.bfloat16), "shard", scatter_dimension=0, tiled=True
        )
        return lax.psum(part, "rep").astype(jnp.float32)

    owned = tuple(over(grad) for grad in (g_qkvw, g_outw, g_in, g_ffo))
    return owned, lax.psum(small, ("rep", "shard"))


def sum_direct(g_qkvw, g_outw, g_in, g_ffo, small):
    biases, gains, in_bias, student, vectors, pool, class_w, class_b = small
    parts = [
        biases.reshape(-1, 128),
        gains.reshape(-1, 128),
        in_bias.reshape(-1, 128),
        vectors.reshape(-1, 128),
        pool.reshape(-1, 128),
        jnp.pad(class_w, ((0, 0), (0, 128 - class_w.shape[1]))),
        jnp.pad(class_b[None], ((0, 0), (0, 128 - class_b.shape[0]))),
    ]
    used = sum(part.shape[0] for part in parts)
    side = jnp.concatenate(parts + [jnp.zeros((D - used, 128), jnp.float32)], 0)
    packed = jnp.concatenate([student, side], 1).astype(jnp.bfloat16)
    low = [grad.astype(jnp.bfloat16) for grad in (g_qkvw, g_outw, g_in, g_ffo)]
    out, summed = sum_gradients(*low, packed)
    out = out.astype(jnp.float32)
    summed = summed.astype(jnp.float32)
    owned = (
        jnp.concatenate([out[9], out[10], out[11]], 1),
        out[8],
        jnp.concatenate([out[4], out[5], out[6], out[7]], 1),
        out[:4].reshape(-1, D),
    )
    result, at = [summed[:, :128]], 0
    for part in parts:
        result.append(summed[at : at + part.shape[0], 128:])
        at += part.shape[0]
    return owned, (
        result[1].reshape(biases.shape),
        result[2].reshape(gains.shape),
        result[3].reshape(in_bias.shape),
        result[0],
        result[4].reshape(vectors.shape),
        result[5].reshape(pool.shape),
        result[6][:, : class_w.shape[1]],
        result[7][0, : class_b.shape[0]],
    )


def body(
    prompt,
    conts,
    prompt_cot,
    cont_cot,
    labels,
    w_qkv,
    w_out,
    w_in,
    w_ffo,
    layer_biases,
    norm_gains,
    bias_in,
    w_student,
    student_vectors,
    w_pool,
    w_class,
    bias_class,
):
    prompt_rows = prompt.shape[1]
    cont_len = conts.shape[2]
    prompt_len = prompt_rows * lax.axis_size("shard")
    direct = (lax.axis_size("rep"), lax.axis_size("shard")) == (8, 4)
    project = project_and_attend if direct else project_native
    w_all, ffo_full, q, kp, vp, kc, vc, attended, log_totals = project(
        prompt[0], conts[0, 0], w_qkv, w_out, w_in, w_ffo, layer_biases
    )
    out_full = w_all[3]
    in_full = jnp.concatenate([w_all[4], w_all[5], w_all[6], w_all[7]], 1)
    tokens = jnp.concatenate([prompt[0], conts[0, 0]], 0)
    tokens_f = tokens.astype(jnp.float32)
    att_b = attended.astype(jnp.bfloat16)
    branch = dot_plain(att_b, out_full) + layer_biases[2]
    resid_one = tokens_f + branch
    first = layer_norm(resid_one, norm_gains[0], layer_biases[4])
    first_b = first.astype(jnp.bfloat16)
    hidden = dot_plain(first_b, in_full) + bias_in
    act_b = gelu_exact(hidden).astype(jnp.bfloat16)
    ffn = dot_plain(act_b, ffo_full) + layer_biases[3]
    resid_two = first + ffn
    output = layer_norm(resid_two, norm_gains[1], layer_biases[5])
    output_b = output.astype(jnp.bfloat16)
    cont_b = output_b[prompt_rows:]
    student_low = w_student.astype(jnp.bfloat16)
    stu = dot_plain(cont_b, student_low) + student_vectors[0]

    def loss_closed(stu_rows, pool_query, bias_pool, pool_weight, class_weight, class_bias):
        return student_loss(
            stu_rows, pool_query, bias_pool, pool_weight, class_weight, class_bias, labels[0, 0]
        )

    loss_value, loss_pull, logit_row = jax.vjp(
        loss_closed,
        stu,
        student_vectors[1],
        student_vectors[2],
        w_pool,
        w_class,
        bias_class,
        has_aux=True,
    )
    g_stu, g_query, g_pbias, g_pool, g_class, g_cbias = loss_pull(jnp.ones((), jnp.float32))
    g_stu_b = g_stu.astype(jnp.bfloat16)
    g_sbias = jnp.sum(g_stu_b.astype(jnp.float32), 0)
    g_student = dot_first(cont_b, g_stu_b)
    student_back = dot_second(g_stu_b, student_low)
    g_output = jnp.concatenate([prompt_cot[0], cont_cot[0, 0]], 0).astype(jnp.float32)
    g_output = g_output + jnp.concatenate(
        [jnp.zeros((prompt_rows, D), jnp.float32), student_back], 0
    )
    out_back, in_back, ffo_back = out_full, in_full, ffo_full
    norm_two, norm_two_pull = jax.vjp(layer_norm, resid_two, norm_gains[1], layer_biases[5])
    g_resid_two, g_gain_two, g_shift_two = norm_two_pull(g_output)
    g_ffn_b = g_resid_two.astype(jnp.bfloat16)
    g_ffo = dot_first(act_b, g_ffn_b)
    g_ffo_bias = jnp.sum(g_ffn_b.astype(jnp.float32), 0)
    g_act = dot_second(g_ffn_b, ffo_back)
    gelu_value, gelu_pull = jax.vjp(gelu_exact, hidden)
    g_hidden_b = gelu_pull(g_act)[0].astype(jnp.bfloat16)
    g_in = dot_first(first_b, g_hidden_b)
    g_in_bias = jnp.sum(g_hidden_b.astype(jnp.float32), 0)
    g_first = g_resid_two + dot_second(g_hidden_b, in_back)
    norm_one, norm_one_pull = jax.vjp(layer_norm, resid_one, norm_gains[0], layer_biases[4])
    g_resid_one, g_gain_one, g_shift_one = norm_one_pull(g_first)
    g_branch_b = g_resid_one.astype(jnp.bfloat16)
    g_outw = dot_first(att_b, g_branch_b)
    g_out_bias = jnp.sum(g_branch_b.astype(jnp.float32), 0)
    g_att_b = dot_second(g_branch_b, out_back).astype(jnp.bfloat16)
    query_grad_b, g_keys_p, g_values_p, g_keys_c, g_values_c = attend_backward(
        q, kp, vp, kc, vc, g_att_b, attended, log_totals, prompt_rows
    )
    cont_kv_b = jnp.concatenate([g_keys_c, g_values_c], 1)
    block_kv_b = jnp.concatenate([g_keys_p, g_values_p], 1)
    kv_weights = jnp.concatenate([w_all[0], w_all[1]], 1)
    g_query_w = dot_first(tokens, query_grad_b)
    g_kv_w = dot_first(tokens[prompt_rows:], cont_kv_b)
    g_tokens = g_resid_one + dot_second(query_grad_b, w_all[2])
    cont_through = dot_second(cont_kv_b, kv_weights)
    kv_summed = lax.psum_scatter(
        block_kv_b,
        "shard",
        scatter_dimension=0,
        tiled=True,
    ).astype(jnp.float32)
    g_kv_w = g_kv_w + lax.dot_general(
        tokens_f[:prompt_rows],
        kv_summed,
        (((0,), (0,)), ((), ())),
        precision=HIGHEST,
        preferred_element_type=jnp.float32,
    )
    prompt_through = jnp.dot(
        kv_summed,
        kv_weights.astype(jnp.float32).T,
        precision=HIGHEST,
        preferred_element_type=jnp.float32,
    )
    value_cols = jnp.sum(kv_summed[:, D:], 0)
    g_tokens = g_tokens + jnp.concatenate([prompt_through, cont_through], 0)
    g_qkvw = jnp.concatenate([g_query_w, g_kv_w], 1)
    g_query_bias = jnp.sum(query_grad_b.astype(jnp.float32), 0)
    g_value_bias = jnp.sum(cont_kv_b[:, D:].astype(jnp.float32), 0) + value_cols
    g_biases = jnp.stack(
        [g_query_bias, g_value_bias, g_out_bias, g_ffo_bias, g_shift_one, g_shift_two]
    )
    g_gains = jnp.stack([g_gain_one, g_gain_two])
    g_vectors = jnp.stack([g_sbias, g_query, g_pbias])
    small = (g_biases, g_gains, g_in_bias, g_student, g_vectors, g_pool, g_class, g_cbias)
    owned, summed = (sum_direct if direct else sum_native)(g_qkvw, g_outw, g_in, g_ffo, small)
    owned_qkv, owned_out, owned_in, owned_ffo = owned
    return (
        output_b[:prompt_rows][None],
        output_b[prompt_rows:][None, None],
        logit_row[None, None],
        g_tokens[:prompt_rows][None],
        g_tokens[prompt_rows:][None, None],
        owned_qkv,
        owned_out,
        owned_in,
        owned_ffo,
        summed[0],
        summed[1],
        summed[2],
        summed[3],
        summed[4],
        summed[5],
        summed[6],
        summed[7],
    )


def solution(mesh):
    return jax.shard_map(
        body,
        mesh=mesh,
        in_specs=(
            P("rep", "shard", None),
            P("rep", "shard", None, None),
            P("rep", "shard", None),
            P("rep", "shard", None, None),
            P("rep", "shard"),
            P("shard", None),
            P("shard", None),
            P("shard", None),
            P("shard", None),
            P(),
            P(),
            P(),
            P(),
            P(),
            P(),
            P(),
            P(),
        ),
        out_specs=(
            P("rep", "shard", None),
            P("rep", "shard", None, None),
            P("rep", "shard", None),
            P("rep", "shard", None),
            P("rep", "shard", None, None),
            P("shard", None),
            P("shard", None),
            P("shard", None),
            P("shard", None),
            P(),
            P(),
            P(),
            P(),
            P(),
            P(),
            P(),
            P(),
        ),
        check_vma=False,
    )
```

```python
import jax
import jax.numpy as jnp
from jax import lax
from jax.experimental import pallas as pl
from jax.experimental.pallas import tpu as pltpu
from jax.sharding import PartitionSpec as P

D = 768
HEADS = 12
DH = 64
STU = 128
SHEADS = 2


HIGHEST = lax.Precision.HIGHEST
NEG_BIG = -1e30


def dot_plain(left, right):
    return jnp.dot(left, right, preferred_element_type=jnp.float32)


def dot_first(left, right):
    return lax.dot_general(
        left, right, (((0,), (0,)), ((), ())), preferred_element_type=jnp.float32
    )


def dot_second(left, right):
    return lax.dot_general(
        left, right, (((1,), (1,)), ((), ())), preferred_element_type=jnp.float32
    )


TILE = 256
PAIR = 128
VMEM_ALL = 62 * 1024 * 1024


def rows_dot(left, right):
    return lax.dot_general(
        left, right, (((1,), (1,)), ((), ())), preferred_element_type=jnp.float32
    )


def low_lanes(shape):
    return lax.broadcasted_iota(jnp.int32, shape, len(shape) - 1) < DH


def attend_fwd_pair(
    shard, prompt_rows, q, kp, vp, kc, vc, att_ref, lse_ref, between=None
):
    cont_len = kc.shape[0]
    prompt_len = kp.shape[0]
    for start in range(0, prompt_rows + cont_len, TILE):
        q_t = q[start : start + TILE, :] * jnp.asarray(DH ** (-0.5), jnp.bfloat16)
        halves = []
        for parity in range(2):
            keep = low_lanes(q_t.shape) == (parity == 0)
            q_h = jnp.where(keep, q_t, jnp.zeros_like(q_t))
            s_p = rows_dot(q_h, kp[...])
            if start < prompt_rows:
                key = lax.broadcasted_iota(jnp.int32, s_p.shape, 1)
                row = lax.broadcasted_iota(jnp.int32, s_p.shape, 0)
                s_p = jnp.where(key <= row + (shard * prompt_rows + start), s_p, NEG_BIG)
                largest = jnp.max(s_p, 1, keepdims=True)
                p_p = jnp.exp(s_p - largest)
                total = jnp.sum(p_p, 1, keepdims=True)
                o = dot_plain(p_p.astype(jnp.bfloat16), vp[...])
            else:
                seen = start - prompt_rows + TILE
                s_c = rows_dot(q_h, kc[:seen, :])
                key = lax.broadcasted_iota(jnp.int32, s_c.shape, 1)
                row = lax.broadcasted_iota(jnp.int32, s_c.shape, 0)
                s_c = jnp.where(key <= row + (start - prompt_rows), s_c, NEG_BIG)
                largest = jnp.maximum(
                    jnp.max(s_p, 1, keepdims=True), jnp.max(s_c, 1, keepdims=True)
                )
                p_p = jnp.exp(s_p - largest)
                p_c = jnp.exp(s_c - largest)
                total = jnp.sum(p_p, 1, keepdims=True) + jnp.sum(p_c, 1, keepdims=True)
                o = dot_plain(p_p.astype(jnp.bfloat16), vp[...]) + dot_plain(
                    p_c.astype(jnp.bfloat16), vc[:seen, :]
                )
            halves.append((o / total, largest + jnp.log(total)))
        keep = low_lanes((TILE, PAIR))
        att_ref[start : start + TILE, :] = jnp.where(keep, halves[0][0], halves[1][0])
        lse = jnp.where(
            keep,
            jnp.broadcast_to(halves[0][1], (TILE, PAIR)),
            jnp.broadcast_to(halves[1][1], (TILE, PAIR)),
        )
        turned = jnp.transpose(lse)
        lse_ref[0:1, start : start + TILE] = turned[0:1, :]
        lse_ref[1:2, start : start + TILE] = turned[DH : DH + 1, :]
        if between is not None:
            between(start // TILE)


def attend_bwd_pair(
    shard, prompt_rows, q, kp, vp, kc, vc, g, att, lse, dq, dkp, dvp, dkc, dvc, accum, between=None
):
    cont_len = kc.shape[0]
    tokens = prompt_rows + cont_len
    prompt_len = kp.shape[0]
    g_t = g[...]
    turned = jnp.transpose(g_t.astype(jnp.float32) * att[...])
    delta = (
        jnp.sum(turned[:DH], 0, keepdims=True),
        jnp.sum(turned[DH:], 0, keepdims=True),
    )
    q_t = q[...] * jnp.asarray(DH ** (-0.5), jnp.bfloat16)
    keep = low_lanes(q_t.shape)
    zero = jnp.zeros_like(q_t)
    q_h = (jnp.where(keep, q_t, zero), jnp.where(keep, zero, q_t))
    g_h = (jnp.where(keep, g_t, zero), jnp.where(keep, zero, g_t))
    accum[...] = jnp.zeros_like(accum)

    def block(key_b, value_b, first, mask):
        key_t = jnp.transpose(key_b.astype(jnp.float32)).astype(jnp.bfloat16)
        g_key = jnp.zeros((TILE, PAIR), jnp.float32)
        g_value = jnp.zeros((TILE, PAIR), jnp.float32)
        for parity in range(2):
            scores = rows_dot(key_b, q_h[parity][first:])
            probs = jnp.exp(scores - lse[parity : parity + 1, first:])
            masked = jnp.where(mask, probs[:, :TILE], 0.0)
            if tokens - first > TILE:
                probs = jnp.concatenate([masked, probs[:, TILE:]], 1)
            else:
                probs = masked
            g_probs = rows_dot(value_b, g_h[parity][first:])
            g_scores = (probs * (g_probs - delta[parity][:, first:])).astype(jnp.bfloat16)
            g_value += dot_plain(probs.astype(jnp.bfloat16), g_h[parity][first:])
            g_key += dot_plain(g_scores, q_h[parity][first:])
            rows = slice(parity * DH, (parity + 1) * DH)
            accum[rows, first:] += dot_plain(key_t[rows], g_scores)
        return g_key.astype(jnp.bfloat16), g_value.astype(jnp.bfloat16)

    ahead = lax.broadcasted_iota(jnp.int32, (TILE, TILE), 0) - lax.broadcasted_iota(
        jnp.int32, (TILE, TILE), 1
    )

    def prompt_block(index, start):
        rows = pl.ds(start, TILE)
        mask = ahead <= shard * prompt_rows - index * TILE
        g_key, g_value = block(kp[rows, :], vp[rows, :], 0, mask)
        dkp[rows, :] = g_key
        dvp[rows, :] = g_value

    blocks = prompt_len // TILE
    if blocks <= 4:
        for index in range(blocks):
            prompt_block(index, index * TILE)
            if between is not None:
                between(index)
    else:

        def step(index, carry):
            prompt_block(index, pl.multiple_of(index * TILE, TILE))
            return carry

        lax.fori_loop(0, blocks, step, 0)
    for start in range(0, cont_len, TILE):
        rows = slice(start, start + TILE)
        g_key, g_value = block(kc[rows, :], vc[rows, :], prompt_rows + start, ahead <= 0)
        dkc[rows, :] = g_key
        dvc[rows, :] = g_value
        if between is not None:
            between(blocks + start // TILE)
    dq[...] = (jnp.transpose(accum[...]) * DH ** (-0.5)).astype(jnp.bfloat16)


def attend_forward(q, kp, vp, kc, vc, prompt_rows):
    tokens, prompt_len, cont_len = q.shape[0], kp.shape[0], kc.shape[0]
    pairs = HEADS // 2

    def kernel(q, kp, vp, kc, vc, att_ref, lse_ref):
        attend_fwd_pair(
            lax.axis_index("shard"), prompt_rows, q, kp, vp, kc, vc, att_ref, lse_ref.at[0]
        )

    def columns(rows):
        return pl.BlockSpec((rows, PAIR), lambda p: (0, p))

    return pl.pallas_call(
        kernel,
        grid=(pairs,),
        in_specs=[columns(rows) for rows in (tokens, prompt_len, prompt_len, cont_len, cont_len)],
        out_specs=[columns(tokens), pl.BlockSpec((1, 8, tokens), lambda p: (p, 0, 0))],
        out_shape=[
            jax.ShapeDtypeStruct((tokens, D), jnp.float32),
            jax.ShapeDtypeStruct((pairs, 8, tokens), jnp.float32),
        ],
        compiler_params=pltpu.CompilerParams(vmem_limit_bytes=VMEM_ALL),
        name="attend_forward",
    )(q, kp, vp, kc, vc)


def attend_backward(q, kp, vp, kc, vc, g_att, att, lse, prompt_rows):
    tokens, prompt_len, cont_len = q.shape[0], kp.shape[0], kc.shape[0]
    pairs = HEADS // 2

    def kernel(q, kp, vp, kc, vc, g, a, ls, dq, dkp, dvp, dkc, dvc, accum):
        attend_bwd_pair(
            lax.axis_index("shard"),
            prompt_rows,
            q,
            kp,
            vp,
            kc,
            vc,
            g,
            a,
            ls.at[0],
            dq,
            dkp,
            dvp,
            dkc,
            dvc,
            accum,
        )

    def columns(rows):
        return pl.BlockSpec((rows, PAIR), lambda p: (0, p))

    sizes = (tokens, prompt_len, prompt_len, cont_len, cont_len)
    return pl.pallas_call(
        kernel,
        grid=(pairs,),
        in_specs=[columns(rows) for rows in sizes + (tokens, tokens)]
        + [pl.BlockSpec((1, 8, tokens), lambda p: (p, 0, 0))],
        out_specs=[columns(rows) for rows in sizes],
        out_shape=[jax.ShapeDtypeStruct((rows, D), jnp.bfloat16) for rows in sizes],
        scratch_shapes=[pltpu.VMEM((PAIR, tokens), jnp.float32)],
        compiler_params=pltpu.CompilerParams(vmem_limit_bytes=VMEM_ALL),
        name="attend_backward",
    )(q, kp, vp, kc, vc, g_att, att, lse)


MESH_ID = pl.DeviceIdType.MESH


def project_and_attend(prompt, conts, w_qkv, w_out, w_in, w_ffo, layer_biases):
    pieces, early = 12, 4
    by_z = (4, 5, 6, 7, 8, 9)
    rows = w_qkv.shape[0]
    p_rows, cont_len = prompt.shape[0], conts.shape[0]
    tokens = p_rows + cont_len
    p_len = 4 * p_rows
    pairs = HEADS // 2
    tiles = tokens // TILE
    chunk = 2 * PAIR
    chunks = D // chunk
    quarter = rows // 4

    def kernel(
        xp, xc, wq, wo, wi, wf, bias, w_all_out, wf_out, q_out, kc_out, vc_out, kp_out, vp_out, att_out, lse,
        stage, w_all, q, kc, vc, kp, vp, att,
        load, c_s, c_r, x_s, x_r, y_s, y_r, z_s, z_r, d_s, d_r, e_s, e_r, w_sem,
        kc_s, kc_r, kx_s, kx_r, kd_s, kd_r, out_sem,
    ):
        rep, shard = lax.axis_index("rep"), lax.axis_index("shard")
        z, y = rep // 2, rep % 2
        x, core = shard // 2, shard % 2
        partner = (rep, 2 * x + 1 - core)
        across = (rep, 2 * (1 - x) + core)
        beside = (2 * z + 1 - y, shard)
        z_low = z % 2
        above = (2 * (z + 1 - 2 * z_low) + y, shard)
        there = 2 * (1 - x) + core

        def remote(ref, send, recv, device):
            return pltpu.make_async_remote_copy(
                src_ref=ref,
                dst_ref=ref,
                send_sem=send,
                recv_sem=recv,
                device_id=device,
                device_id_type=MESH_ID,
            )

        def source(k):
            if k < 3:
                j = (1, 2, 0)[k]
                return wq.at[:, j * D : (j + 1) * D]
            if k < 4:
                return wo
            if k < 8:
                return wi.at[:, (k - 4) * D : (k - 3) * D]
            return wf.at[(k - 8) * rows : (k - 7) * rows, :]

        def loading(k):
            return pltpu.make_async_copy(source(k), stage.at[k], load.at[k])

        for k in range(pieces):
            loading(k).start()
        barrier = pltpu.get_barrier_semaphore()
        for other in (partner, across, beside, above):
            pl.semaphore_signal(barrier, inc=1, device_id=other, device_id_type=MESH_ID)
        pl.semaphore_wait(barrier, 4)

        def part(k, block, first, count):
            start = pl.multiple_of(first * quarter, 16)
            return w_all.at[k, block, pl.ds(start, count * quarter), :]

        def core_copy(k):
            return remote(w_all.at[k, shard], c_s.at[k], c_r.at[k], partner)

        def core_arrival(k):
            return remote(w_all.at[k, 2 * x + 1 - core], c_s.at[k], c_r.at[k], partner)

        def crossing(k, y_at):
            return (2 * z_low + y_at, 1) if k in by_z else (2 * y_at, 2)

        def x_copy(k):
            return remote(part(k, shard, *crossing(k, y)), x_s.at[k], x_r.at[k], across)

        def x_arrival(k):
            return remote(part(k, there, *crossing(k, y)), x_s.at[k], x_r.at[k], across)

        def y_copy(k):
            return remote(part(k, there, *crossing(k, y)), y_s.at[k], y_r.at[k], beside)

        def y_arrival(k):
            return remote(part(k, there, *crossing(k, 1 - y)), y_s.at[k], y_r.at[k], beside)

        def z_copy(k):
            return remote(part(k, there, 2 * z_low, 2), z_s.at[k], z_r.at[k], above)

        def z_arrival(k):
            return remote(part(k, there, 2 * (1 - z_low), 2), z_s.at[k], z_r.at[k], above)

        def halves(k):
            first = 2 * z_low if k in by_z else 2 * y
            return first, 2 - first

        def d_copy(k, block=None):
            block = there if block is None else block
            return remote(part(k, block, halves(k)[0], 2), d_s.at[k], d_r.at[k], partner)

        def e_copy(k, block=None):
            block = there if block is None else block
            return remote(part(k, block, halves(k)[1], 2), e_s.at[k], e_r.at[k], partner)

        far = 2 * (1 - x) + 1 - core

        def send_piece(k):
            x_copy(k).start()
            core_copy(k).start()

        def round_piece(k):
            loading(k).wait()
            w_all[k, shard] = stage[k].astype(jnp.bfloat16)

        def serve_x(k):
            x_arrival(k).wait_recv()
            y_copy(k).start()
            if k not in by_z:
                d_copy(k).start()

        def serve_y(k):
            y_arrival(k).wait_recv()
            if k in by_z:
                z_copy(k).start()
                d_copy(k).start()
            else:
                e_copy(k).start()

        def serve_z(k):
            z_arrival(k).wait_recv()
            e_copy(k).start()

        def w_store(k):
            if k < 8:
                return pltpu.make_async_copy(w_all.at[k], w_all_out.at[k], w_sem.at[k])
            return pltpu.make_async_copy(w_all.at[k], wf_out.at[:, k - 8], w_sem.at[k])

        def complete(k):
            core_arrival(k).wait_recv()
            d_copy(k, far).wait_recv()
            e_copy(k, far).wait_recv()
            w_store(k).start()

        def weight(k):
            return w_all[k].reshape(4 * rows, D)

        for k in range(early):
            round_piece(k)
            send_piece(k)
        for k in range(early, pieces):
            round_piece(k)
        own_rows = pl.ds(pl.multiple_of(shard * p_rows, p_rows), p_rows)
        kv = (kp, vp)

        def kv_part(t, g, block):
            lanes = pl.ds(g * chunk if isinstance(g, int) else pl.multiple_of(g * chunk, chunk), chunk)
            return kv[t].at[pl.ds(pl.multiple_of(block * p_rows, p_rows), p_rows), lanes]

        def kv_core(t, g):
            return remote(kv_part(t, g, shard), kc_s.at[g, t], kc_r.at[g, t], partner)

        def kv_across(t, g):
            return remote(kv_part(t, g, shard), kx_s.at[g, t], kx_r.at[g, t], across)

        def kv_forward(t, g):
            return remote(kv_part(t, g, there), kd_s.at[g, t], kd_r.at[g, t], partner)

        serve_x(0)
        serve_x(1)
        serve_y(0)
        complete(0)
        kp[own_rows, :] = dot_plain(xp[...], weight(0)).astype(jnp.bfloat16)
        kc[...] = dot_plain(xc[...], weight(0)).astype(jnp.bfloat16)
        serve_x(2)
        serve_y(1)
        complete(1)
        vp[own_rows, :] = (dot_plain(xp[...], weight(1)) + bias[1:2, :]).astype(jnp.bfloat16)
        waiting = list(range(early, pieces))
        for g in range(chunks):
            for t in range(2):
                kv_across(t, g).start()
                kv_core(t, g).start()
            for k in waiting[: 2 if g < chunks - 1 else pieces]:
                send_piece(k)
            waiting = waiting[2:]
        vc[...] = (dot_plain(xc[...], weight(1)) + bias[1:2, :]).astype(jnp.bfloat16)
        serve_y(2)
        serve_x(3)
        complete(2)
        q[:p_rows, :] = (dot_plain(xp[...], weight(2)) + bias[0:1, :]).astype(jnp.bfloat16)
        q[p_rows:, :] = (dot_plain(xc[...], weight(2)) + bias[0:1, :]).astype(jnp.bfloat16)

        def keep(ref, target, i):
            return pltpu.make_async_copy(ref, target, out_sem.at[i])

        kept = [(q, q_out, 0), (kc, kc_out, 1), (vc, vc_out, 2)]
        for item in kept:
            keep(*item).start()

        def serve_kv(g):
            for t in range(2):
                remote(kv_part(t, g, there), kx_s.at[g, t], kx_r.at[g, t], across).wait_recv()
                kv_forward(t, g).start()

        def complete_kv(g):
            for t in range(2):
                remote(
                    kv_part(t, g, 2 * x + 1 - core), kc_s.at[g, t], kc_r.at[g, t], partner
                ).wait_recv()
                remote(kv_part(t, g, far), kd_s.at[g, t], kd_r.at[g, t], partner).wait_recv()

        serve_kv(0)
        arrive = {4: 26.3, 5: 27.9, 6: 35.2, 7: 36.8, 8: 44.1, 9: 45.7, 10: 48.9, 11: 52.1}
        work = [(33.6, serve_kv, 1), (42.4, serve_kv, 2), (27.0, serve_y, 3), (30.0, complete, 3)]
        for k in range(4, pieces):
            at = arrive[k]
            work.append((at, serve_x, k))
            if k in by_z:
                work += [(at + 4, serve_y, k), (at + 10, serve_z, k), (at + 13, complete, k)]
            else:
                work += [(at + 6, serve_y, k), (at + 9, complete, k)]
        slots = pairs * tiles
        work = [(max(0, round((at - 26) / 1.37 - 0.6)), act, k) for at, act, k in work]
        work.sort(key=lambda item: item[0])

        def att_store(p):
            lanes = pl.ds(pl.multiple_of(p * PAIR, PAIR), PAIR)
            return pltpu.make_async_copy(att.at[:, lanes], att_out.at[:, lanes], out_sem.at[5 + p])

        def pair(p, carry):
            @pl.when(p % 2 == 0)
            def _():
                complete_kv(p // 2)

            def between(tile):
                for slot, action, k in work:
                    if slot < slots and slot % tiles == tile:

                        @pl.when(p == slot // tiles)
                        def _(action=action, k=k):
                            action(k)

            lanes = pl.ds(pl.multiple_of(p * PAIR, PAIR), PAIR)
            attend_fwd_pair(
                shard,
                p_rows,
                q.at[:, lanes],
                kp.at[:, lanes],
                vp.at[:, lanes],
                kc.at[:, lanes],
                vc.at[:, lanes],
                att.at[:, lanes],
                lse.at[p],
                between,
            )
            att_store(p).start()
            return carry

        lax.fori_loop(0, pairs, pair, 0)
        kept += [(kp, kp_out, 3), (vp, vp_out, 4)]
        for item in kept[3:]:
            keep(*item).start()
        for slot, action, k in work:
            if slot >= slots:
                action(k)
        for item in kept:
            keep(*item).wait()

        def last_pair(p, carry):
            att_store(p).wait()
            return carry

        lax.fori_loop(0, pairs, last_pair, 0)
        for k in range(pieces):
            w_store(k).wait()
            for copy in (core_copy, x_copy, y_copy, d_copy, e_copy):
                copy(k).wait_send()
            if k in by_z:
                z_copy(k).wait_send()
        for g in range(chunks):
            for t in range(2):
                for copy in (kv_core, kv_across, kv_forward):
                    copy(t, g).wait_send()

    def sems(*dims):
        return pltpu.SemaphoreType.DMA(dims)

    def low(*dims):
        return jax.ShapeDtypeStruct(dims, jnp.bfloat16)

    anywhere = pl.BlockSpec(memory_space=pl.ANY)
    vmem = pl.BlockSpec(memory_space=pltpu.VMEM)
    n = pieces
    out = pl.pallas_call(
        kernel,
        in_specs=[vmem, vmem, anywhere, anywhere, anywhere, anywhere, vmem],
        out_specs=[anywhere] * 8 + [vmem],
        out_shape=[
            low(8, 4, rows, D),
            low(4, 4, rows, D),
            low(tokens, D),
            low(cont_len, D),
            low(cont_len, D),
            low(p_len, D),
            low(p_len, D),
            jax.ShapeDtypeStruct((tokens, D), jnp.float32),
            jax.ShapeDtypeStruct((pairs, 8, tokens), jnp.float32),
        ],
        scratch_shapes=[
            pltpu.VMEM((n, rows, D), jnp.float32),
            pltpu.VMEM((n, 4, rows, D), jnp.bfloat16),
            pltpu.VMEM((tokens, D), jnp.bfloat16),
            pltpu.VMEM((cont_len, D), jnp.bfloat16),
            pltpu.VMEM((cont_len, D), jnp.bfloat16),
            pltpu.VMEM((p_len, D), jnp.bfloat16),
            pltpu.VMEM((p_len, D), jnp.bfloat16),
            pltpu.VMEM((tokens, D), jnp.float32),
        ]
        + [sems(n)] * 14
        + [sems(chunks, 2)] * 6
        + [sems(5 + pairs)],
        compiler_params=pltpu.CompilerParams(
            collective_id=1, has_side_effects=True, vmem_limit_bytes=VMEM_ALL
        ),
        name="project_and_attend",
    )(prompt, conts, w_qkv, w_out, w_in, w_ffo, layer_biases)
    w_all, wf, q, kc, vc, kp, vp, att, lse = out
    w_all = w_all.reshape(8, 4 * rows, D)
    return w_all, wf.reshape(16 * rows, D), q, kp, vp, kc, vc, att, lse


def project_native(prompt, conts, w_qkv, w_out, w_in, w_ffo, layer_biases):
    rows = prompt.shape[0]

    def gathered(value):
        return lax.all_gather(value.astype(jnp.bfloat16), "shard", axis=0, tiled=True)

    qkv, out, inner, ffo = (gathered(w) for w in (w_qkv, w_out, w_in, w_ffo))
    tokens = jnp.concatenate([prompt, conts], 0)
    bias = jnp.concatenate([layer_biases[0], jnp.zeros((D,), jnp.float32), layer_biases[1]])
    qkv_b = (dot_plain(tokens, qkv) + bias).astype(jnp.bfloat16)
    q, keys, values = (qkv_b[:, i * D : (i + 1) * D] for i in range(3))
    kp, vp = gathered(keys[:rows]), gathered(values[:rows])
    kc, vc = keys[rows:], values[rows:]
    att, lse = attend_forward(q, kp, vp, kc, vc, rows)
    blocks = [qkv[:, D : 2 * D], qkv[:, 2 * D :], qkv[:, :D], out]
    blocks += [inner[:, i * D : (i + 1) * D] for i in range(inner.shape[1] // D)]
    return jnp.stack(blocks), ffo, q, kp, vp, kc, vc, att, lse


def student_head(label, stu, vectors, w_pool, w_class, bias_class, classes):
    part_w = STU // SHEADS
    low_half = lax.broadcasted_iota(jnp.int32, stu.shape, 1) < part_w
    row_low = lax.broadcasted_iota(jnp.int32, (1, STU), 1) < part_w
    query, bias_pool = vectors[1:2, :], vectors[2:3, :]

    def by_head(values):
        low_sum = jnp.sum(jnp.where(low_half[: values.shape[0]], values, 0.0), 1, keepdims=True)
        high_sum = jnp.sum(jnp.where(low_half[: values.shape[0]], 0.0, values), 1, keepdims=True)
        return jnp.where(low_half[: values.shape[0]], low_sum, high_sum)

    scores = by_head(stu * query) * part_w ** (-0.5)
    largest = jnp.max(scores, 0, keepdims=True)
    expo = jnp.exp(scores - largest)
    weights = expo / jnp.sum(expo, 0, keepdims=True)
    pooled = jnp.sum(weights * stu, 0, keepdims=True)

    def column(row):
        return jnp.transpose(jnp.broadcast_to(row, (STU, STU)))

    def times(row, matrix):
        return jnp.sum(column(row) * matrix, 0, keepdims=True)

    def times_turned(row, matrix):
        total = jnp.sum(matrix * row, 1, keepdims=True)
        return jnp.transpose(jnp.broadcast_to(total, (STU, STU)))[:1]

    top = jnp.tanh(times(pooled, w_pool) + bias_pool)
    lane = lax.broadcasted_iota(jnp.int32, (1, STU), 1)
    logits = times(top, w_class) + bias_class
    seen = jnp.where(lane < classes, logits, NEG_BIG)
    expo_l = jnp.exp(seen - jnp.max(seen, 1, keepdims=True))
    g_logits = expo_l / jnp.sum(expo_l, 1, keepdims=True) - jnp.where(lane == label, 1.0, 0.0)
    g_class = column(top) * g_logits
    g_pre = times_turned(g_logits, w_class) * (1.0 - top * top)
    g_pool = column(pooled) * g_pre
    g_pooled = times_turned(g_pre, w_pool)
    g_weights = by_head(stu * g_pooled)
    mean = jnp.sum(weights * g_weights, 0, keepdims=True)
    g_scores = weights * (g_weights - mean) * part_w ** (-0.5)
    g_stu = weights * g_pooled + g_scores * query
    g_query = jnp.sum(g_scores * stu, 0, keepdims=True)
    return logits, g_stu, g_query, g_pre, g_pool, g_class, g_logits


def middle(
    att, prompt, conts, prompt_cot, cont_cot, labels, w_all, wf,
    biases, gains, bias_in, student, vectors, w_pool, w_class, bias_class,
):
    p_rows, cont_len = prompt.shape[0], conts.shape[0]
    tokens = p_rows + cont_len
    ff = wf.shape[0]
    blocks = ff // D
    steps = tokens // TILE
    wide = D // TILE
    classes = w_class.shape[1]
    w_class_p = jnp.pad(w_class, ((0, 0), (0, STU - classes)))
    bias_class_p = jnp.pad(bias_class[None], ((0, 0), (0, STU - classes)))
    g_names = 2 * blocks + 1

    def kernel(
        label_ref, att_h, xp, xc, cp, cc, w_h, wf_h, bias, gain, b_in, w_stu, vec, w_p, w_c, b_c,
        out_p, out_c, logits_out, grads_h, g_r1_h, g_att_h, small,
        att_v, att_b, w_v, wf_v, norm1, norm2, rstd1, rstd2, x1_b, act, slope, g_res, g_ffn, g_br, g_stu_b, grads,
        sums, in_sum, load, store,
    ):
        def fetch(source, target, i):
            return pltpu.make_async_copy(source, target, load.at[i])

        loads = [
            fetch(att_h, att_v, 0),
            fetch(w_h.at[3], w_v.at[0], 1),
            fetch(w_h.at[pl.ds(4, blocks)], w_v.at[pl.ds(1, blocks)], 2),
            fetch(wf_h, wf_v, 3),
        ]
        for copy in loads:
            copy.start()
        sums[...] = jnp.zeros_like(sums)
        small[...] = jnp.zeros_like(small)

        def row(i):
            return pl.ds(i * TILE, TILE)

        def tokens_of(i):
            return xp[...] if i == 0 else xc[(i - 1) * TILE : i * TILE, :]

        def normalize(values):
            center = values - jnp.mean(values, -1, keepdims=True)
            spread = jnp.mean(center * center, -1, keepdims=True)
            scale = lax.rsqrt(spread + 1e-05)
            return center * scale, scale

        def norm_back(g, gain_row, hat, scale):
            gg = g * gain_row
            return scale * (
                gg
                - jnp.mean(gg, -1, keepdims=True)
                - hat * jnp.mean(gg * hat, -1, keepdims=True)
            )

        def add_sum(i, values):
            sums[i : i + 1, :] += jnp.sum(values, 0, keepdims=True)

        loads[0].wait()
        loads[1].wait()
        for i in range(steps):
            part = att_v[row(i), :].astype(jnp.bfloat16)
            att_b[row(i), :] = part
            branch = dot_plain(part, w_v[0]) + bias[2:3, :]
            hat, scale = normalize(tokens_of(i).astype(jnp.float32) + branch)
            norm1[row(i), :] = hat
            rstd1[row(i), :] = jnp.broadcast_to(scale, (TILE, 128))
            x1_b[row(i), :] = (hat * gain[0:1, :] + bias[4:5, :]).astype(jnp.bfloat16)
        loads[2].wait()

        def inner(i, carry):
            lanes = pl.ds(pl.multiple_of(lax.rem(i, wide) * TILE, TILE), TILE)
            columns = pl.ds(pl.multiple_of(i * TILE, TILE), TILE)
            hidden = dot_plain(x1_b[...], w_v[1 + i // wide, :, lanes]) + b_in[:, columns]
            cdf = 0.5 * (1.0 + lax.erf(hidden * 2.0 ** (-0.5)))
            act[:, columns] = (hidden * cdf).astype(jnp.bfloat16)
            density = jnp.exp(hidden * hidden * (-0.5)) * 0.3989422804014327
            slope[:, columns] = (cdf + hidden * density).astype(jnp.bfloat16)
            return carry

        lax.fori_loop(0, ff // TILE, inner, 0)
        loads[3].wait()
        for i in range(steps):
            ffn = dot_plain(act[row(i), :], wf_v[...]) + bias[3:4, :]
            first = norm1[row(i), :] * gain[0:1, :] + bias[4:5, :]
            hat, scale = normalize(first + ffn)
            norm2[row(i), :] = hat
            rstd2[row(i), :] = jnp.broadcast_to(scale, (TILE, 128))
            out_b = (hat * gain[1:2, :] + bias[5:6, :]).astype(jnp.bfloat16)
            if i == 0:
                out_p[...] = out_b
            else:
                out_c[(i - 1) * TILE : i * TILE, :] = out_b
        w_stu_b = w_stu[...].astype(jnp.bfloat16)
        stu = dot_plain(out_c[...], w_stu_b) + vec[0:1, :]
        logits, g_stu, g_query, g_pre, g_pool, g_class, g_logits = student_head(
            label_ref[0, 0], stu, vec, w_p[...], w_c[...], b_c[...], classes
        )
        logits_out[...] = logits
        g_stu_b[...] = g_stu.astype(jnp.bfloat16)
        small[:, :STU] = dot_first(out_c[...], g_stu_b[...])
        for i in range(steps):
            g = (cp[...] if i == 0 else cc[(i - 1) * TILE : i * TILE, :]).astype(jnp.float32)
            if i > 0:
                g += dot_second(g_stu_b[(i - 1) * TILE : i * TILE, :], w_stu_b)
            hat = norm2[row(i), :]
            add_sum(7, g * hat)
            add_sum(5, g)
            g_r2 = norm_back(g, gain[1:2, :], hat, rstd2[row(i), :1])
            g_res[row(i), :] = g_r2
            low = g_r2.astype(jnp.bfloat16)
            g_ffn[row(i), :] = low
            add_sum(3, low.astype(jnp.float32))

        def piece_store(k):
            return pltpu.make_async_copy(grads.at[k], grads_h.at[k], store.at[k])

        for j in range(blocks):
            product = dot_first(act[:, j * D : (j + 1) * D], g_ffn[...]).astype(jnp.bfloat16)
            rows = D // blocks
            for k in range(blocks):
                grads[k, j * rows : (j + 1) * rows, :] = product[k * rows : (k + 1) * rows]
        for k in range(blocks):
            piece_store(k).start()

        for j in range(blocks):
            columns = slice(j * D, (j + 1) * D)
            total = jnp.zeros((1, D), jnp.float32)
            for i in range(steps):
                g_act = dot_second(g_ffn[row(i), :], wf_v[columns, :])
                low = (g_act * slope[row(i), columns].astype(jnp.float32)).astype(jnp.bfloat16)
                slope[row(i), columns] = low
                total += jnp.sum(low.astype(jnp.float32), 0, keepdims=True)
            in_sum[:, columns] = total
        for j in range(blocks):
            grads[blocks + j] = dot_first(x1_b[...], slope[:, j * D : (j + 1) * D]).astype(
                jnp.bfloat16
            )
            piece_store(blocks + j).start()
        for i in range(steps):
            g = g_res[row(i), :]
            for j in range(blocks):
                g += dot_second(slope[row(i), j * D : (j + 1) * D], w_v[1 + j])
            hat = norm1[row(i), :]
            add_sum(6, g * hat)
            add_sum(4, g)
            g_r1 = norm_back(g, gain[0:1, :], hat, rstd1[row(i), :1])
            g_res[row(i), :] = g_r1
            low = g_r1.astype(jnp.bfloat16)
            g_br[row(i), :] = low
            add_sum(2, low.astype(jnp.float32))
        res_store = pltpu.make_async_copy(g_res, g_r1_h, store.at[g_names])
        res_store.start()
        g_ffn[...] = dot_second(g_br[...], w_v[0]).astype(jnp.bfloat16)
        att_store = pltpu.make_async_copy(g_ffn, g_att_h, store.at[g_names + 1])
        att_store.start()
        grads[2 * blocks] = dot_first(att_b[...], g_br[...]).astype(jnp.bfloat16)
        piece_store(2 * blocks).start()
        across = D // 128
        for i in range(8):
            for part in range(across):
                small[i * across + part : i * across + part + 1, STU:] = sums[
                    i : i + 1, part * 128 : (part + 1) * 128
                ]
        for part in range(ff // 128):
            at = 8 * across + part
            small[at : at + 1, STU:] = in_sum[:, part * 128 : (part + 1) * 128]
        base = 8 * across + ff // 128
        small[base : base + 1, STU:] = jnp.sum(g_stu_b[...].astype(jnp.float32), 0, keepdims=True)
        small[base + 1 : base + 2, STU:] = g_query
        small[base + 2 : base + 3, STU:] = g_pre
        small[base + 3 : base + 4, STU:] = g_logits
        small[base + 8 : base + 8 + STU, STU:] = g_pool
        small[base + 8 + STU : base + 8 + 2 * STU, STU:] = g_class
        res_store.wait()
        att_store.wait()
        for k in range(g_names):
            piece_store(k).wait()

    anywhere = pl.BlockSpec(memory_space=pl.ANY)
    vmem = pl.BlockSpec(memory_space=pltpu.VMEM)
    low = jnp.bfloat16

    def shaped(dims, kind=jnp.float32):
        return jax.ShapeDtypeStruct(dims, kind)

    return pl.pallas_call(
        kernel,
        in_specs=[pl.BlockSpec(memory_space=pltpu.SMEM), anywhere]
        + [vmem] * 4
        + [anywhere] * 2
        + [vmem] * 8,
        out_specs=[vmem, vmem, vmem, anywhere, anywhere, anywhere, vmem],
        out_shape=[
            shaped((p_rows, D), low),
            shaped((cont_len, D), low),
            shaped((1, STU)),
            shaped((g_names, D, D), low),
            shaped((tokens, D)),
            shaped((tokens, D), low),
            shaped((D, 2 * STU)),
        ],
        scratch_shapes=[
            pltpu.VMEM((tokens, D), jnp.float32),
            pltpu.VMEM((tokens, D), low),
            pltpu.VMEM((1 + blocks, D, D), low),
            pltpu.VMEM((ff, D), low),
            pltpu.VMEM((tokens, D), jnp.float32),
            pltpu.VMEM((tokens, D), jnp.float32),
            pltpu.VMEM((tokens, 128), jnp.float32),
            pltpu.VMEM((tokens, 128), jnp.float32),
            pltpu.VMEM((tokens, D), low),
            pltpu.VMEM((tokens, ff), low),
            pltpu.VMEM((tokens, ff), low),
            pltpu.VMEM((tokens, D), jnp.float32),
            pltpu.VMEM((tokens, D), low),
            pltpu.VMEM((tokens, D), low),
            pltpu.VMEM((cont_len, STU), low),
            pltpu.VMEM((g_names, D, D), low),
            pltpu.VMEM((8, D), jnp.float32),
            pltpu.VMEM((1, ff), jnp.float32),
            pltpu.SemaphoreType.DMA((4,)),
            pltpu.SemaphoreType.DMA((g_names + 2,)),
        ],
        compiler_params=pltpu.CompilerParams(vmem_limit_bytes=VMEM_ALL),
        name="middle",
    )(
        labels,
        att,
        prompt,
        conts,
        prompt_cot,
        cont_cot,
        w_all,
        wf,
        biases,
        gains,
        bias_in[None],
        student,
        vectors,
        w_pool,
        w_class_p,
        bias_class_p,
    )


def sum_native(g9, g_qkvw, small):
    blocks = (g9.shape[0] - 1) // 2
    rows = D // blocks
    ffo = g9[:blocks].reshape(blocks, blocks, rows, D).transpose(1, 0, 2, 3).reshape(-1, D)
    inner = jnp.concatenate([g9[blocks + j] for j in range(blocks)], 1)

    def over(grad):
        part = lax.psum_scatter(
            grad.astype(jnp.bfloat16), "shard", scatter_dimension=0, tiled=True
        )
        return lax.psum(part, "rep").astype(jnp.float32)

    owned = tuple(over(grad) for grad in (g_qkvw, g9[2 * blocks], inner, ffo))
    return owned, lax.psum(small, ("rep", "shard"))


def finish(
    q, kp, vp, kc, vc, att, lse, g_att, g9, g_resid, small, w_all, prompt, conts, ff, classes
):
    pieces, ready = 12, 9
    p_rows, cont_len = prompt.shape[0], conts.shape[0]
    tokens = p_rows + cont_len
    p_len = kp.shape[0]
    pairs = HEADS // 2
    rows = D // 4
    half, quarter = D // 2, rows // 4
    s_width = small.shape[1]
    chunk = 2 * PAIR
    chunks = D // chunk
    across_lanes = D // 128

    def kernel(
        q_h, kp_h, vp_h, kc_h, vc_h, att_h, g_att_h, g9, g_res_h, w_h, ls, sm, xp, xc,
        out_pg, out_cg, out_q, out_o, out_i, out_f,
        o_bias, o_gain, o_in, o_stu, o_vec, o_pool, o_class, o_cb,
        qv, kpv, vpv, kcv, vcv, attv, gav, accum, dq, dkp, dvp, dkc, dvc, kr, kx, kvs, wv, g_tok, made, head,
        own, cr, xr, yr, zr, fb, made_s, own_s, cr_s, xr_s, yr_s, zr_s, fb_s, fin_s,
        load, sem_own, c_send, c_recv, x_send, x_recv, y_send, y_recv, z_send, z_recv,
        f_send, f_recv, o_send, o_recv, o_own, g_send, g_recv, kc_s, kc_r, kx_s, kx_r, out_sem,
    ):
        rep, shard = lax.axis_index("rep"), lax.axis_index("shard")
        z, y = rep // 2, rep % 2
        x, core = shard // 2, shard % 2
        partner = (rep, 2 * x + 1 - core)
        across = (rep, 2 * (1 - x) + core)
        beside = (2 * z + 1 - y, shard)
        far = (rep, 2 * (1 - x) + 1 - core)

        def along(step):
            return (2 * lax.rem(z + step, 4) + y, shard)

        def own_copy(k, xx):
            return pltpu.make_async_copy(
                g9.at[k, pl.ds(pl.multiple_of((2 * xx + core) * rows, 16), rows), :],
                own.at[k, xx],
                sem_own.at[k, xx],
            )

        fetched = [(q_h, qv), (kp_h, kpv), (vp_h, vpv), (kc_h, kcv), (vc_h, vcv)]
        fetched += [(att_h, attv), (g_att_h, gav), (w_h.at[pl.ds(0, 3)], wv), (g_res_h, g_tok)]

        def fetch(i):
            return pltpu.make_async_copy(*fetched[i], load.at[i])

        for k in range(2):
            for xx in range(2):
                own_copy(k, xx).start()
        for i in range(7):
            fetch(i).start()
        for k in range(2, ready):
            for xx in range(2):
                own_copy(k, xx).start()
        for i in (7, 8):
            fetch(i).start()

        barrier = pltpu.get_barrier_semaphore()
        others = [partner, across, beside, along(1), along(2), along(3), far]
        for other in others:
            pl.semaphore_signal(barrier, inc=1, device_id=other, device_id_type=MESH_ID)
        pl.semaphore_wait(barrier, len(others))

        def remote(source, target, send, recv, device):
            return pltpu.make_async_remote_copy(
                src_ref=source,
                dst_ref=target,
                send_sem=send,
                recv_sem=recv,
                device_id=device,
                device_id_type=MESH_ID,
            )

        big = (own, cr, xr, yr, zr, fb, half)
        narrow = (own_s, cr_s, xr_s, yr_s, zr_s, fb_s, s_width // 2)

        def bufs(k):
            if isinstance(k, int) and k == pieces:
                return narrow, 0
            return big, k

        def core_copy(k, xx):
            b, i = bufs(k)
            block = 2 * xx + 1 - core
            if not isinstance(k, int):
                source = b[1].at[i, xx]
            elif k < ready:
                source = g9.at[k, pl.ds(pl.multiple_of(block * rows, 16), rows), :]
            elif k < pieces:
                source = made.at[k - ready, block]
            else:
                source = made_s.at[block]
            return remote(source, b[1].at[i, xx], c_send.at[k, xx], c_recv.at[k, xx], partner)

        def x_copy(k):
            b, i = bufs(k)
            return remote(b[0].at[i, 1 - x], b[2].at[i], x_send.at[k], x_recv.at[k], across)

        def lanes_of(b, which):
            return pl.ds(pl.multiple_of(which * b[6], 128), b[6])

        def y_copy(k):
            b, i = bufs(k)
            source = b[0].at[i, x, :, lanes_of(b, 1 - y)]
            return remote(source, b[3].at[i], y_send.at[k], y_recv.at[k], beside)

        def rows_of(which):
            return pl.ds(pl.multiple_of(which * quarter, 16), quarter)

        def zs_copy(k, step):
            b, i = bufs(k)
            source = b[0].at[i, x, rows_of(lax.rem(z + step, 4)), lanes_of(b, y)]
            return remote(
                source, b[4].at[i, z], z_send.at[k, step - 1], z_recv.at[k, z], along(step)
            )

        def zr_wait(k, step):
            b, i = bufs(k)
            slot = lax.rem(z + step, 4)
            target = b[4].at[i, slot]
            remote(
                target, target, z_send.at[k, step - 1], z_recv.at[k, slot], along(step)
            ).wait_recv()

        def fs_copy(k, step):
            b, i = bufs(k)
            block = b[5].at[i, rows_of(z), :]
            return remote(block, block, f_send.at[k, step - 1], f_recv.at[k, z], along(step))

        def fr_wait(k, step):
            b, i = bufs(k)
            slot = lax.rem(z + step, 4)
            block = b[5].at[i, rows_of(slot), :]
            remote(
                block, block, f_send.at[k, step - 1], f_recv.at[k, slot], along(step)
            ).wait_recv()

        def final(k, yy):
            b, _ = bufs(k)
            if k < 4:
                return out_f.at[k * rows : (k + 1) * rows, lanes_of(b, yy)]
            if k == 8:
                return out_o.at[:, lanes_of(b, yy)]
            if k == pieces:
                return fin_s.at[shard, :, lanes_of(b, yy)]
            out, at = (out_i, (k - 4) * D) if k < 8 else (out_q, (k - 9) * D)
            return out.at[:, pl.ds(pl.multiple_of(at + yy * half, 128), half)]

        def o_copy(k):
            b, i = bufs(k)
            return remote(b[5].at[i], final(k, y), o_send.at[k], o_recv.at[k], beside)

        def o_wait(k):
            b, i = bufs(k)
            remote(b[5].at[i], final(k, 1 - y), o_send.at[k], o_recv.at[k], beside).wait_recv()

        def o_local(k):
            b, i = bufs(k)
            return pltpu.make_async_copy(b[5].at[i], final(k, y), o_own.at[k])

        def wide(value):
            return value.astype(jnp.float32)

        def stage_x(k):
            b, i = bufs(k)
            for xx in range(2):
                core_copy(k, xx).wait_recv()
                if not (isinstance(k, int) and k >= ready):
                    own_copy(k, xx).wait()
            b[0][i, 1 - x] = (wide(b[0][i, 1 - x]) + wide(b[1][i, 1 - x])).astype(jnp.bfloat16)
            x_copy(k).start()

        def stage_y(k):
            b, i = bufs(k)
            x_copy(k).wait_recv()
            total = wide(b[0][i, x]) + wide(b[1][i, x]) + wide(b[2][i])
            b[0][i, x] = total.astype(jnp.bfloat16)
            y_copy(k).start()

        def stage_z(k):
            b, i = bufs(k)
            y_copy(k).wait_recv()
            lanes = lanes_of(b, y)
            total = wide(b[0][i, x, :, lanes]) + wide(b[3][i])
            b[0][i, x, :, lanes] = total.astype(jnp.bfloat16)
            for step in (2, 1, 3):
                zs_copy(k, step).start()

        def stage_f(k):
            b, i = bufs(k)
            total = wide(b[0][i, x, rows_of(z), lanes_of(b, y)])
            for step in (1, 2, 3):
                zr_wait(k, step)
                total += wide(b[4][i, lax.rem(z + step, 4)])
            b[5][i, rows_of(z), :] = total.astype(jnp.bfloat16)
            for step in (2, 1, 3):
                fs_copy(k, step).start()

        def stage_o(k):
            for step in (1, 2, 3):
                fr_wait(k, step)
            for kk in range(pieces + 1) if not isinstance(k, int) else [k]:

                def begin(kk=kk):
                    o_copy(kk).start()
                    o_local(kk).start()

                if isinstance(k, int):
                    begin()
                else:
                    pl.when(k == kk)(begin)

        def send_core(k):
            for xx in range(2):
                core_copy(k, xx).start()

        for k in range(ready):
            send_core(k)
        for k in range(2):
            stage_x(k)

        kv = (dkp, dvp)

        def kv_rows(block):
            return pl.ds(pl.multiple_of(block * p_rows, p_rows), p_rows)

        def kv_lanes(g):
            return pl.ds(g * chunk if isinstance(g, int) else pl.multiple_of(g * chunk, chunk), chunk)

        def kv_core(t, g, xx):
            return remote(
                kv[t].at[kv_rows(2 * xx + 1 - core), kv_lanes(g)],
                kr.at[t, xx, :, kv_lanes(g)],
                kc_s.at[g, t, xx],
                kc_r.at[g, t, xx],
                partner,
            )

        def kv_across(t, g):
            return remote(
                kv[t].at[kv_rows(2 * (1 - x) + core), kv_lanes(g)],
                kx.at[t, :, kv_lanes(g)],
                kx_s.at[g, t],
                kx_r.at[g, t],
                across,
            )

        def serve_kv(g):
            block, lanes = kv_rows(2 * (1 - x) + core), kv_lanes(g)
            for t in range(2):
                for xx in range(2):
                    kv_core(t, g, xx).wait_recv()
                total = wide(kv[t][block, lanes]) + wide(kr[t, 1 - x, :, lanes])
                kv[t][block, lanes] = total.astype(jnp.bfloat16)
                kv_across(t, g).start()

        for i in range(7):
            fetch(i).wait()

        def pair(p, carry):
            def between(index):
                if index == 0:
                    pl.when(p + 2 < ready)(lambda: stage_x(p + 2))
                if index == 1:
                    pl.when((p == 2) | (p == 4))(lambda: serve_kv(p // 2 - 1))
                if index == 2:
                    pl.when(p >= 2)(lambda: stage_y(p - 2))
                if index == 3:
                    pl.when(p >= 3)(lambda: stage_z(p - 3))
                if index == 4:
                    pl.when(p >= 4)(lambda: stage_f(p - 4))
                if index == 5:
                    pl.when(p >= 5)(lambda: stage_o(p - 5))

            lanes = pl.ds(pl.multiple_of(p * PAIR, PAIR), PAIR)

            def cut(ref):
                return ref.at[:, lanes]

            attend_bwd_pair(
                shard, p_rows, cut(qv), cut(kpv), cut(vpv), cut(kcv), cut(vcv), cut(gav), cut(attv),
                ls.at[p], cut(dq), cut(dkp), cut(dvp), cut(dkc), cut(dvc), accum, between,
            )

            @pl.when(p % 2 == 1)
            def _():
                for t in range(2):
                    for xx in range(2):
                        kv_core(t, p // 2, xx).start()

            return carry

        lax.fori_loop(0, pairs, pair, 0)

        def keep_piece(k, product):
            for block in range(4):
                made[k - ready, block] = product[block * rows : (block + 1) * rows]
            for xx in range(2):
                own[k, xx] = made[k - ready, 2 * xx + core]
            send_core(k)

        def tick(n, carry):
            stage_y(n)
            stage_z(n - 1)
            stage_f(n - 2)
            stage_o(n - 3)
            return carry

        product = dot_first(xp[...], dq[:p_rows, :]) + dot_first(xc[...], dq[p_rows:, :])
        keep_piece(9, product.astype(jnp.bfloat16))
        serve_kv(chunks - 1)
        stage_x(8)
        for i in (7, 8):
            fetch(i).wait()
        g_tok[...] += dot_second(dq[...], wv[2])
        stage_x(9)
        tick(4, 0)
        g_tok[p_rows:, :] += dot_second(dkc[...], wv[0]) + dot_second(dvc[...], wv[1])
        lax.fori_loop(5, 8, tick, 0)

        for g in range(chunks):
            for t in range(2):
                kv_across(t, g).wait_recv()
        for t in range(2):
            total = wide(kv[t][kv_rows(shard), :]) + wide(kr[t, x]) + wide(kx[t])
            kvs[t] = total.astype(jnp.bfloat16)
        g_bias = jnp.sum(wide(dq[...]), 0, keepdims=True)
        v_bias = jnp.sum(wide(dvc[...]), 0, keepdims=True) + jnp.sum(wide(kvs[1]), 0, keepdims=True)
        head[...] = sm[:16, :]
        for part in range(across_lanes):
            lanes = slice(part * 128, (part + 1) * 128)
            head[part : part + 1, STU:] = g_bias[:, lanes]
            head[across_lanes + part : across_lanes + part + 1, STU:] = v_bias[:, lanes]
        for block in range(4):
            made_s[block] = sm[block * rows : (block + 1) * rows, :].astype(jnp.bfloat16)
        made_s[0, :16] = head[...].astype(jnp.bfloat16)
        for xx in range(2):
            own_s[0, xx] = made_s[2 * xx + core]
        send_core(pieces)
        for t in range(2):
            product = dot_first(xp[...], kvs[t]) + dot_first(xc[...], (dkc, dvc)[t][...])
            keep_piece(10 + t, product.astype(jnp.bfloat16))
        stage_x(pieces)
        stage_x(10)
        stage_x(11)
        g_tok[:p_rows, :] += dot_second(kvs[0], wv[0]) + dot_second(kvs[1], wv[1])
        stores = [
            pltpu.make_async_copy(g_tok.at[:p_rows, :], out_pg, out_sem.at[0]),
            pltpu.make_async_copy(g_tok.at[p_rows:, :], out_cg, out_sem.at[1]),
        ]
        for copy in stores:
            copy.start()

        lax.fori_loop(8, 10, tick, 0)
        stage_y(pieces)
        tick(10, 0)
        stage_z(pieces)
        tick(11, 0)
        stage_f(pieces)
        stage_z(11)
        stage_f(10)
        stage_o(9)
        stage_o(pieces)
        stage_f(11)
        stage_o(10)

        def g_copy(step):
            return remote(
                fin_s.at[shard],
                fin_s.at[shard],
                g_send.at[step - 1],
                g_recv.at[shard],
                (rep, lax.rem(shard + step, 4)),
            )

        o_wait(pieces)
        o_local(pieces).wait()
        for step in (1, 2, 3):
            g_copy(step).start()
        stage_o(11)
        for step in (1, 2, 3):
            slot = lax.rem(shard + step, 4)
            remote(
                fin_s.at[slot], fin_s.at[slot], g_send.at[step - 1], g_recv.at[slot], far
            ).wait_recv()

        for block in range(4):
            o_stu[block * rows : (block + 1) * rows, :] = wide(fin_s[block, :, :STU])

        def side(first, count):
            block, at = first // rows, first % rows
            return wide(fin_s[block, at : at + count, STU:])

        first_rows = side(0, rows)
        for i in range(8):
            target, at = (o_bias, i) if i < 6 else (o_gain, i - 6)
            for part in range(across_lanes):
                r = i * across_lanes + part
                target[at : at + 1, part * 128 : (part + 1) * 128] = first_rows[r : r + 1, :]
        for part in range(ff // 128):
            r = 8 * across_lanes + part
            o_in[:, part * 128 : (part + 1) * 128] = first_rows[r : r + 1, :]
        base = 8 * across_lanes + ff // 128
        o_vec[...] = first_rows[base : base + 3, :]
        o_cb[...] = first_rows[base + 3 : base + 4, :]
        all_side = jnp.concatenate([first_rows, side(rows, rows)], 0)
        o_pool[...] = all_side[base + 8 : base + 8 + STU, :]
        o_class[...] = all_side[base + 8 + STU : base + 8 + 2 * STU, :]

        for k in range(pieces):
            o_wait(k)
            o_local(k).wait()
        for copy in stores:
            copy.wait()

        def sent(k):
            for xx in range(2):
                core_copy(k, xx).wait_send()
            x_copy(k).wait_send()
            y_copy(k).wait_send()
            for step in (1, 2, 3):
                zs_copy(k, step).wait_send()
                fs_copy(k, step).wait_send()

        def sent_step(k, carry):
            sent(k)
            return carry

        lax.fori_loop(0, pieces, sent_step, 0)
        sent(pieces)
        for k in range(pieces + 1):
            o_copy(k).wait_send()
        for step in (1, 2, 3):
            g_copy(step).wait_send()
        for g in range(chunks):
            for t in range(2):
                for xx in range(2):
                    kv_core(t, g, xx).wait_send()
                kv_across(t, g).wait_send()

    def sems(*dims):
        return pltpu.SemaphoreType.DMA(dims)

    def low(*dims):
        return pltpu.VMEM(dims, jnp.bfloat16)

    def full(*dims):
        return pltpu.VMEM(dims, jnp.float32)

    def buffers(count, columns):
        cut = columns // 2
        return [
            low(count, 2, rows, columns),
            low(count, 2, rows, columns),
            low(count, rows, columns),
            low(count, rows, cut),
            low(count, 4, quarter, cut),
            low(count, rows, cut),
        ]

    def shaped(dims, kind=jnp.float32):
        return jax.ShapeDtypeStruct(dims, kind)

    n = pieces + 1
    anywhere = pl.BlockSpec(memory_space=pl.ANY)
    vmem = pl.BlockSpec(memory_space=pltpu.VMEM)
    return pl.pallas_call(
        kernel,
        in_specs=[anywhere] * 10 + [vmem] * 4,
        out_specs=[anywhere] * 6 + [vmem] * 8,
        out_shape=[
            shaped((p_rows, D)),
            shaped((cont_len, D)),
            shaped((rows, 3 * D), jnp.bfloat16),
            shaped((rows, D), jnp.bfloat16),
            shaped((rows, ff), jnp.bfloat16),
            shaped((4 * rows, D), jnp.bfloat16),
            shaped((6, D)),
            shaped((2, D)),
            shaped((1, ff)),
            shaped((D, STU)),
            shaped((3, STU)),
            shaped((STU, STU)),
            shaped((STU, STU)),
            shaped((1, STU)),
        ],
        scratch_shapes=[
            low(tokens, D), low(p_len, D), low(p_len, D), low(cont_len, D), low(cont_len, D),
            full(tokens, D), low(tokens, D), full(PAIR, tokens), low(tokens, D),
            low(p_len, D), low(p_len, D), low(cont_len, D), low(cont_len, D),
            low(2, 2, p_rows, D), low(2, p_rows, D), low(2, p_rows, D), low(3, D, D),
            full(tokens, D), low(3, 4, rows, D), full(16, s_width),
        ]
        + buffers(pieces, D)
        + [low(4, rows, s_width)]
        + buffers(1, s_width)
        + [low(4, rows, s_width)]
        + [
            sems(9), sems(n, 2), sems(n, 2), sems(n, 2), sems(n), sems(n), sems(n), sems(n),
            sems(n, 3), sems(n, 4), sems(n, 3), sems(n, 4), sems(n), sems(n), sems(n),
            sems(3), sems(4), sems(chunks, 2, 2), sems(chunks, 2, 2), sems(chunks, 2),
            sems(chunks, 2), sems(2),
        ],
        compiler_params=pltpu.CompilerParams(
            collective_id=2, has_side_effects=True, vmem_limit_bytes=VMEM_ALL
        ),
        name="finish",
    )(q, kp, vp, kc, vc, att, g_att, g9, g_resid, w_all, lse, small, prompt, conts)


def body(
    prompt,
    conts,
    prompt_cot,
    cont_cot,
    labels,
    w_qkv,
    w_out,
    w_in,
    w_ffo,
    layer_biases,
    norm_gains,
    bias_in,
    w_student,
    student_vectors,
    w_pool,
    w_class,
    bias_class,
):
    prompt_rows = prompt.shape[1]
    direct = (lax.axis_size("rep"), lax.axis_size("shard")) == (8, 4)
    project = project_and_attend if direct else project_native
    w_all, ffo_full, q, kp, vp, kc, vc, attended, log_totals = project(
        prompt[0], conts[0, 0], w_qkv, w_out, w_in, w_ffo, layer_biases
    )
    out_p, out_c, logits, g9, g_resid, g_att, small = middle(
        attended,
        prompt[0],
        conts[0, 0],
        prompt_cot[0],
        cont_cot[0, 0],
        labels,
        w_all,
        ffo_full,
        layer_biases,
        norm_gains,
        bias_in,
        w_student,
        student_vectors,
        w_pool,
        w_class,
        bias_class,
    )
    ff, classes = bias_in.shape[0], w_class.shape[1]
    if direct:
        outs = finish(
            q, kp, vp, kc, vc, attended, log_totals, g_att, g9, g_resid, small, w_all,
            prompt[0], conts[0, 0], ff, classes,
        )
        g_prompt, g_conts = outs[:2]
        owned = [part.astype(jnp.float32) for part in outs[2:6]]
        biases, gains_g, g_in, g_student, g_vectors, g_pool, g_class, g_cb = outs[6:]
    else:
        g_q, g_kp, g_vp, g_kc, g_vc = attend_backward(
            q, kp, vp, kc, vc, g_att, attended, log_totals, prompt_rows
        )
        tokens = jnp.concatenate([prompt[0], conts[0, 0]], 0)
        kv_sum = [
            lax.psum_scatter(part, "shard", scatter_dimension=0, tiled=True)
            for part in (g_kp, g_vp)
        ]
        g_k = jnp.concatenate([kv_sum[0], g_kc], 0)
        g_v = jnp.concatenate([kv_sum[1], g_vc], 0)
        g_tokens = g_resid
        for part, weight in ((g_k, w_all[0]), (g_v, w_all[1]), (g_q, w_all[2])):
            g_tokens = g_tokens + dot_second(part, weight)
        g_prompt, g_conts = g_tokens[:prompt_rows], g_tokens[prompt_rows:]
        g_qkvw = jnp.concatenate([dot_first(tokens, part) for part in (g_q, g_k, g_v)], 1)
        side = small[:, STU:]
        across = D // 128
        for at, part in ((0, g_q), (1, g_v)):
            total = jnp.sum(part.astype(jnp.float32), 0).reshape(across, 128)
            side = lax.dynamic_update_slice(side, total, (at * across, 0))
        small = jnp.concatenate([small[:, :STU], side], 1)
        owned, summed = sum_native(g9, g_qkvw, small)
        side = summed[:, STU:]
        base = 8 * across + ff // 128
        biases = side[: 6 * across].reshape(6, D)
        gains_g = side[6 * across : 8 * across].reshape(2, D)
        g_in = side[8 * across : base]
        g_student, g_vectors = summed[:, :STU], side[base : base + 3]
        g_pool = side[base + 8 : base + 8 + STU]
        g_class = side[base + 8 + STU : base + 8 + 2 * STU]
        g_cb = side[base + 3 : base + 4]
    return (
        out_p[None],
        out_c[None, None],
        logits[None, :, :classes],
        g_prompt[None],
        g_conts[None, None],
        *owned,
        biases,
        gains_g,
        g_in.reshape(ff),
        g_student,
        g_vectors,
        g_pool,
        g_class[:, :classes],
        g_cb[0, :classes],
    )


def solution(mesh):
    return jax.shard_map(
        body,
        mesh=mesh,
        in_specs=(
            P("rep", "shard", None),
            P("rep", "shard", None, None),
            P("rep", "shard", None),
            P("rep", "shard", None, None),
            P("rep", "shard"),
            P("shard", None),
            P("shard", None),
            P("shard", None),
            P("shard", None),
            P(),
            P(),
            P(),
            P(),
            P(),
            P(),
            P(),
            P(),
        ),
        out_specs=(
            P("rep", "shard", None),
            P("rep", "shard", None, None),
            P("rep", "shard", None),
            P("rep", "shard", None),
            P("rep", "shard", None, None),
            P("shard", None),
            P("shard", None),
            P("shard", None),
            P("shard", None),
            P(),
            P(),
            P(),
            P(),
            P(),
            P(),
            P(),
            P(),
        ),
        check_vma=False,
    )
```

```python
import jax
import jax.numpy as jnp
from jax import lax
from jax.experimental import pallas as pl
from jax.experimental.pallas import tpu as pltpu
from jax.sharding import PartitionSpec as P

D = 768
HEADS = 12
DH = 64
STU = 128
SHEADS = 2


HIGHEST = lax.Precision.HIGHEST
NEG_BIG = -1e30


def dot_plain(left, right):
    return jnp.dot(left, right, preferred_element_type=jnp.float32)


def dot_first(left, right):
    return lax.dot_general(
        left, right, (((0,), (0,)), ((), ())), preferred_element_type=jnp.float32
    )


def dot_second(left, right):
    return lax.dot_general(
        left, right, (((1,), (1,)), ((), ())), preferred_element_type=jnp.float32
    )


TILE = 256
PAIR = 128
VMEM_ALL = 62 * 1024 * 1024


def rows_dot(left, right):
    return lax.dot_general(
        left, right, (((1,), (1,)), ((), ())), preferred_element_type=jnp.float32
    )


def low_lanes(shape):
    return lax.broadcasted_iota(jnp.int32, shape, len(shape) - 1) < DH


def attend_fwd_pair(
    shard, prompt_rows, q, kp, vp, kc, vc, att_ref, lse_ref, between=None
):
    cont_len = kc.shape[0]
    prompt_len = kp.shape[0]
    for start in range(0, prompt_rows + cont_len, TILE):
        q_t = q[start : start + TILE, :] * jnp.asarray(DH ** (-0.5), jnp.bfloat16)
        halves = []
        for parity in range(2):
            keep = low_lanes(q_t.shape) == (parity == 0)
            q_h = jnp.where(keep, q_t, jnp.zeros_like(q_t))
            s_p = rows_dot(q_h, kp[...])
            if start < prompt_rows:
                key = lax.broadcasted_iota(jnp.int32, s_p.shape, 1)
                row = lax.broadcasted_iota(jnp.int32, s_p.shape, 0)
                s_p = jnp.where(key <= row + (shard * prompt_rows + start), s_p, NEG_BIG)
                largest = jnp.max(s_p, 1, keepdims=True)
                p_p = jnp.exp(s_p - largest)
                total = jnp.sum(p_p, 1, keepdims=True)
                o = dot_plain(p_p.astype(jnp.bfloat16), vp[...])
            else:
                seen = start - prompt_rows + TILE
                s_c = rows_dot(q_h, kc[:seen, :])
                key = lax.broadcasted_iota(jnp.int32, s_c.shape, 1)
                row = lax.broadcasted_iota(jnp.int32, s_c.shape, 0)
                s_c = jnp.where(key <= row + (start - prompt_rows), s_c, NEG_BIG)
                largest = jnp.maximum(
                    jnp.max(s_p, 1, keepdims=True), jnp.max(s_c, 1, keepdims=True)
                )
                p_p = jnp.exp(s_p - largest)
                p_c = jnp.exp(s_c - largest)
                total = jnp.sum(p_p, 1, keepdims=True) + jnp.sum(p_c, 1, keepdims=True)
                o = dot_plain(p_p.astype(jnp.bfloat16), vp[...]) + dot_plain(
                    p_c.astype(jnp.bfloat16), vc[:seen, :]
                )
            halves.append((o / total, largest + jnp.log(total)))
        keep = low_lanes((TILE, PAIR))
        att_ref[start : start + TILE, :] = jnp.where(keep, halves[0][0], halves[1][0])
        lse = jnp.where(
            keep,
            jnp.broadcast_to(halves[0][1], (TILE, PAIR)),
            jnp.broadcast_to(halves[1][1], (TILE, PAIR)),
        )
        turned = jnp.transpose(lse)
        lse_ref[0:1, start : start + TILE] = turned[0:1, :]
        lse_ref[1:2, start : start + TILE] = turned[DH : DH + 1, :]
        if between is not None:
            between(start // TILE)


def attend_bwd_pair(
    shard, prompt_rows, q, kp, vp, kc, vc, g, att, lse, dq, dkp, dvp, dkc, dvc, accum, between=None
):
    cont_len = kc.shape[0]
    tokens = prompt_rows + cont_len
    prompt_len = kp.shape[0]
    g_t = g[...]
    turned = jnp.transpose(g_t.astype(jnp.float32) * att[...])
    delta = (
        jnp.sum(turned[:DH], 0, keepdims=True),
        jnp.sum(turned[DH:], 0, keepdims=True),
    )
    q_t = q[...] * jnp.asarray(DH ** (-0.5), jnp.bfloat16)
    keep = low_lanes(q_t.shape)
    zero = jnp.zeros_like(q_t)
    q_h = (jnp.where(keep, q_t, zero), jnp.where(keep, zero, q_t))
    g_h = (jnp.where(keep, g_t, zero), jnp.where(keep, zero, g_t))
    accum[...] = jnp.zeros_like(accum)

    def block(key_b, value_b, first, mask):
        key_t = jnp.transpose(key_b.astype(jnp.float32)).astype(jnp.bfloat16)
        g_key = jnp.zeros((TILE, PAIR), jnp.float32)
        g_value = jnp.zeros((TILE, PAIR), jnp.float32)
        for parity in range(2):
            scores = rows_dot(key_b, q_h[parity][first:])
            probs = jnp.exp(scores - lse[parity : parity + 1, first:])
            masked = jnp.where(mask, probs[:, :TILE], 0.0)
            if tokens - first > TILE:
                probs = jnp.concatenate([masked, probs[:, TILE:]], 1)
            else:
                probs = masked
            g_probs = rows_dot(value_b, g_h[parity][first:])
            g_scores = (probs * (g_probs - delta[parity][:, first:])).astype(jnp.bfloat16)
            g_value += dot_plain(probs.astype(jnp.bfloat16), g_h[parity][first:])
            g_key += dot_plain(g_scores, q_h[parity][first:])
            rows = slice(parity * DH, (parity + 1) * DH)
            accum[rows, first:] += dot_plain(key_t[rows], g_scores)
        return g_key.astype(jnp.bfloat16), g_value.astype(jnp.bfloat16)

    ahead = lax.broadcasted_iota(jnp.int32, (TILE, TILE), 0) - lax.broadcasted_iota(
        jnp.int32, (TILE, TILE), 1
    )

    def prompt_block(index, start):
        rows = pl.ds(start, TILE)
        mask = ahead <= shard * prompt_rows - index * TILE
        g_key, g_value = block(kp[rows, :], vp[rows, :], 0, mask)
        dkp[rows, :] = g_key
        dvp[rows, :] = g_value

    blocks = prompt_len // TILE
    if blocks <= 4:
        for index in range(blocks):
            prompt_block(index, index * TILE)
            if between is not None:
                between(index)
    else:

        def step(index, carry):
            prompt_block(index, pl.multiple_of(index * TILE, TILE))
            return carry

        lax.fori_loop(0, blocks, step, 0)
    for start in range(0, cont_len, TILE):
        rows = slice(start, start + TILE)
        g_key, g_value = block(kc[rows, :], vc[rows, :], prompt_rows + start, ahead <= 0)
        dkc[rows, :] = g_key
        dvc[rows, :] = g_value
        if between is not None:
            between(blocks + start // TILE)
    dq[...] = (jnp.transpose(accum[...]) * DH ** (-0.5)).astype(jnp.bfloat16)


def attend_forward(q, kp, vp, kc, vc, prompt_rows):
    tokens, prompt_len, cont_len = q.shape[0], kp.shape[0], kc.shape[0]
    pairs = HEADS // 2

    def kernel(q, kp, vp, kc, vc, att_ref, lse_ref):
        attend_fwd_pair(
            lax.axis_index("shard"), prompt_rows, q, kp, vp, kc, vc, att_ref, lse_ref.at[0]
        )

    def columns(rows):
        return pl.BlockSpec((rows, PAIR), lambda p: (0, p))

    return pl.pallas_call(
        kernel,
        grid=(pairs,),
        in_specs=[columns(rows) for rows in (tokens, prompt_len, prompt_len, cont_len, cont_len)],
        out_specs=[columns(tokens), pl.BlockSpec((1, 8, tokens), lambda p: (p, 0, 0))],
        out_shape=[
            jax.ShapeDtypeStruct((tokens, D), jnp.float32),
            jax.ShapeDtypeStruct((pairs, 8, tokens), jnp.float32),
        ],
        compiler_params=pltpu.CompilerParams(vmem_limit_bytes=VMEM_ALL),
        name="attend_forward",
    )(q, kp, vp, kc, vc)


def attend_backward(q, kp, vp, kc, vc, g_att, att, lse, prompt_rows):
    tokens, prompt_len, cont_len = q.shape[0], kp.shape[0], kc.shape[0]
    pairs = HEADS // 2

    def kernel(q, kp, vp, kc, vc, g, a, ls, dq, dkp, dvp, dkc, dvc, accum):
        attend_bwd_pair(
            lax.axis_index("shard"),
            prompt_rows,
            q,
            kp,
            vp,
            kc,
            vc,
            g,
            a,
            ls.at[0],
            dq,
            dkp,
            dvp,
            dkc,
            dvc,
            accum,
        )

    def columns(rows):
        return pl.BlockSpec((rows, PAIR), lambda p: (0, p))

    sizes = (tokens, prompt_len, prompt_len, cont_len, cont_len)
    return pl.pallas_call(
        kernel,
        grid=(pairs,),
        in_specs=[columns(rows) for rows in sizes + (tokens, tokens)]
        + [pl.BlockSpec((1, 8, tokens), lambda p: (p, 0, 0))],
        out_specs=[columns(rows) for rows in sizes],
        out_shape=[jax.ShapeDtypeStruct((rows, D), jnp.bfloat16) for rows in sizes],
        scratch_shapes=[pltpu.VMEM((PAIR, tokens), jnp.float32)],
        compiler_params=pltpu.CompilerParams(vmem_limit_bytes=VMEM_ALL),
        name="attend_backward",
    )(q, kp, vp, kc, vc, g_att, att, lse)


MESH_ID = pl.DeviceIdType.MESH


def project_and_attend(prompt, conts, w_qkv, w_out, w_in, w_ffo, layer_biases):
    pieces, early = 11, 4
    by_z = (4, 5, 6, 7, 8, 9)
    rows = w_qkv.shape[0]
    p_rows, cont_len = prompt.shape[0], conts.shape[0]
    tokens = p_rows + cont_len
    p_len = 4 * p_rows
    pairs = HEADS // 2
    tiles = tokens // TILE
    chunk = 2 * PAIR
    chunks = D // chunk
    quarter = rows // 4

    def kernel(
        xp, xc, wq, wo, wi, wf, bias, w_all_out, wf_out, q_out, kc_out, vc_out, kp_out, vp_out, att_out, lse,
        stage, w_all, q, kc, vc, kp, vp, att,
        load, c_s, c_r, x_s, x_r, y_s, y_r, z_s, z_r, d_s, d_r, e_s, e_r, w_sem,
        kc_s, kc_r, kx_s, kx_r, kd_s, kd_r, out_sem,
    ):
        rep, shard = lax.axis_index("rep"), lax.axis_index("shard")
        z, y = rep // 2, rep % 2
        x, core = shard // 2, shard % 2
        partner = (rep, 2 * x + 1 - core)
        across = (rep, 2 * (1 - x) + core)
        beside = (2 * z + 1 - y, shard)
        z_low = z % 2
        above = (2 * (z + 1 - 2 * z_low) + y, shard)
        there = 2 * (1 - x) + core

        def remote(ref, send, recv, device):
            return pltpu.make_async_remote_copy(
                src_ref=ref,
                dst_ref=ref,
                send_sem=send,
                recv_sem=recv,
                device_id=device,
                device_id_type=MESH_ID,
            )

        def source(k):
            if k < 3:
                j = (1, 2, 0)[k]
                return wq.at[:, j * D : (j + 1) * D]
            if k < 4:
                return wo
            if k < 8:
                return wi.at[:, (k - 4) * D : (k - 3) * D]
            return wf.at[(k - 8) * rows : (k - 7) * rows, :]

        def loading(k):
            return pltpu.make_async_copy(source(k), stage.at[k], load.at[k])

        for k in range(pieces):
            loading(k).start()
        barrier = pltpu.get_barrier_semaphore()
        for other in (partner, across, beside, above):
            pl.semaphore_signal(barrier, inc=1, device_id=other, device_id_type=MESH_ID)
        pl.semaphore_wait(barrier, 4)

        def part(k, block, first, count):
            start = pl.multiple_of(first * quarter, 16)
            return w_all.at[k, block, pl.ds(start, count * quarter), :]

        def core_copy(k):
            return remote(w_all.at[k, shard], c_s.at[k], c_r.at[k], partner)

        def core_arrival(k):
            return remote(w_all.at[k, 2 * x + 1 - core], c_s.at[k], c_r.at[k], partner)

        def crossing(k, y_at):
            return (2 * z_low + y_at, 1) if k in by_z else (2 * y_at, 2)

        def x_copy(k):
            return remote(part(k, shard, *crossing(k, y)), x_s.at[k], x_r.at[k], across)

        def x_arrival(k):
            return remote(part(k, there, *crossing(k, y)), x_s.at[k], x_r.at[k], across)

        def y_copy(k):
            return remote(part(k, there, *crossing(k, y)), y_s.at[k], y_r.at[k], beside)

        def y_arrival(k):
            return remote(part(k, there, *crossing(k, 1 - y)), y_s.at[k], y_r.at[k], beside)

        def z_copy(k):
            return remote(part(k, there, 2 * z_low, 2), z_s.at[k], z_r.at[k], above)

        def z_arrival(k):
            return remote(part(k, there, 2 * (1 - z_low), 2), z_s.at[k], z_r.at[k], above)

        def halves(k):
            first = 2 * z_low if k in by_z else 2 * y
            return first, 2 - first

        def d_copy(k, block=None):
            block = there if block is None else block
            return remote(part(k, block, halves(k)[0], 2), d_s.at[k], d_r.at[k], partner)

        def e_copy(k, block=None):
            block = there if block is None else block
            return remote(part(k, block, halves(k)[1], 2), e_s.at[k], e_r.at[k], partner)

        far = 2 * (1 - x) + 1 - core

        def send_piece(k):
            x_copy(k).start()
            core_copy(k).start()

        def round_piece(k):
            loading(k).wait()
            w_all[k, shard] = stage[k].astype(jnp.bfloat16)

        def serve_x(k):
            x_arrival(k).wait_recv()
            y_copy(k).start()
            if k not in by_z:
                d_copy(k).start()

        def serve_y(k):
            y_arrival(k).wait_recv()
            if k in by_z:
                z_copy(k).start()
                d_copy(k).start()
            else:
                e_copy(k).start()

        def serve_z(k):
            z_arrival(k).wait_recv()
            e_copy(k).start()

        def w_store(k):
            if k < 8:
                return pltpu.make_async_copy(w_all.at[k], w_all_out.at[k], w_sem.at[k])
            return pltpu.make_async_copy(w_all.at[k], wf_out.at[:, k - 8], w_sem.at[k])

        def complete(k):
            core_arrival(k).wait_recv()
            d_copy(k, far).wait_recv()
            e_copy(k, far).wait_recv()
            w_store(k).start()

        def weight(k):
            return w_all[k].reshape(4 * rows, D)

        for k in range(early):
            round_piece(k)
            send_piece(k)
        for k in range(early, pieces):
            round_piece(k)
        own_rows = pl.ds(pl.multiple_of(shard * p_rows, p_rows), p_rows)
        kv = (kp, vp)

        def kv_part(t, g, block):
            lanes = pl.ds(g * chunk if isinstance(g, int) else pl.multiple_of(g * chunk, chunk), chunk)
            return kv[t].at[pl.ds(pl.multiple_of(block * p_rows, p_rows), p_rows), lanes]

        def kv_core(t, g):
            return remote(kv_part(t, g, shard), kc_s.at[g, t], kc_r.at[g, t], partner)

        def kv_across(t, g):
            return remote(kv_part(t, g, shard), kx_s.at[g, t], kx_r.at[g, t], across)

        def kv_forward(t, g):
            return remote(kv_part(t, g, there), kd_s.at[g, t], kd_r.at[g, t], partner)

        serve_x(0)
        serve_x(1)
        serve_y(0)
        complete(0)
        kp[own_rows, :] = dot_plain(xp[...], weight(0)).astype(jnp.bfloat16)
        kc[...] = dot_plain(xc[...], weight(0)).astype(jnp.bfloat16)
        serve_x(2)
        serve_y(1)
        complete(1)
        vp[own_rows, :] = (dot_plain(xp[...], weight(1)) + bias[1:2, :]).astype(jnp.bfloat16)
        waiting = list(range(early, pieces))
        for g in range(chunks):
            for t in range(2):
                kv_across(t, g).start()
                kv_core(t, g).start()
            for k in waiting[: 2 if g < chunks - 1 else pieces]:
                send_piece(k)
            waiting = waiting[2:]
        vc[...] = (dot_plain(xc[...], weight(1)) + bias[1:2, :]).astype(jnp.bfloat16)
        serve_y(2)
        serve_x(3)
        complete(2)
        q[:p_rows, :] = (dot_plain(xp[...], weight(2)) + bias[0:1, :]).astype(jnp.bfloat16)
        q[p_rows:, :] = (dot_plain(xc[...], weight(2)) + bias[0:1, :]).astype(jnp.bfloat16)

        def keep(ref, target, i):
            return pltpu.make_async_copy(ref, target, out_sem.at[i])

        kept = [(q, q_out, 0), (kc, kc_out, 1), (vc, vc_out, 2)]
        for item in kept:
            keep(*item).start()

        def serve_kv(g):
            for t in range(2):
                remote(kv_part(t, g, there), kx_s.at[g, t], kx_r.at[g, t], across).wait_recv()
                kv_forward(t, g).start()

        def complete_kv(g):
            for t in range(2):
                remote(
                    kv_part(t, g, 2 * x + 1 - core), kc_s.at[g, t], kc_r.at[g, t], partner
                ).wait_recv()
                remote(kv_part(t, g, far), kd_s.at[g, t], kd_r.at[g, t], partner).wait_recv()

        serve_kv(0)
        arrive = {4: 26.3, 5: 27.9, 6: 35.2, 7: 36.8, 8: 44.1, 9: 45.7, 10: 48.9}
        work = [(33.6, serve_kv, 1), (42.4, serve_kv, 2), (27.0, serve_y, 3), (30.0, complete, 3)]
        for k in range(4, pieces):
            at = arrive[k]
            work.append((at, serve_x, k))
            if k in by_z:
                work += [(at + 4, serve_y, k), (at + 10, serve_z, k), (at + 13, complete, k)]
            else:
                work += [(at + 6, serve_y, k), (at + 9, complete, k)]
        slots = pairs * tiles
        work = [(max(0, round((at - 26) / 1.37 - 0.6)), act, k) for at, act, k in work]
        work.sort(key=lambda item: item[0])

        def att_store(p):
            lanes = pl.ds(pl.multiple_of(p * PAIR, PAIR), PAIR)
            return pltpu.make_async_copy(att.at[:, lanes], att_out.at[:, lanes], out_sem.at[5 + p])

        def pair(p, carry):
            @pl.when(p % 2 == 0)
            def _():
                complete_kv(p // 2)

            def between(tile):
                for slot, action, k in work:
                    if slot < slots and slot % tiles == tile:

                        @pl.when(p == slot // tiles)
                        def _(action=action, k=k):
                            action(k)

            lanes = pl.ds(pl.multiple_of(p * PAIR, PAIR), PAIR)
            attend_fwd_pair(
                shard,
                p_rows,
                q.at[:, lanes],
                kp.at[:, lanes],
                vp.at[:, lanes],
                kc.at[:, lanes],
                vc.at[:, lanes],
                att.at[:, lanes],
                lse.at[p],
                between,
            )
            att_store(p).start()
            return carry

        lax.fori_loop(0, pairs, pair, 0)
        kept += [(kp, kp_out, 3), (vp, vp_out, 4)]
        for item in kept[3:]:
            keep(*item).start()
        for slot, action, k in work:
            if slot >= slots:
                action(k)
        for item in kept:
            keep(*item).wait()

        def last_pair(p, carry):
            att_store(p).wait()
            return carry

        lax.fori_loop(0, pairs, last_pair, 0)
        for k in range(pieces):
            w_store(k).wait()
            for copy in (core_copy, x_copy, y_copy, d_copy, e_copy):
                copy(k).wait_send()
            if k in by_z:
                z_copy(k).wait_send()
        for g in range(chunks):
            for t in range(2):
                for copy in (kv_core, kv_across, kv_forward):
                    copy(t, g).wait_send()

    def sems(*dims):
        return pltpu.SemaphoreType.DMA(dims)

    def low(*dims):
        return jax.ShapeDtypeStruct(dims, jnp.bfloat16)

    anywhere = pl.BlockSpec(memory_space=pl.ANY)
    vmem = pl.BlockSpec(memory_space=pltpu.VMEM)
    n = pieces
    out = pl.pallas_call(
        kernel,
        in_specs=[vmem, vmem, anywhere, anywhere, anywhere, anywhere, vmem],
        out_specs=[anywhere] * 8 + [vmem],
        out_shape=[
            low(8, 4, rows, D),
            low(4, 3, rows, D),
            low(tokens, D),
            low(cont_len, D),
            low(cont_len, D),
            low(p_len, D),
            low(p_len, D),
            jax.ShapeDtypeStruct((tokens, D), jnp.float32),
            jax.ShapeDtypeStruct((pairs, 8, tokens), jnp.float32),
        ],
        scratch_shapes=[
            pltpu.VMEM((n, rows, D), jnp.float32),
            pltpu.VMEM((n, 4, rows, D), jnp.bfloat16),
            pltpu.VMEM((tokens, D), jnp.bfloat16),
            pltpu.VMEM((cont_len, D), jnp.bfloat16),
            pltpu.VMEM((cont_len, D), jnp.bfloat16),
            pltpu.VMEM((p_len, D), jnp.bfloat16),
            pltpu.VMEM((p_len, D), jnp.bfloat16),
            pltpu.VMEM((tokens, D), jnp.float32),
        ]
        + [sems(n)] * 14
        + [sems(chunks, 2)] * 6
        + [sems(5 + pairs)],
        compiler_params=pltpu.CompilerParams(
            collective_id=1, has_side_effects=True, vmem_limit_bytes=VMEM_ALL
        ),
        name="project_and_attend",
    )(prompt, conts, w_qkv, w_out, w_in, w_ffo, layer_biases)
    w_all, wf, q, kc, vc, kp, vp, att, lse = out
    w_all = w_all.reshape(8, 4 * rows, D)
    return w_all, wf.reshape(4, 3 * rows, D), q, kp, vp, kc, vc, att, lse


def project_native(prompt, conts, w_qkv, w_out, w_in, w_ffo, layer_biases):
    rows = prompt.shape[0]

    def gathered(value):
        return lax.all_gather(value.astype(jnp.bfloat16), "shard", axis=0, tiled=True)

    qkv, out, inner, ffo = (gathered(w) for w in (w_qkv, w_out, w_in, w_ffo))
    tokens = jnp.concatenate([prompt, conts], 0)
    bias = jnp.concatenate([layer_biases[0], jnp.zeros((D,), jnp.float32), layer_biases[1]])
    qkv_b = (dot_plain(tokens, qkv) + bias).astype(jnp.bfloat16)
    q, keys, values = (qkv_b[:, i * D : (i + 1) * D] for i in range(3))
    kp, vp = gathered(keys[:rows]), gathered(values[:rows])
    kc, vc = keys[rows:], values[rows:]
    att, lse = attend_forward(q, kp, vp, kc, vc, rows)
    blocks = [qkv[:, D : 2 * D], qkv[:, 2 * D :], qkv[:, :D], out]
    blocks += [inner[:, i * D : (i + 1) * D] for i in range(inner.shape[1] // D)]
    return jnp.stack(blocks), ffo, q, kp, vp, kc, vc, att, lse


def student_head(label, stu, vectors, w_pool, w_class, bias_class, classes):
    part_w = STU // SHEADS
    low_half = lax.broadcasted_iota(jnp.int32, stu.shape, 1) < part_w
    row_low = lax.broadcasted_iota(jnp.int32, (1, STU), 1) < part_w
    query, bias_pool = vectors[1:2, :], vectors[2:3, :]

    def by_head(values):
        low_sum = jnp.sum(jnp.where(low_half[: values.shape[0]], values, 0.0), 1, keepdims=True)
        high_sum = jnp.sum(jnp.where(low_half[: values.shape[0]], 0.0, values), 1, keepdims=True)
        return jnp.where(low_half[: values.shape[0]], low_sum, high_sum)

    scores = by_head(stu * query) * part_w ** (-0.5)
    largest = jnp.max(scores, 0, keepdims=True)
    expo = jnp.exp(scores - largest)
    weights = expo / jnp.sum(expo, 0, keepdims=True)
    pooled = jnp.sum(weights * stu, 0, keepdims=True)

    square = (STU, STU)
    on_diagonal = lax.broadcasted_iota(jnp.int32, square, 0) == lax.broadcasted_iota(
        jnp.int32, square, 1
    )

    def column(row):
        return jnp.sum(jnp.where(on_diagonal, row, 0.0), 1, keepdims=True)

    def times(row, matrix):
        return jnp.sum(column(row) * matrix, 0, keepdims=True)

    def times_turned(row, matrix):
        total = jnp.sum(matrix * row, 1, keepdims=True)
        return jnp.sum(jnp.where(on_diagonal, total, 0.0), 0, keepdims=True)

    top = jnp.tanh(times(pooled, w_pool) + bias_pool)
    lane = lax.broadcasted_iota(jnp.int32, (1, STU), 1)
    logits = times(top, w_class) + bias_class
    seen = jnp.where(lane < classes, logits, NEG_BIG)
    expo_l = jnp.exp(seen - jnp.max(seen, 1, keepdims=True))
    g_logits = expo_l / jnp.sum(expo_l, 1, keepdims=True) - jnp.where(lane == label, 1.0, 0.0)
    g_class = column(top) * g_logits
    g_pre = times_turned(g_logits, w_class) * (1.0 - top * top)
    g_pool = column(pooled) * g_pre
    g_pooled = times_turned(g_pre, w_pool)
    g_weights = by_head(stu * g_pooled)
    mean = jnp.sum(weights * g_weights, 0, keepdims=True)
    g_scores = weights * (g_weights - mean) * part_w ** (-0.5)
    g_stu = weights * g_pooled + g_scores * query
    g_query = jnp.sum(g_scores * stu, 0, keepdims=True)
    return logits, g_stu, g_query, g_pre, g_pool, g_class, g_logits


def middle(
    ahead, att, prompt, conts, prompt_cot, cont_cot, labels, w_all, wf, wf_rows,
    biases, gains, bias_in, student, vectors, w_pool, w_class, bias_class,
):
    p_rows, cont_len = prompt.shape[0], conts.shape[0]
    tokens = p_rows + cont_len
    ff = bias_in.shape[0]
    blocks = ff // D
    steps = tokens // TILE
    wide = D // TILE
    classes = w_class.shape[1]
    w_class_p = jnp.pad(w_class, ((0, 0), (0, STU - classes)))
    bias_class_p = jnp.pad(bias_class[None], ((0, 0), (0, STU - classes)))
    g_names = 2 * blocks + 1

    def kernel(
        label_ref, att_h, xp, xc, cp, cc, w_h, wf_h, wf_own, bias, gain, b_in, w_stu, vec, w_p, w_c, b_c,
        out_p, out_c, logits_out, grads_h, g_r1_h, g_att_h, small, totals_h,
        x_v, cot_v, out_v, att_v, att_b, w_v, wf_v, norm1, norm2, rstd1, rstd2, x1_b, act, slope, g_res, g_ffn, g_br, g_stu_b, grads,
        sums, in_sum, load, store, *links,
    ):
        def fetch(source, target, i):
            return pltpu.make_async_copy(source, target, load.at[i])

        loads = [
            fetch(att_h, att_v, 0),
            fetch(w_h.at[3], w_v.at[0], 1),
            fetch(w_h.at[pl.ds(4, blocks)], w_v.at[pl.ds(1, blocks)], 2),
            fetch(wf_h, wf_v.at[:, : wf_h.shape[1]], 3),
            fetch(xp, x_v.at[:p_rows], 4),
            fetch(xc, x_v.at[p_rows:], 5),
            fetch(cp, cot_v.at[:p_rows], 6),
            fetch(cc, cot_v.at[p_rows:], 7),
        ]
        for copy in loads:
            copy.start()
        rows = D // blocks
        if ahead:
            (stage, cr, xr, w_s, w_r, c_s, c_r, x_s, x_r) = links
            own_rows = fetch(wf_own.at[pl.ds(D - rows, rows), :], stage, 8)
            own_rows.start()
            rep, shard = lax.axis_index("rep"), lax.axis_index("shard")
            z, y = rep // 2, rep % 2
            x, core = shard // 2, shard % 2
            partner = (rep, 2 * x + 1 - core)
            across = (rep, 2 * (1 - x) + core)
            beside = (2 * z + 1 - y, shard)
            there, far = 2 * (1 - x) + core, 2 * (1 - x) + 1 - core
            barrier = pltpu.get_barrier_semaphore()
            for other in (partner, across, beside):
                pl.semaphore_signal(barrier, inc=1, device_id=other, device_id_type=MESH_ID)
            pl.semaphore_wait(barrier, 3)

            def remote(source, target, send, recv, device):
                return pltpu.make_async_remote_copy(
                    src_ref=source,
                    dst_ref=target,
                    send_sem=send,
                    recv_sem=recv,
                    device_id=device,
                    device_id_type=MESH_ID,
                )

            def moved(i, block, which, device):
                first = D - rows
                at = pl.ds(first, rows)
                if which is not None:
                    half = rows // 2
                    at = pl.ds(pl.multiple_of(first + which * half, 16), half)
                ref = wf_v.at[block, at, :]
                return remote(ref, ref, w_s.at[i], w_r.at[i], device)

            def core_copy(k, xx):
                block = pl.ds(pl.multiple_of((2 * xx + 1 - core) * rows, 16), rows)
                return remote(
                    grads.at[k, block, :], cr.at[k, xx], c_s.at[k, xx], c_r.at[k, xx], partner
                )

            def mine(xx):
                return pl.ds(pl.multiple_of((2 * xx + core) * rows, 16), rows)

            def x_copy(k):
                return remote(grads.at[k, mine(1 - x), :], xr.at[k], x_s.at[k], x_r.at[k], across)

            own_rows.wait()
            wf_v[shard, D - rows :, :] = stage[...].astype(jnp.bfloat16)
            moved(1, shard, y, across).start()
            moved(0, shard, None, partner).start()

        def serve_across():
            moved(1, there, y, across).wait_recv()
            moved(2, there, y, beside).start()
            moved(3, there, y, partner).start()

        def serve_beside():
            moved(2, there, 1 - y, beside).wait_recv()
            moved(4, there, 1 - y, partner).start()

        def gathered():
            moved(0, 2 * x + 1 - core, None, partner).wait_recv()
            moved(3, far, y, partner).wait_recv()
            moved(4, far, 1 - y, partner).wait_recv()

        def stage_x():
            for k in range(ahead):
                for xx in range(2):
                    core_copy(k, xx).wait_recv()
                block = mine(1 - x)
                total = grads[k, block, :].astype(jnp.float32) + cr[k, 1 - x].astype(jnp.float32)
                grads[k, block, :] = total.astype(jnp.bfloat16)
                x_copy(k).start()

        sums[...] = jnp.zeros_like(sums)
        small[...] = jnp.zeros_like(small)

        def row(i):
            return pl.ds(pl.multiple_of(i * TILE, TILE), TILE)

        def loop(count):
            def run(step):
                def body(i, carry):
                    step(i)
                    return carry

                lax.fori_loop(0, count, body, 0)

            return run

        def normalize(values):
            center = values - jnp.mean(values, -1, keepdims=True)
            spread = jnp.mean(center * center, -1, keepdims=True)
            scale = lax.rsqrt(spread + 1e-05)
            return center * scale, scale

        def norm_back(g, gain_row, hat, scale):
            gg = g * gain_row
            return scale * (
                gg
                - jnp.mean(gg, -1, keepdims=True)
                - hat * jnp.mean(gg * hat, -1, keepdims=True)
            )

        def add_sum(i, values):
            sums[i : i + 1, :] += jnp.sum(values, 0, keepdims=True)

        for i in (0, 1, 4, 5):
            loads[i].wait()

        @loop(steps)
        def _(i):
            part = att_v[row(i), :].astype(jnp.bfloat16)
            att_b[row(i), :] = part
            branch = dot_plain(part, w_v[0]) + bias[2:3, :]
            hat, scale = normalize(x_v[row(i), :].astype(jnp.float32) + branch)
            norm1[row(i), :] = hat
            rstd1[row(i), :] = jnp.broadcast_to(scale, (TILE, 128))
            x1_b[row(i), :] = (hat * gain[0:1, :] + bias[4:5, :]).astype(jnp.bfloat16)

        loads[2].wait()

        def inner(i, carry):
            lanes = pl.ds(pl.multiple_of(lax.rem(i, wide) * TILE, TILE), TILE)
            columns = pl.ds(pl.multiple_of(i * TILE, TILE), TILE)
            hidden = dot_plain(x1_b[...], w_v[1 + i // wide, :, lanes]) + b_in[:, columns]
            cdf = 0.5 * (1.0 + lax.erf(hidden * 2.0 ** (-0.5)))
            act[:, columns] = (hidden * cdf).astype(jnp.bfloat16)
            density = jnp.exp(hidden * hidden * (-0.5)) * 0.3989422804014327
            slope[:, columns] = (cdf + hidden * density).astype(jnp.bfloat16)
            if ahead:
                pl.when(i == 3)(serve_across)
                pl.when(i == 10)(serve_beside)
            return carry

        lax.fori_loop(0, ff // TILE, inner, 0)
        loads[3].wait()
        if ahead:
            gathered()

        @loop(steps)
        def _(i):
            ffn = bias[3:4, :]
            for j in range(blocks):
                ffn = ffn + dot_plain(act[row(i), j * D : (j + 1) * D], wf_v[j])
            first = norm1[row(i), :] * gain[0:1, :] + bias[4:5, :]
            hat, scale = normalize(first + ffn)
            norm2[row(i), :] = hat
            rstd2[row(i), :] = jnp.broadcast_to(scale, (TILE, 128))
            out_v[row(i), :] = (hat * gain[1:2, :] + bias[5:6, :]).astype(jnp.bfloat16)

        out_stores = [
            pltpu.make_async_copy(out_v.at[:p_rows], out_p, store.at[g_names + 2]),
            pltpu.make_async_copy(out_v.at[p_rows:], out_c, store.at[g_names + 3]),
        ]
        for copy in out_stores:
            copy.start()
        base = 8 * (D // 128) + ff // 128
        w_stu_b = w_stu[...].astype(jnp.bfloat16)

        @pl.when(lax.axis_index("rep") >= 0)
        def _():
            stu = dot_plain(out_v[p_rows:, :], w_stu_b) + vec[0:1, :]
            logits, g_stu, g_query, g_pre, g_pool, g_class, g_logits = student_head(
                label_ref[0, 0], stu, vec, w_p[...], w_c[...], b_c[...], classes
            )
            logits_out[...] = logits[:, :classes]
            low = g_stu.astype(jnp.bfloat16)
            g_stu_b[:p_rows, :] = jnp.zeros((p_rows, STU), jnp.bfloat16)
            g_stu_b[p_rows:, :] = low
            small[base : base + 1, STU:] = jnp.sum(low.astype(jnp.float32), 0, keepdims=True)
            small[base + 1 : base + 2, STU:] = g_query
            small[base + 2 : base + 3, STU:] = g_pre
            small[base + 3 : base + 4, STU:] = g_logits
            small[base + 8 : base + 8 + STU, STU:] = g_pool
            small[base + 8 + STU : base + 8 + 2 * STU, STU:] = g_class

        small[:, :STU] = dot_first(out_v[p_rows:, :], g_stu_b[p_rows:, :])
        loads[6].wait()
        loads[7].wait()

        @loop(steps)
        def _(i):
            g = cot_v[row(i), :].astype(jnp.float32) + dot_second(g_stu_b[row(i), :], w_stu_b)
            hat = norm2[row(i), :]
            add_sum(7, g * hat)
            add_sum(5, g)
            g_r2 = norm_back(g, gain[1:2, :], hat, rstd2[row(i), :1])
            g_res[row(i), :] = g_r2
            low = g_r2.astype(jnp.bfloat16)
            g_ffn[row(i), :] = low
            add_sum(3, low.astype(jnp.float32))

        def piece_store(k):
            return pltpu.make_async_copy(grads.at[k], grads_h.at[k], store.at[k])


        @loop(blocks)
        def _(j):
            columns = pl.ds(pl.multiple_of(j * D, D), D)
            product = dot_first(act[:, columns], g_ffn[...]).astype(jnp.bfloat16)
            for k in range(blocks):
                target = pl.ds(pl.multiple_of(j * rows, 16), rows)
                grads[k, target, :] = product[k * rows : (k + 1) * rows]

        for k in range(ahead):
            for xx in range(2):
                core_copy(k, xx).start()
        for k in range(ahead, blocks):
            piece_store(k).start()


        in_sum[...] = jnp.zeros_like(in_sum)

        @loop(steps)
        def _(i):
            for j in range(blocks):
                columns = slice(j * D, (j + 1) * D)
                g_act = dot_second(g_ffn[row(i), :], wf_v[j])
                low = (g_act * slope[row(i), columns].astype(jnp.float32)).astype(jnp.bfloat16)
                slope[row(i), columns] = low
                in_sum[:, columns] += jnp.sum(low.astype(jnp.float32), 0, keepdims=True)
            if ahead:
                pl.when(i == 0)(stage_x)

        @loop(blocks)
        def _(j):
            columns = pl.ds(pl.multiple_of(j * D, D), D)
            grads[blocks + j] = dot_first(x1_b[...], slope[:, columns]).astype(jnp.bfloat16)
            piece_store(blocks + j).start()

        @loop(steps)
        def _(i):
            g = g_res[row(i), :]
            for j in range(blocks):
                g += dot_second(slope[row(i), j * D : (j + 1) * D], w_v[1 + j])
            hat = norm1[row(i), :]
            add_sum(6, g * hat)
            add_sum(4, g)
            g_r1 = norm_back(g, gain[0:1, :], hat, rstd1[row(i), :1])
            g_res[row(i), :] = g_r1
            low = g_r1.astype(jnp.bfloat16)
            g_br[row(i), :] = low
            add_sum(2, low.astype(jnp.float32))

        res_store = pltpu.make_async_copy(g_res, g_r1_h, store.at[g_names])
        res_store.start()
        g_ffn[...] = dot_second(g_br[...], w_v[0]).astype(jnp.bfloat16)
        att_store = pltpu.make_async_copy(g_ffn, g_att_h, store.at[g_names + 1])
        att_store.start()
        grads[2 * blocks] = dot_first(att_b[...], g_br[...]).astype(jnp.bfloat16)
        piece_store(2 * blocks).start()
        spread = D // 128
        for i in range(8):
            for part in range(spread):
                small[i * spread + part : i * spread + part + 1, STU:] = sums[
                    i : i + 1, part * 128 : (part + 1) * 128
                ]
        for part in range(ff // 128):
            at = 8 * spread + part
            small[at : at + 1, STU:] = in_sum[:, part * 128 : (part + 1) * 128]
        res_store.wait()
        att_store.wait()
        for copy in out_stores:
            copy.wait()
        for k in range(ahead):
            x_copy(k).wait_recv()
            total = grads[k, mine(x), :].astype(jnp.float32) + cr[k, x].astype(jnp.float32)
            cr[k, x] = (total + xr[k].astype(jnp.float32)).astype(jnp.bfloat16)
            pltpu.make_async_copy(cr.at[k, x], totals_h.at[k], store.at[k]).start()
        for k in range(ahead, g_names):
            piece_store(k).wait()
        for k in range(ahead):
            pltpu.make_async_copy(cr.at[k, x], totals_h.at[k], store.at[k]).wait()
            for xx in range(2):
                core_copy(k, xx).wait_send()
            x_copy(k).wait_send()
        if ahead:
            moved(0, shard, None, partner).wait_send()
            moved(1, shard, y, across).wait_send()
            moved(2, there, y, beside).wait_send()
            moved(3, there, y, partner).wait_send()
            moved(4, there, 1 - y, partner).wait_send()

    anywhere = pl.BlockSpec(memory_space=pl.ANY)
    vmem = pl.BlockSpec(memory_space=pltpu.VMEM)
    low = jnp.bfloat16

    def shaped(dims, kind=jnp.float32):
        return jax.ShapeDtypeStruct(dims, kind)

    params = pltpu.CompilerParams(vmem_limit_bytes=VMEM_ALL)
    link_scratch = []
    if ahead:
        params = pltpu.CompilerParams(
            collective_id=3, has_side_effects=True, vmem_limit_bytes=VMEM_ALL
        )
        piece = (D // blocks, D)
        link_scratch = [
            pltpu.VMEM(piece, jnp.float32),
            pltpu.VMEM((ahead, 2, *piece), low),
            pltpu.VMEM((ahead, *piece), low),
        ]
        link_scratch += [pltpu.SemaphoreType.DMA((5,))] * 2
        link_scratch += [pltpu.SemaphoreType.DMA((ahead, 2))] * 2
        link_scratch += [pltpu.SemaphoreType.DMA((ahead,))] * 2

    return pl.pallas_call(
        kernel,
        in_specs=[pl.BlockSpec(memory_space=pltpu.SMEM), anywhere]
        + [anywhere] * 7
        + [vmem] * 8,
        out_specs=[anywhere, anywhere, vmem, anywhere, anywhere, anywhere, vmem, anywhere],
        out_shape=[
            shaped((p_rows, D), low),
            shaped((cont_len, D), low),
            shaped((1, classes)),
            shaped((g_names, D, D), low),
            shaped((tokens, D)),
            shaped((tokens, D), low),
            shaped((D, 2 * STU)),
            shaped((max(ahead, 1), D // blocks, D), low),
        ],
        scratch_shapes=[
            pltpu.VMEM((tokens, D), low),
            pltpu.VMEM((tokens, D), low),
            pltpu.VMEM((tokens, D), low),
            pltpu.VMEM((tokens, D), jnp.float32),
            pltpu.VMEM((tokens, D), low),
            pltpu.VMEM((1 + blocks, D, D), low),
            pltpu.VMEM((blocks, D, D), low),
            pltpu.VMEM((tokens, D), jnp.float32),
            pltpu.VMEM((tokens, D), jnp.float32),
            pltpu.VMEM((tokens, 128), jnp.float32),
            pltpu.VMEM((tokens, 128), jnp.float32),
            pltpu.VMEM((tokens, D), low),
            pltpu.VMEM((tokens, ff), low),
            pltpu.VMEM((tokens, ff), low),
            pltpu.VMEM((tokens, D), jnp.float32),
            pltpu.VMEM((tokens, D), low),
            pltpu.VMEM((tokens, D), low),
            pltpu.VMEM((tokens, STU), low),
            pltpu.VMEM((g_names, D, D), low),
            pltpu.VMEM((8, D), jnp.float32),
            pltpu.VMEM((1, ff), jnp.float32),
            pltpu.SemaphoreType.DMA((9,)),
            pltpu.SemaphoreType.DMA((g_names + 4,)),
        ]
        + link_scratch,
        compiler_params=params,
        name="middle",
    )(
        labels,
        att,
        prompt,
        conts,
        prompt_cot,
        cont_cot,
        w_all,
        wf,
        wf_rows,
        biases,
        gains,
        bias_in[None],
        student,
        vectors,
        w_pool,
        w_class_p,
        bias_class_p,
    )


def sum_native(g9, g_qkvw, small):
    blocks = (g9.shape[0] - 1) // 2
    rows = D // blocks
    ffo = g9[:blocks].reshape(blocks, blocks, rows, D).transpose(1, 0, 2, 3).reshape(-1, D)
    inner = jnp.concatenate([g9[blocks + j] for j in range(blocks)], 1)

    def over(grad):
        part = lax.psum_scatter(
            grad.astype(jnp.bfloat16), "shard", scatter_dimension=0, tiled=True
        )
        return lax.psum(part, "rep").astype(jnp.float32)

    owned = tuple(over(grad) for grad in (g_qkvw, g9[2 * blocks], inner, ffo))
    return owned, lax.psum(small, ("rep", "shard"))


def finish(
    ahead, totals, q, kp, vp, kc, vc, att, lse, g_att, g9, g_resid, small, w_all, prompt, conts, ff
):
    pieces, ready = 12, 9
    p_rows, cont_len = prompt.shape[0], conts.shape[0]
    tokens = p_rows + cont_len
    p_len = kp.shape[0]
    pairs = HEADS // 2
    rows = D // 4
    half, quarter = D // 2, rows // 4
    s_width = small.shape[1]
    chunk = 2 * PAIR
    chunks = D // chunk
    across_lanes = D // 128

    def kernel(
        q_h, kp_h, vp_h, kc_h, vc_h, att_h, g_att_h, g9, g_res_h, w_h, totals_h, ls, sm, xp, xc,
        out_pg, out_cg, out_q, out_o, out_i, out_f, fin_s,
        qv, kpv, vpv, kcv, vcv, attv, gav, accum, dq, dkp, dvp, dkc, dvc, kr, kx, kvs, wv, g_tok, made, head,
        own, cr, xr, yr, zr, fb, made_s, own_s, cr_s, xr_s, yr_s, zr_s, fb_s,
        load, sem_own, c_send, c_recv, x_send, x_recv, y_send, y_recv, z_send, z_recv,
        f_send, f_recv, o_send, o_recv, o_own, g_send, g_recv, kc_s, kc_r, kx_s, kx_r, out_sem,
    ):
        rep, shard = lax.axis_index("rep"), lax.axis_index("shard")
        z, y = rep // 2, rep % 2
        x, core = shard // 2, shard % 2
        partner = (rep, 2 * x + 1 - core)
        across = (rep, 2 * (1 - x) + core)
        beside = (2 * z + 1 - y, shard)
        far = (rep, 2 * (1 - x) + 1 - core)

        def along(step):
            return (2 * lax.rem(z + step, 4) + y, shard)

        def own_copy(k, xx):
            return pltpu.make_async_copy(
                g9.at[k, pl.ds(pl.multiple_of((2 * xx + core) * rows, 16), rows), :],
                own.at[k, xx],
                sem_own.at[k, xx],
            )

        fetched = [(q_h, qv), (kp_h, kpv), (vp_h, vpv), (kc_h, kcv), (vc_h, vcv)]
        fetched += [(att_h, attv), (g_att_h, gav), (w_h.at[pl.ds(0, 3)], wv), (g_res_h, g_tok)]

        def fetch(i):
            return pltpu.make_async_copy(*fetched[i], load.at[i])

        def total_copy(k):
            return pltpu.make_async_copy(totals_h.at[k], own.at[k, x], sem_own.at[k, 0])

        for k in range(ahead):
            total_copy(k).start()
        for k in range(ahead, ahead + 2):
            for xx in range(2):
                own_copy(k, xx).start()
        for i in range(7):
            fetch(i).start()
        for k in range(ahead + 2, ready):
            for xx in range(2):
                own_copy(k, xx).start()
        for i in (7, 8):
            fetch(i).start()

        barrier = pltpu.get_barrier_semaphore()
        others = [partner, across, beside, along(1), along(2), along(3), far]
        for other in others:
            pl.semaphore_signal(barrier, inc=1, device_id=other, device_id_type=MESH_ID)
        pl.semaphore_wait(barrier, len(others))

        def remote(source, target, send, recv, device):
            return pltpu.make_async_remote_copy(
                src_ref=source,
                dst_ref=target,
                send_sem=send,
                recv_sem=recv,
                device_id=device,
                device_id_type=MESH_ID,
            )

        big = (own, cr, xr, yr, zr, fb, half)
        narrow = (own_s, cr_s, xr_s, yr_s, zr_s, fb_s, s_width // 2)

        def bufs(k):
            if isinstance(k, int) and k == pieces:
                return narrow, 0
            return big, k

        def core_copy(k, xx):
            b, i = bufs(k)
            block = 2 * xx + 1 - core
            if not isinstance(k, int):
                source = b[1].at[i, xx]
            elif k < ready:
                source = g9.at[k, pl.ds(pl.multiple_of(block * rows, 16), rows), :]
            elif k < pieces:
                source = made.at[k - ready, block]
            else:
                source = made_s.at[block]
            return remote(source, b[1].at[i, xx], c_send.at[k, xx], c_recv.at[k, xx], partner)

        def x_copy(k):
            b, i = bufs(k)
            return remote(b[0].at[i, 1 - x], b[2].at[i], x_send.at[k], x_recv.at[k], across)

        def lanes_of(b, which):
            return pl.ds(pl.multiple_of(which * b[6], 128), b[6])

        def y_copy(k):
            b, i = bufs(k)
            source = b[0].at[i, x, :, lanes_of(b, 1 - y)]
            return remote(source, b[3].at[i], y_send.at[k], y_recv.at[k], beside)

        def rows_of(which):
            return pl.ds(pl.multiple_of(which * quarter, 16), quarter)

        def zs_copy(k, step):
            b, i = bufs(k)
            source = b[0].at[i, x, rows_of(lax.rem(z + step, 4)), lanes_of(b, y)]
            return remote(
                source, b[4].at[i, z], z_send.at[k, step - 1], z_recv.at[k, z], along(step)
            )

        def zr_wait(k, step):
            b, i = bufs(k)
            slot = lax.rem(z + step, 4)
            target = b[4].at[i, slot]
            remote(
                target, target, z_send.at[k, step - 1], z_recv.at[k, slot], along(step)
            ).wait_recv()

        def fs_copy(k, step):
            b, i = bufs(k)
            block = b[5].at[i, rows_of(z), :]
            return remote(block, block, f_send.at[k, step - 1], f_recv.at[k, z], along(step))

        def fr_wait(k, step):
            b, i = bufs(k)
            slot = lax.rem(z + step, 4)
            block = b[5].at[i, rows_of(slot), :]
            remote(
                block, block, f_send.at[k, step - 1], f_recv.at[k, slot], along(step)
            ).wait_recv()

        def final(k, yy):
            b, _ = bufs(k)
            if k < 4:
                return out_f.at[k * rows : (k + 1) * rows, lanes_of(b, yy)]
            if k == 8:
                return out_o.at[:, lanes_of(b, yy)]
            if k == pieces:
                return fin_s.at[shard, :, lanes_of(b, yy)]
            out, at = (out_i, (k - 4) * D) if k < 8 else (out_q, (k - 9) * D)
            return out.at[:, pl.ds(pl.multiple_of(at + yy * half, 128), half)]

        def o_copy(k):
            b, i = bufs(k)
            return remote(b[5].at[i], final(k, y), o_send.at[k], o_recv.at[k], beside)

        def o_wait(k):
            b, i = bufs(k)
            remote(b[5].at[i], final(k, 1 - y), o_send.at[k], o_recv.at[k], beside).wait_recv()

        def o_local(k):
            b, i = bufs(k)
            return pltpu.make_async_copy(b[5].at[i], final(k, y), o_own.at[k])

        def wide(value):
            return value.astype(jnp.float32)

        def stage_x(k):
            b, i = bufs(k)
            for xx in range(2):
                core_copy(k, xx).wait_recv()
                if not isinstance(k, int):
                    pl.when(k < ready)(own_copy(k, xx).wait)
            b[0][i, 1 - x] = (wide(b[0][i, 1 - x]) + wide(b[1][i, 1 - x])).astype(jnp.bfloat16)
            x_copy(k).start()

        def stage_y(k):
            b, i = bufs(k)
            x_copy(k).wait_recv()
            total = wide(b[0][i, x]) + wide(b[1][i, x]) + wide(b[2][i])
            b[0][i, x] = total.astype(jnp.bfloat16)
            y_copy(k).start()

        def stage_z(k):
            b, i = bufs(k)
            y_copy(k).wait_recv()
            lanes = lanes_of(b, y)
            total = wide(b[0][i, x, :, lanes]) + wide(b[3][i])
            b[0][i, x, :, lanes] = total.astype(jnp.bfloat16)
            for step in (2, 1, 3):
                zs_copy(k, step).start()

        def stage_f(k):
            b, i = bufs(k)
            total = wide(b[0][i, x, rows_of(z), lanes_of(b, y)])
            for step in (1, 2, 3):
                zr_wait(k, step)
                total += wide(b[4][i, lax.rem(z + step, 4)])
            b[5][i, rows_of(z), :] = total.astype(jnp.bfloat16)
            for step in (2, 1, 3):
                fs_copy(k, step).start()

        def stage_o(k):
            for step in (1, 2, 3):
                fr_wait(k, step)
            for kk in range(pieces + 1) if not isinstance(k, int) else [k]:

                def begin(kk=kk):
                    o_copy(kk).start()
                    o_local(kk).start()

                if isinstance(k, int):
                    begin()
                else:
                    pl.when(k == kk)(begin)

        def send_core(k):
            for xx in range(2):
                core_copy(k, xx).start()

        for k in range(ahead, ready):
            send_core(k)

        def stages_x(first, last):
            def step(k, carry):
                stage_x(k)
                return carry

            lax.fori_loop(first, last, step, 0)

        for k in range(ahead):
            total_copy(k).wait()
            y_copy(k).start()
        stages_x(ahead, ahead + 2)
        kv = (dkp, dvp)

        def kv_rows(block):
            return pl.ds(pl.multiple_of(block * p_rows, p_rows), p_rows)

        def kv_lanes(g):
            return pl.ds(g * chunk if isinstance(g, int) else pl.multiple_of(g * chunk, chunk), chunk)

        def kv_core(t, g, xx):
            return remote(
                kv[t].at[kv_rows(2 * xx + 1 - core), kv_lanes(g)],
                kr.at[t, xx, :, kv_lanes(g)],
                kc_s.at[g, t, xx],
                kc_r.at[g, t, xx],
                partner,
            )

        def kv_across(t, g):
            return remote(
                kv[t].at[kv_rows(2 * (1 - x) + core), kv_lanes(g)],
                kx.at[t, :, kv_lanes(g)],
                kx_s.at[g, t],
                kx_r.at[g, t],
                across,
            )

        def serve_kv(g):
            block, lanes = kv_rows(2 * (1 - x) + core), kv_lanes(g)
            for t in range(2):
                for xx in range(2):
                    kv_core(t, g, xx).wait_recv()
                total = wide(kv[t][block, lanes]) + wide(kr[t, 1 - x, :, lanes])
                kv[t][block, lanes] = total.astype(jnp.bfloat16)
                kv_across(t, g).start()

        for i in range(7):
            fetch(i).wait()

        def pair(p, carry):
            def between(index):
                if index == 0:
                    pl.when(p + ahead + 2 < ready)(lambda: stage_x(p + ahead + 2))
                if index == 1:
                    pl.when((p == 2) | (p == 4))(lambda: serve_kv(p // 2 - 1))
                if index == 2:
                    pl.when(p >= 1)(lambda: stage_y(p + ahead - 1))
                if index == 3:
                    stage_z(p)
                if index == 4:
                    pl.when(p >= 1)(lambda: stage_f(p - 1))
                if index == 5:
                    pl.when(p >= 2)(lambda: stage_o(p - 2))

            lanes = pl.ds(pl.multiple_of(p * PAIR, PAIR), PAIR)

            def cut(ref):
                return ref.at[:, lanes]

            attend_bwd_pair(
                shard, p_rows, cut(qv), cut(kpv), cut(vpv), cut(kcv), cut(vcv), cut(gav), cut(attv),
                ls.at[p], cut(dq), cut(dkp), cut(dvp), cut(dkc), cut(dvc), accum, between,
            )

            @pl.when(p % 2 == 1)
            def _():
                for t in range(2):
                    for xx in range(2):
                        kv_core(t, p // 2, xx).start()

            return carry

        lax.fori_loop(0, pairs, pair, 0)

        def keep_piece(k, product):
            for block in range(4):
                made[k - ready, block] = product[block * rows : (block + 1) * rows]
            for xx in range(2):
                own[k, xx] = made[k - ready, 2 * xx + core]
            send_core(k)

        product = dot_first(xp[...], dq[:p_rows, :]) + dot_first(xc[...], dq[p_rows:, :])
        keep_piece(9, product.astype(jnp.bfloat16))
        serve_kv(chunks - 1)
        for i in (7, 8):
            fetch(i).wait()
        stages_x(9, 10)
        g_tok[...] += dot_second(dq[...], wv[2])
        stores = [
            pltpu.make_async_copy(g_tok.at[:p_rows, :], out_pg, out_sem.at[0]),
            pltpu.make_async_copy(g_tok.at[p_rows:, :], out_cg, out_sem.at[1]),
        ]

        def with_kv():
            for g in range(chunks):
                for t in range(2):
                    kv_across(t, g).wait_recv()
            for t in range(2):
                total = wide(kv[t][kv_rows(shard), :]) + wide(kr[t, x]) + wide(kx[t])
                kvs[t] = total.astype(jnp.bfloat16)
            g_bias = jnp.sum(wide(dq[...]), 0, keepdims=True)
            v_bias = jnp.sum(wide(dvc[...]), 0, keepdims=True)
            v_bias += jnp.sum(wide(kvs[1]), 0, keepdims=True)
            head[...] = sm[:16, :]
            for part in range(across_lanes):
                lanes = slice(part * 128, (part + 1) * 128)
                head[part : part + 1, STU:] = g_bias[:, lanes]
                head[across_lanes + part : across_lanes + part + 1, STU:] = v_bias[:, lanes]
            for block in range(4):
                made_s[block] = sm[block * rows : (block + 1) * rows, :].astype(jnp.bfloat16)
            made_s[0, :16] = head[...].astype(jnp.bfloat16)
            for xx in range(2):
                own_s[0, xx] = made_s[2 * xx + core]
            send_core(pieces)
            for t in range(2):
                product = dot_first(xp[...], kvs[t]) + dot_first(xc[...], (dkc, dvc)[t][...])
                keep_piece(10 + t, product.astype(jnp.bfloat16))
            stage_x(pieces)
            stages_x(10, 12)
            g_tok[:p_rows, :] += dot_second(kvs[0], wv[0]) + dot_second(kvs[1], wv[1])
            for copy in stores:
                copy.start()

        def cont_part():
            g_tok[p_rows:, :] += dot_second(dkc[...], wv[0]) + dot_second(dvc[...], wv[1])

        def tick(n, carry):
            pl.when(n == 9)(with_kv)
            pl.when((n >= 8) & (n < pieces))(lambda: stage_y(n))
            pl.when(n == 10)(lambda: stage_y(pieces))
            pl.when(n < pieces + 1)(lambda: stage_z(n - 1))
            pl.when(n == 11)(lambda: stage_z(pieces))
            pl.when(n < pieces + 2)(lambda: stage_f(n - 2))
            pl.when(n == 12)(lambda: stage_f(pieces))
            stage_o(n - 3)
            pl.when(n == 13)(lambda: stage_o(pieces))
            pl.when(n == 7)(cont_part)
            return carry

        def g_copy(step):
            return remote(
                fin_s.at[shard],
                fin_s.at[shard],
                g_send.at[step - 1],
                g_recv.at[shard],
                (rep, lax.rem(shard + step, 4)),
            )

        def stage_g():
            o_wait(pieces)
            o_local(pieces).wait()
            for step in (1, 2, 3):
                g_copy(step).start()

        lax.fori_loop(pieces - 5, pieces + 3, tick, 0)
        stage_g()
        for step in (1, 2, 3):
            slot = lax.rem(shard + step, 4)
            remote(
                fin_s.at[slot], fin_s.at[slot], g_send.at[step - 1], g_recv.at[slot], far
            ).wait_recv()

        for k in range(pieces):
            o_wait(k)
            o_local(k).wait()
        for copy in stores:
            copy.wait()

        def sent(k):
            def two():
                for xx in range(2):
                    core_copy(k, xx).wait_send()
                x_copy(k).wait_send()

            if isinstance(k, int):
                two()
            else:
                pl.when(k >= ahead)(two)
            y_copy(k).wait_send()
            for step in (1, 2, 3):
                zs_copy(k, step).wait_send()
                fs_copy(k, step).wait_send()

        def sent_step(k, carry):
            sent(k)
            return carry

        lax.fori_loop(0, pieces, sent_step, 0)
        sent(pieces)
        for k in range(pieces + 1):
            o_copy(k).wait_send()
        for step in (1, 2, 3):
            g_copy(step).wait_send()
        for g in range(chunks):
            for t in range(2):
                for xx in range(2):
                    kv_core(t, g, xx).wait_send()
                kv_across(t, g).wait_send()

    def sems(*dims):
        return pltpu.SemaphoreType.DMA(dims)

    def low(*dims):
        return pltpu.VMEM(dims, jnp.bfloat16)

    def full(*dims):
        return pltpu.VMEM(dims, jnp.float32)

    def buffers(count, columns):
        cut = columns // 2
        return [
            low(count, 2, rows, columns),
            low(count, 2, rows, columns),
            low(count, rows, columns),
            low(count, rows, cut),
            low(count, 4, quarter, cut),
            low(count, rows, cut),
        ]

    def shaped(dims, kind=jnp.float32):
        return jax.ShapeDtypeStruct(dims, kind)

    n = pieces + 1
    anywhere = pl.BlockSpec(memory_space=pl.ANY)
    vmem = pl.BlockSpec(memory_space=pltpu.VMEM)
    return pl.pallas_call(
        kernel,
        in_specs=[anywhere] * 11 + [vmem] * 4,
        out_specs=[anywhere] * 6 + [vmem],
        out_shape=[
            shaped((p_rows, D)),
            shaped((cont_len, D)),
            shaped((rows, 3 * D), jnp.bfloat16),
            shaped((rows, D), jnp.bfloat16),
            shaped((rows, ff), jnp.bfloat16),
            shaped((4 * rows, D), jnp.bfloat16),
            shaped((4, rows, s_width), jnp.bfloat16),
        ],
        scratch_shapes=[
            low(tokens, D), low(p_len, D), low(p_len, D), low(cont_len, D), low(cont_len, D),
            full(tokens, D), low(tokens, D), full(PAIR, tokens), low(tokens, D),
            low(p_len, D), low(p_len, D), low(cont_len, D), low(cont_len, D),
            low(2, 2, p_rows, D), low(2, p_rows, D), low(2, p_rows, D), low(3, D, D),
            full(tokens, D), low(3, 4, rows, D), full(16, s_width),
        ]
        + buffers(pieces, D)
        + [low(4, rows, s_width)]
        + buffers(1, s_width)
        + [
            sems(9), sems(n, 2), sems(n, 2), sems(n, 2), sems(n), sems(n), sems(n), sems(n),
            sems(n, 3), sems(n, 4), sems(n, 3), sems(n, 4), sems(n), sems(n), sems(n),
            sems(3), sems(4), sems(chunks, 2, 2), sems(chunks, 2, 2), sems(chunks, 2),
            sems(chunks, 2), sems(2),
        ],
        compiler_params=pltpu.CompilerParams(
            collective_id=2, has_side_effects=True, vmem_limit_bytes=VMEM_ALL
        ),
        name="finish",
    )(q, kp, vp, kc, vc, att, g_att, g9, g_resid, w_all, totals, lse, small, prompt, conts)


def place(g_prompt, g_conts, owned, summed, ff, classes):
    big = [g_prompt, g_conts, *owned]
    rows, across = summed.shape[1], D // 128

    def kernel(*refs):
        sources, fin = refs[:6], refs[6]
        targets, (o_bias, o_gain, o_in, o_stu, o_vec, o_pool, o_class, o_cb) = (
            refs[7:13],
            refs[13:21],
        )
        held, turned, sem_in, sem_out = refs[21:27], refs[27:31], refs[31], refs[32]
        reads = [
            pltpu.make_async_copy(sources[i], held[i], sem_in.at[i]) for i in (2, 4, 5, 3, 1, 0)
        ]
        for copy in reads:
            copy.start()

        def side(block):
            return fin[block, :, STU:].astype(jnp.float32)

        first = side(0)
        for i in range(8):
            target, at = (o_bias, i) if i < 6 else (o_gain, i - 6)
            for part in range(across):
                r = i * across + part
                target[at : at + 1, part * 128 : (part + 1) * 128] = first[r : r + 1, :]
        for part in range(ff // 128):
            r = 8 * across + part
            o_in[:, part * 128 : (part + 1) * 128] = first[r : r + 1, :]
        base = 8 * across + ff // 128
        o_vec[...] = first[base : base + 3, :]
        o_cb[...] = first[base + 3 : base + 4, :classes]
        every = jnp.concatenate([first, side(1)], 0)
        o_pool[...] = every[base + 8 : base + 8 + STU, :]
        o_class[...] = every[base + 8 + STU : base + 8 + 2 * STU, :classes]
        for block in range(4):
            o_stu[block * rows : (block + 1) * rows, :] = fin[block, :, :STU].astype(jnp.float32)
        writes = []
        for copy, i in zip(reads, (2, 4, 5, 3, 1, 0)):
            copy.wait()
            source = held[i]
            if i >= 2:
                source = turned[i - 2]
                source[...] = held[i][...].astype(jnp.float32)
            writes.append(pltpu.make_async_copy(source, targets[i], sem_out.at[i]))
            writes[-1].start()
        for copy in writes:
            copy.wait()

    def shaped(*dims):
        return jax.ShapeDtypeStruct(dims, jnp.float32)

    anywhere = pl.BlockSpec(memory_space=pl.ANY)
    vmem = pl.BlockSpec(memory_space=pltpu.VMEM)
    return pl.pallas_call(
        kernel,
        in_specs=[anywhere] * 6 + [vmem],
        out_specs=[anywhere] * 6 + [vmem] * 8,
        out_shape=[shaped(*part.shape) for part in big]
        + [
            shaped(6, D),
            shaped(2, D),
            shaped(1, ff),
            shaped(D, STU),
            shaped(3, STU),
            shaped(STU, STU),
            shaped(STU, classes),
            shaped(1, classes),
        ],
        scratch_shapes=[pltpu.VMEM(part.shape, part.dtype) for part in big]
        + [pltpu.VMEM(part.shape, jnp.float32) for part in owned]
        + [pltpu.SemaphoreType.DMA((6,)), pltpu.SemaphoreType.DMA((6,))],
        compiler_params=pltpu.CompilerParams(vmem_limit_bytes=VMEM_ALL),
        name="place",
    )(*big, summed)


def body(
    prompt,
    conts,
    prompt_cot,
    cont_cot,
    labels,
    w_qkv,
    w_out,
    w_in,
    w_ffo,
    layer_biases,
    norm_gains,
    bias_in,
    w_student,
    student_vectors,
    w_pool,
    w_class,
    bias_class,
):
    prompt_rows = prompt.shape[1]
    direct = (lax.axis_size("rep"), lax.axis_size("shard")) == (8, 4)
    project = project_and_attend if direct else project_native
    w_all, ffo_full, q, kp, vp, kc, vc, attended, log_totals = project(
        prompt[0], conts[0, 0], w_qkv, w_out, w_in, w_ffo, layer_biases
    )
    ahead = 3 if direct else 0
    out_p, out_c, logits, g9, g_resid, g_att, small, totals = middle(
        ahead,
        attended,
        prompt[0],
        conts[0, 0],
        prompt_cot[0],
        cont_cot[0, 0],
        labels,
        w_all,
        ffo_full if direct else ffo_full.reshape(-1, D, D),
        w_ffo,
        layer_biases,
        norm_gains,
        bias_in,
        w_student,
        student_vectors,
        w_pool,
        w_class,
        bias_class,
    )
    ff, classes = bias_in.shape[0], w_class.shape[1]
    if direct:
        outs = finish(
            ahead, totals, q, kp, vp, kc, vc, attended, log_totals, g_att, g9, g_resid, small, w_all,
            prompt[0], conts[0, 0], ff,
        )
        placed = place(outs[0], outs[1], outs[2:6], outs[6], ff, classes)
        g_prompt, g_conts, owned = placed[0], placed[1], placed[2:6]
        biases, gains_g, g_in, g_student, g_vectors, g_pool, g_class, g_cb = placed[6:]
    else:
        g_q, g_kp, g_vp, g_kc, g_vc = attend_backward(
            q, kp, vp, kc, vc, g_att, attended, log_totals, prompt_rows
        )
        tokens = jnp.concatenate([prompt[0], conts[0, 0]], 0)
        kv_sum = [
            lax.psum_scatter(part, "shard", scatter_dimension=0, tiled=True)
            for part in (g_kp, g_vp)
        ]
        g_k = jnp.concatenate([kv_sum[0], g_kc], 0)
        g_v = jnp.concatenate([kv_sum[1], g_vc], 0)
        g_tokens = g_resid
        for part, weight in ((g_k, w_all[0]), (g_v, w_all[1]), (g_q, w_all[2])):
            g_tokens = g_tokens + dot_second(part, weight)
        g_prompt, g_conts = g_tokens[:prompt_rows], g_tokens[prompt_rows:]
        g_qkvw = jnp.concatenate([dot_first(tokens, part) for part in (g_q, g_k, g_v)], 1)
        side = small[:, STU:]
        across = D // 128
        for at, part in ((0, g_q), (1, g_v)):
            total = jnp.sum(part.astype(jnp.float32), 0).reshape(across, 128)
            side = lax.dynamic_update_slice(side, total, (at * across, 0))
        small = jnp.concatenate([small[:, :STU], side], 1)
        owned, summed = sum_native(g9, g_qkvw, small)
        side = summed[:, STU:]
        base = 8 * across + ff // 128
        biases = side[: 6 * across].reshape(6, D)
        gains_g = side[6 * across : 8 * across].reshape(2, D)
        g_in = side[8 * across : base]
        g_student, g_vectors = summed[:, :STU], side[base : base + 3]
        g_pool = side[base + 8 : base + 8 + STU]
        g_class = side[base + 8 + STU : base + 8 + 2 * STU]
        g_cb = side[base + 3 : base + 4]
    return (
        out_p[None],
        out_c[None, None],
        logits[None],
        g_prompt[None],
        g_conts[None, None],
        *owned,
        biases,
        gains_g,
        g_in.reshape(ff),
        g_student,
        g_vectors,
        g_pool,
        g_class[:, :classes],
        g_cb[0, :classes],
    )


def solution(mesh):
    return jax.shard_map(
        body,
        mesh=mesh,
        in_specs=(
            P("rep", "shard", None),
            P("rep", "shard", None, None),
            P("rep", "shard", None),
            P("rep", "shard", None, None),
            P("rep", "shard"),
            P("shard", None),
            P("shard", None),
            P("shard", None),
            P("shard", None),
            P(),
            P(),
            P(),
            P(),
            P(),
            P(),
            P(),
            P(),
        ),
        out_specs=(
            P("rep", "shard", None),
            P("rep", "shard", None, None),
            P("rep", "shard", None),
            P("rep", "shard", None),
            P("rep", "shard", None, None),
            P("shard", None),
            P("shard", None),
            P("shard", None),
            P("shard", None),
            P(),
            P(),
            P(),
            P(),
            P(),
            P(),
            P(),
            P(),
        ),
        check_vma=False,
    )
```

```python
import functools

import jax
import jax.numpy as jnp
from jax import lax
from jax.experimental import pallas as pl
from jax.experimental.pallas import tpu as pltpu
from jax.sharding import PartitionSpec as P

D = 768
HEADS = 12
DH = 64
STU = 128
SHEADS = 2


HIGHEST = lax.Precision.HIGHEST
NEG_BIG = -1e30


def dot_plain(left, right):
    return jnp.dot(left, right, preferred_element_type=jnp.float32)


def dot_first(left, right):
    return lax.dot_general(
        left, right, (((0,), (0,)), ((), ())), preferred_element_type=jnp.float32
    )


def dot_second(left, right):
    return lax.dot_general(
        left, right, (((1,), (1,)), ((), ())), preferred_element_type=jnp.float32
    )


TILE = 256
PAIR = 128
VMEM_ALL = 62 * 1024 * 1024


def rows_dot(left, right):
    return lax.dot_general(
        left, right, (((1,), (1,)), ((), ())), preferred_element_type=jnp.float32
    )


def low_lanes(shape):
    return lax.broadcasted_iota(jnp.int32, shape, len(shape) - 1) < DH


def attend_fwd_pair(
    shard, prompt_rows, q, kp, vp, kc, vc, att_ref, lse_ref, between=None
):
    cont_len = kc.shape[0]
    prompt_len = kp.shape[0]
    for start in range(0, prompt_rows + cont_len, TILE):
        q_t = q[start : start + TILE, :] * jnp.asarray(DH ** (-0.5), jnp.bfloat16)
        halves = []
        for parity in range(2):
            keep = low_lanes(q_t.shape) == (parity == 0)
            q_h = jnp.where(keep, q_t, jnp.zeros_like(q_t))
            s_p = rows_dot(q_h, kp[...])
            if start < prompt_rows:
                key = lax.broadcasted_iota(jnp.int32, s_p.shape, 1)
                row = lax.broadcasted_iota(jnp.int32, s_p.shape, 0)
                s_p = jnp.where(key <= row + (shard * prompt_rows + start), s_p, NEG_BIG)
                largest = jnp.max(s_p, 1, keepdims=True)
                p_p = jnp.exp(s_p - largest)
                total = jnp.sum(p_p, 1, keepdims=True)
                o = dot_plain(p_p.astype(jnp.bfloat16), vp[...])
            else:
                seen = start - prompt_rows + TILE
                s_c = rows_dot(q_h, kc[:seen, :])
                key = lax.broadcasted_iota(jnp.int32, s_c.shape, 1)
                row = lax.broadcasted_iota(jnp.int32, s_c.shape, 0)
                s_c = jnp.where(key <= row + (start - prompt_rows), s_c, NEG_BIG)
                largest = jnp.maximum(
                    jnp.max(s_p, 1, keepdims=True), jnp.max(s_c, 1, keepdims=True)
                )
                p_p = jnp.exp(s_p - largest)
                p_c = jnp.exp(s_c - largest)
                total = jnp.sum(p_p, 1, keepdims=True) + jnp.sum(p_c, 1, keepdims=True)
                o = dot_plain(p_p.astype(jnp.bfloat16), vp[...]) + dot_plain(
                    p_c.astype(jnp.bfloat16), vc[:seen, :]
                )
            halves.append((o / total, largest + jnp.log(total)))
        keep = low_lanes((TILE, PAIR))
        att_ref[start : start + TILE, :] = jnp.where(keep, halves[0][0], halves[1][0])
        lse = jnp.where(
            keep,
            jnp.broadcast_to(halves[0][1], (TILE, PAIR)),
            jnp.broadcast_to(halves[1][1], (TILE, PAIR)),
        )
        turned = jnp.transpose(lse)
        lse_ref[0:1, start : start + TILE] = turned[0:1, :]
        lse_ref[1:2, start : start + TILE] = turned[DH : DH + 1, :]
        if between is not None:
            between(start // TILE)


def attend_bwd_pair(
    shard, prompt_rows, q, kp, vp, kc, vc, g, att, lse, dq, dkp, dvp, dkc, dvc, accum, between=None
):
    cont_len = kc.shape[0]
    tokens = prompt_rows + cont_len
    prompt_len = kp.shape[0]
    g_t = g[...]
    turned = jnp.transpose(g_t.astype(jnp.float32) * att[...])
    delta = (
        jnp.sum(turned[:DH], 0, keepdims=True),
        jnp.sum(turned[DH:], 0, keepdims=True),
    )
    q_t = q[...] * jnp.asarray(DH ** (-0.5), jnp.bfloat16)
    keep = low_lanes(q_t.shape)
    zero = jnp.zeros_like(q_t)
    q_h = (jnp.where(keep, q_t, zero), jnp.where(keep, zero, q_t))
    g_h = (jnp.where(keep, g_t, zero), jnp.where(keep, zero, g_t))
    accum[...] = jnp.zeros_like(accum)

    def block(key_b, value_b, first, mask):
        key_t = jnp.transpose(key_b.astype(jnp.float32)).astype(jnp.bfloat16)
        g_key = jnp.zeros((TILE, PAIR), jnp.float32)
        g_value = jnp.zeros((TILE, PAIR), jnp.float32)
        for parity in range(2):
            scores = rows_dot(key_b, q_h[parity][first:])
            probs = jnp.exp(scores - lse[parity : parity + 1, first:])
            masked = jnp.where(mask, probs[:, :TILE], 0.0)
            if tokens - first > TILE:
                probs = jnp.concatenate([masked, probs[:, TILE:]], 1)
            else:
                probs = masked
            g_probs = rows_dot(value_b, g_h[parity][first:])
            g_scores = (probs * (g_probs - delta[parity][:, first:])).astype(jnp.bfloat16)
            g_value += dot_plain(probs.astype(jnp.bfloat16), g_h[parity][first:])
            g_key += dot_plain(g_scores, q_h[parity][first:])
            rows = slice(parity * DH, (parity + 1) * DH)
            accum[rows, first:] += dot_plain(key_t[rows], g_scores)
        return g_key.astype(jnp.bfloat16), g_value.astype(jnp.bfloat16)

    ahead = lax.broadcasted_iota(jnp.int32, (TILE, TILE), 0) - lax.broadcasted_iota(
        jnp.int32, (TILE, TILE), 1
    )

    def prompt_block(index, start):
        rows = pl.ds(start, TILE)
        mask = ahead <= shard * prompt_rows - index * TILE
        g_key, g_value = block(kp[rows, :], vp[rows, :], 0, mask)
        dkp[rows, :] = g_key
        dvp[rows, :] = g_value

    blocks = prompt_len // TILE
    if blocks <= 4:
        for index in range(blocks):
            prompt_block(index, index * TILE)
            if between is not None:
                between(index)
    else:

        def step(index, carry):
            prompt_block(index, pl.multiple_of(index * TILE, TILE))
            return carry

        lax.fori_loop(0, blocks, step, 0)
    for start in range(0, cont_len, TILE):
        rows = slice(start, start + TILE)
        g_key, g_value = block(kc[rows, :], vc[rows, :], prompt_rows + start, ahead <= 0)
        dkc[rows, :] = g_key
        dvc[rows, :] = g_value
        if between is not None:
            between(blocks + start // TILE)
    dq[...] = (jnp.transpose(accum[...]) * DH ** (-0.5)).astype(jnp.bfloat16)


def attend_forward(q, kp, vp, kc, vc, prompt_rows):
    tokens, prompt_len, cont_len = q.shape[0], kp.shape[0], kc.shape[0]
    pairs = HEADS // 2

    def kernel(q, kp, vp, kc, vc, att_ref, lse_ref):
        attend_fwd_pair(
            lax.axis_index("shard"), prompt_rows, q, kp, vp, kc, vc, att_ref, lse_ref.at[0]
        )

    def columns(rows):
        return pl.BlockSpec((rows, PAIR), lambda p: (0, p))

    return pl.pallas_call(
        kernel,
        grid=(pairs,),
        in_specs=[columns(rows) for rows in (tokens, prompt_len, prompt_len, cont_len, cont_len)],
        out_specs=[columns(tokens), pl.BlockSpec((1, 8, tokens), lambda p: (p, 0, 0))],
        out_shape=[
            jax.ShapeDtypeStruct((tokens, D), jnp.float32),
            jax.ShapeDtypeStruct((pairs, 8, tokens), jnp.float32),
        ],
        compiler_params=pltpu.CompilerParams(vmem_limit_bytes=VMEM_ALL),
        name="attend_forward",
    )(q, kp, vp, kc, vc)


def attend_backward(q, kp, vp, kc, vc, g_att, att, lse, prompt_rows):
    tokens, prompt_len, cont_len = q.shape[0], kp.shape[0], kc.shape[0]
    pairs = HEADS // 2

    def kernel(q, kp, vp, kc, vc, g, a, ls, dq, dkp, dvp, dkc, dvc, accum):
        attend_bwd_pair(
            lax.axis_index("shard"),
            prompt_rows,
            q,
            kp,
            vp,
            kc,
            vc,
            g,
            a,
            ls.at[0],
            dq,
            dkp,
            dvp,
            dkc,
            dvc,
            accum,
        )

    def columns(rows):
        return pl.BlockSpec((rows, PAIR), lambda p: (0, p))

    sizes = (tokens, prompt_len, prompt_len, cont_len, cont_len)
    return pl.pallas_call(
        kernel,
        grid=(pairs,),
        in_specs=[columns(rows) for rows in sizes + (tokens, tokens)]
        + [pl.BlockSpec((1, 8, tokens), lambda p: (p, 0, 0))],
        out_specs=[columns(rows) for rows in sizes],
        out_shape=[jax.ShapeDtypeStruct((rows, D), jnp.bfloat16) for rows in sizes],
        scratch_shapes=[pltpu.VMEM((PAIR, tokens), jnp.float32)],
        compiler_params=pltpu.CompilerParams(vmem_limit_bytes=VMEM_ALL),
        name="attend_backward",
    )(q, kp, vp, kc, vc, g_att, att, lse)


MESH_ID = pl.DeviceIdType.MESH


def project_and_attend(
    prompt, conts, w_qkv, w_out, w_in, w_ffo, layer_biases, norm_gains, bias_in
):
    pieces, early = 12, 4
    ff = bias_in.shape[0]
    wide = D // TILE
    inner_steps = ff // TILE
    by_z = (4, 5, 6, 7, 8, 9)
    rows = w_qkv.shape[0]
    p_rows, cont_len = prompt.shape[0], conts.shape[0]
    tokens = p_rows + cont_len
    p_len = 4 * p_rows
    pairs = HEADS // 2
    tiles = tokens // TILE
    steps = tokens // TILE
    chunk = 2 * PAIR
    chunks = D // chunk
    quarter = rows // 4

    def kernel(
        xp, xc, wq, wo, wi, wf, bias, gain, b_in, w_all_out, wf_out, q_out, kc_out, vc_out, kp_out, vp_out, att_out,
        norm_out, x1_out, act_out, slope_out, att_b_out, lse, rstd_out,
        stage, w_all, q, kc, vc, kp, vp, att, norm1, x1_b, act, slope, att_b,
        load, c_s, c_r, x_s, x_r, y_s, y_r, z_s, z_r, d_s, d_r, e_s, e_r, w_sem,
        kc_s, kc_r, kx_s, kx_r, kd_s, kd_r, out_sem, ff_sem, row_sem,
    ):
        rep, shard = lax.axis_index("rep"), lax.axis_index("shard")
        z, y = rep // 2, rep % 2
        x, core = shard // 2, shard % 2
        partner = (rep, 2 * x + 1 - core)
        across = (rep, 2 * (1 - x) + core)
        beside = (2 * z + 1 - y, shard)
        z_low = z % 2
        above = (2 * (z + 1 - 2 * z_low) + y, shard)
        there = 2 * (1 - x) + core

        def remote(ref, send, recv, device):
            return pltpu.make_async_remote_copy(
                src_ref=ref,
                dst_ref=ref,
                send_sem=send,
                recv_sem=recv,
                device_id=device,
                device_id_type=MESH_ID,
            )

        def source(k):
            if k < 3:
                j = (1, 2, 0)[k]
                return wq.at[:, j * D : (j + 1) * D]
            if k < 4:
                return wo
            if k < 8:
                return wi.at[:, (k - 4) * D : (k - 3) * D]
            return wf.at[(k - 8) * rows : (k - 7) * rows, :]

        def loading(k):
            return pltpu.make_async_copy(source(k), stage.at[k], load.at[k])

        for k in range(pieces):
            loading(k).start()
        barrier = pltpu.get_barrier_semaphore()
        for other in (partner, across, beside, above):
            pl.semaphore_signal(barrier, inc=1, device_id=other, device_id_type=MESH_ID)
        pl.semaphore_wait(barrier, 4)

        def part(k, block, first, count):
            start = pl.multiple_of(first * quarter, 16)
            return w_all.at[k, block, pl.ds(start, count * quarter), :]

        def core_copy(k):
            return remote(w_all.at[k, shard], c_s.at[k], c_r.at[k], partner)

        def core_arrival(k):
            return remote(w_all.at[k, 2 * x + 1 - core], c_s.at[k], c_r.at[k], partner)

        def crossing(k, y_at):
            return (2 * z_low + y_at, 1) if k in by_z else (2 * y_at, 2)

        def x_copy(k):
            return remote(part(k, shard, *crossing(k, y)), x_s.at[k], x_r.at[k], across)

        def x_arrival(k):
            return remote(part(k, there, *crossing(k, y)), x_s.at[k], x_r.at[k], across)

        def y_copy(k):
            return remote(part(k, there, *crossing(k, y)), y_s.at[k], y_r.at[k], beside)

        def y_arrival(k):
            return remote(part(k, there, *crossing(k, 1 - y)), y_s.at[k], y_r.at[k], beside)

        def z_copy(k):
            return remote(part(k, there, 2 * z_low, 2), z_s.at[k], z_r.at[k], above)

        def z_arrival(k):
            return remote(part(k, there, 2 * (1 - z_low), 2), z_s.at[k], z_r.at[k], above)

        def halves(k):
            first = 2 * z_low if k in by_z else 2 * y
            return first, 2 - first

        def d_copy(k, block=None):
            block = there if block is None else block
            return remote(part(k, block, halves(k)[0], 2), d_s.at[k], d_r.at[k], partner)

        def e_copy(k, block=None):
            block = there if block is None else block
            return remote(part(k, block, halves(k)[1], 2), e_s.at[k], e_r.at[k], partner)

        far = 2 * (1 - x) + 1 - core

        def send_piece(k):
            x_copy(k).start()
            core_copy(k).start()

        def round_piece(k):
            loading(k).wait()
            w_all[k, shard] = stage[k].astype(jnp.bfloat16)

        def serve_x(k):
            x_arrival(k).wait_recv()
            y_copy(k).start()
            if k not in by_z:
                d_copy(k).start()

        def serve_y(k):
            y_arrival(k).wait_recv()
            if k in by_z:
                z_copy(k).start()
                d_copy(k).start()
            else:
                e_copy(k).start()

        def serve_z(k):
            z_arrival(k).wait_recv()
            e_copy(k).start()

        def w_store(k):
            if k < 8:
                return pltpu.make_async_copy(w_all.at[k], w_all_out.at[k], w_sem.at[k])
            return pltpu.make_async_copy(w_all.at[k], wf_out.at[:, k - 8], w_sem.at[k])

        def complete(k):
            core_arrival(k).wait_recv()
            d_copy(k, far).wait_recv()
            e_copy(k, far).wait_recv()
            w_store(k).start()

        def weight(k):
            return w_all[k].reshape(4 * rows, D)

        for k in range(early):
            round_piece(k)
            send_piece(k)
        for k in range(early, pieces):
            round_piece(k)
        own_rows = pl.ds(pl.multiple_of(shard * p_rows, p_rows), p_rows)
        kv = (kp, vp)

        def kv_part(t, g, block):
            lanes = pl.ds(g * chunk if isinstance(g, int) else pl.multiple_of(g * chunk, chunk), chunk)
            return kv[t].at[pl.ds(pl.multiple_of(block * p_rows, p_rows), p_rows), lanes]

        def kv_core(t, g):
            return remote(kv_part(t, g, shard), kc_s.at[g, t], kc_r.at[g, t], partner)

        def kv_across(t, g):
            return remote(kv_part(t, g, shard), kx_s.at[g, t], kx_r.at[g, t], across)

        def kv_forward(t, g):
            return remote(kv_part(t, g, there), kd_s.at[g, t], kd_r.at[g, t], partner)

        serve_x(0)
        serve_x(1)
        serve_y(0)
        complete(0)
        kp[own_rows, :] = dot_plain(xp[...], weight(0)).astype(jnp.bfloat16)
        kc[...] = dot_plain(xc[...], weight(0)).astype(jnp.bfloat16)
        serve_x(2)
        serve_y(1)
        complete(1)
        vp[own_rows, :] = (dot_plain(xp[...], weight(1)) + bias[1:2, :]).astype(jnp.bfloat16)
        waiting = list(range(early, pieces))
        for g in range(chunks):
            for t in range(2):
                kv_across(t, g).start()
                kv_core(t, g).start()
            for k in waiting[: 2 if g < chunks - 1 else pieces]:
                send_piece(k)
            waiting = waiting[2:]
        vc[...] = (dot_plain(xc[...], weight(1)) + bias[1:2, :]).astype(jnp.bfloat16)
        serve_y(2)
        serve_x(3)
        complete(2)
        q[:p_rows, :] = (dot_plain(xp[...], weight(2)) + bias[0:1, :]).astype(jnp.bfloat16)
        q[p_rows:, :] = (dot_plain(xc[...], weight(2)) + bias[0:1, :]).astype(jnp.bfloat16)

        def keep(ref, target, i):
            return pltpu.make_async_copy(ref, target, out_sem.at[i])

        kept = [(q, q_out, 0), (kc, kc_out, 1), (vc, vc_out, 2)]
        for item in kept:
            keep(*item).start()

        def serve_kv(g):
            for t in range(2):
                remote(kv_part(t, g, there), kx_s.at[g, t], kx_r.at[g, t], across).wait_recv()
                kv_forward(t, g).start()

        def complete_kv(g):
            for t in range(2):
                remote(
                    kv_part(t, g, 2 * x + 1 - core), kc_s.at[g, t], kc_r.at[g, t], partner
                ).wait_recv()
                remote(kv_part(t, g, far), kd_s.at[g, t], kd_r.at[g, t], partner).wait_recv()

        serve_kv(0)
        arrive = {4: 26.3, 5: 27.9, 6: 35.2, 7: 36.8, 8: 44.1, 9: 45.7, 10: 48.9, 11: 52.1}
        work = [(33.6, serve_kv, 1), (42.4, serve_kv, 2), (27.0, serve_y, 3), (30.0, complete, 3)]
        for k in range(4, pieces):
            at = arrive[k]
            work.append((at, serve_x, k))
            if k in by_z:
                work += [(at + 4, serve_y, k), (at + 10, serve_z, k), (at + 13, complete, k)]
            else:
                work += [(at + 6, serve_y, k), (at + 9, complete, k)]
        slots = pairs * tiles
        work.sort(key=lambda item: item[0])
        later = [item for item in work if item[0] > 26 + 1.37 * slots]
        work = [(max(0, round((at - 26) / 1.37 - 0.6)), job, k) for at, job, k in work if at <= 26 + 1.37 * slots]
        work = [(min(slot, slots - 1), job, k) for slot, job, k in work]

        def att_store(p):
            lanes = pl.ds(pl.multiple_of(p * PAIR, PAIR), PAIR)
            return pltpu.make_async_copy(att.at[:, lanes], att_out.at[:, lanes], out_sem.at[5 + p])

        def pair(p, carry):
            @pl.when(p % 2 == 0)
            def _():
                complete_kv(p // 2)

            def between(tile):
                for slot, action, k in work:
                    if slot < slots and slot % tiles == tile:

                        @pl.when(p == slot // tiles)
                        def _(action=action, k=k):
                            action(k)

            lanes = pl.ds(pl.multiple_of(p * PAIR, PAIR), PAIR)
            attend_fwd_pair(
                shard,
                p_rows,
                q.at[:, lanes],
                kp.at[:, lanes],
                vp.at[:, lanes],
                kc.at[:, lanes],
                vc.at[:, lanes],
                att.at[:, lanes],
                lse.at[p],
                between,
            )
            att_store(p).start()
            return carry

        lax.fori_loop(0, pairs, pair, 0)
        kept += [(kp, kp_out, 3), (vp, vp_out, 4)]
        for item in kept[3:]:
            keep(*item).start()

        def row(i):
            return pl.ds(pl.multiple_of(i * TILE, TILE), TILE)

        def row_stores(i):
            pairs_of = [(norm1, norm_out), (x1_b, x1_out), (att_b, att_b_out)]
            return [
                pltpu.make_async_copy(ref.at[row(i), :], out.at[row(i), :], row_sem.at[n, i])
                for n, (ref, out) in enumerate(pairs_of)
            ]

        def normalized(i, carry):
            part = att[row(i), :].astype(jnp.bfloat16)
            att_b[row(i), :] = part
            values = dot_plain(part, weight(3)) + bias[2:3, :] + norm1[row(i), :]
            center = values - jnp.mean(values, -1, keepdims=True)
            spread = jnp.mean(center * center, -1, keepdims=True)
            scale = lax.rsqrt(spread + 1e-05)
            hat = center * scale
            norm1[row(i), :] = hat
            rstd_out[row(i), :] = jnp.broadcast_to(scale, (TILE, 128))
            x1_b[row(i), :] = (hat * gain[0:1, :] + bias[4:5, :]).astype(jnp.bfloat16)
            for copy in row_stores(i):
                copy.start()
            return carry

        norm1[:p_rows, :] = xp[...].astype(jnp.float32)
        norm1[p_rows:, :] = xc[...].astype(jnp.float32)
        lax.fori_loop(0, steps, normalized, 0)

        def ff_stores(i):
            columns = pl.ds(pl.multiple_of(i * TILE, TILE), TILE)
            return [
                pltpu.make_async_copy(ref.at[:, columns], out.at[:, columns], ff_sem.at[n, i])
                for n, (ref, out) in enumerate([(act, act_out), (slope, slope_out)])
            ]

        def inner(i, carry):
            lanes = pl.ds(pl.multiple_of(lax.rem(i, wide) * TILE, TILE), TILE)
            columns = pl.ds(pl.multiple_of(i * TILE, TILE), TILE)
            block = w_all[4 + i // wide, :, :, lanes].reshape(D, TILE)
            hidden = dot_plain(x1_b[...], block) + b_in[:, columns]
            cdf = 0.5 * (1.0 + lax.erf(hidden * 2.0 ** (-0.5)))
            act[:, columns] = (hidden * cdf).astype(jnp.bfloat16)
            density = jnp.exp(hidden * hidden * (-0.5)) * 0.3989422804014327
            slope[:, columns] = (cdf + hidden * density).astype(jnp.bfloat16)
            for copy in ff_stores(i):
                copy.start()
            for at, job, k in later:
                step = min(max(0, round((at - 54.5) / 0.73 - 0.5)), inner_steps - 1)
                pl.when(i == step)(functools.partial(job, k))
            return carry

        lax.fori_loop(0, inner_steps, inner, 0)

        def ff_wait(i, carry):
            for copy in ff_stores(i):
                copy.wait()
            return carry

        lax.fori_loop(0, inner_steps, ff_wait, 0)

        def row_wait(i, carry):
            for copy in row_stores(i):
                copy.wait()
            return carry

        lax.fori_loop(0, steps, row_wait, 0)
        for item in kept:
            keep(*item).wait()

        def last_pair(p, carry):
            att_store(p).wait()
            return carry

        lax.fori_loop(0, pairs, last_pair, 0)
        for k in range(pieces):
            w_store(k).wait()
            for copy in (core_copy, x_copy, y_copy, d_copy, e_copy):
                copy(k).wait_send()
            if k in by_z:
                z_copy(k).wait_send()
        for g in range(chunks):
            for t in range(2):
                for copy in (kv_core, kv_across, kv_forward):
                    copy(t, g).wait_send()

    def sems(*dims):
        return pltpu.SemaphoreType.DMA(dims)

    def low(*dims):
        return jax.ShapeDtypeStruct(dims, jnp.bfloat16)

    anywhere = pl.BlockSpec(memory_space=pl.ANY)
    vmem = pl.BlockSpec(memory_space=pltpu.VMEM)
    n = pieces
    out = pl.pallas_call(
        kernel,
        in_specs=[vmem, vmem, anywhere, anywhere, anywhere, anywhere, vmem, vmem, vmem],
        out_specs=[anywhere] * 13 + [vmem] * 2,
        out_shape=[
            low(8, 4, rows, D),
            low(4, 4, rows, D),
            low(tokens, D),
            low(cont_len, D),
            low(cont_len, D),
            low(p_len, D),
            low(p_len, D),
            jax.ShapeDtypeStruct((tokens, D), jnp.float32),
            jax.ShapeDtypeStruct((tokens, D), jnp.float32),
            low(tokens, D),
            low(tokens, ff),
            low(tokens, ff),
            low(tokens, D),
            jax.ShapeDtypeStruct((pairs, 8, tokens), jnp.float32),
            jax.ShapeDtypeStruct((tokens, 128), jnp.float32),
        ],
        scratch_shapes=[
            pltpu.VMEM((n, rows, D), jnp.float32),
            pltpu.VMEM((n, 4, rows, D), jnp.bfloat16),
            pltpu.VMEM((tokens, D), jnp.bfloat16),
            pltpu.VMEM((cont_len, D), jnp.bfloat16),
            pltpu.VMEM((cont_len, D), jnp.bfloat16),
            pltpu.VMEM((p_len, D), jnp.bfloat16),
            pltpu.VMEM((p_len, D), jnp.bfloat16),
            pltpu.VMEM((tokens, D), jnp.float32),
            pltpu.VMEM((tokens, D), jnp.float32),
            pltpu.VMEM((tokens, D), jnp.bfloat16),
            pltpu.VMEM((tokens, ff), jnp.bfloat16),
            pltpu.VMEM((tokens, ff), jnp.bfloat16),
            pltpu.VMEM((tokens, D), jnp.bfloat16),
        ]
        + [sems(n)] * 14
        + [sems(chunks, 2)] * 6
        + [sems(5 + pairs), sems(2, inner_steps), sems(3, steps)],
        compiler_params=pltpu.CompilerParams(
            collective_id=1, has_side_effects=True, vmem_limit_bytes=VMEM_ALL
        ),
        name="project_and_attend",
    )(prompt, conts, w_qkv, w_out, w_in, w_ffo, layer_biases, norm_gains, bias_in[None])
    w_all, wf, q, kc, vc, kp, vp, att, norm1, x1_b, act, slope, att_b, lse, rstd1 = out
    w_all = w_all.reshape(8, 4 * rows, D)
    wf = wf.reshape(4, 4 * rows, D)
    return w_all, wf, q, kp, vp, kc, vc, att, lse, (norm1, rstd1, x1_b, act, slope, att_b)


def project_native(
    prompt, conts, w_qkv, w_out, w_in, w_ffo, layer_biases, norm_gains, bias_in
):
    rows = prompt.shape[0]

    def gathered(value):
        return lax.all_gather(value.astype(jnp.bfloat16), "shard", axis=0, tiled=True)

    qkv, out, inner, ffo = (gathered(w) for w in (w_qkv, w_out, w_in, w_ffo))
    tokens = jnp.concatenate([prompt, conts], 0)
    bias = jnp.concatenate([layer_biases[0], jnp.zeros((D,), jnp.float32), layer_biases[1]])
    qkv_b = (dot_plain(tokens, qkv) + bias).astype(jnp.bfloat16)
    q, keys, values = (qkv_b[:, i * D : (i + 1) * D] for i in range(3))
    kp, vp = gathered(keys[:rows]), gathered(values[:rows])
    kc, vc = keys[rows:], values[rows:]
    att, lse = attend_forward(q, kp, vp, kc, vc, rows)
    blocks = [qkv[:, D : 2 * D], qkv[:, 2 * D :], qkv[:, :D], out]
    blocks += [inner[:, i * D : (i + 1) * D] for i in range(inner.shape[1] // D)]
    att_b = att.astype(jnp.bfloat16)
    values = tokens.astype(jnp.float32) + dot_plain(att_b, out) + layer_biases[2]
    center = values - jnp.mean(values, -1, keepdims=True)
    scale = lax.rsqrt(jnp.mean(center * center, -1, keepdims=True) + 1e-05)
    norm1 = center * scale
    x1_b = (norm1 * norm_gains[0] + layer_biases[4]).astype(jnp.bfloat16)
    hidden = dot_plain(x1_b, inner) + bias_in
    cdf = 0.5 * (1.0 + lax.erf(hidden * 2.0 ** (-0.5)))
    density = jnp.exp(hidden * hidden * (-0.5)) * 0.3989422804014327
    act = (hidden * cdf).astype(jnp.bfloat16)
    slope = (cdf + hidden * density).astype(jnp.bfloat16)
    rstd1 = jnp.broadcast_to(scale, (tokens.shape[0], 128))
    state = (norm1, rstd1, x1_b, act, slope, att_b)
    ffo = ffo.reshape(-1, D, D)
    return jnp.stack(blocks), ffo, q, kp, vp, kc, vc, att, lse, state


def student_head(label, stu, vectors, w_pool, w_class, bias_class, classes):
    part_w = STU // SHEADS
    low_half = lax.broadcasted_iota(jnp.int32, stu.shape, 1) < part_w
    row_low = lax.broadcasted_iota(jnp.int32, (1, STU), 1) < part_w
    query, bias_pool = vectors[1:2, :], vectors[2:3, :]

    def by_head(values):
        low_sum = jnp.sum(jnp.where(low_half[: values.shape[0]], values, 0.0), 1, keepdims=True)
        high_sum = jnp.sum(jnp.where(low_half[: values.shape[0]], 0.0, values), 1, keepdims=True)
        return jnp.where(low_half[: values.shape[0]], low_sum, high_sum)

    scores = by_head(stu * query) * part_w ** (-0.5)
    largest = jnp.max(scores, 0, keepdims=True)
    expo = jnp.exp(scores - largest)
    weights = expo / jnp.sum(expo, 0, keepdims=True)
    pooled = jnp.sum(weights * stu, 0, keepdims=True)

    square = (STU, STU)
    on_diagonal = lax.broadcasted_iota(jnp.int32, square, 0) == lax.broadcasted_iota(
        jnp.int32, square, 1
    )

    def column(row):
        return jnp.sum(jnp.where(on_diagonal, row, 0.0), 1, keepdims=True)

    def times(row, matrix):
        return jnp.sum(column(row) * matrix, 0, keepdims=True)

    def times_turned(row, matrix):
        total = jnp.sum(matrix * row, 1, keepdims=True)
        return jnp.sum(jnp.where(on_diagonal, total, 0.0), 0, keepdims=True)

    top = jnp.tanh(times(pooled, w_pool) + bias_pool)
    lane = lax.broadcasted_iota(jnp.int32, (1, STU), 1)
    logits = times_turned(top, w_class) + bias_class
    seen = jnp.where(lane < classes, logits, NEG_BIG)
    expo_l = jnp.exp(seen - jnp.max(seen, 1, keepdims=True))
    g_logits = expo_l / jnp.sum(expo_l, 1, keepdims=True) - jnp.where(lane == label, 1.0, 0.0)
    g_class = column(g_logits) * top
    g_pre = times(g_logits, w_class) * (1.0 - top * top)
    g_pool = column(pooled) * g_pre
    g_pooled = times_turned(g_pre, w_pool)
    g_weights = by_head(stu * g_pooled)
    mean = jnp.sum(weights * g_weights, 0, keepdims=True)
    g_scores = weights * (g_weights - mean) * part_w ** (-0.5)
    g_stu = weights * g_pooled + g_scores * query
    g_query = jnp.sum(g_scores * stu, 0, keepdims=True)
    return logits, g_stu, g_query, g_pre, g_pool, g_class, g_logits


def middle(
    ahead, state, prompt_cot, cont_cot, labels, w_all, wf,
    biases, gains, bias_in, student, vectors, w_pool, w_class, bias_class,
):
    p_rows, cont_len = prompt_cot.shape[0], cont_cot.shape[0]
    tokens = p_rows + cont_len
    ff = bias_in.shape[0]
    blocks = ff // D
    steps = tokens // TILE
    wide = D // TILE
    classes = w_class.shape[1]
    g_names = 2 * blocks + 1

    def kernel(
        label_ref, norm_h, rstd_h, x1_h, act_h, slope_h, att_b_h, cp, cc, w_h, wf_h, bias, gain, w_stu, vec, w_p, w_c, b_c,
        out_p, out_c, logits_out, grads_h, g_r1_h, g_att_h, small, totals_h,
        cot_v, out_v, w_c_v, b_c_v, att_b, w_v, wf_v, norm1, norm2, rstd1, rstd2, x1_b, act, slope, g_res, g_ffn, g_br, g_stu_b, grads,
        sums, in_sum, load, store, *links,
    ):
        def fetch(source, target, i):
            return pltpu.make_async_copy(source, target, load.at[i])

        loads = [
            fetch(act_h, act, 0),
            fetch(wf_h, wf_v, 1),
            fetch(norm_h, norm1, 2),
            fetch(cp, cot_v.at[:p_rows], 3),
            fetch(cc, cot_v.at[p_rows:], 4),
            fetch(slope_h, slope, 5),
            fetch(x1_h, x1_b, 6),
            fetch(rstd_h, rstd1, 7),
            fetch(w_h.at[pl.ds(3, 1 + blocks)], w_v, 8),
            fetch(att_b_h, att_b, 9),
        ]
        for copy in loads:
            copy.start()
        rows = D // blocks
        if ahead:
            (cr, xr, c_s, c_r, x_s, x_r) = links
            rep, shard = lax.axis_index("rep"), lax.axis_index("shard")
            x, core = shard // 2, shard % 2
            partner = (rep, 2 * x + 1 - core)
            across = (rep, 2 * (1 - x) + core)
            barrier = pltpu.get_barrier_semaphore()
            for other in (partner, across):
                pl.semaphore_signal(barrier, inc=1, device_id=other, device_id_type=MESH_ID)
            pl.semaphore_wait(barrier, 2)

            def remote(source, target, send, recv, device):
                return pltpu.make_async_remote_copy(
                    src_ref=source,
                    dst_ref=target,
                    send_sem=send,
                    recv_sem=recv,
                    device_id=device,
                    device_id_type=MESH_ID,
                )

            def core_copy(k, xx):
                block = pl.ds(pl.multiple_of((2 * xx + 1 - core) * rows, 16), rows)
                return remote(
                    grads.at[k, block, :], cr.at[k, xx], c_s.at[k, xx], c_r.at[k, xx], partner
                )

            def mine(xx):
                return pl.ds(pl.multiple_of((2 * xx + core) * rows, 16), rows)

            def x_copy(k):
                return remote(grads.at[k, mine(1 - x), :], xr.at[k], x_s.at[k], x_r.at[k], across)

        def stage_x():
            for k in range(ahead):
                for xx in range(2):
                    core_copy(k, xx).wait_recv()
                block = mine(1 - x)
                total = grads[k, block, :].astype(jnp.float32) + cr[k, 1 - x].astype(jnp.float32)
                grads[k, block, :] = total.astype(jnp.bfloat16)
                x_copy(k).start()

        sums[...] = jnp.zeros_like(sums)
        small[...] = jnp.zeros_like(small)

        def row(i):
            return pl.ds(pl.multiple_of(i * TILE, TILE), TILE)

        def loop(count):
            def run(step):
                def body(i, carry):
                    step(i)
                    return carry

                lax.fori_loop(0, count, body, 0)

            return run

        def normalize(values):
            center = values - jnp.mean(values, -1, keepdims=True)
            spread = jnp.mean(center * center, -1, keepdims=True)
            scale = lax.rsqrt(spread + 1e-05)
            return center * scale, scale

        def norm_back(g, gain_row, hat, scale):
            gg = g * gain_row
            return scale * (
                gg
                - jnp.mean(gg, -1, keepdims=True)
                - hat * jnp.mean(gg * hat, -1, keepdims=True)
            )

        def add_sum(i, values):
            sums[i : i + 1, :] += jnp.sum(values, 0, keepdims=True)

        for i in range(3):
            loads[i].wait()

        @loop(steps)
        def _(i):
            ffn = bias[3:4, :]
            for j in range(blocks):
                ffn = ffn + dot_plain(act[row(i), j * D : (j + 1) * D], wf_v[j])
            first = norm1[row(i), :] * gain[0:1, :] + bias[4:5, :]
            hat, scale = normalize(first + ffn)
            norm2[row(i), :] = hat
            rstd2[row(i), :] = jnp.broadcast_to(scale, (TILE, 128))
            out_v[row(i), :] = (hat * gain[1:2, :] + bias[5:6, :]).astype(jnp.bfloat16)

        out_stores = [
            pltpu.make_async_copy(out_v.at[:p_rows], out_p, store.at[g_names + 2]),
            pltpu.make_async_copy(out_v.at[p_rows:], out_c, store.at[g_names + 3]),
        ]
        for copy in out_stores:
            copy.start()
        base = 8 * (D // 128) + ff // 128
        w_stu_b = w_stu[...].astype(jnp.bfloat16)

        w_c_v[...] = jnp.zeros_like(w_c_v)
        b_c_v[...] = jnp.zeros_like(b_c_v)
        w_c_v[:classes, :] = w_c[...]
        b_c_v[:1, :classes] = b_c[...]

        @pl.when(lax.axis_index("rep") >= 0)
        def _():
            stu = dot_plain(out_v[p_rows:, :], w_stu_b) + vec[0:1, :]
            logits, g_stu, g_query, g_pre, g_pool, g_class, g_logits = student_head(
                label_ref[0, 0], stu, vec, w_p[...], w_c_v[...], b_c_v[:1, :], classes
            )
            logits_out[...] = logits[:, :classes]
            low = g_stu.astype(jnp.bfloat16)
            g_stu_b[:p_rows, :] = jnp.zeros((p_rows, STU), jnp.bfloat16)
            g_stu_b[p_rows:, :] = low
            small[base : base + 1, STU:] = jnp.sum(low.astype(jnp.float32), 0, keepdims=True)
            small[base + 1 : base + 2, STU:] = g_query
            small[base + 2 : base + 3, STU:] = g_pre
            small[base + 3 : base + 4, STU:] = g_logits
            small[base + 8 : base + 8 + STU, STU:] = g_pool
            small[base + 8 + STU : base + 24 + STU, STU:] = g_class[:16]

        small[:, :STU] = dot_first(out_v[p_rows:, :], g_stu_b[p_rows:, :])
        for i in range(3, 10):
            loads[i].wait()

        @loop(steps)
        def _(i):
            g = cot_v[row(i), :].astype(jnp.float32) + dot_second(g_stu_b[row(i), :], w_stu_b)
            hat = norm2[row(i), :]
            add_sum(7, g * hat)
            add_sum(5, g)
            g_r2 = norm_back(g, gain[1:2, :], hat, rstd2[row(i), :1])
            g_res[row(i), :] = g_r2
            low = g_r2.astype(jnp.bfloat16)
            g_ffn[row(i), :] = low
            add_sum(3, low.astype(jnp.float32))

        def piece_store(k):
            return pltpu.make_async_copy(grads.at[k], grads_h.at[k], store.at[k])


        @loop(blocks)
        def _(j):
            columns = pl.ds(pl.multiple_of(j * D, D), D)
            product = dot_first(act[:, columns], g_ffn[...]).astype(jnp.bfloat16)
            for k in range(blocks):
                target = pl.ds(pl.multiple_of(j * rows, 16), rows)
                grads[k, target, :] = product[k * rows : (k + 1) * rows]

        for k in range(ahead):
            for xx in range(2):
                core_copy(k, xx).start()
        for k in range(ahead, blocks):
            piece_store(k).start()


        in_sum[...] = jnp.zeros_like(in_sum)

        @loop(steps)
        def _(i):
            for j in range(blocks):
                columns = slice(j * D, (j + 1) * D)
                g_act = dot_second(g_ffn[row(i), :], wf_v[j])
                low = (g_act * slope[row(i), columns].astype(jnp.float32)).astype(jnp.bfloat16)
                slope[row(i), columns] = low
                in_sum[:, columns] += jnp.sum(low.astype(jnp.float32), 0, keepdims=True)
            if ahead:
                pl.when(i == 0)(stage_x)

        @loop(blocks)
        def _(j):
            columns = pl.ds(pl.multiple_of(j * D, D), D)
            grads[blocks + j] = dot_first(x1_b[...], slope[:, columns]).astype(jnp.bfloat16)
            piece_store(blocks + j).start()

        @loop(steps)
        def _(i):
            g = g_res[row(i), :]
            for j in range(blocks):
                g += dot_second(slope[row(i), j * D : (j + 1) * D], w_v[1 + j])
            hat = norm1[row(i), :]
            add_sum(6, g * hat)
            add_sum(4, g)
            g_r1 = norm_back(g, gain[0:1, :], hat, rstd1[row(i), :1])
            g_res[row(i), :] = g_r1
            low = g_r1.astype(jnp.bfloat16)
            g_br[row(i), :] = low
            add_sum(2, low.astype(jnp.float32))

        res_store = pltpu.make_async_copy(g_res, g_r1_h, store.at[g_names])
        res_store.start()
        g_ffn[...] = dot_second(g_br[...], w_v[0]).astype(jnp.bfloat16)
        att_store = pltpu.make_async_copy(g_ffn, g_att_h, store.at[g_names + 1])
        att_store.start()
        grads[2 * blocks] = dot_first(att_b[...], g_br[...]).astype(jnp.bfloat16)
        piece_store(2 * blocks).start()
        spread = D // 128
        for i in range(8):
            for part in range(spread):
                small[i * spread + part : i * spread + part + 1, STU:] = sums[
                    i : i + 1, part * 128 : (part + 1) * 128
                ]
        for part in range(ff // 128):
            at = 8 * spread + part
            small[at : at + 1, STU:] = in_sum[:, part * 128 : (part + 1) * 128]
        res_store.wait()
        att_store.wait()
        for copy in out_stores:
            copy.wait()
        for k in range(ahead):
            x_copy(k).wait_recv()
            total = grads[k, mine(x), :].astype(jnp.float32) + cr[k, x].astype(jnp.float32)
            cr[k, x] = (total + xr[k].astype(jnp.float32)).astype(jnp.bfloat16)
            pltpu.make_async_copy(cr.at[k, x], totals_h.at[k], store.at[k]).start()
        for k in range(ahead, g_names):
            piece_store(k).wait()
        for k in range(ahead):
            pltpu.make_async_copy(cr.at[k, x], totals_h.at[k], store.at[k]).wait()
            for xx in range(2):
                core_copy(k, xx).wait_send()
            x_copy(k).wait_send()

    anywhere = pl.BlockSpec(memory_space=pl.ANY)
    vmem = pl.BlockSpec(memory_space=pltpu.VMEM)
    low = jnp.bfloat16

    def shaped(dims, kind=jnp.float32):
        return jax.ShapeDtypeStruct(dims, kind)

    params = pltpu.CompilerParams(vmem_limit_bytes=VMEM_ALL)
    link_scratch = []
    if ahead:
        params = pltpu.CompilerParams(
            collective_id=3, has_side_effects=True, vmem_limit_bytes=VMEM_ALL
        )
        piece = (D // blocks, D)
        link_scratch = [
            pltpu.VMEM((ahead, 2, *piece), low),
            pltpu.VMEM((ahead, *piece), low),
        ]
        link_scratch += [pltpu.SemaphoreType.DMA((ahead, 2))] * 2
        link_scratch += [pltpu.SemaphoreType.DMA((ahead,))] * 2

    return pl.pallas_call(
        kernel,
        in_specs=[pl.BlockSpec(memory_space=pltpu.SMEM)] + [anywhere] * 10 + [vmem] * 7,
        out_specs=[anywhere, anywhere, vmem, anywhere, anywhere, anywhere, vmem, anywhere],
        out_shape=[
            shaped((p_rows, D), low),
            shaped((cont_len, D), low),
            shaped((1, classes)),
            shaped((g_names, D, D), low),
            shaped((tokens, D)),
            shaped((tokens, D), low),
            shaped((D, 2 * STU)),
            shaped((max(ahead, 1), D // blocks, D), low),
        ],
        scratch_shapes=[
            pltpu.VMEM((tokens, D), low),
            pltpu.VMEM((tokens, D), low),
            pltpu.VMEM((STU, STU), jnp.float32),
            pltpu.VMEM((8, STU), jnp.float32),
            pltpu.VMEM((tokens, D), low),
            pltpu.VMEM((1 + blocks, D, D), low),
            pltpu.VMEM((blocks, D, D), low),
            pltpu.VMEM((tokens, D), jnp.float32),
            pltpu.VMEM((tokens, D), jnp.float32),
            pltpu.VMEM((tokens, 128), jnp.float32),
            pltpu.VMEM((tokens, 128), jnp.float32),
            pltpu.VMEM((tokens, D), low),
            pltpu.VMEM((tokens, ff), low),
            pltpu.VMEM((tokens, ff), low),
            pltpu.VMEM((tokens, D), jnp.float32),
            pltpu.VMEM((tokens, D), low),
            pltpu.VMEM((tokens, D), low),
            pltpu.VMEM((tokens, STU), low),
            pltpu.VMEM((g_names, D, D), low),
            pltpu.VMEM((8, D), jnp.float32),
            pltpu.VMEM((1, ff), jnp.float32),
            pltpu.SemaphoreType.DMA((10,)),
            pltpu.SemaphoreType.DMA((g_names + 4,)),
        ]
        + link_scratch,
        compiler_params=params,
        name="middle",
    )(
        labels,
        *state,
        prompt_cot,
        cont_cot,
        w_all,
        wf,
        biases,
        gains,
        student,
        vectors,
        w_pool,
        w_class.T,
        bias_class[None],
    )


def sum_native(g9, g_qkvw, small):
    blocks = (g9.shape[0] - 1) // 2
    rows = D // blocks
    ffo = g9[:blocks].reshape(blocks, blocks, rows, D).transpose(1, 0, 2, 3).reshape(-1, D)
    inner = jnp.concatenate([g9[blocks + j] for j in range(blocks)], 1)

    def over(grad):
        part = lax.psum_scatter(
            grad.astype(jnp.bfloat16), "shard", scatter_dimension=0, tiled=True
        )
        return lax.psum(part, "rep").astype(jnp.float32)

    owned = tuple(over(grad) for grad in (g_qkvw, g9[2 * blocks], inner, ffo))
    return owned, lax.psum(small, ("rep", "shard"))


def finish(
    ahead, totals, q, kp, vp, kc, vc, att, lse, g_att, g9, g_resid, small, w_all, prompt, conts, ff
):
    pieces, ready = 12, 9
    p_rows, cont_len = prompt.shape[0], conts.shape[0]
    tokens = p_rows + cont_len
    p_len = kp.shape[0]
    pairs = HEADS // 2
    rows = D // 4
    half, quarter = D // 2, rows // 4
    s_width = small.shape[1]
    chunk = 2 * PAIR
    chunks = D // chunk
    across_lanes = D // 128

    def kernel(
        q_h, kp_h, vp_h, kc_h, vc_h, att_h, g_att_h, g9, g_res_h, w_h, totals_h, ls, sm, xp, xc,
        out_pg, out_cg, out_q, out_o, out_i, out_f, fin_s,
        qv, kpv, vpv, kcv, vcv, attv, gav, accum, dq, dkp, dvp, dkc, dvc, kr, kx, kvs, wv, g_tok, made, head,
        own, cr, xr, yr, zr, fb, made_s, own_s, cr_s, xr_s, yr_s, zr_s, fb_s,
        load, sem_own, c_send, c_recv, x_send, x_recv, y_send, y_recv, z_send, z_recv,
        f_send, f_recv, o_send, o_recv, o_own, g_send, g_recv, kc_s, kc_r, kx_s, kx_r, out_sem,
    ):
        rep, shard = lax.axis_index("rep"), lax.axis_index("shard")
        z, y = rep // 2, rep % 2
        x, core = shard // 2, shard % 2
        partner = (rep, 2 * x + 1 - core)
        across = (rep, 2 * (1 - x) + core)
        beside = (2 * z + 1 - y, shard)
        far = (rep, 2 * (1 - x) + 1 - core)

        def along(step):
            return (2 * lax.rem(z + step, 4) + y, shard)

        def own_copy(k, xx):
            return pltpu.make_async_copy(
                g9.at[k, pl.ds(pl.multiple_of((2 * xx + core) * rows, 16), rows), :],
                own.at[k, xx],
                sem_own.at[k, xx],
            )

        fetched = [(q_h, qv), (kp_h, kpv), (vp_h, vpv), (kc_h, kcv), (vc_h, vcv)]
        fetched += [(att_h, attv), (g_att_h, gav), (w_h.at[pl.ds(0, 3)], wv), (g_res_h, g_tok)]

        def fetch(i):
            return pltpu.make_async_copy(*fetched[i], load.at[i])

        def total_copy(k):
            return pltpu.make_async_copy(totals_h.at[k], own.at[k, x], sem_own.at[k, 0])

        for k in range(ahead):
            total_copy(k).start()
        for k in range(ahead, ahead + 2):
            for xx in range(2):
                own_copy(k, xx).start()
        for i in range(7):
            fetch(i).start()
        for k in range(ahead + 2, ready):
            for xx in range(2):
                own_copy(k, xx).start()
        for i in (7, 8):
            fetch(i).start()

        barrier = pltpu.get_barrier_semaphore()
        others = [partner, across, beside, along(1), along(2), along(3), far]
        for other in others:
            pl.semaphore_signal(barrier, inc=1, device_id=other, device_id_type=MESH_ID)
        pl.semaphore_wait(barrier, len(others))

        def remote(source, target, send, recv, device):
            return pltpu.make_async_remote_copy(
                src_ref=source,
                dst_ref=target,
                send_sem=send,
                recv_sem=recv,
                device_id=device,
                device_id_type=MESH_ID,
            )

        big = (own, cr, xr, yr, zr, fb, half)
        narrow = (own_s, cr_s, xr_s, yr_s, zr_s, fb_s, s_width // 2)

        def bufs(k):
            if isinstance(k, int) and k == pieces:
                return narrow, 0
            return big, k

        def core_copy(k, xx):
            b, i = bufs(k)
            block = 2 * xx + 1 - core
            if not isinstance(k, int):
                source = b[1].at[i, xx]
            elif k < ready:
                source = g9.at[k, pl.ds(pl.multiple_of(block * rows, 16), rows), :]
            elif k < pieces:
                source = made.at[k - ready, block]
            else:
                source = made_s.at[block]
            return remote(source, b[1].at[i, xx], c_send.at[k, xx], c_recv.at[k, xx], partner)

        def x_copy(k):
            b, i = bufs(k)
            return remote(b[0].at[i, 1 - x], b[2].at[i], x_send.at[k], x_recv.at[k], across)

        def lanes_of(b, which):
            return pl.ds(pl.multiple_of(which * b[6], 128), b[6])

        def y_copy(k):
            b, i = bufs(k)
            source = b[0].at[i, x, :, lanes_of(b, 1 - y)]
            return remote(source, b[3].at[i], y_send.at[k], y_recv.at[k], beside)

        def rows_of(which):
            return pl.ds(pl.multiple_of(which * quarter, 16), quarter)

        def zs_copy(k, step):
            b, i = bufs(k)
            source = b[0].at[i, x, rows_of(lax.rem(z + step, 4)), lanes_of(b, y)]
            return remote(
                source, b[4].at[i, z], z_send.at[k, step - 1], z_recv.at[k, z], along(step)
            )

        def zr_wait(k, step):
            b, i = bufs(k)
            slot = lax.rem(z + step, 4)
            target = b[4].at[i, slot]
            remote(
                target, target, z_send.at[k, step - 1], z_recv.at[k, slot], along(step)
            ).wait_recv()

        def fs_copy(k, step):
            b, i = bufs(k)
            block = b[5].at[i, rows_of(z), :]
            return remote(block, block, f_send.at[k, step - 1], f_recv.at[k, z], along(step))

        def fr_wait(k, step):
            b, i = bufs(k)
            slot = lax.rem(z + step, 4)
            block = b[5].at[i, rows_of(slot), :]
            remote(
                block, block, f_send.at[k, step - 1], f_recv.at[k, slot], along(step)
            ).wait_recv()

        def final(k, yy):
            b, _ = bufs(k)
            if k < 4:
                return out_f.at[k * rows : (k + 1) * rows, lanes_of(b, yy)]
            if k == 8:
                return out_o.at[:, lanes_of(b, yy)]
            if k == pieces:
                return fin_s.at[shard, :, lanes_of(b, yy)]
            out, at = (out_i, (k - 4) * D) if k < 8 else (out_q, (k - 9) * D)
            return out.at[:, pl.ds(pl.multiple_of(at + yy * half, 128), half)]

        def o_copy(k):
            b, i = bufs(k)
            return remote(b[5].at[i], final(k, y), o_send.at[k], o_recv.at[k], beside)

        def o_wait(k):
            b, i = bufs(k)
            remote(b[5].at[i], final(k, 1 - y), o_send.at[k], o_recv.at[k], beside).wait_recv()

        def o_local(k):
            b, i = bufs(k)
            return pltpu.make_async_copy(b[5].at[i], final(k, y), o_own.at[k])

        def wide(value):
            return value.astype(jnp.float32)

        def stage_x(k):
            b, i = bufs(k)
            for xx in range(2):
                core_copy(k, xx).wait_recv()
                if not isinstance(k, int):
                    pl.when(k < ready)(own_copy(k, xx).wait)
            b[0][i, 1 - x] = (wide(b[0][i, 1 - x]) + wide(b[1][i, 1 - x])).astype(jnp.bfloat16)
            x_copy(k).start()

        def stage_y(k):
            b, i = bufs(k)
            x_copy(k).wait_recv()
            total = wide(b[0][i, x]) + wide(b[1][i, x]) + wide(b[2][i])
            b[0][i, x] = total.astype(jnp.bfloat16)
            y_copy(k).start()

        def stage_z(k):
            b, i = bufs(k)
            y_copy(k).wait_recv()
            lanes = lanes_of(b, y)
            total = wide(b[0][i, x, :, lanes]) + wide(b[3][i])
            b[0][i, x, :, lanes] = total.astype(jnp.bfloat16)
            for step in (2, 1, 3):
                zs_copy(k, step).start()

        def stage_f(k):
            b, i = bufs(k)
            total = wide(b[0][i, x, rows_of(z), lanes_of(b, y)])
            for step in (1, 2, 3):
                zr_wait(k, step)
                total += wide(b[4][i, lax.rem(z + step, 4)])
            b[5][i, rows_of(z), :] = total.astype(jnp.bfloat16)
            for step in (2, 1, 3):
                fs_copy(k, step).start()

        def stage_o(k):
            for step in (1, 2, 3):
                fr_wait(k, step)
            for kk in range(pieces + 1) if not isinstance(k, int) else [k]:

                def begin(kk=kk):
                    o_copy(kk).start()
                    o_local(kk).start()

                if isinstance(k, int):
                    begin()
                else:
                    pl.when(k == kk)(begin)

        def send_core(k):
            for xx in range(2):
                core_copy(k, xx).start()

        for k in range(ahead, ready):
            send_core(k)

        def stages_x(first, last):
            def step(k, carry):
                stage_x(k)
                return carry

            lax.fori_loop(first, last, step, 0)

        for k in range(ahead):
            total_copy(k).wait()
            y_copy(k).start()
        stages_x(ahead, ahead + 2)
        kv = (dkp, dvp)

        def kv_rows(block):
            return pl.ds(pl.multiple_of(block * p_rows, p_rows), p_rows)

        def kv_lanes(g):
            return pl.ds(g * chunk if isinstance(g, int) else pl.multiple_of(g * chunk, chunk), chunk)

        def kv_core(t, g, xx):
            return remote(
                kv[t].at[kv_rows(2 * xx + 1 - core), kv_lanes(g)],
                kr.at[t, xx, :, kv_lanes(g)],
                kc_s.at[g, t, xx],
                kc_r.at[g, t, xx],
                partner,
            )

        def kv_across(t, g):
            return remote(
                kv[t].at[kv_rows(2 * (1 - x) + core), kv_lanes(g)],
                kx.at[t, :, kv_lanes(g)],
                kx_s.at[g, t],
                kx_r.at[g, t],
                across,
            )

        def serve_kv(g):
            block, lanes = kv_rows(2 * (1 - x) + core), kv_lanes(g)
            for t in range(2):
                for xx in range(2):
                    kv_core(t, g, xx).wait_recv()
                total = wide(kv[t][block, lanes]) + wide(kr[t, 1 - x, :, lanes])
                kv[t][block, lanes] = total.astype(jnp.bfloat16)
                kv_across(t, g).start()

        for i in range(7):
            fetch(i).wait()

        def pair(p, carry):
            def between(index):
                if index == 0:
                    pl.when(p + ahead + 2 < ready)(lambda: stage_x(p + ahead + 2))
                if index == 1:
                    pl.when((p == 2) | (p == 4))(lambda: serve_kv(p // 2 - 1))
                if index == 2:
                    pl.when(p >= 1)(lambda: stage_y(p + ahead - 1))
                if index == 3:
                    stage_z(p)
                if index == 4:
                    pl.when(p >= 1)(lambda: stage_f(p - 1))
                if index == 5:
                    pl.when(p >= 2)(lambda: stage_o(p - 2))

            lanes = pl.ds(pl.multiple_of(p * PAIR, PAIR), PAIR)

            def cut(ref):
                return ref.at[:, lanes]

            attend_bwd_pair(
                shard, p_rows, cut(qv), cut(kpv), cut(vpv), cut(kcv), cut(vcv), cut(gav), cut(attv),
                ls.at[p], cut(dq), cut(dkp), cut(dvp), cut(dkc), cut(dvc), accum, between,
            )

            @pl.when(p % 2 == 1)
            def _():
                for t in range(2):
                    for xx in range(2):
                        kv_core(t, p // 2, xx).start()

            return carry

        lax.fori_loop(0, pairs, pair, 0)

        def keep_piece(k, product):
            for block in range(4):
                made[k - ready, block] = product[block * rows : (block + 1) * rows]
            for xx in range(2):
                own[k, xx] = made[k - ready, 2 * xx + core]
            send_core(k)

        product = dot_first(xp[...], dq[:p_rows, :]) + dot_first(xc[...], dq[p_rows:, :])
        keep_piece(9, product.astype(jnp.bfloat16))
        serve_kv(chunks - 1)
        for i in (7, 8):
            fetch(i).wait()
        stages_x(9, 10)
        g_tok[...] += dot_second(dq[...], wv[2])
        stores = [
            pltpu.make_async_copy(g_tok.at[:p_rows, :], out_pg, out_sem.at[0]),
            pltpu.make_async_copy(g_tok.at[p_rows:, :], out_cg, out_sem.at[1]),
        ]

        def with_kv():
            for g in range(chunks):
                for t in range(2):
                    kv_across(t, g).wait_recv()
            for t in range(2):
                total = wide(kv[t][kv_rows(shard), :]) + wide(kr[t, x]) + wide(kx[t])
                kvs[t] = total.astype(jnp.bfloat16)
            g_bias = jnp.sum(wide(dq[...]), 0, keepdims=True)
            v_bias = jnp.sum(wide(dvc[...]), 0, keepdims=True)
            v_bias += jnp.sum(wide(kvs[1]), 0, keepdims=True)
            head[...] = sm[:16, :]
            for part in range(across_lanes):
                lanes = slice(part * 128, (part + 1) * 128)
                head[part : part + 1, STU:] = g_bias[:, lanes]
                head[across_lanes + part : across_lanes + part + 1, STU:] = v_bias[:, lanes]
            for block in range(4):
                made_s[block] = sm[block * rows : (block + 1) * rows, :].astype(jnp.bfloat16)
            made_s[0, :16] = head[...].astype(jnp.bfloat16)
            for xx in range(2):
                own_s[0, xx] = made_s[2 * xx + core]
            send_core(pieces)
            for t in range(2):
                product = dot_first(xp[...], kvs[t]) + dot_first(xc[...], (dkc, dvc)[t][...])
                keep_piece(10 + t, product.astype(jnp.bfloat16))
            stage_x(pieces)
            stages_x(10, 12)
            g_tok[:p_rows, :] += dot_second(kvs[0], wv[0]) + dot_second(kvs[1], wv[1])
            for copy in stores:
                copy.start()

        def cont_part():
            g_tok[p_rows:, :] += dot_second(dkc[...], wv[0]) + dot_second(dvc[...], wv[1])

        def tick(n, carry):
            pl.when(n == 9)(with_kv)
            pl.when((n >= 8) & (n < pieces))(lambda: stage_y(n))
            pl.when(n == 10)(lambda: stage_y(pieces))
            pl.when(n < pieces + 1)(lambda: stage_z(n - 1))
            pl.when(n == 11)(lambda: stage_z(pieces))
            pl.when(n < pieces + 2)(lambda: stage_f(n - 2))
            pl.when(n == 12)(lambda: stage_f(pieces))
            stage_o(n - 3)
            pl.when(n == 13)(lambda: stage_o(pieces))
            pl.when(n == 7)(cont_part)
            return carry

        def g_copy(step):
            return remote(
                fin_s.at[shard],
                fin_s.at[shard],
                g_send.at[step - 1],
                g_recv.at[shard],
                (rep, lax.rem(shard + step, 4)),
            )

        def stage_g():
            o_wait(pieces)
            o_local(pieces).wait()
            for step in (1, 2, 3):
                g_copy(step).start()

        lax.fori_loop(pieces - 5, pieces + 3, tick, 0)
        stage_g()
        for step in (1, 2, 3):
            slot = lax.rem(shard + step, 4)
            remote(
                fin_s.at[slot], fin_s.at[slot], g_send.at[step - 1], g_recv.at[slot], far
            ).wait_recv()

        for k in range(pieces):
            o_wait(k)
            o_local(k).wait()
        for copy in stores:
            copy.wait()

        def sent(k):
            def two():
                for xx in range(2):
                    core_copy(k, xx).wait_send()
                x_copy(k).wait_send()

            if isinstance(k, int):
                two()
            else:
                pl.when(k >= ahead)(two)
            y_copy(k).wait_send()
            for step in (1, 2, 3):
                zs_copy(k, step).wait_send()
                fs_copy(k, step).wait_send()

        def sent_step(k, carry):
            sent(k)
            return carry

        lax.fori_loop(0, pieces, sent_step, 0)
        sent(pieces)
        for k in range(pieces + 1):
            o_copy(k).wait_send()
        for step in (1, 2, 3):
            g_copy(step).wait_send()
        for g in range(chunks):
            for t in range(2):
                for xx in range(2):
                    kv_core(t, g, xx).wait_send()
                kv_across(t, g).wait_send()

    def sems(*dims):
        return pltpu.SemaphoreType.DMA(dims)

    def low(*dims):
        return pltpu.VMEM(dims, jnp.bfloat16)

    def full(*dims):
        return pltpu.VMEM(dims, jnp.float32)

    def buffers(count, columns):
        cut = columns // 2
        return [
            low(count, 2, rows, columns),
            low(count, 2, rows, columns),
            low(count, rows, columns),
            low(count, rows, cut),
            low(count, 4, quarter, cut),
            low(count, rows, cut),
        ]

    def shaped(dims, kind=jnp.float32):
        return jax.ShapeDtypeStruct(dims, kind)

    n = pieces + 1
    anywhere = pl.BlockSpec(memory_space=pl.ANY)
    vmem = pl.BlockSpec(memory_space=pltpu.VMEM)
    return pl.pallas_call(
        kernel,
        in_specs=[anywhere] * 11 + [vmem] * 4,
        out_specs=[anywhere] * 6 + [vmem],
        out_shape=[
            shaped((p_rows, D)),
            shaped((cont_len, D)),
            shaped((rows, 3 * D), jnp.bfloat16),
            shaped((rows, D), jnp.bfloat16),
            shaped((rows, ff), jnp.bfloat16),
            shaped((4 * rows, D), jnp.bfloat16),
            shaped((4, rows, s_width), jnp.bfloat16),
        ],
        scratch_shapes=[
            low(tokens, D), low(p_len, D), low(p_len, D), low(cont_len, D), low(cont_len, D),
            full(tokens, D), low(tokens, D), full(PAIR, tokens), low(tokens, D),
            low(p_len, D), low(p_len, D), low(cont_len, D), low(cont_len, D),
            low(2, 2, p_rows, D), low(2, p_rows, D), low(2, p_rows, D), low(3, D, D),
            full(tokens, D), low(3, 4, rows, D), full(16, s_width),
        ]
        + buffers(pieces, D)
        + [low(4, rows, s_width)]
        + buffers(1, s_width)
        + [
            sems(9), sems(n, 2), sems(n, 2), sems(n, 2), sems(n), sems(n), sems(n), sems(n),
            sems(n, 3), sems(n, 4), sems(n, 3), sems(n, 4), sems(n), sems(n), sems(n),
            sems(3), sems(4), sems(chunks, 2, 2), sems(chunks, 2, 2), sems(chunks, 2),
            sems(chunks, 2), sems(2),
        ],
        compiler_params=pltpu.CompilerParams(
            collective_id=2, has_side_effects=True, vmem_limit_bytes=VMEM_ALL
        ),
        name="finish",
    )(q, kp, vp, kc, vc, att, g_att, g9, g_resid, w_all, totals, lse, small, prompt, conts)


def place(g_prompt, g_conts, owned, out_p, out_c, logits, summed, ff, classes):
    big = [g_prompt, g_conts, *owned, out_p, out_c]
    count = len(big)
    order = (2, 4, 5, 3, 1, 0, 7, 6)
    rows, across = summed.shape[1], D // 128

    def kernel(*refs):
        sources, fin, logits_in = refs[:count], refs[count], refs[count + 1]
        outs = refs[count + 2 :]
        targets = outs[:count]
        o_bias, o_gain, o_in, o_stu, o_vec, o_pool, o_class, o_cb, o_logits = outs[count : count + 9]
        scratch = outs[count + 9 :]
        held, turned, (sem_in, sem_out) = scratch[:count], scratch[count:-2], scratch[-2:]
        reads = [pltpu.make_async_copy(sources[i], held[i], sem_in.at[i]) for i in order]
        for copy in reads:
            copy.start()

        def side(block):
            return fin[block, :, STU:].astype(jnp.float32)

        first = side(0)
        for i in range(8):
            target, at = (o_bias, i) if i < 6 else (o_gain, i - 6)
            for part in range(across):
                r = i * across + part
                target[at : at + 1, part * 128 : (part + 1) * 128] = first[r : r + 1, :]
        for part in range(ff // 128):
            r = 8 * across + part
            o_in[:, part * 128 : (part + 1) * 128] = first[r : r + 1, :]
        base = 8 * across + ff // 128
        o_vec[...] = first[base : base + 3, :]
        o_cb[...] = first[base + 3 : base + 4, :classes]
        every = jnp.concatenate([first, side(1)], 0)
        o_pool[...] = every[base + 8 : base + 8 + STU, :]
        o_class[...] = every[base + 8 + STU : base + 8 + STU + classes, :]
        for block in range(4):
            o_stu[block * rows : (block + 1) * rows, :] = fin[block, :, :STU].astype(jnp.float32)
        writes = []
        o_logits[...] = logits_in[...]
        for copy, i in zip(reads, order):
            copy.wait()
            source = held[i]
            if 2 <= i < 6:
                source = turned[i - 2]
                source[...] = held[i][...].astype(jnp.float32)
            writes.append(pltpu.make_async_copy(source, targets[i], sem_out.at[i]))
            writes[-1].start()
        for copy in writes:
            copy.wait()

    def shaped(*dims):
        return jax.ShapeDtypeStruct(dims, jnp.float32)

    anywhere = pl.BlockSpec(memory_space=pl.ANY)
    vmem = pl.BlockSpec(memory_space=pltpu.VMEM)
    return pl.pallas_call(
        kernel,
        in_specs=[anywhere] * count + [vmem] * 2,
        out_specs=[anywhere] * count + [vmem] * 9,
        out_shape=[shaped(*part.shape) for part in big[:6]]
        + [jax.ShapeDtypeStruct(part.shape, part.dtype) for part in big[6:]]
        + [
            shaped(6, D),
            shaped(2, D),
            shaped(1, ff),
            shaped(D, STU),
            shaped(3, STU),
            shaped(STU, STU),
            shaped(classes, STU),
            shaped(1, classes),
            shaped(1, classes),
        ],
        scratch_shapes=[pltpu.VMEM(part.shape, part.dtype) for part in big]
        + [pltpu.VMEM(part.shape, jnp.float32) for part in owned]
        + [pltpu.SemaphoreType.DMA((count,)), pltpu.SemaphoreType.DMA((count,))],
        compiler_params=pltpu.CompilerParams(vmem_limit_bytes=VMEM_ALL),
        name="place",
    )(*big, summed, logits)


def body(
    prompt,
    conts,
    prompt_cot,
    cont_cot,
    labels,
    w_qkv,
    w_out,
    w_in,
    w_ffo,
    layer_biases,
    norm_gains,
    bias_in,
    w_student,
    student_vectors,
    w_pool,
    w_class,
    bias_class,
):
    prompt_rows = prompt.shape[1]
    direct = (lax.axis_size("rep"), lax.axis_size("shard")) == (8, 4)
    project = project_and_attend if direct else project_native
    w_all, ffo_full, q, kp, vp, kc, vc, attended, log_totals, state = project(
        prompt[0], conts[0, 0], w_qkv, w_out, w_in, w_ffo, layer_biases, norm_gains, bias_in
    )
    ahead = 3 if direct else 0
    out_p, out_c, logits, g9, g_resid, g_att, small, totals = middle(
        ahead,
        state,
        prompt_cot[0],
        cont_cot[0, 0],
        labels,
        w_all,
        ffo_full,
        layer_biases,
        norm_gains,
        bias_in,
        w_student,
        student_vectors,
        w_pool,
        w_class,
        bias_class,
    )
    ff, classes = bias_in.shape[0], w_class.shape[1]
    if direct:
        outs = finish(
            ahead, totals, q, kp, vp, kc, vc, attended, log_totals, g_att, g9, g_resid, small, w_all,
            prompt[0], conts[0, 0], ff,
        )
        placed = place(outs[0], outs[1], outs[2:6], out_p, out_c, logits, outs[6], ff, classes)
        g_prompt, g_conts, owned, out_p, out_c = placed[0], placed[1], placed[2:6], *placed[6:8]
        biases, gains_g, g_in, g_student, g_vectors, g_pool, g_class, g_cb, logits = placed[8:]
    else:
        g_q, g_kp, g_vp, g_kc, g_vc = attend_backward(
            q, kp, vp, kc, vc, g_att, attended, log_totals, prompt_rows
        )
        tokens = jnp.concatenate([prompt[0], conts[0, 0]], 0)
        kv_sum = [
            lax.psum_scatter(part, "shard", scatter_dimension=0, tiled=True)
            for part in (g_kp, g_vp)
        ]
        g_k = jnp.concatenate([kv_sum[0], g_kc], 0)
        g_v = jnp.concatenate([kv_sum[1], g_vc], 0)
        g_tokens = g_resid
        for part, weight in ((g_k, w_all[0]), (g_v, w_all[1]), (g_q, w_all[2])):
            g_tokens = g_tokens + dot_second(part, weight)
        g_prompt, g_conts = g_tokens[:prompt_rows], g_tokens[prompt_rows:]
        g_qkvw = jnp.concatenate([dot_first(tokens, part) for part in (g_q, g_k, g_v)], 1)
        side = small[:, STU:]
        across = D // 128
        for at, part in ((0, g_q), (1, g_v)):
            total = jnp.sum(part.astype(jnp.float32), 0).reshape(across, 128)
            side = lax.dynamic_update_slice(side, total, (at * across, 0))
        small = jnp.concatenate([small[:, :STU], side], 1)
        owned, summed = sum_native(g9, g_qkvw, small)
        side = summed[:, STU:]
        base = 8 * across + ff // 128
        biases = side[: 6 * across].reshape(6, D)
        gains_g = side[6 * across : 8 * across].reshape(2, D)
        g_in = side[8 * across : base]
        g_student, g_vectors = summed[:, :STU], side[base : base + 3]
        g_pool = side[base + 8 : base + 8 + STU]
        g_class = side[base + 8 + STU : base + 8 + STU + classes]
        g_cb = side[base + 3 : base + 4]
    return (
        out_p[None],
        out_c[None, None],
        logits[None],
        g_prompt[None],
        g_conts[None, None],
        *owned,
        biases,
        gains_g,
        g_in.reshape(ff),
        g_student,
        g_vectors,
        g_pool,
        g_class.T,
        g_cb[0, :classes],
    )


def solution(mesh):
    return jax.shard_map(
        body,
        mesh=mesh,
        in_specs=(
            P("rep", "shard", None),
            P("rep", "shard", None, None),
            P("rep", "shard", None),
            P("rep", "shard", None, None),
            P("rep", "shard"),
            P("shard", None),
            P("shard", None),
            P("shard", None),
            P("shard", None),
            P(),
            P(),
            P(),
            P(),
            P(),
            P(),
            P(),
            P(),
        ),
        out_specs=(
            P("rep", "shard", None),
            P("rep", "shard", None, None),
            P("rep", "shard", None),
            P("rep", "shard", None),
            P("rep", "shard", None, None),
            P("shard", None),
            P("shard", None),
            P("shard", None),
            P("shard", None),
            P(),
            P(),
            P(),
            P(),
            P(),
            P(),
            P(),
            P(),
        ),
        check_vma=False,
    )
```

```python
import functools

import jax
import jax.numpy as jnp
from jax import lax
from jax.experimental import pallas as pl
from jax.experimental.pallas import tpu as pltpu
from jax.sharding import PartitionSpec as P

D = 768
HEADS = 12
DH = 64
STU = 128
SHEADS = 2


HIGHEST = lax.Precision.HIGHEST
NEG_BIG = -1e30


def dot_plain(left, right):
    return jnp.dot(left, right, preferred_element_type=jnp.float32)


def dot_first(left, right):
    return lax.dot_general(
        left, right, (((0,), (0,)), ((), ())), preferred_element_type=jnp.float32
    )


def dot_second(left, right):
    return lax.dot_general(
        left, right, (((1,), (1,)), ((), ())), preferred_element_type=jnp.float32
    )


TILE = 256
PAIR = 128
VMEM_ALL = 62 * 1024 * 1024


def rows_dot(left, right):
    return lax.dot_general(
        left, right, (((1,), (1,)), ((), ())), preferred_element_type=jnp.float32
    )


def low_lanes(shape):
    return lax.broadcasted_iota(jnp.int32, shape, len(shape) - 1) < DH


def attend_fwd_pair(
    shard, prompt_rows, q, kp, vp, kc, vc, att_ref, lse_ref, between=None
):
    cont_len = kc.shape[0]
    prompt_len = kp.shape[0]
    for start in range(0, prompt_rows + cont_len, TILE):
        q_t = q[start : start + TILE, :] * jnp.asarray(DH ** (-0.5), jnp.bfloat16)
        halves = []
        for parity in range(2):
            keep = low_lanes(q_t.shape) == (parity == 0)
            q_h = jnp.where(keep, q_t, jnp.zeros_like(q_t))
            s_p = rows_dot(q_h, kp[...])
            if start < prompt_rows:
                key = lax.broadcasted_iota(jnp.int32, s_p.shape, 1)
                row = lax.broadcasted_iota(jnp.int32, s_p.shape, 0)
                s_p = jnp.where(key <= row + (shard * prompt_rows + start), s_p, NEG_BIG)
                largest = jnp.max(s_p, 1, keepdims=True)
                p_p = jnp.exp(s_p - largest)
                total = jnp.sum(p_p, 1, keepdims=True)
                o = dot_plain(p_p.astype(jnp.bfloat16), vp[...])
            else:
                seen = start - prompt_rows + TILE
                s_c = rows_dot(q_h, kc[:seen, :])
                key = lax.broadcasted_iota(jnp.int32, s_c.shape, 1)
                row = lax.broadcasted_iota(jnp.int32, s_c.shape, 0)
                s_c = jnp.where(key <= row + (start - prompt_rows), s_c, NEG_BIG)
                largest = jnp.maximum(
                    jnp.max(s_p, 1, keepdims=True), jnp.max(s_c, 1, keepdims=True)
                )
                p_p = jnp.exp(s_p - largest)
                p_c = jnp.exp(s_c - largest)
                total = jnp.sum(p_p, 1, keepdims=True) + jnp.sum(p_c, 1, keepdims=True)
                o = dot_plain(p_p.astype(jnp.bfloat16), vp[...]) + dot_plain(
                    p_c.astype(jnp.bfloat16), vc[:seen, :]
                )
            halves.append((o / total, largest + jnp.log(total)))
        keep = low_lanes((TILE, PAIR))
        att_ref[start : start + TILE, :] = jnp.where(keep, halves[0][0], halves[1][0])
        lse = jnp.where(
            keep,
            jnp.broadcast_to(halves[0][1], (TILE, PAIR)),
            jnp.broadcast_to(halves[1][1], (TILE, PAIR)),
        )
        turned = jnp.transpose(lse)
        lse_ref[0:1, start : start + TILE] = turned[0:1, :]
        lse_ref[1:2, start : start + TILE] = turned[DH : DH + 1, :]
        if between is not None:
            between(start // TILE)


def attend_bwd_pair(
    shard, prompt_rows, q, kp, vp, kc, vc, g, att, lse, dq, dkp, dvp, dkc, dvc, accum, between=None
):
    cont_len = kc.shape[0]
    tokens = prompt_rows + cont_len
    prompt_len = kp.shape[0]
    g_t = g[...]
    turned = jnp.transpose(g_t.astype(jnp.float32) * att[...])
    delta = (
        jnp.sum(turned[:DH], 0, keepdims=True),
        jnp.sum(turned[DH:], 0, keepdims=True),
    )
    q_t = q[...] * jnp.asarray(DH ** (-0.5), jnp.bfloat16)
    keep = low_lanes(q_t.shape)
    zero = jnp.zeros_like(q_t)
    q_h = (jnp.where(keep, q_t, zero), jnp.where(keep, zero, q_t))
    g_h = (jnp.where(keep, g_t, zero), jnp.where(keep, zero, g_t))
    accum[...] = jnp.zeros_like(accum)

    def block(key_b, value_b, first, mask):
        key_t = jnp.transpose(key_b.astype(jnp.float32)).astype(jnp.bfloat16)
        g_key = jnp.zeros((TILE, PAIR), jnp.float32)
        g_value = jnp.zeros((TILE, PAIR), jnp.float32)
        for parity in range(2):
            scores = rows_dot(key_b, q_h[parity][first:])
            probs = jnp.exp(scores - lse[parity : parity + 1, first:])
            masked = jnp.where(mask, probs[:, :TILE], 0.0)
            if tokens - first > TILE:
                probs = jnp.concatenate([masked, probs[:, TILE:]], 1)
            else:
                probs = masked
            g_probs = rows_dot(value_b, g_h[parity][first:])
            g_scores = (probs * (g_probs - delta[parity][:, first:])).astype(jnp.bfloat16)
            g_value += dot_plain(probs.astype(jnp.bfloat16), g_h[parity][first:])
            g_key += dot_plain(g_scores, q_h[parity][first:])
            rows = slice(parity * DH, (parity + 1) * DH)
            accum[rows, first:] += dot_plain(key_t[rows], g_scores)
        return g_key.astype(jnp.bfloat16), g_value.astype(jnp.bfloat16)

    ahead = lax.broadcasted_iota(jnp.int32, (TILE, TILE), 0) - lax.broadcasted_iota(
        jnp.int32, (TILE, TILE), 1
    )

    def prompt_block(index, start):
        rows = pl.ds(start, TILE)
        mask = ahead <= shard * prompt_rows - index * TILE
        g_key, g_value = block(kp[rows, :], vp[rows, :], 0, mask)
        dkp[rows, :] = g_key
        dvp[rows, :] = g_value

    blocks = prompt_len // TILE
    if blocks <= 4:
        for index in range(blocks):
            prompt_block(index, index * TILE)
            if between is not None:
                between(index)
    else:

        def step(index, carry):
            prompt_block(index, pl.multiple_of(index * TILE, TILE))
            return carry

        lax.fori_loop(0, blocks, step, 0)
    for start in range(0, cont_len, TILE):
        rows = slice(start, start + TILE)
        g_key, g_value = block(kc[rows, :], vc[rows, :], prompt_rows + start, ahead <= 0)
        dkc[rows, :] = g_key
        dvc[rows, :] = g_value
        if between is not None:
            between(blocks + start // TILE)
    dq[...] = (jnp.transpose(accum[...]) * DH ** (-0.5)).astype(jnp.bfloat16)


def attend_forward(q, kp, vp, kc, vc, prompt_rows):
    tokens, prompt_len, cont_len = q.shape[0], kp.shape[0], kc.shape[0]
    pairs = HEADS // 2

    def kernel(q, kp, vp, kc, vc, att_ref, lse_ref):
        attend_fwd_pair(
            lax.axis_index("shard"), prompt_rows, q, kp, vp, kc, vc, att_ref, lse_ref.at[0]
        )

    def columns(rows):
        return pl.BlockSpec((rows, PAIR), lambda p: (0, p))

    return pl.pallas_call(
        kernel,
        grid=(pairs,),
        in_specs=[columns(rows) for rows in (tokens, prompt_len, prompt_len, cont_len, cont_len)],
        out_specs=[columns(tokens), pl.BlockSpec((1, 8, tokens), lambda p: (p, 0, 0))],
        out_shape=[
            jax.ShapeDtypeStruct((tokens, D), jnp.float32),
            jax.ShapeDtypeStruct((pairs, 8, tokens), jnp.float32),
        ],
        compiler_params=pltpu.CompilerParams(vmem_limit_bytes=VMEM_ALL),
        name="attend_forward",
    )(q, kp, vp, kc, vc)


def attend_backward(q, kp, vp, kc, vc, g_att, att, lse, prompt_rows):
    tokens, prompt_len, cont_len = q.shape[0], kp.shape[0], kc.shape[0]
    pairs = HEADS // 2

    def kernel(q, kp, vp, kc, vc, g, a, ls, dq, dkp, dvp, dkc, dvc, accum):
        attend_bwd_pair(
            lax.axis_index("shard"),
            prompt_rows,
            q,
            kp,
            vp,
            kc,
            vc,
            g,
            a,
            ls.at[0],
            dq,
            dkp,
            dvp,
            dkc,
            dvc,
            accum,
        )

    def columns(rows):
        return pl.BlockSpec((rows, PAIR), lambda p: (0, p))

    sizes = (tokens, prompt_len, prompt_len, cont_len, cont_len)
    return pl.pallas_call(
        kernel,
        grid=(pairs,),
        in_specs=[columns(rows) for rows in sizes + (tokens, tokens)]
        + [pl.BlockSpec((1, 8, tokens), lambda p: (p, 0, 0))],
        out_specs=[columns(rows) for rows in sizes],
        out_shape=[jax.ShapeDtypeStruct((rows, D), jnp.bfloat16) for rows in sizes],
        scratch_shapes=[pltpu.VMEM((PAIR, tokens), jnp.float32)],
        compiler_params=pltpu.CompilerParams(vmem_limit_bytes=VMEM_ALL),
        name="attend_backward",
    )(q, kp, vp, kc, vc, g_att, att, lse)


MESH_ID = pl.DeviceIdType.MESH


def project_and_attend(
    prompt, conts, w_qkv, w_out, w_in, w_ffo, layer_biases, norm_gains, bias_in
):
    pieces, early = 12, 4
    ff = bias_in.shape[0]
    wide = D // TILE
    inner_steps = ff // TILE
    by_z = (4, 5, 6, 7, 8, 9)
    rows = w_qkv.shape[0]
    p_rows, cont_len = prompt.shape[0], conts.shape[0]
    tokens = p_rows + cont_len
    p_len = 4 * p_rows
    pairs = HEADS // 2
    tiles = tokens // TILE
    steps = tokens // TILE
    chunk = PAIR
    chunks = D // chunk
    quarter = rows // 4

    def kernel(
        xp, xc, wq, wo, wi, wf, bias, gain, b_in, w_all_out, wf_out, q_out, kc_out, vc_out, kp_out, vp_out, att_out,
        norm_out, x1_out, act_out, slope_out, att_b_out, lse, rstd_out,
        stage, w_all, q, kc, vc, kp, vp, att, norm1, x1_b, act, slope, att_b,
        load, c_s, c_r, x_s, x_r, y_s, y_r, z_s, z_r, d_s, d_r, e_s, e_r, w_sem,
        kc_s, kc_r, kx_s, kx_r, kd_s, kd_r, out_sem, ff_sem, row_sem,
    ):
        rep, shard = lax.axis_index("rep"), lax.axis_index("shard")
        z, y = rep // 2, rep % 2
        x, core = shard // 2, shard % 2
        partner = (rep, 2 * x + 1 - core)
        across = (rep, 2 * (1 - x) + core)
        beside = (2 * z + 1 - y, shard)
        z_low = z % 2
        above = (2 * (z + 1 - 2 * z_low) + y, shard)
        there = 2 * (1 - x) + core

        def remote(ref, send, recv, device):
            return pltpu.make_async_remote_copy(
                src_ref=ref,
                dst_ref=ref,
                send_sem=send,
                recv_sem=recv,
                device_id=device,
                device_id_type=MESH_ID,
            )

        def source(k):
            if k < 3:
                j = (1, 2, 0)[k]
                return wq.at[:, j * D : (j + 1) * D]
            if k < 4:
                return wo
            if k < 8:
                return wi.at[:, (k - 4) * D : (k - 3) * D]
            return wf.at[(k - 8) * rows : (k - 7) * rows, :]

        def loading(k):
            return pltpu.make_async_copy(source(k), stage.at[k], load.at[k])

        for k in range(pieces):
            loading(k).start()
        barrier = pltpu.get_barrier_semaphore()
        for other in (partner, across, beside, above):
            pl.semaphore_signal(barrier, inc=1, device_id=other, device_id_type=MESH_ID)
        pl.semaphore_wait(barrier, 4)

        def part(k, block, first, count):
            start = pl.multiple_of(first * quarter, 16)
            return w_all.at[k, block, pl.ds(start, count * quarter), :]

        def core_copy(k):
            return remote(w_all.at[k, shard], c_s.at[k], c_r.at[k], partner)

        def core_arrival(k):
            return remote(w_all.at[k, 2 * x + 1 - core], c_s.at[k], c_r.at[k], partner)

        def crossing(k, y_at):
            return (2 * z_low + y_at, 1) if k in by_z else (2 * y_at, 2)

        def x_copy(k):
            return remote(part(k, shard, *crossing(k, y)), x_s.at[k], x_r.at[k], across)

        def x_arrival(k):
            return remote(part(k, there, *crossing(k, y)), x_s.at[k], x_r.at[k], across)

        def y_copy(k):
            return remote(part(k, there, *crossing(k, y)), y_s.at[k], y_r.at[k], beside)

        def y_arrival(k):
            return remote(part(k, there, *crossing(k, 1 - y)), y_s.at[k], y_r.at[k], beside)

        def z_copy(k):
            return remote(part(k, there, 2 * z_low, 2), z_s.at[k], z_r.at[k], above)

        def z_arrival(k):
            return remote(part(k, there, 2 * (1 - z_low), 2), z_s.at[k], z_r.at[k], above)

        def halves(k):
            first = 2 * z_low if k in by_z else 2 * y
            return first, 2 - first

        def d_copy(k, block=None):
            block = there if block is None else block
            return remote(part(k, block, halves(k)[0], 2), d_s.at[k], d_r.at[k], partner)

        def e_copy(k, block=None):
            block = there if block is None else block
            return remote(part(k, block, halves(k)[1], 2), e_s.at[k], e_r.at[k], partner)

        far = 2 * (1 - x) + 1 - core

        def send_piece(k):
            x_copy(k).start()
            core_copy(k).start()

        def round_piece(k):
            loading(k).wait()
            w_all[k, shard] = stage[k].astype(jnp.bfloat16)

        def serve_x(k):
            x_arrival(k).wait_recv()
            y_copy(k).start()
            if k not in by_z:
                d_copy(k).start()

        def serve_y(k):
            y_arrival(k).wait_recv()
            if k in by_z:
                z_copy(k).start()
                d_copy(k).start()
            else:
                e_copy(k).start()

        def serve_z(k):
            z_arrival(k).wait_recv()
            e_copy(k).start()

        def w_store(k):
            if k < 8:
                return pltpu.make_async_copy(w_all.at[k], w_all_out.at[k], w_sem.at[k])
            return pltpu.make_async_copy(w_all.at[k], wf_out.at[:, k - 8], w_sem.at[k])

        def complete(k):
            core_arrival(k).wait_recv()
            d_copy(k, far).wait_recv()
            e_copy(k, far).wait_recv()
            w_store(k).start()

        def weight(k):
            return w_all[k].reshape(4 * rows, D)

        for k in range(early):
            round_piece(k)
            send_piece(k)
        for k in range(early, pieces):
            round_piece(k)
        own_rows = pl.ds(pl.multiple_of(shard * p_rows, p_rows), p_rows)
        kv = (kp, vp)

        def kv_part(t, g, block):
            lanes = pl.ds(g * chunk if isinstance(g, int) else pl.multiple_of(g * chunk, chunk), chunk)
            return kv[t].at[pl.ds(pl.multiple_of(block * p_rows, p_rows), p_rows), lanes]

        def kv_core(t, g):
            return remote(kv_part(t, g, shard), kc_s.at[g, t], kc_r.at[g, t], partner)

        def kv_across(t, g):
            return remote(kv_part(t, g, shard), kx_s.at[g, t], kx_r.at[g, t], across)

        def kv_forward(t, g):
            return remote(kv_part(t, g, there), kd_s.at[g, t], kd_r.at[g, t], partner)

        serve_x(0)
        serve_x(1)
        serve_y(0)
        complete(0)
        kp[own_rows, :] = dot_plain(xp[...], weight(0)).astype(jnp.bfloat16)
        kc[...] = dot_plain(xc[...], weight(0)).astype(jnp.bfloat16)
        serve_x(2)
        serve_y(1)
        complete(1)
        vp[own_rows, :] = (dot_plain(xp[...], weight(1)) + bias[1:2, :]).astype(jnp.bfloat16)
        waiting = list(range(early, pieces))
        for g in range(chunks):
            for t in range(2):
                kv_across(t, g).start()
                kv_core(t, g).start()
            sent = 0 if g == 0 else 1 if g < chunks - 1 else pieces
            for k in waiting[:sent]:
                send_piece(k)
            waiting = waiting[sent:]
        vc[...] = (dot_plain(xc[...], weight(1)) + bias[1:2, :]).astype(jnp.bfloat16)
        serve_y(2)
        serve_x(3)
        complete(2)
        q[:p_rows, :] = (dot_plain(xp[...], weight(2)) + bias[0:1, :]).astype(jnp.bfloat16)
        q[p_rows:, :] = (dot_plain(xc[...], weight(2)) + bias[0:1, :]).astype(jnp.bfloat16)

        def keep(ref, target, i):
            return pltpu.make_async_copy(ref, target, out_sem.at[i])

        kept = [(q, q_out, 0), (kc, kc_out, 1), (vc, vc_out, 2)]
        for item in kept:
            keep(*item).start()

        def serve_kv(g):
            for t in range(2):
                remote(kv_part(t, g, there), kx_s.at[g, t], kx_r.at[g, t], across).wait_recv()
                kv_forward(t, g).start()

        def complete_kv(g):
            for t in range(2):
                remote(
                    kv_part(t, g, 2 * x + 1 - core), kc_s.at[g, t], kc_r.at[g, t], partner
                ).wait_recv()
                remote(kv_part(t, g, far), kd_s.at[g, t], kd_r.at[g, t], partner).wait_recv()

        serve_kv(0)
        arrive = {4: 26.2, 5: 30.6, 6: 35.1, 7: 39.5, 8: 43.9, 9: 45.5, 10: 48.7, 11: 51.9}
        work = [(27.0, serve_y, 3), (30.0, complete, 3)]
        forward = (27.0, 31.1, 35.5, 39.9, 44.3)
        work += [(at, serve_kv, g + 1) for g, at in enumerate(forward)]
        for k in range(4, pieces):
            at = arrive[k]
            work.append((at, serve_x, k))
            if k in by_z:
                work += [(at + 4, serve_y, k), (at + 10, serve_z, k), (at + 13, complete, k)]
            else:
                work += [(at + 6, serve_y, k), (at + 9, complete, k)]
        slots = pairs * tiles
        work.sort(key=lambda item: item[0])
        later = [item for item in work if item[0] > 26 + 1.37 * slots]
        work = [(max(0, round((at - 26) / 1.37 - 0.6)), job, k) for at, job, k in work if at <= 26 + 1.37 * slots]
        work = [(min(slot, slots - 1), job, k) for slot, job, k in work]

        def att_store(p):
            lanes = pl.ds(pl.multiple_of(p * PAIR, PAIR), PAIR)
            return pltpu.make_async_copy(att.at[:, lanes], att_out.at[:, lanes], out_sem.at[5 + p])

        def pair(p, carry):
            complete_kv(p)

            def between(tile):
                for slot, action, k in work:
                    if slot < slots and slot % tiles == tile:

                        @pl.when(p == slot // tiles)
                        def _(action=action, k=k):
                            action(k)

            lanes = pl.ds(pl.multiple_of(p * PAIR, PAIR), PAIR)
            attend_fwd_pair(
                shard,
                p_rows,
                q.at[:, lanes],
                kp.at[:, lanes],
                vp.at[:, lanes],
                kc.at[:, lanes],
                vc.at[:, lanes],
                att.at[:, lanes],
                lse.at[p],
                between,
            )
            att_store(p).start()
            return carry

        lax.fori_loop(0, pairs, pair, 0)
        kept += [(kp, kp_out, 3), (vp, vp_out, 4)]
        for item in kept[3:]:
            keep(*item).start()

        def row(i):
            return pl.ds(pl.multiple_of(i * TILE, TILE), TILE)

        def row_stores(i):
            pairs_of = [(norm1, norm_out), (x1_b, x1_out), (att_b, att_b_out)]
            return [
                pltpu.make_async_copy(ref.at[row(i), :], out.at[row(i), :], row_sem.at[n, i])
                for n, (ref, out) in enumerate(pairs_of)
            ]

        def normalized(i, carry):
            part = att[row(i), :].astype(jnp.bfloat16)
            att_b[row(i), :] = part
            values = dot_plain(part, weight(3)) + bias[2:3, :] + norm1[row(i), :]
            center = values - jnp.mean(values, -1, keepdims=True)
            spread = jnp.mean(center * center, -1, keepdims=True)
            scale = lax.rsqrt(spread + 1e-05)
            hat = center * scale
            norm1[row(i), :] = hat
            rstd_out[row(i), :] = jnp.broadcast_to(scale, (TILE, 128))
            x1_b[row(i), :] = (hat * gain[0:1, :] + bias[4:5, :]).astype(jnp.bfloat16)
            for copy in row_stores(i):
                copy.start()
            return carry

        norm1[:p_rows, :] = xp[...].astype(jnp.float32)
        norm1[p_rows:, :] = xc[...].astype(jnp.float32)
        lax.fori_loop(0, steps, normalized, 0)

        def ff_stores(i):
            columns = pl.ds(pl.multiple_of(i * TILE, TILE), TILE)
            return [
                pltpu.make_async_copy(ref.at[:, columns], out.at[:, columns], ff_sem.at[n, i])
                for n, (ref, out) in enumerate([(act, act_out), (slope, slope_out)])
            ]

        def inner(i, carry):
            lanes = pl.ds(pl.multiple_of(lax.rem(i, wide) * TILE, TILE), TILE)
            columns = pl.ds(pl.multiple_of(i * TILE, TILE), TILE)
            block = w_all[4 + i // wide, :, :, lanes].reshape(D, TILE)
            hidden = dot_plain(x1_b[...], block) + b_in[:, columns]
            cdf = 0.5 * (1.0 + lax.erf(hidden * 2.0 ** (-0.5)))
            act[:, columns] = (hidden * cdf).astype(jnp.bfloat16)
            density = jnp.exp(hidden * hidden * (-0.5)) * 0.3989422804014327
            slope[:, columns] = (cdf + hidden * density).astype(jnp.bfloat16)
            for copy in ff_stores(i):
                copy.start()
            for at, job, k in later:
                step = min(max(0, round((at - 54.5) / 0.73 - 0.5)), inner_steps - 1)
                pl.when(i == step)(functools.partial(job, k))
            return carry

        lax.fori_loop(0, inner_steps, inner, 0)

        def ff_wait(i, carry):
            for copy in ff_stores(i):
                copy.wait()
            return carry

        lax.fori_loop(0, inner_steps, ff_wait, 0)

        def row_wait(i, carry):
            for copy in row_stores(i):
                copy.wait()
            return carry

        lax.fori_loop(0, steps, row_wait, 0)
        for item in kept:
            keep(*item).wait()

        def last_pair(p, carry):
            att_store(p).wait()
            return carry

        lax.fori_loop(0, pairs, last_pair, 0)
        for k in range(pieces):
            w_store(k).wait()
            for copy in (core_copy, x_copy, y_copy, d_copy, e_copy):
                copy(k).wait_send()
            if k in by_z:
                z_copy(k).wait_send()
        for g in range(chunks):
            for t in range(2):
                for copy in (kv_core, kv_across, kv_forward):
                    copy(t, g).wait_send()

    def sems(*dims):
        return pltpu.SemaphoreType.DMA(dims)

    def low(*dims):
        return jax.ShapeDtypeStruct(dims, jnp.bfloat16)

    anywhere = pl.BlockSpec(memory_space=pl.ANY)
    vmem = pl.BlockSpec(memory_space=pltpu.VMEM)
    n = pieces
    out = pl.pallas_call(
        kernel,
        in_specs=[vmem, vmem, anywhere, anywhere, anywhere, anywhere, vmem, vmem, vmem],
        out_specs=[anywhere] * 13 + [vmem] * 2,
        out_shape=[
            low(8, 4, rows, D),
            low(4, 4, rows, D),
            low(tokens, D),
            low(cont_len, D),
            low(cont_len, D),
            low(p_len, D),
            low(p_len, D),
            jax.ShapeDtypeStruct((tokens, D), jnp.float32),
            jax.ShapeDtypeStruct((tokens, D), jnp.float32),
            low(tokens, D),
            low(tokens, ff),
            low(tokens, ff),
            low(tokens, D),
            jax.ShapeDtypeStruct((pairs, 8, tokens), jnp.float32),
            jax.ShapeDtypeStruct((tokens, 128), jnp.float32),
        ],
        scratch_shapes=[
            pltpu.VMEM((n, rows, D), jnp.float32),
            pltpu.VMEM((n, 4, rows, D), jnp.bfloat16),
            pltpu.VMEM((tokens, D), jnp.bfloat16),
            pltpu.VMEM((cont_len, D), jnp.bfloat16),
            pltpu.VMEM((cont_len, D), jnp.bfloat16),
            pltpu.VMEM((p_len, D), jnp.bfloat16),
            pltpu.VMEM((p_len, D), jnp.bfloat16),
            pltpu.VMEM((tokens, D), jnp.float32),
            pltpu.VMEM((tokens, D), jnp.float32),
            pltpu.VMEM((tokens, D), jnp.bfloat16),
            pltpu.VMEM((tokens, ff), jnp.bfloat16),
            pltpu.VMEM((tokens, ff), jnp.bfloat16),
            pltpu.VMEM((tokens, D), jnp.bfloat16),
        ]
        + [sems(n)] * 14
        + [sems(chunks, 2)] * 6
        + [sems(5 + pairs), sems(2, inner_steps), sems(3, steps)],
        compiler_params=pltpu.CompilerParams(
            collective_id=1, has_side_effects=True, vmem_limit_bytes=VMEM_ALL
        ),
        name="project_and_attend",
    )(prompt, conts, w_qkv, w_out, w_in, w_ffo, layer_biases, norm_gains, bias_in[None])
    w_all, wf, q, kc, vc, kp, vp, att, norm1, x1_b, act, slope, att_b, lse, rstd1 = out
    w_all = w_all.reshape(8, 4 * rows, D)
    wf = wf.reshape(4, 4 * rows, D)
    return w_all, wf, q, kp, vp, kc, vc, att, lse, (norm1, rstd1, x1_b, act, slope, att_b)


def project_native(
    prompt, conts, w_qkv, w_out, w_in, w_ffo, layer_biases, norm_gains, bias_in
):
    rows = prompt.shape[0]

    def gathered(value):
        return lax.all_gather(value.astype(jnp.bfloat16), "shard", axis=0, tiled=True)

    qkv, out, inner, ffo = (gathered(w) for w in (w_qkv, w_out, w_in, w_ffo))
    tokens = jnp.concatenate([prompt, conts], 0)
    bias = jnp.concatenate([layer_biases[0], jnp.zeros((D,), jnp.float32), layer_biases[1]])
    qkv_b = (dot_plain(tokens, qkv) + bias).astype(jnp.bfloat16)
    q, keys, values = (qkv_b[:, i * D : (i + 1) * D] for i in range(3))
    kp, vp = gathered(keys[:rows]), gathered(values[:rows])
    kc, vc = keys[rows:], values[rows:]
    att, lse = attend_forward(q, kp, vp, kc, vc, rows)
    blocks = [qkv[:, D : 2 * D], qkv[:, 2 * D :], qkv[:, :D], out]
    blocks += [inner[:, i * D : (i + 1) * D] for i in range(inner.shape[1] // D)]
    att_b = att.astype(jnp.bfloat16)
    values = tokens.astype(jnp.float32) + dot_plain(att_b, out) + layer_biases[2]
    center = values - jnp.mean(values, -1, keepdims=True)
    scale = lax.rsqrt(jnp.mean(center * center, -1, keepdims=True) + 1e-05)
    norm1 = center * scale
    x1_b = (norm1 * norm_gains[0] + layer_biases[4]).astype(jnp.bfloat16)
    hidden = dot_plain(x1_b, inner) + bias_in
    cdf = 0.5 * (1.0 + lax.erf(hidden * 2.0 ** (-0.5)))
    density = jnp.exp(hidden * hidden * (-0.5)) * 0.3989422804014327
    act = (hidden * cdf).astype(jnp.bfloat16)
    slope = (cdf + hidden * density).astype(jnp.bfloat16)
    rstd1 = jnp.broadcast_to(scale, (tokens.shape[0], 128))
    state = (norm1, rstd1, x1_b, act, slope, att_b)
    ffo = ffo.reshape(-1, D, D)
    return jnp.stack(blocks), ffo, q, kp, vp, kc, vc, att, lse, state


def student_head(label, stu, vectors, w_pool, w_class, bias_class, classes):
    part_w = STU // SHEADS
    low_half = lax.broadcasted_iota(jnp.int32, stu.shape, 1) < part_w
    row_low = lax.broadcasted_iota(jnp.int32, (1, STU), 1) < part_w
    query, bias_pool = vectors[1:2, :], vectors[2:3, :]

    def by_head(values):
        low_sum = jnp.sum(jnp.where(low_half[: values.shape[0]], values, 0.0), 1, keepdims=True)
        high_sum = jnp.sum(jnp.where(low_half[: values.shape[0]], 0.0, values), 1, keepdims=True)
        return jnp.where(low_half[: values.shape[0]], low_sum, high_sum)

    scores = by_head(stu * query) * part_w ** (-0.5)
    largest = jnp.max(scores, 0, keepdims=True)
    expo = jnp.exp(scores - largest)
    weights = expo / jnp.sum(expo, 0, keepdims=True)
    pooled = jnp.sum(weights * stu, 0, keepdims=True)

    square = (STU, STU)
    on_diagonal = lax.broadcasted_iota(jnp.int32, square, 0) == lax.broadcasted_iota(
        jnp.int32, square, 1
    )

    def column(row):
        return jnp.sum(jnp.where(on_diagonal, row, 0.0), 1, keepdims=True)

    def times(row, matrix):
        return jnp.sum(column(row) * matrix, 0, keepdims=True)

    def times_turned(row, matrix):
        total = jnp.sum(matrix * row, 1, keepdims=True)
        return jnp.sum(jnp.where(on_diagonal, total, 0.0), 0, keepdims=True)

    top = jnp.tanh(times(pooled, w_pool) + bias_pool)
    lane = lax.broadcasted_iota(jnp.int32, (1, STU), 1)
    logits = times_turned(top, w_class) + bias_class
    seen = jnp.where(lane < classes, logits, NEG_BIG)
    expo_l = jnp.exp(seen - jnp.max(seen, 1, keepdims=True))
    g_logits = expo_l / jnp.sum(expo_l, 1, keepdims=True) - jnp.where(lane == label, 1.0, 0.0)
    g_class = column(g_logits) * top
    g_pre = times(g_logits, w_class) * (1.0 - top * top)
    g_pool = column(pooled) * g_pre
    g_pooled = times_turned(g_pre, w_pool)
    g_weights = by_head(stu * g_pooled)
    mean = jnp.sum(weights * g_weights, 0, keepdims=True)
    g_scores = weights * (g_weights - mean) * part_w ** (-0.5)
    g_stu = weights * g_pooled + g_scores * query
    g_query = jnp.sum(g_scores * stu, 0, keepdims=True)
    return logits, g_stu, g_query, g_pre, g_pool, g_class, g_logits


def middle(
    ahead, state, prompt_cot, cont_cot, labels, w_all, wf,
    biases, gains, bias_in, student, vectors, w_pool, w_class, bias_class,
):
    p_rows, cont_len = prompt_cot.shape[0], cont_cot.shape[0]
    tokens = p_rows + cont_len
    ff = bias_in.shape[0]
    blocks = ff // D
    steps = tokens // TILE
    wide = D // TILE
    classes = w_class.shape[1]
    g_names = 2 * blocks + 1

    def kernel(
        label_ref, norm_h, rstd_h, x1_h, act_h, slope_h, att_b_h, cp, cc, w_h, wf_h, bias, gain, w_stu, vec, w_p, w_c, b_c,
        out_p, out_c, logits_out, grads_h, g_r1_h, g_att_h, small, totals_h,
        cot_v, out_v, w_c_v, b_c_v, att_b, w_v, wf_v, norm1, norm2, rstd1, rstd2, x1_b, act, slope, g_res, g_ffn, g_br, g_stu_b, grads,
        sums, in_sum, load, store, *links,
    ):
        def fetch(source, target, i):
            return pltpu.make_async_copy(source, target, load.at[i])

        loads = [
            fetch(act_h, act, 0),
            fetch(wf_h, wf_v, 1),
            fetch(norm_h, norm1, 2),
            fetch(cp, cot_v.at[:p_rows], 3),
            fetch(cc, cot_v.at[p_rows:], 4),
            fetch(slope_h, slope, 5),
            fetch(x1_h, x1_b, 6),
            fetch(rstd_h, rstd1, 7),
            fetch(w_h.at[pl.ds(3, 1 + blocks)], w_v, 8),
            fetch(att_b_h, att_b, 9),
        ]
        for copy in loads:
            copy.start()
        rows = D // blocks
        if ahead:
            (cr, xr, c_s, c_r, x_s, x_r) = links
            rep, shard = lax.axis_index("rep"), lax.axis_index("shard")
            x, core = shard // 2, shard % 2
            partner = (rep, 2 * x + 1 - core)
            across = (rep, 2 * (1 - x) + core)
            barrier = pltpu.get_barrier_semaphore()
            for other in (partner, across):
                pl.semaphore_signal(barrier, inc=1, device_id=other, device_id_type=MESH_ID)
            pl.semaphore_wait(barrier, 2)

            def remote(source, target, send, recv, device):
                return pltpu.make_async_remote_copy(
                    src_ref=source,
                    dst_ref=target,
                    send_sem=send,
                    recv_sem=recv,
                    device_id=device,
                    device_id_type=MESH_ID,
                )

            def core_copy(k, xx):
                block = pl.ds(pl.multiple_of((2 * xx + 1 - core) * rows, 16), rows)
                return remote(
                    grads.at[k, block, :], cr.at[k, xx], c_s.at[k, xx], c_r.at[k, xx], partner
                )

            def mine(xx):
                return pl.ds(pl.multiple_of((2 * xx + core) * rows, 16), rows)

            def x_copy(k):
                return remote(grads.at[k, mine(1 - x), :], xr.at[k], x_s.at[k], x_r.at[k], across)

        def stage_x():
            for k in range(ahead):
                for xx in range(2):
                    core_copy(k, xx).wait_recv()
                block = mine(1 - x)
                total = grads[k, block, :].astype(jnp.float32) + cr[k, 1 - x].astype(jnp.float32)
                grads[k, block, :] = total.astype(jnp.bfloat16)
                x_copy(k).start()

        sums[...] = jnp.zeros_like(sums)
        small[...] = jnp.zeros_like(small)

        def row(i):
            return pl.ds(pl.multiple_of(i * TILE, TILE), TILE)

        def loop(count):
            def run(step):
                def body(i, carry):
                    step(i)
                    return carry

                lax.fori_loop(0, count, body, 0)

            return run

        def normalize(values):
            center = values - jnp.mean(values, -1, keepdims=True)
            spread = jnp.mean(center * center, -1, keepdims=True)
            scale = lax.rsqrt(spread + 1e-05)
            return center * scale, scale

        def norm_back(g, gain_row, hat, scale):
            gg = g * gain_row
            return scale * (
                gg
                - jnp.mean(gg, -1, keepdims=True)
                - hat * jnp.mean(gg * hat, -1, keepdims=True)
            )

        def add_sum(i, values):
            sums[i : i + 1, :] += jnp.sum(values, 0, keepdims=True)

        for i in range(3):
            loads[i].wait()

        @loop(steps)
        def _(i):
            ffn = bias[3:4, :]
            for j in range(blocks):
                ffn = ffn + dot_plain(act[row(i), j * D : (j + 1) * D], wf_v[j])
            first = norm1[row(i), :] * gain[0:1, :] + bias[4:5, :]
            hat, scale = normalize(first + ffn)
            norm2[row(i), :] = hat
            rstd2[row(i), :] = jnp.broadcast_to(scale, (TILE, 128))
            out_v[row(i), :] = (hat * gain[1:2, :] + bias[5:6, :]).astype(jnp.bfloat16)

        out_stores = [
            pltpu.make_async_copy(out_v.at[:p_rows], out_p, store.at[g_names + 2]),
            pltpu.make_async_copy(out_v.at[p_rows:], out_c, store.at[g_names + 3]),
        ]
        for copy in out_stores:
            copy.start()
        base = 8 * (D // 128) + ff // 128
        w_stu_b = w_stu[...].astype(jnp.bfloat16)

        w_c_v[...] = jnp.zeros_like(w_c_v)
        b_c_v[...] = jnp.zeros_like(b_c_v)
        w_c_v[:classes, :] = w_c[...]
        b_c_v[:1, :classes] = b_c[...]

        @pl.when(lax.axis_index("rep") >= 0)
        def _():
            stu = dot_plain(out_v[p_rows:, :], w_stu_b) + vec[0:1, :]
            logits, g_stu, g_query, g_pre, g_pool, g_class, g_logits = student_head(
                label_ref[0, 0], stu, vec, w_p[...], w_c_v[...], b_c_v[:1, :], classes
            )
            logits_out[...] = logits[:, :classes]
            low = g_stu.astype(jnp.bfloat16)
            g_stu_b[:p_rows, :] = jnp.zeros((p_rows, STU), jnp.bfloat16)
            g_stu_b[p_rows:, :] = low
            small[base : base + 1, STU:] = jnp.sum(low.astype(jnp.float32), 0, keepdims=True)
            small[base + 1 : base + 2, STU:] = g_query
            small[base + 2 : base + 3, STU:] = g_pre
            small[base + 3 : base + 4, STU:] = g_logits
            small[base + 8 : base + 8 + STU, STU:] = g_pool
            small[base + 8 + STU : base + 24 + STU, STU:] = g_class[:16]

        small[:, :STU] = dot_first(out_v[p_rows:, :], g_stu_b[p_rows:, :])
        for i in range(3, 10):
            loads[i].wait()

        @loop(steps)
        def _(i):
            g = cot_v[row(i), :].astype(jnp.float32) + dot_second(g_stu_b[row(i), :], w_stu_b)
            hat = norm2[row(i), :]
            add_sum(7, g * hat)
            add_sum(5, g)
            g_r2 = norm_back(g, gain[1:2, :], hat, rstd2[row(i), :1])
            g_res[row(i), :] = g_r2
            low = g_r2.astype(jnp.bfloat16)
            g_ffn[row(i), :] = low
            add_sum(3, low.astype(jnp.float32))

        def piece_store(k):
            return pltpu.make_async_copy(grads.at[k], grads_h.at[k], store.at[k])


        @loop(blocks)
        def _(j):
            columns = pl.ds(pl.multiple_of(j * D, D), D)
            product = dot_first(act[:, columns], g_ffn[...]).astype(jnp.bfloat16)
            for k in range(blocks):
                target = pl.ds(pl.multiple_of(j * rows, 16), rows)
                grads[k, target, :] = product[k * rows : (k + 1) * rows]

        for k in range(ahead):
            for xx in range(2):
                core_copy(k, xx).start()
        for k in range(ahead, blocks):
            piece_store(k).start()


        in_sum[...] = jnp.zeros_like(in_sum)

        @loop(steps)
        def _(i):
            for j in range(blocks):
                columns = slice(j * D, (j + 1) * D)
                g_act = dot_second(g_ffn[row(i), :], wf_v[j])
                low = (g_act * slope[row(i), columns].astype(jnp.float32)).astype(jnp.bfloat16)
                slope[row(i), columns] = low
                in_sum[:, columns] += jnp.sum(low.astype(jnp.float32), 0, keepdims=True)
            if ahead:
                pl.when(i == 0)(stage_x)

        @loop(blocks)
        def _(j):
            columns = pl.ds(pl.multiple_of(j * D, D), D)
            grads[blocks + j] = dot_first(x1_b[...], slope[:, columns]).astype(jnp.bfloat16)
            piece_store(blocks + j).start()

        @loop(steps)
        def _(i):
            g = g_res[row(i), :]
            for j in range(blocks):
                g += dot_second(slope[row(i), j * D : (j + 1) * D], w_v[1 + j])
            hat = norm1[row(i), :]
            add_sum(6, g * hat)
            add_sum(4, g)
            g_r1 = norm_back(g, gain[0:1, :], hat, rstd1[row(i), :1])
            g_res[row(i), :] = g_r1
            low = g_r1.astype(jnp.bfloat16)
            g_br[row(i), :] = low
            add_sum(2, low.astype(jnp.float32))

        res_store = pltpu.make_async_copy(g_res, g_r1_h, store.at[g_names])
        res_store.start()
        g_ffn[...] = dot_second(g_br[...], w_v[0]).astype(jnp.bfloat16)
        att_store = pltpu.make_async_copy(g_ffn, g_att_h, store.at[g_names + 1])
        att_store.start()
        grads[2 * blocks] = dot_first(att_b[...], g_br[...]).astype(jnp.bfloat16)
        piece_store(2 * blocks).start()
        spread = D // 128
        for i in range(8):
            for part in range(spread):
                small[i * spread + part : i * spread + part + 1, STU:] = sums[
                    i : i + 1, part * 128 : (part + 1) * 128
                ]
        for part in range(ff // 128):
            at = 8 * spread + part
            small[at : at + 1, STU:] = in_sum[:, part * 128 : (part + 1) * 128]
        res_store.wait()
        att_store.wait()
        for copy in out_stores:
            copy.wait()
        for k in range(ahead):
            x_copy(k).wait_recv()
            total = grads[k, mine(x), :].astype(jnp.float32) + cr[k, x].astype(jnp.float32)
            cr[k, x] = (total + xr[k].astype(jnp.float32)).astype(jnp.bfloat16)
            pltpu.make_async_copy(cr.at[k, x], totals_h.at[k], store.at[k]).start()
        for k in range(ahead, g_names):
            piece_store(k).wait()
        for k in range(ahead):
            pltpu.make_async_copy(cr.at[k, x], totals_h.at[k], store.at[k]).wait()
            for xx in range(2):
                core_copy(k, xx).wait_send()
            x_copy(k).wait_send()

    anywhere = pl.BlockSpec(memory_space=pl.ANY)
    vmem = pl.BlockSpec(memory_space=pltpu.VMEM)
    low = jnp.bfloat16

    def shaped(dims, kind=jnp.float32):
        return jax.ShapeDtypeStruct(dims, kind)

    params = pltpu.CompilerParams(vmem_limit_bytes=VMEM_ALL)
    link_scratch = []
    if ahead:
        params = pltpu.CompilerParams(
            collective_id=3, has_side_effects=True, vmem_limit_bytes=VMEM_ALL
        )
        piece = (D // blocks, D)
        link_scratch = [
            pltpu.VMEM((ahead, 2, *piece), low),
            pltpu.VMEM((ahead, *piece), low),
        ]
        link_scratch += [pltpu.SemaphoreType.DMA((ahead, 2))] * 2
        link_scratch += [pltpu.SemaphoreType.DMA((ahead,))] * 2

    return pl.pallas_call(
        kernel,
        in_specs=[pl.BlockSpec(memory_space=pltpu.SMEM)] + [anywhere] * 10 + [vmem] * 7,
        out_specs=[anywhere, anywhere, vmem, anywhere, anywhere, anywhere, vmem, anywhere],
        out_shape=[
            shaped((p_rows, D), low),
            shaped((cont_len, D), low),
            shaped((1, classes)),
            shaped((g_names, D, D), low),
            shaped((tokens, D)),
            shaped((tokens, D), low),
            shaped((D, 2 * STU)),
            shaped((max(ahead, 1), D // blocks, D), low),
        ],
        scratch_shapes=[
            pltpu.VMEM((tokens, D), low),
            pltpu.VMEM((tokens, D), low),
            pltpu.VMEM((STU, STU), jnp.float32),
            pltpu.VMEM((8, STU), jnp.float32),
            pltpu.VMEM((tokens, D), low),
            pltpu.VMEM((1 + blocks, D, D), low),
            pltpu.VMEM((blocks, D, D), low),
            pltpu.VMEM((tokens, D), jnp.float32),
            pltpu.VMEM((tokens, D), jnp.float32),
            pltpu.VMEM((tokens, 128), jnp.float32),
            pltpu.VMEM((tokens, 128), jnp.float32),
            pltpu.VMEM((tokens, D), low),
            pltpu.VMEM((tokens, ff), low),
            pltpu.VMEM((tokens, ff), low),
            pltpu.VMEM((tokens, D), jnp.float32),
            pltpu.VMEM((tokens, D), low),
            pltpu.VMEM((tokens, D), low),
            pltpu.VMEM((tokens, STU), low),
            pltpu.VMEM((g_names, D, D), low),
            pltpu.VMEM((8, D), jnp.float32),
            pltpu.VMEM((1, ff), jnp.float32),
            pltpu.SemaphoreType.DMA((10,)),
            pltpu.SemaphoreType.DMA((g_names + 4,)),
        ]
        + link_scratch,
        compiler_params=params,
        name="middle",
    )(
        labels,
        *state,
        prompt_cot,
        cont_cot,
        w_all,
        wf,
        biases,
        gains,
        student,
        vectors,
        w_pool,
        w_class.T,
        bias_class[None],
    )


def sum_native(g9, g_qkvw, small):
    blocks = (g9.shape[0] - 1) // 2
    rows = D // blocks
    ffo = g9[:blocks].reshape(blocks, blocks, rows, D).transpose(1, 0, 2, 3).reshape(-1, D)
    inner = jnp.concatenate([g9[blocks + j] for j in range(blocks)], 1)

    def over(grad):
        part = lax.psum_scatter(
            grad.astype(jnp.bfloat16), "shard", scatter_dimension=0, tiled=True
        )
        return lax.psum(part, "rep").astype(jnp.float32)

    owned = tuple(over(grad) for grad in (g_qkvw, g9[2 * blocks], inner, ffo))
    return owned, lax.psum(small, ("rep", "shard"))


def finish(
    ahead, totals, q, kp, vp, kc, vc, att, lse, g_att, g9, g_resid, small, w_all, prompt, conts, ff
):
    pieces, ready = 12, 9
    p_rows, cont_len = prompt.shape[0], conts.shape[0]
    tokens = p_rows + cont_len
    p_len = kp.shape[0]
    pairs = HEADS // 2
    rows = D // 4
    half, quarter = D // 2, rows // 4
    s_width = small.shape[1]
    chunk = 2 * PAIR
    chunks = D // chunk
    across_lanes = D // 128

    def kernel(
        q_h, kp_h, vp_h, kc_h, vc_h, att_h, g_att_h, g9, g_res_h, w_h, totals_h, ls, sm, xp, xc,
        out_pg, out_cg, out_q, out_o, out_i, out_f, fin_s,
        qv, kpv, vpv, kcv, vcv, attv, gav, accum, dq, dkp, dvp, dkc, dvc, kr, kx, kvs, wv, g_tok, made, head,
        own, cr, xr, yr, zr, fb, made_s, own_s, cr_s, xr_s, yr_s, zr_s, fb_s,
        load, sem_own, c_send, c_recv, x_send, x_recv, y_send, y_recv, z_send, z_recv,
        f_send, f_recv, o_send, o_recv, o_own, g_send, g_recv, kc_s, kc_r, kx_s, kx_r, out_sem,
    ):
        rep, shard = lax.axis_index("rep"), lax.axis_index("shard")
        z, y = rep // 2, rep % 2
        x, core = shard // 2, shard % 2
        partner = (rep, 2 * x + 1 - core)
        across = (rep, 2 * (1 - x) + core)
        beside = (2 * z + 1 - y, shard)
        far = (rep, 2 * (1 - x) + 1 - core)

        def along(step):
            return (2 * lax.rem(z + step, 4) + y, shard)

        def own_copy(k, xx):
            return pltpu.make_async_copy(
                g9.at[k, pl.ds(pl.multiple_of((2 * xx + core) * rows, 16), rows), :],
                own.at[k, xx],
                sem_own.at[k, xx],
            )

        fetched = [(q_h, qv), (kp_h, kpv), (vp_h, vpv), (kc_h, kcv), (vc_h, vcv)]
        fetched += [(att_h, attv), (g_att_h, gav), (w_h.at[pl.ds(0, 3)], wv), (g_res_h, g_tok)]

        def fetch(i):
            return pltpu.make_async_copy(*fetched[i], load.at[i])

        def total_copy(k):
            return pltpu.make_async_copy(totals_h.at[k], own.at[k, x], sem_own.at[k, 0])

        for k in range(ahead):
            total_copy(k).start()
        for k in range(ahead, ahead + 2):
            for xx in range(2):
                own_copy(k, xx).start()
        for i in range(7):
            fetch(i).start()
        for k in range(ahead + 2, ready):
            for xx in range(2):
                own_copy(k, xx).start()
        for i in (7, 8):
            fetch(i).start()

        barrier = pltpu.get_barrier_semaphore()
        others = [partner, across, beside, along(1), along(2), along(3), far]
        for other in others:
            pl.semaphore_signal(barrier, inc=1, device_id=other, device_id_type=MESH_ID)
        pl.semaphore_wait(barrier, len(others))

        def remote(source, target, send, recv, device):
            return pltpu.make_async_remote_copy(
                src_ref=source,
                dst_ref=target,
                send_sem=send,
                recv_sem=recv,
                device_id=device,
                device_id_type=MESH_ID,
            )

        big = (own, cr, xr, yr, zr, fb, half)
        narrow = (own_s, cr_s, xr_s, yr_s, zr_s, fb_s, s_width // 2)

        def bufs(k):
            if isinstance(k, int) and k == pieces:
                return narrow, 0
            return big, k

        def core_copy(k, xx):
            b, i = bufs(k)
            block = 2 * xx + 1 - core
            if not isinstance(k, int):
                source = b[1].at[i, xx]
            elif k < ready:
                source = g9.at[k, pl.ds(pl.multiple_of(block * rows, 16), rows), :]
            elif k < pieces:
                source = made.at[k - ready, block]
            else:
                source = made_s.at[block]
            return remote(source, b[1].at[i, xx], c_send.at[k, xx], c_recv.at[k, xx], partner)

        def x_copy(k):
            b, i = bufs(k)
            return remote(b[0].at[i, 1 - x], b[2].at[i], x_send.at[k], x_recv.at[k], across)

        def lanes_of(b, which):
            return pl.ds(pl.multiple_of(which * b[6], 128), b[6])

        def y_copy(k):
            b, i = bufs(k)
            source = b[0].at[i, x, :, lanes_of(b, 1 - y)]
            return remote(source, b[3].at[i], y_send.at[k], y_recv.at[k], beside)

        def rows_of(which):
            return pl.ds(pl.multiple_of(which * quarter, 16), quarter)

        def zs_copy(k, step):
            b, i = bufs(k)
            source = b[0].at[i, x, rows_of(lax.rem(z + step, 4)), lanes_of(b, y)]
            return remote(
                source, b[4].at[i, z], z_send.at[k, step - 1], z_recv.at[k, z], along(step)
            )

        def zr_wait(k, step):
            b, i = bufs(k)
            slot = lax.rem(z + step, 4)
            target = b[4].at[i, slot]
            remote(
                target, target, z_send.at[k, step - 1], z_recv.at[k, slot], along(step)
            ).wait_recv()

        def fs_copy(k, step):
            b, i = bufs(k)
            block = b[5].at[i, rows_of(z), :]
            return remote(block, block, f_send.at[k, step - 1], f_recv.at[k, z], along(step))

        def fr_wait(k, step):
            b, i = bufs(k)
            slot = lax.rem(z + step, 4)
            block = b[5].at[i, rows_of(slot), :]
            remote(
                block, block, f_send.at[k, step - 1], f_recv.at[k, slot], along(step)
            ).wait_recv()

        def final(k, yy):
            b, _ = bufs(k)
            if k < 4:
                return out_f.at[k * rows : (k + 1) * rows, lanes_of(b, yy)]
            if k == 8:
                return out_o.at[:, lanes_of(b, yy)]
            if k == pieces:
                return fin_s.at[shard, :, lanes_of(b, yy)]
            out, at = (out_i, (k - 4) * D) if k < 8 else (out_q, (k - 9) * D)
            return out.at[:, pl.ds(pl.multiple_of(at + yy * half, 128), half)]

        def o_copy(k):
            b, i = bufs(k)
            return remote(b[5].at[i], final(k, y), o_send.at[k], o_recv.at[k], beside)

        def o_wait(k):
            b, i = bufs(k)
            remote(b[5].at[i], final(k, 1 - y), o_send.at[k], o_recv.at[k], beside).wait_recv()

        def o_local(k):
            b, i = bufs(k)
            return pltpu.make_async_copy(b[5].at[i], final(k, y), o_own.at[k])

        def wide(value):
            return value.astype(jnp.float32)

        def stage_x(k):
            b, i = bufs(k)
            for xx in range(2):
                core_copy(k, xx).wait_recv()
                if not isinstance(k, int):
                    pl.when(k < ready)(own_copy(k, xx).wait)
            b[0][i, 1 - x] = (wide(b[0][i, 1 - x]) + wide(b[1][i, 1 - x])).astype(jnp.bfloat16)
            x_copy(k).start()

        def stage_y(k):
            b, i = bufs(k)
            x_copy(k).wait_recv()
            total = wide(b[0][i, x]) + wide(b[1][i, x]) + wide(b[2][i])
            b[0][i, x] = total.astype(jnp.bfloat16)
            y_copy(k).start()

        def stage_z(k):
            b, i = bufs(k)
            y_copy(k).wait_recv()
            lanes = lanes_of(b, y)
            total = wide(b[0][i, x, :, lanes]) + wide(b[3][i])
            b[0][i, x, :, lanes] = total.astype(jnp.bfloat16)
            for step in (2, 1, 3):
                zs_copy(k, step).start()

        def stage_f(k):
            b, i = bufs(k)
            total = wide(b[0][i, x, rows_of(z), lanes_of(b, y)])
            for step in (1, 2, 3):
                zr_wait(k, step)
                total += wide(b[4][i, lax.rem(z + step, 4)])
            b[5][i, rows_of(z), :] = total.astype(jnp.bfloat16)
            for step in (2, 1, 3):
                fs_copy(k, step).start()

        def stage_o(k):
            for step in (1, 2, 3):
                fr_wait(k, step)
            for kk in range(pieces + 1) if not isinstance(k, int) else [k]:

                def begin(kk=kk):
                    o_copy(kk).start()
                    o_local(kk).start()

                if isinstance(k, int):
                    begin()
                else:
                    pl.when(k == kk)(begin)

        def send_core(k):
            for xx in range(2):
                core_copy(k, xx).start()

        for k in range(ahead, ready):
            send_core(k)

        def stages_x(first, last):
            def step(k, carry):
                stage_x(k)
                return carry

            lax.fori_loop(first, last, step, 0)

        for k in range(ahead):
            total_copy(k).wait()
            y_copy(k).start()
        stages_x(ahead, ahead + 2)
        kv = (dkp, dvp)

        def kv_rows(block):
            return pl.ds(pl.multiple_of(block * p_rows, p_rows), p_rows)

        def kv_lanes(g):
            return pl.ds(g * chunk if isinstance(g, int) else pl.multiple_of(g * chunk, chunk), chunk)

        def kv_core(t, g, xx):
            return remote(
                kv[t].at[kv_rows(2 * xx + 1 - core), kv_lanes(g)],
                kr.at[t, xx, :, kv_lanes(g)],
                kc_s.at[g, t, xx],
                kc_r.at[g, t, xx],
                partner,
            )

        def kv_across(t, g):
            return remote(
                kv[t].at[kv_rows(2 * (1 - x) + core), kv_lanes(g)],
                kx.at[t, :, kv_lanes(g)],
                kx_s.at[g, t],
                kx_r.at[g, t],
                across,
            )

        def serve_kv(g):
            block, lanes = kv_rows(2 * (1 - x) + core), kv_lanes(g)
            for t in range(2):
                for xx in range(2):
                    kv_core(t, g, xx).wait_recv()
                total = wide(kv[t][block, lanes]) + wide(kr[t, 1 - x, :, lanes])
                kv[t][block, lanes] = total.astype(jnp.bfloat16)
                kv_across(t, g).start()

        for i in range(7):
            fetch(i).wait()

        def pair(p, carry):
            def between(index):
                if index == 0:
                    pl.when(p + ahead + 2 < ready)(lambda: stage_x(p + ahead + 2))
                if index == 1:
                    pl.when((p == 2) | (p == 4))(lambda: serve_kv(p // 2 - 1))
                if index == 2:
                    pl.when(p >= 1)(lambda: stage_y(p + ahead - 1))
                if index == 3:
                    stage_z(p)
                if index == 4:
                    pl.when(p >= 1)(lambda: stage_f(p - 1))
                if index == 5:
                    pl.when(p >= 2)(lambda: stage_o(p - 2))

            lanes = pl.ds(pl.multiple_of(p * PAIR, PAIR), PAIR)

            def cut(ref):
                return ref.at[:, lanes]

            attend_bwd_pair(
                shard, p_rows, cut(qv), cut(kpv), cut(vpv), cut(kcv), cut(vcv), cut(gav), cut(attv),
                ls.at[p], cut(dq), cut(dkp), cut(dvp), cut(dkc), cut(dvc), accum, between,
            )

            @pl.when(p % 2 == 1)
            def _():
                for t in range(2):
                    for xx in range(2):
                        kv_core(t, p // 2, xx).start()

            return carry

        lax.fori_loop(0, pairs, pair, 0)

        def keep_piece(k, product):
            for block in range(4):
                made[k - ready, block] = product[block * rows : (block + 1) * rows]
            for xx in range(2):
                own[k, xx] = made[k - ready, 2 * xx + core]
            send_core(k)

        product = dot_first(xp[...], dq[:p_rows, :]) + dot_first(xc[...], dq[p_rows:, :])
        keep_piece(9, product.astype(jnp.bfloat16))
        serve_kv(chunks - 1)
        for i in (7, 8):
            fetch(i).wait()
        stages_x(9, 10)
        g_tok[...] += dot_second(dq[...], wv[2])
        stores = [
            pltpu.make_async_copy(g_tok.at[:p_rows, :], out_pg, out_sem.at[0]),
            pltpu.make_async_copy(g_tok.at[p_rows:, :], out_cg, out_sem.at[1]),
        ]

        def with_kv():
            for g in range(chunks):
                for t in range(2):
                    kv_across(t, g).wait_recv()
            for t in range(2):
                total = wide(kv[t][kv_rows(shard), :]) + wide(kr[t, x]) + wide(kx[t])
                kvs[t] = total.astype(jnp.bfloat16)
            g_bias = jnp.sum(wide(dq[...]), 0, keepdims=True)
            v_bias = jnp.sum(wide(dvc[...]), 0, keepdims=True)
            v_bias += jnp.sum(wide(kvs[1]), 0, keepdims=True)
            head[...] = sm[:16, :]
            for part in range(across_lanes):
                lanes = slice(part * 128, (part + 1) * 128)
                head[part : part + 1, STU:] = g_bias[:, lanes]
                head[across_lanes + part : across_lanes + part + 1, STU:] = v_bias[:, lanes]
            for block in range(4):
                made_s[block] = sm[block * rows : (block + 1) * rows, :].astype(jnp.bfloat16)
            made_s[0, :16] = head[...].astype(jnp.bfloat16)
            for xx in range(2):
                own_s[0, xx] = made_s[2 * xx + core]
            send_core(pieces)
            for t in range(2):
                product = dot_first(xp[...], kvs[t]) + dot_first(xc[...], (dkc, dvc)[t][...])
                keep_piece(10 + t, product.astype(jnp.bfloat16))
            stage_x(pieces)
            stages_x(10, 12)
            g_tok[:p_rows, :] += dot_second(kvs[0], wv[0]) + dot_second(kvs[1], wv[1])
            for copy in stores:
                copy.start()

        def cont_part():
            g_tok[p_rows:, :] += dot_second(dkc[...], wv[0]) + dot_second(dvc[...], wv[1])

        def tick(n, carry):
            pl.when(n == 9)(with_kv)
            pl.when((n >= 8) & (n < pieces))(lambda: stage_y(n))
            pl.when(n == 10)(lambda: stage_y(pieces))
            pl.when(n < pieces + 1)(lambda: stage_z(n - 1))
            pl.when(n == 11)(lambda: stage_z(pieces))
            pl.when(n < pieces + 2)(lambda: stage_f(n - 2))
            pl.when(n == 12)(lambda: stage_f(pieces))
            stage_o(n - 3)
            pl.when(n == 13)(lambda: stage_o(pieces))
            pl.when(n == 7)(cont_part)
            return carry

        def g_copy(step):
            return remote(
                fin_s.at[shard],
                fin_s.at[shard],
                g_send.at[step - 1],
                g_recv.at[shard],
                (rep, lax.rem(shard + step, 4)),
            )

        def stage_g():
            o_wait(pieces)
            o_local(pieces).wait()
            for step in (1, 2, 3):
                g_copy(step).start()

        lax.fori_loop(pieces - 5, pieces + 3, tick, 0)
        stage_g()
        for step in (1, 2, 3):
            slot = lax.rem(shard + step, 4)
            remote(
                fin_s.at[slot], fin_s.at[slot], g_send.at[step - 1], g_recv.at[slot], far
            ).wait_recv()

        for k in range(pieces):
            o_wait(k)
            o_local(k).wait()
        for copy in stores:
            copy.wait()

        def sent(k):
            def two():
                for xx in range(2):
                    core_copy(k, xx).wait_send()
                x_copy(k).wait_send()

            if isinstance(k, int):
                two()
            else:
                pl.when(k >= ahead)(two)
            y_copy(k).wait_send()
            for step in (1, 2, 3):
                zs_copy(k, step).wait_send()
                fs_copy(k, step).wait_send()

        def sent_step(k, carry):
            sent(k)
            return carry

        lax.fori_loop(0, pieces, sent_step, 0)
        sent(pieces)
        for k in range(pieces + 1):
            o_copy(k).wait_send()
        for step in (1, 2, 3):
            g_copy(step).wait_send()
        for g in range(chunks):
            for t in range(2):
                for xx in range(2):
                    kv_core(t, g, xx).wait_send()
                kv_across(t, g).wait_send()

    def sems(*dims):
        return pltpu.SemaphoreType.DMA(dims)

    def low(*dims):
        return pltpu.VMEM(dims, jnp.bfloat16)

    def full(*dims):
        return pltpu.VMEM(dims, jnp.float32)

    def buffers(count, columns):
        cut = columns // 2
        return [
            low(count, 2, rows, columns),
            low(count, 2, rows, columns),
            low(count, rows, columns),
            low(count, rows, cut),
            low(count, 4, quarter, cut),
            low(count, rows, cut),
        ]

    def shaped(dims, kind=jnp.float32):
        return jax.ShapeDtypeStruct(dims, kind)

    n = pieces + 1
    anywhere = pl.BlockSpec(memory_space=pl.ANY)
    vmem = pl.BlockSpec(memory_space=pltpu.VMEM)
    return pl.pallas_call(
        kernel,
        in_specs=[anywhere] * 11 + [vmem] * 4,
        out_specs=[anywhere] * 6 + [vmem],
        out_shape=[
            shaped((p_rows, D)),
            shaped((cont_len, D)),
            shaped((rows, 3 * D), jnp.bfloat16),
            shaped((rows, D), jnp.bfloat16),
            shaped((rows, ff), jnp.bfloat16),
            shaped((4 * rows, D), jnp.bfloat16),
            shaped((4, rows, s_width), jnp.bfloat16),
        ],
        scratch_shapes=[
            low(tokens, D), low(p_len, D), low(p_len, D), low(cont_len, D), low(cont_len, D),
            full(tokens, D), low(tokens, D), full(PAIR, tokens), low(tokens, D),
            low(p_len, D), low(p_len, D), low(cont_len, D), low(cont_len, D),
            low(2, 2, p_rows, D), low(2, p_rows, D), low(2, p_rows, D), low(3, D, D),
            full(tokens, D), low(3, 4, rows, D), full(16, s_width),
        ]
        + buffers(pieces, D)
        + [low(4, rows, s_width)]
        + buffers(1, s_width)
        + [
            sems(9), sems(n, 2), sems(n, 2), sems(n, 2), sems(n), sems(n), sems(n), sems(n),
            sems(n, 3), sems(n, 4), sems(n, 3), sems(n, 4), sems(n), sems(n), sems(n),
            sems(3), sems(4), sems(chunks, 2, 2), sems(chunks, 2, 2), sems(chunks, 2),
            sems(chunks, 2), sems(2),
        ],
        compiler_params=pltpu.CompilerParams(
            collective_id=2, has_side_effects=True, vmem_limit_bytes=VMEM_ALL
        ),
        name="finish",
    )(q, kp, vp, kc, vc, att, g_att, g9, g_resid, w_all, totals, lse, small, prompt, conts)


def place(g_prompt, g_conts, owned, out_p, out_c, logits, summed, ff, classes):
    big = [g_prompt, g_conts, *owned, out_p, out_c]
    count = len(big)
    order = (2, 4, 5, 3, 1, 0, 7, 6)
    rows, across = summed.shape[1], D // 128

    def kernel(*refs):
        sources, fin, logits_in = refs[:count], refs[count], refs[count + 1]
        outs = refs[count + 2 :]
        targets = outs[:count]
        o_bias, o_gain, o_in, o_stu, o_vec, o_pool, o_class, o_cb, o_logits = outs[count : count + 9]
        scratch = outs[count + 9 :]
        held, turned, (sem_in, sem_out) = scratch[:count], scratch[count:-2], scratch[-2:]
        reads = [pltpu.make_async_copy(sources[i], held[i], sem_in.at[i]) for i in order]
        for copy in reads:
            copy.start()

        def side(block):
            return fin[block, :, STU:].astype(jnp.float32)

        first = side(0)
        for i in range(8):
            target, at = (o_bias, i) if i < 6 else (o_gain, i - 6)
            for part in range(across):
                r = i * across + part
                target[at : at + 1, part * 128 : (part + 1) * 128] = first[r : r + 1, :]
        for part in range(ff // 128):
            r = 8 * across + part
            o_in[:, part * 128 : (part + 1) * 128] = first[r : r + 1, :]
        base = 8 * across + ff // 128
        o_vec[...] = first[base : base + 3, :]
        o_cb[...] = first[base + 3 : base + 4, :classes]
        every = jnp.concatenate([first, side(1)], 0)
        o_pool[...] = every[base + 8 : base + 8 + STU, :]
        o_class[...] = every[base + 8 + STU : base + 8 + STU + classes, :]
        for block in range(4):
            o_stu[block * rows : (block + 1) * rows, :] = fin[block, :, :STU].astype(jnp.float32)
        writes = []
        o_logits[...] = logits_in[...]
        for copy, i in zip(reads, order):
            copy.wait()
            source = held[i]
            if 2 <= i < 6:
                source = turned[i - 2]
                source[...] = held[i][...].astype(jnp.float32)
            writes.append(pltpu.make_async_copy(source, targets[i], sem_out.at[i]))
            writes[-1].start()
        for copy in writes:
            copy.wait()

    def shaped(*dims):
        return jax.ShapeDtypeStruct(dims, jnp.float32)

    anywhere = pl.BlockSpec(memory_space=pl.ANY)
    vmem = pl.BlockSpec(memory_space=pltpu.VMEM)
    return pl.pallas_call(
        kernel,
        in_specs=[anywhere] * count + [vmem] * 2,
        out_specs=[anywhere] * count + [vmem] * 9,
        out_shape=[shaped(*part.shape) for part in big[:6]]
        + [jax.ShapeDtypeStruct(part.shape, part.dtype) for part in big[6:]]
        + [
            shaped(6, D),
            shaped(2, D),
            shaped(1, ff),
            shaped(D, STU),
            shaped(3, STU),
            shaped(STU, STU),
            shaped(classes, STU),
            shaped(1, classes),
            shaped(1, classes),
        ],
        scratch_shapes=[pltpu.VMEM(part.shape, part.dtype) for part in big]
        + [pltpu.VMEM(part.shape, jnp.float32) for part in owned]
        + [pltpu.SemaphoreType.DMA((count,)), pltpu.SemaphoreType.DMA((count,))],
        compiler_params=pltpu.CompilerParams(vmem_limit_bytes=VMEM_ALL),
        name="place",
    )(*big, summed, logits)


def body(
    prompt,
    conts,
    prompt_cot,
    cont_cot,
    labels,
    w_qkv,
    w_out,
    w_in,
    w_ffo,
    layer_biases,
    norm_gains,
    bias_in,
    w_student,
    student_vectors,
    w_pool,
    w_class,
    bias_class,
):
    prompt_rows = prompt.shape[1]
    direct = (lax.axis_size("rep"), lax.axis_size("shard")) == (8, 4)
    project = project_and_attend if direct else project_native
    w_all, ffo_full, q, kp, vp, kc, vc, attended, log_totals, state = project(
        prompt[0], conts[0, 0], w_qkv, w_out, w_in, w_ffo, layer_biases, norm_gains, bias_in
    )
    ahead = 3 if direct else 0
    out_p, out_c, logits, g9, g_resid, g_att, small, totals = middle(
        ahead,
        state,
        prompt_cot[0],
        cont_cot[0, 0],
        labels,
        w_all,
        ffo_full,
        layer_biases,
        norm_gains,
        bias_in,
        w_student,
        student_vectors,
        w_pool,
        w_class,
        bias_class,
    )
    ff, classes = bias_in.shape[0], w_class.shape[1]
    if direct:
        outs = finish(
            ahead, totals, q, kp, vp, kc, vc, attended, log_totals, g_att, g9, g_resid, small, w_all,
            prompt[0], conts[0, 0], ff,
        )
        placed = place(outs[0], outs[1], outs[2:6], out_p, out_c, logits, outs[6], ff, classes)
        g_prompt, g_conts, owned, out_p, out_c = placed[0], placed[1], placed[2:6], *placed[6:8]
        biases, gains_g, g_in, g_student, g_vectors, g_pool, g_class, g_cb, logits = placed[8:]
    else:
        g_q, g_kp, g_vp, g_kc, g_vc = attend_backward(
            q, kp, vp, kc, vc, g_att, attended, log_totals, prompt_rows
        )
        tokens = jnp.concatenate([prompt[0], conts[0, 0]], 0)
        kv_sum = [
            lax.psum_scatter(part, "shard", scatter_dimension=0, tiled=True)
            for part in (g_kp, g_vp)
        ]
        g_k = jnp.concatenate([kv_sum[0], g_kc], 0)
        g_v = jnp.concatenate([kv_sum[1], g_vc], 0)
        g_tokens = g_resid
        for part, weight in ((g_k, w_all[0]), (g_v, w_all[1]), (g_q, w_all[2])):
            g_tokens = g_tokens + dot_second(part, weight)
        g_prompt, g_conts = g_tokens[:prompt_rows], g_tokens[prompt_rows:]
        g_qkvw = jnp.concatenate([dot_first(tokens, part) for part in (g_q, g_k, g_v)], 1)
        side = small[:, STU:]
        across = D // 128
        for at, part in ((0, g_q), (1, g_v)):
            total = jnp.sum(part.astype(jnp.float32), 0).reshape(across, 128)
            side = lax.dynamic_update_slice(side, total, (at * across, 0))
        small = jnp.concatenate([small[:, :STU], side], 1)
        owned, summed = sum_native(g9, g_qkvw, small)
        side = summed[:, STU:]
        base = 8 * across + ff // 128
        biases = side[: 6 * across].reshape(6, D)
        gains_g = side[6 * across : 8 * across].reshape(2, D)
        g_in = side[8 * across : base]
        g_student, g_vectors = summed[:, :STU], side[base : base + 3]
        g_pool = side[base + 8 : base + 8 + STU]
        g_class = side[base + 8 + STU : base + 8 + STU + classes]
        g_cb = side[base + 3 : base + 4]
    return (
        out_p[None],
        out_c[None, None],
        logits[None],
        g_prompt[None],
        g_conts[None, None],
        *owned,
        biases,
        gains_g,
        g_in.reshape(ff),
        g_student,
        g_vectors,
        g_pool,
        g_class.T,
        g_cb[0, :classes],
    )


def solution(mesh):
    return jax.shard_map(
        body,
        mesh=mesh,
        in_specs=(
            P("rep", "shard", None),
            P("rep", "shard", None, None),
            P("rep", "shard", None),
            P("rep", "shard", None, None),
            P("rep", "shard"),
            P("shard", None),
            P("shard", None),
            P("shard", None),
            P("shard", None),
            P(),
            P(),
            P(),
            P(),
            P(),
            P(),
            P(),
            P(),
        ),
        out_specs=(
            P("rep", "shard", None),
            P("rep", "shard", None, None),
            P("rep", "shard", None),
            P("rep", "shard", None),
            P("rep", "shard", None, None),
            P("shard", None),
            P("shard", None),
            P("shard", None),
            P("shard", None),
            P(),
            P(),
            P(),
            P(),
            P(),
            P(),
            P(),
            P(),
        ),
        check_vma=False,
    )
```

```python
import functools

import jax
import jax.numpy as jnp
from jax import lax
from jax.experimental import pallas as pl
from jax.experimental.pallas import tpu as pltpu
from jax.sharding import PartitionSpec as P

D = 768
HEADS = 12
DH = 64
STU = 128
SHEADS = 2


HIGHEST = lax.Precision.HIGHEST
NEG_BIG = -1e30


def dot_plain(left, right):
    return jnp.dot(left, right, preferred_element_type=jnp.float32)


def dot_first(left, right):
    return lax.dot_general(
        left, right, (((0,), (0,)), ((), ())), preferred_element_type=jnp.float32
    )


def dot_second(left, right):
    return lax.dot_general(
        left, right, (((1,), (1,)), ((), ())), preferred_element_type=jnp.float32
    )


TILE = 256
PAIR = 128
VMEM_ALL = 62 * 1024 * 1024


def rows_dot(left, right):
    return lax.dot_general(
        left, right, (((1,), (1,)), ((), ())), preferred_element_type=jnp.float32
    )


def low_lanes(shape):
    return lax.broadcasted_iota(jnp.int32, shape, len(shape) - 1) < DH


def attend_fwd_pair(
    shard, prompt_rows, q, kp, vp, kc, vc, att_ref, lse_ref, between=None
):
    cont_len = kc.shape[0]
    prompt_len = kp.shape[0]
    for start in range(0, prompt_rows + cont_len, TILE):
        q_t = q[start : start + TILE, :] * jnp.asarray(DH ** (-0.5), jnp.bfloat16)
        halves = []
        for parity in range(2):
            keep = low_lanes(q_t.shape) == (parity == 0)
            q_h = jnp.where(keep, q_t, jnp.zeros_like(q_t))
            s_p = rows_dot(q_h, kp[...])
            if start < prompt_rows:
                key = lax.broadcasted_iota(jnp.int32, s_p.shape, 1)
                row = lax.broadcasted_iota(jnp.int32, s_p.shape, 0)
                s_p = jnp.where(key <= row + (shard * prompt_rows + start), s_p, NEG_BIG)
                largest = jnp.max(s_p, 1, keepdims=True)
                p_p = jnp.exp(s_p - largest)
                total = jnp.sum(p_p, 1, keepdims=True)
                o = dot_plain(p_p.astype(jnp.bfloat16), vp[...])
            else:
                seen = start - prompt_rows + TILE
                s_c = rows_dot(q_h, kc[:seen, :])
                key = lax.broadcasted_iota(jnp.int32, s_c.shape, 1)
                row = lax.broadcasted_iota(jnp.int32, s_c.shape, 0)
                s_c = jnp.where(key <= row + (start - prompt_rows), s_c, NEG_BIG)
                largest = jnp.maximum(
                    jnp.max(s_p, 1, keepdims=True), jnp.max(s_c, 1, keepdims=True)
                )
                p_p = jnp.exp(s_p - largest)
                p_c = jnp.exp(s_c - largest)
                total = jnp.sum(p_p, 1, keepdims=True) + jnp.sum(p_c, 1, keepdims=True)
                o = dot_plain(p_p.astype(jnp.bfloat16), vp[...]) + dot_plain(
                    p_c.astype(jnp.bfloat16), vc[:seen, :]
                )
            halves.append((o / total, largest + jnp.log(total)))
        keep = low_lanes((TILE, PAIR))
        att_ref[start : start + TILE, :] = jnp.where(keep, halves[0][0], halves[1][0])
        lse = jnp.where(
            keep,
            jnp.broadcast_to(halves[0][1], (TILE, PAIR)),
            jnp.broadcast_to(halves[1][1], (TILE, PAIR)),
        )
        turned = jnp.transpose(lse)
        lse_ref[0:1, start : start + TILE] = turned[0:1, :]
        lse_ref[1:2, start : start + TILE] = turned[DH : DH + 1, :]
        if between is not None:
            between(start // TILE)


def attend_bwd_pair(
    shard, prompt_rows, q, kp, vp, kc, vc, g, att, lse, dq, dkp, dvp, dkc, dvc, accum, between=None
):
    cont_len = kc.shape[0]
    tokens = prompt_rows + cont_len
    prompt_len = kp.shape[0]
    g_t = g[...]
    turned = jnp.transpose(g_t.astype(jnp.float32) * att[...])
    delta = (
        jnp.sum(turned[:DH], 0, keepdims=True),
        jnp.sum(turned[DH:], 0, keepdims=True),
    )
    q_t = q[...] * jnp.asarray(DH ** (-0.5), jnp.bfloat16)
    keep = low_lanes(q_t.shape)
    zero = jnp.zeros_like(q_t)
    q_h = (jnp.where(keep, q_t, zero), jnp.where(keep, zero, q_t))
    g_h = (jnp.where(keep, g_t, zero), jnp.where(keep, zero, g_t))
    accum[...] = jnp.zeros_like(accum)

    def block(key_b, value_b, first, mask):
        key_t = jnp.transpose(key_b.astype(jnp.float32)).astype(jnp.bfloat16)
        g_key = jnp.zeros((TILE, PAIR), jnp.float32)
        g_value = jnp.zeros((TILE, PAIR), jnp.float32)
        for parity in range(2):
            scores = rows_dot(key_b, q_h[parity][first:])
            probs = jnp.exp(scores - lse[parity : parity + 1, first:])
            masked = jnp.where(mask, probs[:, :TILE], 0.0)
            if tokens - first > TILE:
                probs = jnp.concatenate([masked, probs[:, TILE:]], 1)
            else:
                probs = masked
            g_probs = rows_dot(value_b, g_h[parity][first:])
            g_scores = (probs * (g_probs - delta[parity][:, first:])).astype(jnp.bfloat16)
            g_value += dot_plain(probs.astype(jnp.bfloat16), g_h[parity][first:])
            g_key += dot_plain(g_scores, q_h[parity][first:])
            rows = slice(parity * DH, (parity + 1) * DH)
            accum[rows, first:] += dot_plain(key_t[rows], g_scores)
        return g_key.astype(jnp.bfloat16), g_value.astype(jnp.bfloat16)

    ahead = lax.broadcasted_iota(jnp.int32, (TILE, TILE), 0) - lax.broadcasted_iota(
        jnp.int32, (TILE, TILE), 1
    )

    def prompt_block(index, start):
        rows = pl.ds(start, TILE)
        mask = ahead <= shard * prompt_rows - index * TILE
        g_key, g_value = block(kp[rows, :], vp[rows, :], 0, mask)
        dkp[rows, :] = g_key
        dvp[rows, :] = g_value

    blocks = prompt_len // TILE
    if blocks <= 4:
        for index in range(blocks):
            prompt_block(index, index * TILE)
            if between is not None:
                between(index)
    else:

        def step(index, carry):
            prompt_block(index, pl.multiple_of(index * TILE, TILE))
            return carry

        lax.fori_loop(0, blocks, step, 0)
    for start in range(0, cont_len, TILE):
        rows = slice(start, start + TILE)
        g_key, g_value = block(kc[rows, :], vc[rows, :], prompt_rows + start, ahead <= 0)
        dkc[rows, :] = g_key
        dvc[rows, :] = g_value
        if between is not None:
            between(blocks + start // TILE)
    dq[...] = (jnp.transpose(accum[...]) * DH ** (-0.5)).astype(jnp.bfloat16)


def attend_forward(q, kp, vp, kc, vc, prompt_rows):
    tokens, prompt_len, cont_len = q.shape[0], kp.shape[0], kc.shape[0]
    pairs = HEADS // 2

    def kernel(q, kp, vp, kc, vc, att_ref, lse_ref):
        attend_fwd_pair(
            lax.axis_index("shard"), prompt_rows, q, kp, vp, kc, vc, att_ref, lse_ref.at[0]
        )

    def columns(rows):
        return pl.BlockSpec((rows, PAIR), lambda p: (0, p))

    return pl.pallas_call(
        kernel,
        grid=(pairs,),
        in_specs=[columns(rows) for rows in (tokens, prompt_len, prompt_len, cont_len, cont_len)],
        out_specs=[columns(tokens), pl.BlockSpec((1, 8, tokens), lambda p: (p, 0, 0))],
        out_shape=[
            jax.ShapeDtypeStruct((tokens, D), jnp.float32),
            jax.ShapeDtypeStruct((pairs, 8, tokens), jnp.float32),
        ],
        compiler_params=pltpu.CompilerParams(vmem_limit_bytes=VMEM_ALL),
        name="attend_forward",
    )(q, kp, vp, kc, vc)


def attend_backward(q, kp, vp, kc, vc, g_att, att, lse, prompt_rows):
    tokens, prompt_len, cont_len = q.shape[0], kp.shape[0], kc.shape[0]
    pairs = HEADS // 2

    def kernel(q, kp, vp, kc, vc, g, a, ls, dq, dkp, dvp, dkc, dvc, accum):
        attend_bwd_pair(
            lax.axis_index("shard"),
            prompt_rows,
            q,
            kp,
            vp,
            kc,
            vc,
            g,
            a,
            ls.at[0],
            dq,
            dkp,
            dvp,
            dkc,
            dvc,
            accum,
        )

    def columns(rows):
        return pl.BlockSpec((rows, PAIR), lambda p: (0, p))

    sizes = (tokens, prompt_len, prompt_len, cont_len, cont_len)
    return pl.pallas_call(
        kernel,
        grid=(pairs,),
        in_specs=[columns(rows) for rows in sizes + (tokens, tokens)]
        + [pl.BlockSpec((1, 8, tokens), lambda p: (p, 0, 0))],
        out_specs=[columns(rows) for rows in sizes],
        out_shape=[jax.ShapeDtypeStruct((rows, D), jnp.bfloat16) for rows in sizes],
        scratch_shapes=[pltpu.VMEM((PAIR, tokens), jnp.float32)],
        compiler_params=pltpu.CompilerParams(vmem_limit_bytes=VMEM_ALL),
        name="attend_backward",
    )(q, kp, vp, kc, vc, g_att, att, lse)


MESH_ID = pl.DeviceIdType.MESH


def project_and_attend(
    prompt, conts, w_qkv, w_out, w_in, w_ffo, layer_biases, norm_gains, bias_in
):
    pieces, early = 12, 4
    ff = bias_in.shape[0]
    wide = D // TILE
    inner_steps = ff // TILE
    by_z = (4, 5, 6, 7, 8, 9)
    rows = w_qkv.shape[0]
    p_rows, cont_len = prompt.shape[0], conts.shape[0]
    tokens = p_rows + cont_len
    p_len = 4 * p_rows
    pairs = HEADS // 2
    tiles = tokens // TILE
    steps = tokens // TILE
    chunk = PAIR
    chunks = D // chunk
    quarter = rows // 4

    def kernel(
        xp, xc, wq, wo, wi, wf, bias, gain, b_in, w_all_out, wf_out, q_out, kc_out, vc_out, kp_out, vp_out, att_out,
        norm_out, x1_out, act_out, slope_out, att_b_out, lse, rstd_out,
        stage, w_all, q, kc, vc, kp, vp, att, norm1, x1_b, act, slope, att_b,
        load, c_s, c_r, x_s, x_r, y_s, y_r, z_s, z_r, d_s, d_r, e_s, e_r, w_sem,
        kc_s, kc_r, kx_s, kx_r, kd_s, kd_r, out_sem, ff_sem, row_sem,
    ):
        rep, shard = lax.axis_index("rep"), lax.axis_index("shard")
        z, y = rep // 2, rep % 2
        x, core = shard // 2, shard % 2
        partner = (rep, 2 * x + 1 - core)
        across = (rep, 2 * (1 - x) + core)
        beside = (2 * z + 1 - y, shard)
        z_low = z % 2
        above = (2 * (z + 1 - 2 * z_low) + y, shard)
        there = 2 * (1 - x) + core

        def remote(ref, send, recv, device):
            return pltpu.make_async_remote_copy(
                src_ref=ref,
                dst_ref=ref,
                send_sem=send,
                recv_sem=recv,
                device_id=device,
                device_id_type=MESH_ID,
            )

        def source(k):
            if k < 3:
                j = (1, 2, 0)[k]
                return wq.at[:, j * D : (j + 1) * D]
            if k < 4:
                return wo
            if k < 8:
                return wi.at[:, (k - 4) * D : (k - 3) * D]
            return wf.at[(k - 8) * rows : (k - 7) * rows, :]

        def loading(k):
            return pltpu.make_async_copy(source(k), stage.at[k], load.at[k])

        for k in range(pieces):
            loading(k).start()
        barrier = pltpu.get_barrier_semaphore()
        for other in (partner, across, beside, above):
            pl.semaphore_signal(barrier, inc=1, device_id=other, device_id_type=MESH_ID)
        pl.semaphore_wait(barrier, 4)

        def part(k, block, first, count):
            start = pl.multiple_of(first * quarter, 16)
            return w_all.at[k, block, pl.ds(start, count * quarter), :]

        def core_copy(k):
            return remote(w_all.at[k, shard], c_s.at[k], c_r.at[k], partner)

        def core_arrival(k):
            return remote(w_all.at[k, 2 * x + 1 - core], c_s.at[k], c_r.at[k], partner)

        def crossing(k, y_at):
            return (2 * z_low + y_at, 1) if k in by_z else (2 * y_at, 2)

        def x_copy(k):
            return remote(part(k, shard, *crossing(k, y)), x_s.at[k], x_r.at[k], across)

        def x_arrival(k):
            return remote(part(k, there, *crossing(k, y)), x_s.at[k], x_r.at[k], across)

        def y_copy(k):
            return remote(part(k, there, *crossing(k, y)), y_s.at[k], y_r.at[k], beside)

        def y_arrival(k):
            return remote(part(k, there, *crossing(k, 1 - y)), y_s.at[k], y_r.at[k], beside)

        def z_copy(k):
            return remote(part(k, there, 2 * z_low, 2), z_s.at[k], z_r.at[k], above)

        def z_arrival(k):
            return remote(part(k, there, 2 * (1 - z_low), 2), z_s.at[k], z_r.at[k], above)

        def halves(k):
            first = 2 * z_low if k in by_z else 2 * y
            return first, 2 - first

        def d_copy(k, block=None):
            block = there if block is None else block
            return remote(part(k, block, halves(k)[0], 2), d_s.at[k], d_r.at[k], partner)

        def e_copy(k, block=None):
            block = there if block is None else block
            return remote(part(k, block, halves(k)[1], 2), e_s.at[k], e_r.at[k], partner)

        far = 2 * (1 - x) + 1 - core

        def send_piece(k):
            x_copy(k).start()
            core_copy(k).start()

        def round_piece(k):
            loading(k).wait()
            w_all[k, shard] = stage[k].astype(jnp.bfloat16)

        def serve_x(k):
            x_arrival(k).wait_recv()
            y_copy(k).start()
            if k not in by_z:
                d_copy(k).start()

        def serve_y(k):
            y_arrival(k).wait_recv()
            if k in by_z:
                z_copy(k).start()
                d_copy(k).start()
            else:
                e_copy(k).start()

        def serve_z(k):
            z_arrival(k).wait_recv()
            e_copy(k).start()

        def w_store(k):
            if k < 8:
                return pltpu.make_async_copy(w_all.at[k], w_all_out.at[k], w_sem.at[k])
            return pltpu.make_async_copy(w_all.at[k], wf_out.at[:, k - 8], w_sem.at[k])

        def complete(k):
            core_arrival(k).wait_recv()
            d_copy(k, far).wait_recv()
            e_copy(k, far).wait_recv()
            w_store(k).start()

        def weight(k):
            return w_all[k].reshape(4 * rows, D)

        for k in range(early):
            round_piece(k)
            send_piece(k)
        for k in range(early, pieces):
            round_piece(k)
        own_rows = pl.ds(pl.multiple_of(shard * p_rows, p_rows), p_rows)
        kv = (kp, vp)

        def kv_part(t, g, block):
            lanes = pl.ds(g * chunk if isinstance(g, int) else pl.multiple_of(g * chunk, chunk), chunk)
            return kv[t].at[pl.ds(pl.multiple_of(block * p_rows, p_rows), p_rows), lanes]

        def kv_core(t, g):
            return remote(kv_part(t, g, shard), kc_s.at[g, t], kc_r.at[g, t], partner)

        def kv_across(t, g):
            return remote(kv_part(t, g, shard), kx_s.at[g, t], kx_r.at[g, t], across)

        def kv_forward(t, g):
            return remote(kv_part(t, g, there), kd_s.at[g, t], kd_r.at[g, t], partner)

        serve_x(0)
        serve_x(1)
        serve_y(0)
        complete(0)
        kp[own_rows, :] = dot_plain(xp[...], weight(0)).astype(jnp.bfloat16)
        kc[...] = dot_plain(xc[...], weight(0)).astype(jnp.bfloat16)
        serve_x(2)
        serve_y(1)
        complete(1)
        vp[own_rows, :] = (dot_plain(xp[...], weight(1)) + bias[1:2, :]).astype(jnp.bfloat16)
        waiting = list(range(early, pieces))
        for g in range(chunks):
            for t in range(2):
                kv_across(t, g).start()
                kv_core(t, g).start()
            sent = 0 if g == 0 else 1 if g < chunks - 1 else pieces
            for k in waiting[:sent]:
                send_piece(k)
            waiting = waiting[sent:]
        vc[...] = (dot_plain(xc[...], weight(1)) + bias[1:2, :]).astype(jnp.bfloat16)
        serve_y(2)
        serve_x(3)
        complete(2)
        q[:p_rows, :] = (dot_plain(xp[...], weight(2)) + bias[0:1, :]).astype(jnp.bfloat16)
        q[p_rows:, :] = (dot_plain(xc[...], weight(2)) + bias[0:1, :]).astype(jnp.bfloat16)

        def keep(ref, target, i):
            return pltpu.make_async_copy(ref, target, out_sem.at[i])

        kept = [(q, q_out, 0), (kc, kc_out, 1), (vc, vc_out, 2)]
        for item in kept:
            keep(*item).start()

        def serve_kv(g):
            for t in range(2):
                remote(kv_part(t, g, there), kx_s.at[g, t], kx_r.at[g, t], across).wait_recv()
                kv_forward(t, g).start()

        def complete_kv(g):
            for t in range(2):
                remote(
                    kv_part(t, g, 2 * x + 1 - core), kc_s.at[g, t], kc_r.at[g, t], partner
                ).wait_recv()
                remote(kv_part(t, g, far), kd_s.at[g, t], kd_r.at[g, t], partner).wait_recv()

        serve_kv(0)
        arrive = {4: 26.2, 5: 30.6, 6: 35.1, 7: 39.5, 8: 43.9, 9: 45.5, 10: 48.7, 11: 51.9}
        work = [(27.0, serve_y, 3), (30.0, complete, 3)]
        forward = (27.0, 31.1, 35.5, 39.9, 44.3)
        work += [(at, serve_kv, g + 1) for g, at in enumerate(forward)]
        for k in range(4, pieces):
            at = arrive[k]
            work.append((at, serve_x, k))
            if k in by_z:
                work += [(at + 4, serve_y, k), (at + 10, serve_z, k), (at + 13, complete, k)]
            else:
                work += [(at + 6, serve_y, k), (at + 9, complete, k)]
        slots = pairs * tiles
        work.sort(key=lambda item: item[0])
        later = [item for item in work if item[0] > 26 + 1.37 * slots]
        work = [(max(0, round((at - 26) / 1.37 - 0.6)), job, k) for at, job, k in work if at <= 26 + 1.37 * slots]
        work = [(min(slot, slots - 1), job, k) for slot, job, k in work]

        def att_store(p):
            lanes = pl.ds(pl.multiple_of(p * PAIR, PAIR), PAIR)
            return pltpu.make_async_copy(att.at[:, lanes], att_out.at[:, lanes], out_sem.at[5 + p])

        def pair(p, carry):
            complete_kv(p)

            def between(tile):
                for slot, action, k in work:
                    if slot < slots and slot % tiles == tile:

                        @pl.when(p == slot // tiles)
                        def _(action=action, k=k):
                            action(k)

            lanes = pl.ds(pl.multiple_of(p * PAIR, PAIR), PAIR)
            attend_fwd_pair(
                shard,
                p_rows,
                q.at[:, lanes],
                kp.at[:, lanes],
                vp.at[:, lanes],
                kc.at[:, lanes],
                vc.at[:, lanes],
                att.at[:, lanes],
                lse.at[p],
                between,
            )
            att_store(p).start()
            return carry

        lax.fori_loop(0, pairs, pair, 0)
        kept += [(kp, kp_out, 3), (vp, vp_out, 4)]
        for item in kept[3:]:
            keep(*item).start()

        def row(i):
            return pl.ds(pl.multiple_of(i * TILE, TILE), TILE)

        def row_stores(i):
            pairs_of = [(norm1, norm_out), (x1_b, x1_out), (att_b, att_b_out)]
            return [
                pltpu.make_async_copy(ref.at[row(i), :], out.at[row(i), :], row_sem.at[n, i])
                for n, (ref, out) in enumerate(pairs_of)
            ]

        def normalized(i, carry):
            part = att[row(i), :].astype(jnp.bfloat16)
            att_b[row(i), :] = part
            values = dot_plain(part, weight(3)) + bias[2:3, :] + norm1[row(i), :]
            center = values - jnp.mean(values, -1, keepdims=True)
            spread = jnp.mean(center * center, -1, keepdims=True)
            scale = lax.rsqrt(spread + 1e-05)
            hat = center * scale
            norm1[row(i), :] = hat
            rstd_out[row(i), :] = jnp.broadcast_to(scale, (TILE, 128))
            x1_b[row(i), :] = (hat * gain[0:1, :] + bias[4:5, :]).astype(jnp.bfloat16)
            for copy in row_stores(i):
                copy.start()
            return carry

        norm1[:p_rows, :] = xp[...].astype(jnp.float32)
        norm1[p_rows:, :] = xc[...].astype(jnp.float32)
        lax.fori_loop(0, steps, normalized, 0)

        def ff_stores(i):
            columns = pl.ds(pl.multiple_of(i * TILE, TILE), TILE)
            return [
                pltpu.make_async_copy(ref.at[:, columns], out.at[:, columns], ff_sem.at[n, i])
                for n, (ref, out) in enumerate([(act, act_out), (slope, slope_out)])
            ]

        def inner(i, carry):
            lanes = pl.ds(pl.multiple_of(lax.rem(i, wide) * TILE, TILE), TILE)
            columns = pl.ds(pl.multiple_of(i * TILE, TILE), TILE)
            block = w_all[4 + i // wide, :, :, lanes].reshape(D, TILE)
            hidden = dot_plain(x1_b[...], block) + b_in[:, columns]
            cdf = 0.5 * (1.0 + lax.erf(hidden * 2.0 ** (-0.5)))
            act[:, columns] = (hidden * cdf).astype(jnp.bfloat16)
            density = jnp.exp(hidden * hidden * (-0.5)) * 0.3989422804014327
            slope[:, columns] = (cdf + hidden * density).astype(jnp.bfloat16)
            for copy in ff_stores(i):
                copy.start()
            for at, job, k in later:
                step = min(max(0, round((at - 54.5) / 0.73 - 0.5)), inner_steps - 1)
                pl.when(i == step)(functools.partial(job, k))
            return carry

        lax.fori_loop(0, inner_steps, inner, 0)

        def ff_wait(i, carry):
            for copy in ff_stores(i):
                copy.wait()
            return carry

        lax.fori_loop(0, inner_steps, ff_wait, 0)

        def row_wait(i, carry):
            for copy in row_stores(i):
                copy.wait()
            return carry

        lax.fori_loop(0, steps, row_wait, 0)
        for item in kept:
            keep(*item).wait()

        def last_pair(p, carry):
            att_store(p).wait()
            return carry

        lax.fori_loop(0, pairs, last_pair, 0)
        for k in range(pieces):
            w_store(k).wait()
            for copy in (core_copy, x_copy, y_copy, d_copy, e_copy):
                copy(k).wait_send()
            if k in by_z:
                z_copy(k).wait_send()
        for g in range(chunks):
            for t in range(2):
                for copy in (kv_core, kv_across, kv_forward):
                    copy(t, g).wait_send()

    def sems(*dims):
        return pltpu.SemaphoreType.DMA(dims)

    def low(*dims):
        return jax.ShapeDtypeStruct(dims, jnp.bfloat16)

    anywhere = pl.BlockSpec(memory_space=pl.ANY)
    vmem = pl.BlockSpec(memory_space=pltpu.VMEM)
    n = pieces
    out = pl.pallas_call(
        kernel,
        in_specs=[vmem, vmem, anywhere, anywhere, anywhere, anywhere, vmem, vmem, vmem],
        out_specs=[anywhere] * 13 + [vmem] * 2,
        out_shape=[
            low(8, 4, rows, D),
            low(4, 4, rows, D),
            low(tokens, D),
            low(cont_len, D),
            low(cont_len, D),
            low(p_len, D),
            low(p_len, D),
            jax.ShapeDtypeStruct((tokens, D), jnp.float32),
            jax.ShapeDtypeStruct((tokens, D), jnp.float32),
            low(tokens, D),
            low(tokens, ff),
            low(tokens, ff),
            low(tokens, D),
            jax.ShapeDtypeStruct((pairs, 8, tokens), jnp.float32),
            jax.ShapeDtypeStruct((tokens, 128), jnp.float32),
        ],
        scratch_shapes=[
            pltpu.VMEM((n, rows, D), jnp.float32),
            pltpu.VMEM((n, 4, rows, D), jnp.bfloat16),
            pltpu.VMEM((tokens, D), jnp.bfloat16),
            pltpu.VMEM((cont_len, D), jnp.bfloat16),
            pltpu.VMEM((cont_len, D), jnp.bfloat16),
            pltpu.VMEM((p_len, D), jnp.bfloat16),
            pltpu.VMEM((p_len, D), jnp.bfloat16),
            pltpu.VMEM((tokens, D), jnp.float32),
            pltpu.VMEM((tokens, D), jnp.float32),
            pltpu.VMEM((tokens, D), jnp.bfloat16),
            pltpu.VMEM((tokens, ff), jnp.bfloat16),
            pltpu.VMEM((tokens, ff), jnp.bfloat16),
            pltpu.VMEM((tokens, D), jnp.bfloat16),
        ]
        + [sems(n)] * 14
        + [sems(chunks, 2)] * 6
        + [sems(5 + pairs), sems(2, inner_steps), sems(3, steps)],
        compiler_params=pltpu.CompilerParams(
            collective_id=1, has_side_effects=True, vmem_limit_bytes=VMEM_ALL
        ),
        name="project_and_attend",
    )(prompt, conts, w_qkv, w_out, w_in, w_ffo, layer_biases, norm_gains, bias_in[None])
    w_all, wf, q, kc, vc, kp, vp, att, norm1, x1_b, act, slope, att_b, lse, rstd1 = out
    w_all = w_all.reshape(8, 4 * rows, D)
    wf = wf.reshape(4, 4 * rows, D)
    return w_all, wf, q, kp, vp, kc, vc, att, lse, (norm1, rstd1, x1_b, act, slope, att_b)


def project_native(
    prompt, conts, w_qkv, w_out, w_in, w_ffo, layer_biases, norm_gains, bias_in
):
    rows = prompt.shape[0]

    def gathered(value):
        return lax.all_gather(value.astype(jnp.bfloat16), "shard", axis=0, tiled=True)

    qkv, out, inner, ffo = (gathered(w) for w in (w_qkv, w_out, w_in, w_ffo))
    tokens = jnp.concatenate([prompt, conts], 0)
    bias = jnp.concatenate([layer_biases[0], jnp.zeros((D,), jnp.float32), layer_biases[1]])
    qkv_b = (dot_plain(tokens, qkv) + bias).astype(jnp.bfloat16)
    q, keys, values = (qkv_b[:, i * D : (i + 1) * D] for i in range(3))
    kp, vp = gathered(keys[:rows]), gathered(values[:rows])
    kc, vc = keys[rows:], values[rows:]
    att, lse = attend_forward(q, kp, vp, kc, vc, rows)
    blocks = [qkv[:, D : 2 * D], qkv[:, 2 * D :], qkv[:, :D], out]
    blocks += [inner[:, i * D : (i + 1) * D] for i in range(inner.shape[1] // D)]
    att_b = att.astype(jnp.bfloat16)
    values = tokens.astype(jnp.float32) + dot_plain(att_b, out) + layer_biases[2]
    center = values - jnp.mean(values, -1, keepdims=True)
    scale = lax.rsqrt(jnp.mean(center * center, -1, keepdims=True) + 1e-05)
    norm1 = center * scale
    x1_b = (norm1 * norm_gains[0] + layer_biases[4]).astype(jnp.bfloat16)
    hidden = dot_plain(x1_b, inner) + bias_in
    cdf = 0.5 * (1.0 + lax.erf(hidden * 2.0 ** (-0.5)))
    density = jnp.exp(hidden * hidden * (-0.5)) * 0.3989422804014327
    act = (hidden * cdf).astype(jnp.bfloat16)
    slope = (cdf + hidden * density).astype(jnp.bfloat16)
    rstd1 = jnp.broadcast_to(scale, (tokens.shape[0], 128))
    state = (norm1, rstd1, x1_b, act, slope, att_b)
    ffo = ffo.reshape(-1, D, D)
    return jnp.stack(blocks), ffo, q, kp, vp, kc, vc, att, lse, state


def student_head(label, stu, vectors, w_pool, w_class, bias_class, classes):
    part_w = STU // SHEADS
    low_half = lax.broadcasted_iota(jnp.int32, stu.shape, 1) < part_w
    row_low = lax.broadcasted_iota(jnp.int32, (1, STU), 1) < part_w
    query, bias_pool = vectors[1:2, :], vectors[2:3, :]

    def by_head(values):
        low_sum = jnp.sum(jnp.where(low_half[: values.shape[0]], values, 0.0), 1, keepdims=True)
        high_sum = jnp.sum(jnp.where(low_half[: values.shape[0]], 0.0, values), 1, keepdims=True)
        return jnp.where(low_half[: values.shape[0]], low_sum, high_sum)

    scores = by_head(stu * query) * part_w ** (-0.5)
    largest = jnp.max(scores, 0, keepdims=True)
    expo = jnp.exp(scores - largest)
    weights = expo / jnp.sum(expo, 0, keepdims=True)
    pooled = jnp.sum(weights * stu, 0, keepdims=True)

    square = (STU, STU)
    on_diagonal = lax.broadcasted_iota(jnp.int32, square, 0) == lax.broadcasted_iota(
        jnp.int32, square, 1
    )

    def column(row):
        return jnp.sum(jnp.where(on_diagonal, row, 0.0), 1, keepdims=True)

    def times(row, matrix):
        return jnp.sum(column(row) * matrix, 0, keepdims=True)

    def times_turned(row, matrix):
        total = jnp.sum(matrix * row, 1, keepdims=True)
        return jnp.sum(jnp.where(on_diagonal, total, 0.0), 0, keepdims=True)

    top = jnp.tanh(times(pooled, w_pool) + bias_pool)
    lane = lax.broadcasted_iota(jnp.int32, (1, STU), 1)
    logits = times_turned(top, w_class) + bias_class
    seen = jnp.where(lane < classes, logits, NEG_BIG)
    expo_l = jnp.exp(seen - jnp.max(seen, 1, keepdims=True))
    g_logits = expo_l / jnp.sum(expo_l, 1, keepdims=True) - jnp.where(lane == label, 1.0, 0.0)
    g_class = column(g_logits) * top
    g_pre = times(g_logits, w_class) * (1.0 - top * top)
    g_pool = column(pooled) * g_pre
    g_pooled = times_turned(g_pre, w_pool)
    g_weights = by_head(stu * g_pooled)
    mean = jnp.sum(weights * g_weights, 0, keepdims=True)
    g_scores = weights * (g_weights - mean) * part_w ** (-0.5)
    g_stu = weights * g_pooled + g_scores * query
    g_query = jnp.sum(g_scores * stu, 0, keepdims=True)
    return logits, g_stu, g_query, g_pre, g_pool, g_class, g_logits


def middle(
    ahead, state, prompt_cot, cont_cot, labels, w_all, wf,
    biases, gains, bias_in, student, vectors, w_pool, w_class, bias_class,
):
    p_rows, cont_len = prompt_cot.shape[0], cont_cot.shape[0]
    tokens = p_rows + cont_len
    ff = bias_in.shape[0]
    blocks = ff // D
    steps = tokens // TILE
    wide = D // TILE
    classes = w_class.shape[1]
    g_names = 2 * blocks + 1

    def kernel(
        label_ref, norm_h, rstd_h, x1_h, act_h, slope_h, att_b_h, cp, cc, w_h, wf_h, bias, gain, w_stu, vec, w_p, w_c, b_c,
        out_p, out_c, logits_out, grads_h, g_r1_h, g_att_h, small, totals_h,
        cot_v, out_v, w_c_v, b_c_v, att_b, w_v, wf_v, norm1, norm2, rstd1, rstd2, x1_b, act, slope, g_res, g_ffn, g_br, g_stu_b, grads,
        sums, in_sum, load, store, *links,
    ):
        def fetch(source, target, i):
            return pltpu.make_async_copy(source, target, load.at[i])

        loads = [
            fetch(act_h, act, 0),
            fetch(wf_h, wf_v, 1),
            fetch(norm_h, norm1, 2),
            fetch(cp, cot_v.at[:p_rows], 3),
            fetch(cc, cot_v.at[p_rows:], 4),
            fetch(slope_h, slope, 5),
            fetch(x1_h, x1_b, 6),
            fetch(rstd_h, rstd1, 7),
            fetch(w_h.at[pl.ds(3, 1 + blocks)], w_v, 8),
            fetch(att_b_h, att_b, 9),
        ]
        for copy in loads:
            copy.start()
        rows = D // blocks
        if ahead:
            (cr, xr, c_s, c_r, x_s, x_r) = links
            rep, shard = lax.axis_index("rep"), lax.axis_index("shard")
            x, core = shard // 2, shard % 2
            partner = (rep, 2 * x + 1 - core)
            across = (rep, 2 * (1 - x) + core)
            barrier = pltpu.get_barrier_semaphore()
            for other in (partner, across):
                pl.semaphore_signal(barrier, inc=1, device_id=other, device_id_type=MESH_ID)
            pl.semaphore_wait(barrier, 2)

            def remote(source, target, send, recv, device):
                return pltpu.make_async_remote_copy(
                    src_ref=source,
                    dst_ref=target,
                    send_sem=send,
                    recv_sem=recv,
                    device_id=device,
                    device_id_type=MESH_ID,
                )

            def core_copy(k, xx):
                block = pl.ds(pl.multiple_of((2 * xx + 1 - core) * rows, 16), rows)
                return remote(
                    grads.at[k, block, :], cr.at[k, xx], c_s.at[k, xx], c_r.at[k, xx], partner
                )

            def mine(xx):
                return pl.ds(pl.multiple_of((2 * xx + core) * rows, 16), rows)

            def x_copy(k):
                return remote(grads.at[k, mine(1 - x), :], xr.at[k], x_s.at[k], x_r.at[k], across)

        def stage_x():
            for k in range(ahead):
                for xx in range(2):
                    core_copy(k, xx).wait_recv()
                block = mine(1 - x)
                total = grads[k, block, :].astype(jnp.float32) + cr[k, 1 - x].astype(jnp.float32)
                grads[k, block, :] = total.astype(jnp.bfloat16)
                x_copy(k).start()

        sums[...] = jnp.zeros_like(sums)
        small[...] = jnp.zeros_like(small)

        def row(i):
            return pl.ds(pl.multiple_of(i * TILE, TILE), TILE)

        def loop(count):
            def run(step):
                def body(i, carry):
                    step(i)
                    return carry

                lax.fori_loop(0, count, body, 0)

            return run

        def normalize(values):
            center = values - jnp.mean(values, -1, keepdims=True)
            spread = jnp.mean(center * center, -1, keepdims=True)
            scale = lax.rsqrt(spread + 1e-05)
            return center * scale, scale

        def norm_back(g, gain_row, hat, scale):
            gg = g * gain_row
            return scale * (
                gg
                - jnp.mean(gg, -1, keepdims=True)
                - hat * jnp.mean(gg * hat, -1, keepdims=True)
            )

        def add_sum(i, values):
            sums[i : i + 1, :] += jnp.sum(values, 0, keepdims=True)

        for i in range(3):
            loads[i].wait()

        @loop(steps)
        def _(i):
            ffn = bias[3:4, :]
            for j in range(blocks):
                ffn = ffn + dot_plain(act[row(i), j * D : (j + 1) * D], wf_v[j])
            first = norm1[row(i), :] * gain[0:1, :] + bias[4:5, :]
            hat, scale = normalize(first + ffn)
            norm2[row(i), :] = hat
            rstd2[row(i), :] = jnp.broadcast_to(scale, (TILE, 128))
            out_v[row(i), :] = (hat * gain[1:2, :] + bias[5:6, :]).astype(jnp.bfloat16)

        out_stores = [
            pltpu.make_async_copy(out_v.at[:p_rows], out_p, store.at[g_names + 2]),
            pltpu.make_async_copy(out_v.at[p_rows:], out_c, store.at[g_names + 3]),
        ]
        for copy in out_stores:
            copy.start()
        base = 8 * (D // 128) + ff // 128
        w_stu_b = w_stu[...].astype(jnp.bfloat16)

        w_c_v[...] = jnp.zeros_like(w_c_v)
        b_c_v[...] = jnp.zeros_like(b_c_v)
        w_c_v[:classes, :] = w_c[...]
        b_c_v[:1, :classes] = b_c[...]

        @pl.when(lax.axis_index("rep") >= 0)
        def _():
            stu = dot_plain(out_v[p_rows:, :], w_stu_b) + vec[0:1, :]
            logits, g_stu, g_query, g_pre, g_pool, g_class, g_logits = student_head(
                label_ref[0, 0], stu, vec, w_p[...], w_c_v[...], b_c_v[:1, :], classes
            )
            logits_out[...] = logits[:, :classes]
            low = g_stu.astype(jnp.bfloat16)
            g_stu_b[:p_rows, :] = jnp.zeros((p_rows, STU), jnp.bfloat16)
            g_stu_b[p_rows:, :] = low
            small[base : base + 1, STU:] = jnp.sum(low.astype(jnp.float32), 0, keepdims=True)
            small[base + 1 : base + 2, STU:] = g_query
            small[base + 2 : base + 3, STU:] = g_pre
            small[base + 3 : base + 4, STU:] = g_logits
            small[base + 8 : base + 8 + STU, STU:] = g_pool
            small[base + 8 + STU : base + 24 + STU, STU:] = g_class[:16]

        small[:, :STU] = dot_first(out_v[p_rows:, :], g_stu_b[p_rows:, :])
        for i in range(3, 10):
            loads[i].wait()

        @loop(steps)
        def _(i):
            g = cot_v[row(i), :].astype(jnp.float32) + dot_second(g_stu_b[row(i), :], w_stu_b)
            hat = norm2[row(i), :]
            add_sum(7, g * hat)
            add_sum(5, g)
            g_r2 = norm_back(g, gain[1:2, :], hat, rstd2[row(i), :1])
            g_res[row(i), :] = g_r2
            low = g_r2.astype(jnp.bfloat16)
            g_ffn[row(i), :] = low
            add_sum(3, low.astype(jnp.float32))

        def piece_store(k):
            return pltpu.make_async_copy(grads.at[k], grads_h.at[k], store.at[k])


        @loop(blocks)
        def _(j):
            columns = pl.ds(pl.multiple_of(j * D, D), D)
            product = dot_first(act[:, columns], g_ffn[...]).astype(jnp.bfloat16)
            for k in range(blocks):
                target = pl.ds(pl.multiple_of(j * rows, 16), rows)
                grads[k, target, :] = product[k * rows : (k + 1) * rows]

        for k in range(ahead):
            for xx in range(2):
                core_copy(k, xx).start()
        for k in range(ahead, blocks):
            piece_store(k).start()


        in_sum[...] = jnp.zeros_like(in_sum)

        @loop(steps)
        def _(i):
            for j in range(blocks):
                columns = slice(j * D, (j + 1) * D)
                g_act = dot_second(g_ffn[row(i), :], wf_v[j])
                low = (g_act * slope[row(i), columns].astype(jnp.float32)).astype(jnp.bfloat16)
                slope[row(i), columns] = low
                in_sum[:, columns] += jnp.sum(low.astype(jnp.float32), 0, keepdims=True)
            if ahead:
                pl.when(i == 0)(stage_x)

        @loop(blocks)
        def _(j):
            columns = pl.ds(pl.multiple_of(j * D, D), D)
            grads[blocks + j] = dot_first(x1_b[...], slope[:, columns]).astype(jnp.bfloat16)
            piece_store(blocks + j).start()

        @loop(steps)
        def _(i):
            g = g_res[row(i), :]
            for j in range(blocks):
                g += dot_second(slope[row(i), j * D : (j + 1) * D], w_v[1 + j])
            hat = norm1[row(i), :]
            add_sum(6, g * hat)
            add_sum(4, g)
            g_r1 = norm_back(g, gain[0:1, :], hat, rstd1[row(i), :1])
            g_res[row(i), :] = g_r1
            low = g_r1.astype(jnp.bfloat16)
            g_br[row(i), :] = low
            add_sum(2, low.astype(jnp.float32))

        res_store = pltpu.make_async_copy(g_res, g_r1_h, store.at[g_names])
        res_store.start()
        g_ffn[...] = dot_second(g_br[...], w_v[0]).astype(jnp.bfloat16)
        att_store = pltpu.make_async_copy(g_ffn, g_att_h, store.at[g_names + 1])
        att_store.start()
        grads[2 * blocks] = dot_first(att_b[...], g_br[...]).astype(jnp.bfloat16)
        piece_store(2 * blocks).start()
        spread = D // 128
        for i in range(8):
            for part in range(spread):
                small[i * spread + part : i * spread + part + 1, STU:] = sums[
                    i : i + 1, part * 128 : (part + 1) * 128
                ]
        for part in range(ff // 128):
            at = 8 * spread + part
            small[at : at + 1, STU:] = in_sum[:, part * 128 : (part + 1) * 128]
        res_store.wait()
        att_store.wait()
        for copy in out_stores:
            copy.wait()
        for k in range(ahead):
            x_copy(k).wait_recv()
            total = grads[k, mine(x), :].astype(jnp.float32) + cr[k, x].astype(jnp.float32)
            cr[k, x] = (total + xr[k].astype(jnp.float32)).astype(jnp.bfloat16)
            pltpu.make_async_copy(cr.at[k, x], totals_h.at[k], store.at[k]).start()
        for k in range(ahead, g_names):
            piece_store(k).wait()
        for k in range(ahead):
            pltpu.make_async_copy(cr.at[k, x], totals_h.at[k], store.at[k]).wait()
            for xx in range(2):
                core_copy(k, xx).wait_send()
            x_copy(k).wait_send()

    anywhere = pl.BlockSpec(memory_space=pl.ANY)
    vmem = pl.BlockSpec(memory_space=pltpu.VMEM)
    low = jnp.bfloat16

    def shaped(dims, kind=jnp.float32):
        return jax.ShapeDtypeStruct(dims, kind)

    params = pltpu.CompilerParams(vmem_limit_bytes=VMEM_ALL)
    link_scratch = []
    if ahead:
        params = pltpu.CompilerParams(
            collective_id=3, has_side_effects=True, vmem_limit_bytes=VMEM_ALL
        )
        piece = (D // blocks, D)
        link_scratch = [
            pltpu.VMEM((ahead, 2, *piece), low),
            pltpu.VMEM((ahead, *piece), low),
        ]
        link_scratch += [pltpu.SemaphoreType.DMA((ahead, 2))] * 2
        link_scratch += [pltpu.SemaphoreType.DMA((ahead,))] * 2

    return pl.pallas_call(
        kernel,
        in_specs=[pl.BlockSpec(memory_space=pltpu.SMEM)] + [anywhere] * 10 + [vmem] * 7,
        out_specs=[anywhere, anywhere, vmem, anywhere, anywhere, anywhere, vmem, anywhere],
        out_shape=[
            shaped((p_rows, D), low),
            shaped((cont_len, D), low),
            shaped((1, classes)),
            shaped((g_names, D, D), low),
            shaped((tokens, D)),
            shaped((tokens, D), low),
            shaped((D, 2 * STU)),
            shaped((max(ahead, 1), D // blocks, D), low),
        ],
        scratch_shapes=[
            pltpu.VMEM((tokens, D), low),
            pltpu.VMEM((tokens, D), low),
            pltpu.VMEM((STU, STU), jnp.float32),
            pltpu.VMEM((8, STU), jnp.float32),
            pltpu.VMEM((tokens, D), low),
            pltpu.VMEM((1 + blocks, D, D), low),
            pltpu.VMEM((blocks, D, D), low),
            pltpu.VMEM((tokens, D), jnp.float32),
            pltpu.VMEM((tokens, D), jnp.float32),
            pltpu.VMEM((tokens, 128), jnp.float32),
            pltpu.VMEM((tokens, 128), jnp.float32),
            pltpu.VMEM((tokens, D), low),
            pltpu.VMEM((tokens, ff), low),
            pltpu.VMEM((tokens, ff), low),
            pltpu.VMEM((tokens, D), jnp.float32),
            pltpu.VMEM((tokens, D), low),
            pltpu.VMEM((tokens, D), low),
            pltpu.VMEM((tokens, STU), low),
            pltpu.VMEM((g_names, D, D), low),
            pltpu.VMEM((8, D), jnp.float32),
            pltpu.VMEM((1, ff), jnp.float32),
            pltpu.SemaphoreType.DMA((10,)),
            pltpu.SemaphoreType.DMA((g_names + 4,)),
        ]
        + link_scratch,
        compiler_params=params,
        name="middle",
    )(
        labels,
        *state,
        prompt_cot,
        cont_cot,
        w_all,
        wf,
        biases,
        gains,
        student,
        vectors,
        w_pool,
        w_class.T,
        bias_class[None],
    )


def sum_native(g9, g_qkvw, small):
    blocks = (g9.shape[0] - 1) // 2
    rows = D // blocks
    ffo = g9[:blocks].reshape(blocks, blocks, rows, D).transpose(1, 0, 2, 3).reshape(-1, D)
    inner = jnp.concatenate([g9[blocks + j] for j in range(blocks)], 1)

    def over(grad):
        part = lax.psum_scatter(
            grad.astype(jnp.bfloat16), "shard", scatter_dimension=0, tiled=True
        )
        return lax.psum(part, "rep").astype(jnp.float32)

    owned = tuple(over(grad) for grad in (g_qkvw, g9[2 * blocks], inner, ffo))
    return owned, lax.psum(small, ("rep", "shard"))


def finish(
    ahead, totals, q, kp, vp, kc, vc, att, lse, g_att, g9, g_resid, small, w_all, prompt, conts, ff
):
    pieces, ready = 12, 9
    p_rows, cont_len = prompt.shape[0], conts.shape[0]
    tokens = p_rows + cont_len
    p_len = kp.shape[0]
    pairs = HEADS // 2
    rows = D // 4
    half, quarter = D // 2, rows // 4
    s_width = small.shape[1]
    chunk = 2 * PAIR
    chunks = D // chunk
    across_lanes = D // 128

    def kernel(
        q_h, kp_h, vp_h, kc_h, vc_h, att_h, g_att_h, g9, g_res_h, w_h, totals_h, ls, sm, xp, xc,
        out_pg, out_cg, out_q, out_o, out_i, out_f, fin_s,
        qv, kpv, vpv, kcv, vcv, attv, gav, accum, dq, dkp, dvp, dkc, dvc, kr, kx, kvs, wv, g_tok, made, head,
        own, cr, xr, yr, zr, fb, made_s, own_s, cr_s, xr_s, yr_s, zr_s, fb_s,
        load, sem_own, c_send, c_recv, x_send, x_recv, y_send, y_recv, z_send, z_recv,
        f_send, f_recv, o_send, o_recv, o_own, g_send, g_recv, kc_s, kc_r, kx_s, kx_r, out_sem,
    ):
        rep, shard = lax.axis_index("rep"), lax.axis_index("shard")
        z, y = rep // 2, rep % 2
        x, core = shard // 2, shard % 2
        partner = (rep, 2 * x + 1 - core)
        across = (rep, 2 * (1 - x) + core)
        beside = (2 * z + 1 - y, shard)
        far = (rep, 2 * (1 - x) + 1 - core)

        def along(step):
            return (2 * lax.rem(z + step, 4) + y, shard)

        def own_copy(k, xx):
            return pltpu.make_async_copy(
                g9.at[k, pl.ds(pl.multiple_of((2 * xx + core) * rows, 16), rows), :],
                own.at[k, xx],
                sem_own.at[k, xx],
            )

        fetched = [(q_h, qv), (kp_h, kpv), (vp_h, vpv), (kc_h, kcv), (vc_h, vcv)]
        fetched += [(att_h, attv), (g_att_h, gav), (w_h.at[pl.ds(0, 3)], wv), (g_res_h, g_tok)]

        def fetch(i):
            return pltpu.make_async_copy(*fetched[i], load.at[i])

        def total_copy(k):
            return pltpu.make_async_copy(totals_h.at[k], own.at[k, x], sem_own.at[k, 0])

        for k in range(ahead):
            total_copy(k).start()
        for k in range(ahead, ahead + 2):
            for xx in range(2):
                own_copy(k, xx).start()
        for i in range(7):
            fetch(i).start()
        for k in range(ahead + 2, ready):
            for xx in range(2):
                own_copy(k, xx).start()
        for i in (7, 8):
            fetch(i).start()

        barrier = pltpu.get_barrier_semaphore()
        others = [partner, across, beside, along(1), along(2), along(3), far]
        for other in others:
            pl.semaphore_signal(barrier, inc=1, device_id=other, device_id_type=MESH_ID)
        pl.semaphore_wait(barrier, len(others))

        def remote(source, target, send, recv, device):
            return pltpu.make_async_remote_copy(
                src_ref=source,
                dst_ref=target,
                send_sem=send,
                recv_sem=recv,
                device_id=device,
                device_id_type=MESH_ID,
            )

        big = (own, cr, xr, yr, zr, fb, half)
        narrow = (own_s, cr_s, xr_s, yr_s, zr_s, fb_s, s_width // 2)

        def bufs(k):
            if isinstance(k, int) and k == pieces:
                return narrow, 0
            return big, k

        def core_copy(k, xx):
            b, i = bufs(k)
            block = 2 * xx + 1 - core
            if not isinstance(k, int):
                source = b[1].at[i, xx]
            elif k < ready:
                source = g9.at[k, pl.ds(pl.multiple_of(block * rows, 16), rows), :]
            elif k < pieces:
                source = made.at[k - ready, block]
            else:
                source = made_s.at[block]
            return remote(source, b[1].at[i, xx], c_send.at[k, xx], c_recv.at[k, xx], partner)

        def x_copy(k):
            b, i = bufs(k)
            return remote(b[0].at[i, 1 - x], b[2].at[i], x_send.at[k], x_recv.at[k], across)

        def lanes_of(b, which):
            return pl.ds(pl.multiple_of(which * b[6], 128), b[6])

        def y_copy(k):
            b, i = bufs(k)
            source = b[0].at[i, x, :, lanes_of(b, 1 - y)]
            return remote(source, b[3].at[i], y_send.at[k], y_recv.at[k], beside)

        def rows_of(which):
            return pl.ds(pl.multiple_of(which * quarter, 16), quarter)

        def zs_copy(k, step):
            b, i = bufs(k)
            source = b[0].at[i, x, rows_of(lax.rem(z + step, 4)), lanes_of(b, y)]
            return remote(
                source, b[4].at[i, z], z_send.at[k, step - 1], z_recv.at[k, z], along(step)
            )

        def zr_wait(k, step):
            b, i = bufs(k)
            slot = lax.rem(z + step, 4)
            target = b[4].at[i, slot]
            remote(
                target, target, z_send.at[k, step - 1], z_recv.at[k, slot], along(step)
            ).wait_recv()

        def fs_copy(k, step):
            b, i = bufs(k)
            block = b[5].at[i, rows_of(z), :]
            return remote(block, block, f_send.at[k, step - 1], f_recv.at[k, z], along(step))

        def fr_wait(k, step):
            b, i = bufs(k)
            slot = lax.rem(z + step, 4)
            block = b[5].at[i, rows_of(slot), :]
            remote(
                block, block, f_send.at[k, step - 1], f_recv.at[k, slot], along(step)
            ).wait_recv()

        def final(k, yy):
            b, _ = bufs(k)
            if k < 4:
                return out_f.at[k * rows : (k + 1) * rows, lanes_of(b, yy)]
            if k == 8:
                return out_o.at[:, lanes_of(b, yy)]
            if k == pieces:
                return fin_s.at[shard, :, lanes_of(b, yy)]
            out, at = (out_i, (k - 4) * D) if k < 8 else (out_q, (k - 9) * D)
            return out.at[:, pl.ds(pl.multiple_of(at + yy * half, 128), half)]

        def o_copy(k):
            b, i = bufs(k)
            return remote(b[5].at[i], final(k, y), o_send.at[k], o_recv.at[k], beside)

        def o_wait(k):
            b, i = bufs(k)
            remote(b[5].at[i], final(k, 1 - y), o_send.at[k], o_recv.at[k], beside).wait_recv()

        def o_local(k):
            b, i = bufs(k)
            return pltpu.make_async_copy(b[5].at[i], final(k, y), o_own.at[k])

        def wide(value):
            return value.astype(jnp.float32)

        def stage_x(k):
            b, i = bufs(k)
            for xx in range(2):
                core_copy(k, xx).wait_recv()
                if not isinstance(k, int):
                    pl.when(k < ready)(own_copy(k, xx).wait)
            b[0][i, 1 - x] = (wide(b[0][i, 1 - x]) + wide(b[1][i, 1 - x])).astype(jnp.bfloat16)
            x_copy(k).start()

        def stage_y(k):
            b, i = bufs(k)
            x_copy(k).wait_recv()
            total = wide(b[0][i, x]) + wide(b[1][i, x]) + wide(b[2][i])
            b[0][i, x] = total.astype(jnp.bfloat16)
            y_copy(k).start()

        def stage_z(k):
            b, i = bufs(k)
            y_copy(k).wait_recv()
            lanes = lanes_of(b, y)
            total = wide(b[0][i, x, :, lanes]) + wide(b[3][i])
            b[0][i, x, :, lanes] = total.astype(jnp.bfloat16)
            for step in (2, 1, 3):
                zs_copy(k, step).start()

        def stage_f(k):
            b, i = bufs(k)
            total = wide(b[0][i, x, rows_of(z), lanes_of(b, y)])
            for step in (1, 2, 3):
                zr_wait(k, step)
                total += wide(b[4][i, lax.rem(z + step, 4)])
            b[5][i, rows_of(z), :] = total.astype(jnp.bfloat16)
            for step in (2, 1, 3):
                fs_copy(k, step).start()

        def stage_o(k):
            for step in (1, 2, 3):
                fr_wait(k, step)
            for kk in range(pieces + 1) if not isinstance(k, int) else [k]:

                def begin(kk=kk):
                    o_copy(kk).start()
                    o_local(kk).start()

                if isinstance(k, int):
                    begin()
                else:
                    pl.when(k == kk)(begin)

        def send_core(k):
            for xx in range(2):
                core_copy(k, xx).start()

        for k in range(ahead, ready):
            send_core(k)

        def stages_x(first, last):
            def step(k, carry):
                stage_x(k)
                return carry

            lax.fori_loop(first, last, step, 0)

        for k in range(ahead):
            total_copy(k).wait()
            y_copy(k).start()
        stages_x(ahead, ahead + 2)
        kv = (dkp, dvp)

        def kv_rows(block):
            return pl.ds(pl.multiple_of(block * p_rows, p_rows), p_rows)

        def kv_lanes(g):
            return pl.ds(g * chunk if isinstance(g, int) else pl.multiple_of(g * chunk, chunk), chunk)

        def kv_core(t, g, xx):
            return remote(
                kv[t].at[kv_rows(2 * xx + 1 - core), kv_lanes(g)],
                kr.at[t, xx, :, kv_lanes(g)],
                kc_s.at[g, t, xx],
                kc_r.at[g, t, xx],
                partner,
            )

        def kv_across(t, g):
            return remote(
                kv[t].at[kv_rows(2 * (1 - x) + core), kv_lanes(g)],
                kx.at[t, :, kv_lanes(g)],
                kx_s.at[g, t],
                kx_r.at[g, t],
                across,
            )

        def serve_kv(g):
            block, lanes = kv_rows(2 * (1 - x) + core), kv_lanes(g)
            for t in range(2):
                for xx in range(2):
                    kv_core(t, g, xx).wait_recv()
                total = wide(kv[t][block, lanes]) + wide(kr[t, 1 - x, :, lanes])
                kv[t][block, lanes] = total.astype(jnp.bfloat16)
                kv_across(t, g).start()

        for i in range(7):
            fetch(i).wait()

        def pair(p, carry):
            def between(index):
                if index == 0:
                    pl.when(p + ahead + 2 < ready)(lambda: stage_x(p + ahead + 2))
                if index == 1:
                    pl.when((p == 2) | (p == 4))(lambda: serve_kv(p // 2 - 1))
                if index == 2:
                    pl.when(p >= 1)(lambda: stage_y(p + ahead - 1))
                if index == 3:
                    stage_z(p)
                if index == 4:
                    pl.when(p >= 1)(lambda: stage_f(p - 1))
                if index == 5:
                    pl.when(p >= 2)(lambda: stage_o(p - 2))

            lanes = pl.ds(pl.multiple_of(p * PAIR, PAIR), PAIR)

            def cut(ref):
                return ref.at[:, lanes]

            attend_bwd_pair(
                shard, p_rows, cut(qv), cut(kpv), cut(vpv), cut(kcv), cut(vcv), cut(gav), cut(attv),
                ls.at[p], cut(dq), cut(dkp), cut(dvp), cut(dkc), cut(dvc), accum, between,
            )

            @pl.when(p % 2 == 1)
            def _():
                for t in range(2):
                    for xx in range(2):
                        kv_core(t, p // 2, xx).start()

            return carry

        lax.fori_loop(0, pairs, pair, 0)

        def keep_piece(k, product):
            for block in range(4):
                made[k - ready, block] = product[block * rows : (block + 1) * rows]
            for xx in range(2):
                own[k, xx] = made[k - ready, 2 * xx + core]
            send_core(k)

        product = dot_first(xp[...], dq[:p_rows, :]) + dot_first(xc[...], dq[p_rows:, :])
        keep_piece(9, product.astype(jnp.bfloat16))
        serve_kv(chunks - 1)
        for i in (7, 8):
            fetch(i).wait()
        stages_x(9, 10)
        g_tok[...] += dot_second(dq[...], wv[2])
        stores = [
            pltpu.make_async_copy(g_tok.at[:p_rows, :], out_pg, out_sem.at[0]),
            pltpu.make_async_copy(g_tok.at[p_rows:, :], out_cg, out_sem.at[1]),
        ]

        def with_kv():
            for g in range(chunks):
                for t in range(2):
                    kv_across(t, g).wait_recv()
            for t in range(2):
                total = wide(kv[t][kv_rows(shard), :]) + wide(kr[t, x]) + wide(kx[t])
                kvs[t] = total.astype(jnp.bfloat16)
            g_bias = jnp.sum(wide(dq[...]), 0, keepdims=True)
            v_bias = jnp.sum(wide(dvc[...]), 0, keepdims=True)
            v_bias += jnp.sum(wide(kvs[1]), 0, keepdims=True)
            head[...] = sm[:16, :]
            for part in range(across_lanes):
                lanes = slice(part * 128, (part + 1) * 128)
                head[part : part + 1, STU:] = g_bias[:, lanes]
                head[across_lanes + part : across_lanes + part + 1, STU:] = v_bias[:, lanes]
            for block in range(4):
                made_s[block] = sm[block * rows : (block + 1) * rows, :].astype(jnp.bfloat16)
            made_s[0, :16] = head[...].astype(jnp.bfloat16)
            for xx in range(2):
                own_s[0, xx] = made_s[2 * xx + core]
            send_core(pieces)
            for t in range(2):
                product = dot_first(xp[...], kvs[t]) + dot_first(xc[...], (dkc, dvc)[t][...])
                keep_piece(10 + t, product.astype(jnp.bfloat16))
            stage_x(pieces)
            stages_x(10, 12)
            g_tok[:p_rows, :] += dot_second(kvs[0], wv[0]) + dot_second(kvs[1], wv[1])
            for copy in stores:
                copy.start()

        def cont_part():
            g_tok[p_rows:, :] += dot_second(dkc[...], wv[0]) + dot_second(dvc[...], wv[1])

        def tick(n, carry):
            pl.when(n == 9)(with_kv)
            pl.when((n >= 8) & (n < pieces))(lambda: stage_y(n))
            pl.when(n == 10)(lambda: stage_y(pieces))
            pl.when(n < pieces + 1)(lambda: stage_z(n - 1))
            pl.when(n == 11)(lambda: stage_z(pieces))
            pl.when(n < pieces + 2)(lambda: stage_f(n - 2))
            pl.when(n == 12)(lambda: stage_f(pieces))
            pl.when(n == 14)(stage_g)
            stage_o(n - 3)
            pl.when(n == 13)(lambda: stage_o(pieces))
            pl.when(n == 7)(cont_part)
            return carry

        def g_copy(step):
            return remote(
                fin_s.at[shard],
                fin_s.at[shard],
                g_send.at[step - 1],
                g_recv.at[shard],
                (rep, lax.rem(shard + step, 4)),
            )

        def stage_g():
            o_wait(pieces)
            o_local(pieces).wait()
            for step in (1, 2, 3):
                g_copy(step).start()

        lax.fori_loop(pieces - 5, pieces + 3, tick, 0)
        for step in (1, 2, 3):
            slot = lax.rem(shard + step, 4)
            remote(
                fin_s.at[slot], fin_s.at[slot], g_send.at[step - 1], g_recv.at[slot], far
            ).wait_recv()

        for k in range(pieces):
            o_wait(k)
            o_local(k).wait()
        for copy in stores:
            copy.wait()

        def sent(k):
            def two():
                for xx in range(2):
                    core_copy(k, xx).wait_send()
                x_copy(k).wait_send()

            if isinstance(k, int):
                two()
            else:
                pl.when(k >= ahead)(two)
            y_copy(k).wait_send()
            for step in (1, 2, 3):
                zs_copy(k, step).wait_send()
                fs_copy(k, step).wait_send()

        def sent_step(k, carry):
            sent(k)
            return carry

        lax.fori_loop(0, pieces, sent_step, 0)
        sent(pieces)
        for k in range(pieces + 1):
            o_copy(k).wait_send()
        for step in (1, 2, 3):
            g_copy(step).wait_send()
        for g in range(chunks):
            for t in range(2):
                for xx in range(2):
                    kv_core(t, g, xx).wait_send()
                kv_across(t, g).wait_send()

    def sems(*dims):
        return pltpu.SemaphoreType.DMA(dims)

    def low(*dims):
        return pltpu.VMEM(dims, jnp.bfloat16)

    def full(*dims):
        return pltpu.VMEM(dims, jnp.float32)

    def buffers(count, columns):
        cut = columns // 2
        return [
            low(count, 2, rows, columns),
            low(count, 2, rows, columns),
            low(count, rows, columns),
            low(count, rows, cut),
            low(count, 4, quarter, cut),
            low(count, rows, cut),
        ]

    def shaped(dims, kind=jnp.float32):
        return jax.ShapeDtypeStruct(dims, kind)

    n = pieces + 1
    anywhere = pl.BlockSpec(memory_space=pl.ANY)
    vmem = pl.BlockSpec(memory_space=pltpu.VMEM)
    return pl.pallas_call(
        kernel,
        in_specs=[anywhere] * 11 + [vmem] * 4,
        out_specs=[anywhere] * 6 + [vmem],
        out_shape=[
            shaped((p_rows, D)),
            shaped((cont_len, D)),
            shaped((rows, 3 * D), jnp.bfloat16),
            shaped((rows, D), jnp.bfloat16),
            shaped((rows, ff), jnp.bfloat16),
            shaped((4 * rows, D), jnp.bfloat16),
            shaped((4, rows, s_width), jnp.bfloat16),
        ],
        scratch_shapes=[
            low(tokens, D), low(p_len, D), low(p_len, D), low(cont_len, D), low(cont_len, D),
            full(tokens, D), low(tokens, D), full(PAIR, tokens), low(tokens, D),
            low(p_len, D), low(p_len, D), low(cont_len, D), low(cont_len, D),
            low(2, 2, p_rows, D), low(2, p_rows, D), low(2, p_rows, D), low(3, D, D),
            full(tokens, D), low(3, 4, rows, D), full(16, s_width),
        ]
        + buffers(pieces, D)
        + [low(4, rows, s_width)]
        + buffers(1, s_width)
        + [
            sems(9), sems(n, 2), sems(n, 2), sems(n, 2), sems(n), sems(n), sems(n), sems(n),
            sems(n, 3), sems(n, 4), sems(n, 3), sems(n, 4), sems(n), sems(n), sems(n),
            sems(3), sems(4), sems(chunks, 2, 2), sems(chunks, 2, 2), sems(chunks, 2),
            sems(chunks, 2), sems(2),
        ],
        compiler_params=pltpu.CompilerParams(
            collective_id=2, has_side_effects=True, vmem_limit_bytes=VMEM_ALL
        ),
        name="finish",
    )(q, kp, vp, kc, vc, att, g_att, g9, g_resid, w_all, totals, lse, small, prompt, conts)


def place(g_prompt, g_conts, owned, out_p, out_c, logits, summed, ff, classes):
    big = [g_prompt, g_conts, *owned, out_p, out_c]
    count = len(big)
    order = (2, 4, 5, 3, 1, 0, 7, 6)
    rows, across = summed.shape[1], D // 128

    def kernel(*refs):
        sources, fin_h, logits_in = refs[:count], refs[count], refs[count + 1]
        outs = refs[count + 2 :]
        targets = outs[:count]
        o_bias, o_gain, o_in, o_stu, o_vec, o_pool, o_class, o_cb, o_logits = outs[count : count + 9]
        scratch = outs[count + 9 :]
        held, turned, (fin, sem_in, sem_out) = scratch[:count], scratch[count:-3], scratch[-3:]
        reads = [pltpu.make_async_copy(sources[i], held[i], sem_in.at[i]) for i in order]
        small = pltpu.make_async_copy(fin_h, fin, sem_in.at[count])
        small.start()
        for copy in reads:
            copy.start()
        small.wait()

        def side(block):
            return fin[block, :, STU:].astype(jnp.float32)

        first = side(0)
        for i in range(8):
            target, at = (o_bias, i) if i < 6 else (o_gain, i - 6)
            for part in range(across):
                r = i * across + part
                target[at : at + 1, part * 128 : (part + 1) * 128] = first[r : r + 1, :]
        for part in range(ff // 128):
            r = 8 * across + part
            o_in[:, part * 128 : (part + 1) * 128] = first[r : r + 1, :]
        base = 8 * across + ff // 128
        o_vec[...] = first[base : base + 3, :]
        o_cb[...] = first[base + 3 : base + 4, :classes]
        every = jnp.concatenate([first, side(1)], 0)
        o_pool[...] = every[base + 8 : base + 8 + STU, :]
        o_class[...] = every[base + 8 + STU : base + 8 + STU + classes, :]
        for block in range(4):
            o_stu[block * rows : (block + 1) * rows, :] = fin[block, :, :STU].astype(jnp.float32)
        writes = []
        o_logits[...] = logits_in[...]
        for copy, i in zip(reads, order):
            copy.wait()
            source = held[i]
            if 2 <= i < 6:
                source = turned[i - 2]
                source[...] = held[i][...].astype(jnp.float32)
            writes.append(pltpu.make_async_copy(source, targets[i], sem_out.at[i]))
            writes[-1].start()
        for copy in writes:
            copy.wait()

    def shaped(*dims):
        return jax.ShapeDtypeStruct(dims, jnp.float32)

    anywhere = pl.BlockSpec(memory_space=pl.ANY)
    vmem = pl.BlockSpec(memory_space=pltpu.VMEM)
    return pl.pallas_call(
        kernel,
        in_specs=[anywhere] * (count + 1) + [vmem],
        out_specs=[anywhere] * count + [vmem] * 9,
        out_shape=[shaped(*part.shape) for part in big[:6]]
        + [jax.ShapeDtypeStruct(part.shape, part.dtype) for part in big[6:]]
        + [
            shaped(6, D),
            shaped(2, D),
            shaped(1, ff),
            shaped(D, STU),
            shaped(3, STU),
            shaped(STU, STU),
            shaped(classes, STU),
            shaped(1, classes),
            shaped(1, classes),
        ],
        scratch_shapes=[pltpu.VMEM(part.shape, part.dtype) for part in big]
        + [pltpu.VMEM(part.shape, jnp.float32) for part in owned]
        + [pltpu.VMEM(summed.shape, summed.dtype)]
        + [pltpu.SemaphoreType.DMA((count + 1,)), pltpu.SemaphoreType.DMA((count,))],
        compiler_params=pltpu.CompilerParams(vmem_limit_bytes=VMEM_ALL),
        name="place",
    )(*big, summed, logits)


def body(
    prompt,
    conts,
    prompt_cot,
    cont_cot,
    labels,
    w_qkv,
    w_out,
    w_in,
    w_ffo,
    layer_biases,
    norm_gains,
    bias_in,
    w_student,
    student_vectors,
    w_pool,
    w_class,
    bias_class,
):
    prompt_rows = prompt.shape[1]
    direct = (lax.axis_size("rep"), lax.axis_size("shard")) == (8, 4)
    project = project_and_attend if direct else project_native
    w_all, ffo_full, q, kp, vp, kc, vc, attended, log_totals, state = project(
        prompt[0], conts[0, 0], w_qkv, w_out, w_in, w_ffo, layer_biases, norm_gains, bias_in
    )
    ahead = 3 if direct else 0
    out_p, out_c, logits, g9, g_resid, g_att, small, totals = middle(
        ahead,
        state,
        prompt_cot[0],
        cont_cot[0, 0],
        labels,
        w_all,
        ffo_full,
        layer_biases,
        norm_gains,
        bias_in,
        w_student,
        student_vectors,
        w_pool,
        w_class,
        bias_class,
    )
    ff, classes = bias_in.shape[0], w_class.shape[1]
    if direct:
        outs = finish(
            ahead, totals, q, kp, vp, kc, vc, attended, log_totals, g_att, g9, g_resid, small, w_all,
            prompt[0], conts[0, 0], ff,
        )
        placed = place(outs[0], outs[1], outs[2:6], out_p, out_c, logits, outs[6], ff, classes)
        g_prompt, g_conts, owned, out_p, out_c = placed[0], placed[1], placed[2:6], *placed[6:8]
        biases, gains_g, g_in, g_student, g_vectors, g_pool, g_class, g_cb, logits = placed[8:]
    else:
        g_q, g_kp, g_vp, g_kc, g_vc = attend_backward(
            q, kp, vp, kc, vc, g_att, attended, log_totals, prompt_rows
        )
        tokens = jnp.concatenate([prompt[0], conts[0, 0]], 0)
        kv_sum = [
            lax.psum_scatter(part, "shard", scatter_dimension=0, tiled=True)
            for part in (g_kp, g_vp)
        ]
        g_k = jnp.concatenate([kv_sum[0], g_kc], 0)
        g_v = jnp.concatenate([kv_sum[1], g_vc], 0)
        g_tokens = g_resid
        for part, weight in ((g_k, w_all[0]), (g_v, w_all[1]), (g_q, w_all[2])):
            g_tokens = g_tokens + dot_second(part, weight)
        g_prompt, g_conts = g_tokens[:prompt_rows], g_tokens[prompt_rows:]
        g_qkvw = jnp.concatenate([dot_first(tokens, part) for part in (g_q, g_k, g_v)], 1)
        side = small[:, STU:]
        across = D // 128
        for at, part in ((0, g_q), (1, g_v)):
            total = jnp.sum(part.astype(jnp.float32), 0).reshape(across, 128)
            side = lax.dynamic_update_slice(side, total, (at * across, 0))
        small = jnp.concatenate([small[:, :STU], side], 1)
        owned, summed = sum_native(g9, g_qkvw, small)
        side = summed[:, STU:]
        base = 8 * across + ff // 128
        biases = side[: 6 * across].reshape(6, D)
        gains_g = side[6 * across : 8 * across].reshape(2, D)
        g_in = side[8 * across : base]
        g_student, g_vectors = summed[:, :STU], side[base : base + 3]
        g_pool = side[base + 8 : base + 8 + STU]
        g_class = side[base + 8 + STU : base + 8 + STU + classes]
        g_cb = side[base + 3 : base + 4]
    return (
        out_p[None],
        out_c[None, None],
        logits[None],
        g_prompt[None],
        g_conts[None, None],
        *owned,
        biases,
        gains_g,
        g_in.reshape(ff),
        g_student,
        g_vectors,
        g_pool,
        g_class.T,
        g_cb[0, :classes],
    )


def solution(mesh):
    return jax.shard_map(
        body,
        mesh=mesh,
        in_specs=(
            P("rep", "shard", None),
            P("rep", "shard", None, None),
            P("rep", "shard", None),
            P("rep", "shard", None, None),
            P("rep", "shard"),
            P("shard", None),
            P("shard", None),
            P("shard", None),
            P("shard", None),
            P(),
            P(),
            P(),
            P(),
            P(),
            P(),
            P(),
            P(),
        ),
        out_specs=(
            P("rep", "shard", None),
            P("rep", "shard", None, None),
            P("rep", "shard", None),
            P("rep", "shard", None),
            P("rep", "shard", None, None),
            P("shard", None),
            P("shard", None),
            P("shard", None),
            P("shard", None),
            P(),
            P(),
            P(),
            P(),
            P(),
            P(),
            P(),
            P(),
        ),
        check_vma=False,
    )
```
